32 devices in a mesh: seq: 2 (over y), fsdp: 16 (over z, x, core).
Axes of the slice: x: 2, y: 2, z: 4, core: 2. Of those that a mesh axis runs over, the one named last changes fastest.
Arguments:
- tokens: bfloat16 [16, 1024, 1024], P('fsdp', 'seq'), may hold values from -6 to 6
- grad_out: bfloat16 [16, 1024, 1024], P('fsdp', 'seq'), may hold values from -6 to 6
- segments: int32 [16, 1024], P('fsdp'), may hold values from 0 to 1, as said below
- padding: int32 [16, 1024], P('fsdp'), may hold values from 0 to 1, as said below
- adapter_ids: int32 [16, 1], P('fsdp'), may hold values from 0 to 7
- norm1_gain: bfloat16 [1024], P('fsdp'), may hold values from 0.5 to 1.5
- norm1_bias: bfloat16 [1024], P('fsdp'), may hold values from -1.1953125 to 1.1953125
- w_qkv: bfloat16 [1024, 3072], P('fsdp'), may hold values from -0.1875 to 0.1875
- w_proj: bfloat16 [1024, 1024], P('fsdp'), may hold values from -3 to 3
- proj_bias: bfloat16 [1024], P('fsdp'), may hold values from -1.796875 to 1.796875
- norm2_gain: bfloat16 [1024], P('fsdp'), may hold values from 0.5 to 1.5
- norm2_bias: bfloat16 [1024], P('fsdp'), may hold values from -1.1953125 to 1.1953125
- w_fc1: bfloat16 [1024, 4096], P('fsdp'), may hold values from -0.1875 to 0.1875
- fc1_bias: bfloat16 [4096], P('fsdp'), may hold values from -3 to 3
- w_fc2: bfloat16 [4096, 1024], P('fsdp'), may hold values from -0.09375 to 0.09375
- fc2_bias: bfloat16 [1024], P('fsdp'), may hold values from -1.796875 to 1.796875
- qkv_down: bfloat16 [1024, 128], replicated, may hold values from -0.1875 to 0.1875
- qkv_up: bfloat16 [128, 3072], replicated, may hold values from -1.5 to 1.5
- proj_down: bfloat16 [1024, 128], replicated, may hold values from -3 to 3
- proj_up: bfloat16 [128, 1024], replicated, may hold values from -1.5 to 1.5
- fc1_down: bfloat16 [1024, 128], replicated, may hold values from -0.1875 to 0.1875
- fc1_up: bfloat16 [128, 4096], replicated, may hold values from -1.5 to 1.5
- fc2_down: bfloat16 [4096, 128], replicated, may hold values from -0.09375 to 0.09375
- fc2_up: bfloat16 [128, 1024], replicated, may hold values from -1.5 to 1.5
Outputs:
- output: bfloat16 [16, 1024, 1024], P('fsdp', 'seq')
- grad_tokens: float32 [16, 1024, 1024], P('fsdp', 'seq')
- grad_qkv_down: float32 [1024, 128], replicated
- grad_qkv_up: float32 [128, 3072], replicated
- grad_proj_down: float32 [1024, 128], replicated
- grad_proj_up: float32 [128, 1024], replicated
- grad_fc1_down: float32 [1024, 128], replicated
- grad_fc1_up: float32 [128, 4096], replicated
- grad_fc2_down: float32 [4096, 128], replicated
- grad_fc2_up: float32 [128, 1024], replicated
The draws below stay inside these ranges and needn't reach their ends.
Inputs may be any that keep to these rules, and one draw needn't show every extreme that they name: `segments`: in each pack the tokens with padding 1 form 1 runs of exactly 577 tokens, in order; a token's segment number is the count of runs that begin at or before it, so run s has number s and padding takes the number of the run before it, or 0. `padding`: 1 exactly on the tokens of the runs. `adapter_ids`: entry s - 1 is the adapter of run s of the pack.
All inputs are finite; a program needn't handle non-finite values.
Results may differ from the reference program's by a relative error of at most 0.014.
The reference program's roundings to bfloat16 on the way count: a program that leaves them out, or rounds other values in their place, can miss the bound.
Values may be sent and summed in bfloat16 or wider, within the bound.
A program may use at most 192 MiB of HBM per device.

```python
import jax
import jax.numpy as jnp
from jax import lax

D = 1024
HEADS = 16
HEAD_DIM = 64
FF = 4096
IMG = 577
ADAPTERS = 8
RANK = 16
PACK_TOK = 1024
PACKS = 16
NIMG = 1
ADAPT_COLS = 128


def image_starts(key):
    spare_tokens = PACK_TOK - NIMG * IMG
    cuts = jax.random.randint(jax.random.fold_in(key, 11), (PACKS, NIMG), 0, spare_tokens + 1)
    ordered = lax.top_k(cuts, NIMG)[0][:, ::-1]
    return ordered + jnp.arange(NIMG, dtype=jnp.int32)[None, :] * IMG


def draw_segments(key, part):
    starts = image_starts(key)
    places = jnp.arange(PACK_TOK, dtype=jnp.int32)
    begun = places[None, :, None] >= starts[:, None, :]
    return jnp.sum(begun.astype(jnp.int32), axis=2)


def draw_padding(key, part):
    starts = image_starts(key)
    places = jnp.arange(PACK_TOK, dtype=jnp.int32)
    inside = (places[None, :, None] >= starts[:, None, :]) & (places[None, :, None] < starts[:, None, :] + IMG)
    return jnp.any(inside, axis=2).astype(jnp.int32)


def plant(values, own_key, low, largest):
    longest = values.shape.index(max(values.shape))
    spots = []
    for shift in (0, 1):
        where = [jax.random.randint(jax.random.fold_in(own_key, axis), (), 0, length) for axis, length in enumerate(values.shape)]
        where[longest] = (where[longest] + shift) % values.shape[longest]
        spots.append(tuple(where))
    return values.at[spots[0]].set(low).at[spots[1]].set(largest)


def shard_levels(rng, shape, cuts, least, top_value):
    def one(axis_at, parts):
        steps = jax.random.uniform(jax.random.fold_in(jax.random.fold_in(rng, 6), axis_at), (parts,), jnp.float32, least / len(cuts), top_value / len(cuts))
        return jnp.repeat(jnp.exp(steps), shape[axis_at] // parts).reshape((-1,) + (1,) * (len(shape) - axis_at - 1))

    level = one(*cuts[0])
    for cut in cuts[1:]:
        level = level * one(*cut)
    return level


def normal_values(key, extent, scale, limit, pieces=(), kind=jnp.bfloat16):
    values = scale * jax.random.normal(key, extent, jnp.float32)
    if pieces:
        values = values * shard_levels(key, extent, pieces, -0.22, 0.18)
    return jnp.clip(values, -limit, limit).astype(kind)


def setup_inputs(seed: int = 0) -> dict:
    key_list = jax.random.split(jax.random.key(seed), 25)
    return {
        "tokens": normal_values(key_list[0], (PACKS, PACK_TOK, D), 1.0, 6.0, ((0, 16), (1, 2))),
        "grad_out": normal_values(key_list[1], (PACKS, PACK_TOK, D), 1.0, 6.0, ((0, 16), (1, 2))),
        "segments": draw_segments(jax.random.fold_in(key_list[24], 71), 0),
        "padding": draw_padding(jax.random.fold_in(key_list[24], 71), 0),
        "adapter_ids": plant(jax.random.randint(key_list[4], (PACKS, NIMG), 0, ADAPTERS), jax.random.fold_in(key_list[4], 1), 0, ADAPTERS - 1).astype(jnp.int32),
        "norm1_gain": jnp.clip(1.0 + 0.1 * jax.random.normal(key_list[5], (D,), jnp.float32), 0.5, 1.5).astype(jnp.bfloat16),
        "norm1_bias": normal_values(key_list[6], (D,), 0.2, 1.1953125, ((0, 16),)),
        "w_qkv": normal_values(key_list[7], (D, 3 * D), D ** -0.5, 0.1875, ((0, 16),)),
        "w_proj": normal_values(key_list[8], (D, D), (max(D // 256, 1)) ** -0.5, 3.0, ((0, 16),)),
        "proj_bias": normal_values(key_list[9], (D,), 0.3, 1.796875, ((0, 16),)),
        "norm2_gain": jnp.clip(1.0 + 0.1 * jax.random.normal(key_list[10], (D,), jnp.float32), 0.5, 1.5).astype(jnp.bfloat16),
        "norm2_bias": normal_values(key_list[11], (D,), 0.2, 1.1953125, ((0, 16),)),
        "w_fc1": normal_values(key_list[12], (D, FF), D ** -0.5, 0.1875, ((0, 16),)),
        "fc1_bias": normal_values(key_list[13], (FF,), 0.5, 3.0, ((0, 16),)),
        "w_fc2": normal_values(key_list[14], (FF, D), FF ** -0.5, 0.09375, ((0, 16),)),
        "fc2_bias": normal_values(key_list[15], (D,), 0.3, 1.796875, ((0, 16),)),
        "qkv_down": normal_values(key_list[16], (D, ADAPT_COLS), D ** -0.5, 0.1875),
        "qkv_up": normal_values(key_list[17], (ADAPT_COLS, 3 * D), RANK ** -0.5, 1.5),
        "proj_down": normal_values(key_list[18], (D, ADAPT_COLS), (max(D // 256, 1)) ** -0.5, 3.0),
        "proj_up": normal_values(key_list[19], (ADAPT_COLS, D), RANK ** -0.5, 1.5),
        "fc1_down": normal_values(key_list[20], (D, ADAPT_COLS), D ** -0.5, 0.1875),
        "fc1_up": normal_values(key_list[21], (ADAPT_COLS, FF), RANK ** -0.5, 1.5),
        "fc2_down": normal_values(key_list[22], (FF, ADAPT_COLS), FF ** -0.5, 0.09375),
        "fc2_up": normal_values(key_list[23], (ADAPT_COLS, D), RANK ** -0.5, 1.5),
    }


highest_precision = lax.Precision.HIGHEST
norm_eps = 1e-06
masked_score = -1e+30

@jax.custom_vjp
def low(v):
    return lax.optimization_barrier(v.astype(jnp.bfloat16)).astype(jnp.float32)

@jax.custom_vjp
def low_back(v):
    return v

def low_keep(v):
    return (low(v), None)

def low_pass(kept, grad):
    return (grad,)

def back_keep(v):
    return (v, None)

def back_low(kept, grad):
    return (low(grad),)
low.defvjp(low_keep, low_pass)
low_back.defvjp(back_keep, back_low)

def matmul(left_side, right_side):
    return jnp.dot(left_side, right_side, precision=highest_precision, preferred_element_type=jnp.float32)

def layer_norm(values, norm_gain, norm_shift):
    centre = lax.optimization_barrier(jnp.mean(values, axis=-1, keepdims=True))
    centred = values - centre
    spread = lax.optimization_barrier(jnp.mean(centred * centred, axis=-1, keepdims=True))
    return centred * lax.rsqrt(spread + norm_eps) * norm_gain + norm_shift

def adapted(inputs, weight, down_map, up_map, select):
    inner_term = low(low_back(matmul(inputs, down_map)) * select)
    return matmul(inputs, weight) + matmul(inner_term, up_map)

def selection(segments, adapter_ids):
    images = jnp.arange(NIMG, dtype=jnp.int32)
    image_match = segments[:, :, None] - 1 == images[None, None, :]
    token_adapter = lax.optimization_barrier(jnp.sum(jnp.where(image_match, adapter_ids[:, None, :], 0), axis=2))
    present = jnp.any(image_match, axis=2)
    column = jnp.arange(ADAPTERS * RANK, dtype=jnp.int32) // RANK
    chosen = (token_adapter[:, :, None] == column[None, None, :]) & present[:, :, None]
    return chosen.astype(jnp.float32).reshape(PACKS * PACK_TOK, ADAPTERS * RANK)

def head_attention(query_heads, key_heads, value_heads, allowed):
    score_scale = HEAD_DIM ** (-0.5)
    scores = low_back(matmul(query_heads, key_heads.T) * score_scale)
    scores = jnp.where(allowed, scores, masked_score)
    row_max = lax.optimization_barrier(jnp.max(scores, axis=1, keepdims=True))
    weights = jnp.exp(scores - row_max)
    weights = weights / lax.optimization_barrier(jnp.sum(weights, axis=1, keepdims=True))
    return matmul(low(weights), value_heads)

def pack_attention(packed):
    qkv_rows, segment, keep_flags = packed
    allowed = (segment[:, None] == segment[None, :]) & (keep_flags[None, :] == 1)
    split_heads = qkv_rows.reshape(PACK_TOK, 3, HEADS, HEAD_DIM).transpose(1, 2, 0, 3)
    checked = jax.checkpoint(head_attention)

    def per_head(triple):
        return checked(triple[0], triple[1], triple[2], allowed)
    result = lax.map(per_head, (split_heads[0], split_heads[1], split_heads[2]))
    result = result.transpose(1, 0, 2).reshape(PACK_TOK, D)
    return result * keep_flags[:, None].astype(jnp.float32)

def reference(tokens, grad_out, segments, padding, adapter_ids, norm1_gain, norm1_bias, w_qkv, w_proj, proj_bias, norm2_gain, norm2_bias, w_fc1, fc1_bias, w_fc2, fc2_bias, qkv_down, qkv_up, proj_down, proj_up, fc1_down, fc1_up, fc2_down, fc2_up):
    select = selection(segments, adapter_ids)
    layer_in = tokens.astype(jnp.float32).reshape(PACKS * PACK_TOK, D)
    gain_one = norm1_gain.astype(jnp.float32)
    shift_one = norm1_bias.astype(jnp.float32)
    gain_two = norm2_gain.astype(jnp.float32)
    shift_two = norm2_bias.astype(jnp.float32)
    weight_qkv = w_qkv.astype(jnp.float32)
    weight_proj = w_proj.astype(jnp.float32)
    weight_fc1 = w_fc1.astype(jnp.float32)
    weight_fc2 = w_fc2.astype(jnp.float32)
    shift_proj = proj_bias.astype(jnp.float32)
    shift_fc1 = fc1_bias.astype(jnp.float32)
    shift_fc2 = fc2_bias.astype(jnp.float32)

    def forward(block_in, down_qkv, up_qkv, down_proj, up_proj, down_fc1, up_fc1, down_fc2, up_fc2):
        normed_one = low(layer_norm(block_in, gain_one, shift_one))
        qkv_rows = low(low_back(adapted(normed_one, weight_qkv, down_qkv, up_qkv, select)))
        packed = qkv_rows.reshape(PACKS, PACK_TOK, 3 * D)
        attended = lax.map(jax.checkpoint(pack_attention), (packed, segments, padding))
        attended = low(low_back(attended.reshape(PACKS * PACK_TOK, D)))
        branch_one = adapted(attended, weight_proj, down_proj, up_proj, select) + shift_proj
        middle = block_in + low_back(branch_one)
        normed_two = low(layer_norm(middle, gain_two, shift_two))
        hidden = low_back(adapted(normed_two, weight_fc1, down_fc1, up_fc1, select) + shift_fc1)
        active = low(jax.nn.gelu(hidden, approximate=False))
        branch_two = adapted(active, weight_fc2, down_fc2, up_fc2, select) + shift_fc2
        return middle + low_back(branch_two)
    factors = (qkv_down, qkv_up, proj_down, proj_up, fc1_down, fc1_up, fc2_down, fc2_up)
    factors = tuple((factor.astype(jnp.float32) for factor in factors))
    result, pullback = jax.vjp(forward, layer_in, *factors)
    grads = pullback(grad_out.astype(jnp.float32).reshape(PACKS * PACK_TOK, D))
    output = result.reshape(PACKS, PACK_TOK, D).astype(jnp.bfloat16)
    grad_tokens = grads[0].reshape(PACKS, PACK_TOK, D)
    return (output, grad_tokens, grads[1], grads[2], grads[3], grads[4], grads[5], grads[6], grads[7], grads[8])
```

```python
from functools import partial

import jax
import jax.numpy as jnp
from jax import lax
from jax.experimental import pallas as pl
from jax.experimental.pallas import tpu as pltpu
from jax.sharding import PartitionSpec as P

HEAD_DIM = 64
IMG = 577
RANK = 16
QBLOCK = 512


norm_eps = 1e-06
masked_score = -1e30


def matmul(left_side, right_side):
    return jnp.dot(left_side, right_side, preferred_element_type=jnp.float32)


def matmul_nt(left_side, right_side):
    return jnp.einsum("tk,jk->tj", left_side, right_side, preferred_element_type=jnp.float32)


def matmul_tn(left_side, right_side):
    return jnp.einsum("ti,to->io", left_side, right_side, preferred_element_type=jnp.float32)


def layer_norm(values, norm_gain, norm_shift):
    centre = jnp.mean(values, axis=-1, keepdims=True)
    centred = values - centre
    spread = jnp.mean(centred * centred, axis=-1, keepdims=True)
    return centred * lax.rsqrt(spread + norm_eps) * norm_gain + norm_shift


def norm_backward(values, norm_gain, norm_shift, grad_in):

    def apply_norm(inputs):
        return layer_norm(inputs, norm_gain, norm_shift)

    unused, pullback = jax.vjp(apply_norm, values)
    return pullback(grad_in)[0]


def selection(seg_own, image_adapters, columns):
    images = jnp.arange(image_adapters.shape[0], dtype=jnp.int32)
    image_match = seg_own[:, None] - 1 == images[None, :]
    token_adapter = jnp.sum(jnp.where(image_match, image_adapters[None, :], 0), axis=1)
    present = jnp.any(image_match, axis=1)
    column = jnp.arange(columns, dtype=jnp.int32) // RANK
    chosen = (token_adapter[:, None] == column[None, :]) & present[:, None]
    return chosen.astype(jnp.float32)


def adapter_forward(inputs_b, weight, down_map, up_map, select):
    inner_term = (matmul(inputs_b, down_map) * select).astype(jnp.bfloat16)
    return (matmul(inputs_b, weight) + matmul(inner_term, up_map), inner_term)


def adapter_backward(inputs_b, inner_term, grad_in, weight, down_map, up_map, select):
    grad_up = matmul_tn(inner_term, grad_in)
    grad_inner = (matmul_nt(grad_in, up_map) * select).astype(jnp.bfloat16)
    grad_down = matmul_tn(inputs_b, grad_inner)
    grad_inputs = matmul_nt(grad_in, weight) + matmul_nt(grad_inner, down_map)
    return (grad_inputs, grad_down, grad_up)


def block_scores(query_block, key_heads, seg_block, seg_keys, keep_keys):
    score_scale = HEAD_DIM ** (-0.5)
    scores = (
        jnp.einsum("qhd,khd->hqk", query_block, key_heads, preferred_element_type=jnp.float32)
        * score_scale
    )
    allowed = (seg_block[:, None] == seg_keys[None, :]) & (keep_keys[None, :] == 1)
    return jnp.where(allowed[None, :, :], scores, masked_score)


def split_heads(head_rows):
    all_rows = head_rows.shape[0]
    local_heads = head_rows.shape[2] // HEAD_DIM
    query_heads = head_rows[:, 0].reshape(all_rows, local_heads, HEAD_DIM)
    key_heads = head_rows[:, 1].reshape(all_rows, local_heads, HEAD_DIM)
    value_heads = head_rows[:, 2].reshape(all_rows, local_heads, HEAD_DIM)
    return (query_heads, key_heads, value_heads)


def key_window(all_rows):
    return min(all_rows, (QBLOCK + 2 * IMG - 2 + 127) // 128 * 128)


def window_start(block_index, all_rows, window):
    first = block_index * QBLOCK - (IMG - 1)
    return jnp.clip(first, 0, all_rows - window)


def attention_forward(head_rows, seg_all, keep_all):
    all_rows = head_rows.shape[0]
    block_count = all_rows // QBLOCK
    window = key_window(all_rows)
    query_heads, key_heads, value_heads = split_heads(head_rows)
    local_heads = query_heads.shape[1]

    def one_block(block_parts):
        query_block, seg_block, keep_block, block_index = block_parts
        start = window_start(block_index, all_rows, window)
        keys_near = lax.dynamic_slice_in_dim(key_heads, start, window, 0)
        values_near = lax.dynamic_slice_in_dim(value_heads, start, window, 0)
        seg_near = lax.dynamic_slice_in_dim(seg_all, start, window, 0)
        keep_near = lax.dynamic_slice_in_dim(keep_all, start, window, 0)
        scores = block_scores(query_block, keys_near, seg_block, seg_near, keep_near)
        row_max = jnp.max(scores, axis=2, keepdims=True)
        weights = jnp.exp(scores - row_max)
        row_sum = jnp.sum(weights, axis=2, keepdims=True)
        probs_low = (weights / row_sum).astype(jnp.bfloat16)
        result = jnp.einsum(
            "hqk,khd->qhd", probs_low, values_near, preferred_element_type=jnp.float32
        )
        result = result * keep_block[:, None, None].astype(jnp.float32)
        return (result.astype(jnp.bfloat16), row_max, row_sum)

    block_ids = jnp.arange(block_count, dtype=jnp.int32)
    blocked = (
        query_heads.reshape(block_count, QBLOCK, local_heads, HEAD_DIM),
        seg_all.reshape(block_count, QBLOCK),
        keep_all.reshape(block_count, QBLOCK),
        block_ids,
    )
    results, block_max, block_sums = lax.map(one_block, blocked)
    return (results.reshape(all_rows, local_heads * HEAD_DIM), block_max, block_sums)


def attention_backward(head_rows, grad_rows, seg_all, keep_all, block_max, block_sums):
    all_rows = head_rows.shape[0]
    block_count = all_rows // QBLOCK
    window = key_window(all_rows)
    query_heads, key_heads, value_heads = split_heads(head_rows)
    local_heads = query_heads.shape[1]
    score_scale = HEAD_DIM ** (-0.5)

    def one_block(running, block_parts):
        grad_keys, grad_values = running
        query_block, seg_block, keep_block, grad_block, row_max, row_sum, block_index = block_parts
        start = window_start(block_index, all_rows, window)
        keys_near = lax.dynamic_slice_in_dim(key_heads, start, window, 0)
        values_near = lax.dynamic_slice_in_dim(value_heads, start, window, 0)
        seg_near = lax.dynamic_slice_in_dim(seg_all, start, window, 0)
        keep_near = lax.dynamic_slice_in_dim(keep_all, start, window, 0)
        scores = block_scores(query_block, keys_near, seg_block, seg_near, keep_near)
        probs = jnp.exp(scores - row_max) / row_sum
        grad_result = grad_block * keep_block[:, None, None].astype(jnp.bfloat16)
        values_term = jnp.einsum(
            "hqk,qhd->khd",
            probs.astype(jnp.bfloat16),
            grad_result,
            preferred_element_type=jnp.float32,
        )
        grad_probs = jnp.einsum(
            "qhd,khd->hqk", grad_result, values_near, preferred_element_type=jnp.float32
        )
        row_inner = jnp.sum(probs * grad_probs, axis=2, keepdims=True)
        grad_scores = (probs * (grad_probs - row_inner)).astype(jnp.bfloat16)
        grad_query = (
            jnp.einsum("hqk,khd->qhd", grad_scores, keys_near, preferred_element_type=jnp.float32)
            * score_scale
        )
        keys_term = (
            jnp.einsum("hqk,qhd->khd", grad_scores, query_block, preferred_element_type=jnp.float32)
            * score_scale
        )
        grad_keys = lax.dynamic_update_slice_in_dim(
            grad_keys, lax.dynamic_slice_in_dim(grad_keys, start, window, 0) + keys_term, start, 0
        )
        grad_values = lax.dynamic_update_slice_in_dim(
            grad_values,
            lax.dynamic_slice_in_dim(grad_values, start, window, 0) + values_term,
            start,
            0,
        )
        return ((grad_keys, grad_values), grad_query)

    zero_heads = jnp.zeros((all_rows, local_heads, HEAD_DIM), jnp.float32)
    block_ids = jnp.arange(block_count, dtype=jnp.int32)
    blocked = (
        query_heads.reshape(block_count, QBLOCK, local_heads, HEAD_DIM),
        seg_all.reshape(block_count, QBLOCK),
        keep_all.reshape(block_count, QBLOCK),
        grad_rows.reshape(block_count, QBLOCK, local_heads, HEAD_DIM),
        block_max,
        block_sums,
        block_ids,
    )
    (grad_keys, grad_values), grad_queries = lax.scan(one_block, (zero_heads, zero_heads), blocked)
    flat_width = local_heads * HEAD_DIM
    stacked = jnp.stack(
        [
            grad_queries.reshape(all_rows, flat_width),
            grad_keys.reshape(all_rows, flat_width),
            grad_values.reshape(all_rows, flat_width),
        ],
        axis=1,
    )
    return stacked.astype(jnp.bfloat16)


def per_device(
    tokens,
    grad_out,
    segments,
    padding,
    adapter_ids,
    norm1_gain,
    norm1_bias,
    w_qkv,
    w_proj,
    proj_bias,
    norm2_gain,
    norm2_bias,
    w_fc1,
    fc1_bias,
    w_fc2,
    fc2_bias,
    qkv_down,
    qkv_up,
    proj_down,
    proj_up,
    fc1_down,
    fc1_up,
    fc2_down,
    fc2_up,
):
    tok_rows = tokens.shape[1]
    feat_width = tokens.shape[2]
    inputs = tokens[0].astype(jnp.float32)
    seg_all = segments[0]
    keep_all = padding[0]
    offset = lax.axis_index("seq") * tok_rows
    seg_own = lax.dynamic_slice_in_dim(seg_all, offset, tok_rows)
    select = selection(seg_own, adapter_ids[0], qkv_down.shape[1])
    gain_one, shift_one, qkv_weight, proj_weight, proj_shift = (
        lax.all_gather(norm1_gain, "fsdp", axis=0, tiled=True),
        lax.all_gather(norm1_bias, "fsdp", axis=0, tiled=True),
        lax.all_gather(w_qkv, "fsdp", axis=0, tiled=True),
        lax.all_gather(w_proj, "fsdp", axis=0, tiled=True),
        lax.all_gather(proj_bias, "fsdp", axis=0, tiled=True),
    )
    gain_one = gain_one.astype(jnp.float32)
    shift_one = shift_one.astype(jnp.float32)
    normed_one = layer_norm(inputs, gain_one, shift_one).astype(jnp.bfloat16)
    qkv_main, inner_one = adapter_forward(normed_one, qkv_weight, qkv_down, qkv_up, select)
    qkv_low = qkv_main.astype(jnp.bfloat16).reshape(tok_rows, 3, feat_width)
    head_rows = lax.all_to_all(qkv_low, "seq", split_axis=2, concat_axis=0, tiled=True)
    attended_heads, block_max, block_sums = attention_forward(head_rows, seg_all, keep_all)
    attended = lax.all_to_all(attended_heads, "seq", split_axis=0, concat_axis=1, tiled=True)
    branch_one, inner_two = adapter_forward(attended, proj_weight, proj_down, proj_up, select)
    middle = inputs + (branch_one + proj_shift.astype(jnp.float32))
    gain_two, shift_two, fc1_weight, fc2_shift, fc2_weight, fc1_shift = (
        lax.all_gather(norm2_gain, "fsdp", axis=0, tiled=True),
        lax.all_gather(norm2_bias, "fsdp", axis=0, tiled=True),
        lax.all_gather(w_fc1, "fsdp", axis=0, tiled=True),
        lax.all_gather(fc2_bias, "fsdp", axis=0, tiled=True),
        lax.all_gather(w_fc2, "fsdp", axis=0, tiled=True),
        lax.all_gather(fc1_bias, "fsdp", axis=0, tiled=True),
    )
    gain_two = gain_two.astype(jnp.float32)
    shift_two = shift_two.astype(jnp.float32)
    normed_two = layer_norm(middle, gain_two, shift_two).astype(jnp.bfloat16)
    hidden_main, inner_three = adapter_forward(normed_two, fc1_weight, fc1_down, fc1_up, select)
    hidden = hidden_main + fc1_shift.astype(jnp.float32)
    active = jax.nn.gelu(hidden, approximate=False).astype(jnp.bfloat16)
    branch_two, inner_four = adapter_forward(active, fc2_weight, fc2_down, fc2_up, select)
    output = (middle + (branch_two + fc2_shift.astype(jnp.float32))).astype(jnp.bfloat16)
    fc1_back, fc2_back = (
        lax.all_gather(w_fc1, "fsdp", axis=0, tiled=True),
        lax.all_gather(w_fc2, "fsdp", axis=0, tiled=True),
    )
    grad_top = grad_out[0]
    grad_active, grad_fc2_down, grad_fc2_up = adapter_backward(
        active, inner_four, grad_top, fc2_back, fc2_down, fc2_up, select
    )
    unused, gelu_back = jax.vjp(partial(jax.nn.gelu, approximate=False), hidden)
    grad_hidden = gelu_back(grad_active)[0].astype(jnp.bfloat16)
    grad_normed_two, grad_fc1_down, grad_fc1_up = adapter_backward(
        normed_two, inner_three, grad_hidden, fc1_back, fc1_down, fc1_up, select
    )
    grad_middle = grad_top.astype(jnp.float32) + norm_backward(
        middle, gain_two, shift_two, grad_normed_two
    )
    qkv_back, proj_back = (
        lax.all_gather(w_qkv, "fsdp", axis=0, tiled=True),
        lax.all_gather(w_proj, "fsdp", axis=0, tiled=True),
    )
    grad_branch_one = grad_middle.astype(jnp.bfloat16)
    grad_attended, grad_proj_down, grad_proj_up = adapter_backward(
        attended, inner_two, grad_branch_one, proj_back, proj_down, proj_up, select
    )
    grad_head_rows = lax.all_to_all(
        grad_attended.astype(jnp.bfloat16), "seq", split_axis=1, concat_axis=0, tiled=True
    )
    grad_qkv_heads = attention_backward(
        head_rows, grad_head_rows, seg_all, keep_all, block_max, block_sums
    )
    grad_qkv = lax.all_to_all(
        grad_qkv_heads, "seq", split_axis=0, concat_axis=2, tiled=True
    ).reshape(tok_rows, 3 * feat_width)
    grad_normed_one, grad_qkv_down, grad_qkv_up = adapter_backward(
        normed_one, inner_one, grad_qkv, qkv_back, qkv_down, qkv_up, select
    )
    grad_tokens = grad_middle + norm_backward(inputs, gain_one, shift_one, grad_normed_one)
    summed = lax.psum(
        (
            grad_qkv_down,
            grad_qkv_up,
            grad_proj_down,
            grad_proj_up,
            grad_fc1_down,
            grad_fc1_up,
            grad_fc2_down,
            grad_fc2_up,
        ),
        ("seq", "fsdp"),
    )
    return (
        output[None],
        grad_tokens[None],
        summed[0],
        summed[1],
        summed[2],
        summed[3],
        summed[4],
        summed[5],
        summed[6],
        summed[7],
    )


F32 = jnp.float32
BF16 = jnp.bfloat16
MESH = pl.DeviceIdType.MESH
VMEM_LIMIT = 64 * 1000 * 1000


def mm(a, b):
    return lax.dot_general(a, b, (((1,), (0,)), ((), ())), preferred_element_type=F32)


def mm_nt(a, b):
    return lax.dot_general(a, b, (((1,), (1,)), ((), ())), preferred_element_type=F32)


def mm_tn(a, b):
    return lax.dot_general(a, b, (((0,), (0,)), ((), ())), preferred_element_type=F32)


def norm_parts(v):
    mean = jnp.mean(v, axis=-1, keepdims=True)
    centred = v - mean
    r = lax.rsqrt(jnp.mean(centred * centred, axis=-1, keepdims=True) + norm_eps)
    return centred * r, r


def norm_grad(v, gain, grad_y):
    h, r = norm_parts(v)
    d = grad_y * gain
    return r * (d - jnp.mean(d, axis=-1, keepdims=True) - h * jnp.mean(d * h, axis=-1, keepdims=True))


class Net:
    def __init__(self):
        self.s = lax.axis_index("seq")
        self.f = lax.axis_index("fsdp")
        self.z = self.f // 4
        self.x = (self.f // 2) % 2
        self.c = self.f % 2
        self.partner = {"seq": 1 - self.s}
        self.x_peer = {"fsdp": self.block(self.z, 1 - self.x, self.c)}
        self.c_peer = {"fsdp": self.block(self.z, self.x, 1 - self.c)}

    def block(self, z, x, c):
        return (z * 2 + x) * 2 + c

    def z_peer(self, d):
        return {"fsdp": self.block((self.z + d) % 4, self.x, self.c)}

    def barrier(self):
        sem = pltpu.get_barrier_semaphore()
        peers = [self.partner, self.x_peer, self.c_peer] + [self.z_peer(d) for d in (1, 2, 3)]
        for peer in peers:
            pl.semaphore_signal(sem, inc=1, device_id=peer, device_id_type=MESH)
        pl.semaphore_wait(sem, len(peers))


class Gather:
    def __init__(self, net, items, send_sem, recv_sem, own_sem):
        self.net, self.items = net, items
        self.send_sem, self.recv_sem, self.own_sem = send_sem, recv_sem, own_sem
        self.sent, self.own = [], []

    def _copy(self, i, src, block, k, peer):
        return pltpu.make_async_remote_copy(
            src_ref=src, dst_ref=self.items[i][1](block), send_sem=self.send_sem.at[i, k],
            recv_sem=self.recv_sem.at[i, block], device_id=peer, device_id_type=MESH)

    def _send(self, i, src, block, k, peer):
        copy = self._copy(i, src, block, k, peer)
        copy.start()
        self.sent.append(copy)

    def _arrive(self, i, block):
        piece = self.items[i][1](block)
        self._copy(i, piece, block, 0, self.net.c_peer).wait_recv()
        return piece

    def start(self, i):
        net = self.net
        src = self.items[i][0]
        for d in (2, 1, 3):
            self._send(i, src, net.f, d - 1, net.z_peer(d))
        self._send(i, src, net.f, 3, net.x_peer)
        self._send(i, src, net.f, 4, net.c_peer)
        own = pltpu.make_async_copy(src, self.items[i][1](net.f), self.own_sem.at[i])
        own.start()
        self.own.append(own)

    def from_z(self, i):
        net = self.net
        for n, d in enumerate((1, 3, 2)):
            block = net.block((net.z + d) % 4, net.x, net.c)
            piece = self._arrive(i, block)
            self._send(i, piece, block, 5 + 2 * n, net.x_peer)
            self._send(i, piece, block, 6 + 2 * n, net.c_peer)

    def from_x(self, i):
        net = self.net
        for n, d in enumerate((0, 1, 3, 2)):
            block = net.block((net.z + d) % 4, 1 - net.x, net.c)
            piece = self._arrive(i, block)
            self._send(i, piece, block, 11 + n, net.c_peer)

    def from_core(self, i):
        net = self.net
        for d in (0, 1, 3, 2):
            for x in (net.x, 1 - net.x):
                self._arrive(i, net.block((net.z + d) % 4, x, 1 - net.c))
        self.own[i].wait()

    def finish(self):
        for copy in self.sent:
            copy.wait_send()


def full_vector(vec_ref, row, blocks=16, rows=16):
    parts = []
    for k in range(blocks // 2):
        even = vec_ref[2 * k * rows + row:2 * k * rows + row + 1, :]
        odd = vec_ref[(2 * k + 1) * rows + row:(2 * k + 1) * rows + row + 1, :]
        parts.append(even + odd)
    return jnp.concatenate(parts, axis=1)


WINDOW = 640
STEP = 64
PAD = 384
QROWS = 320


def choose(pick_ref, load):
    total = None
    for k in range(PAD // STEP + 1):
        value = load(k * STEP)
        value = value * pick_ref[k:k + 1, 0:1].astype(value.dtype)
        total = value if total is None else total + value
    return total


def lane_halves():
    lane = lax.broadcasted_iota(jnp.int32, (1, 128), 1)
    return [(lane < 64).astype(F32), (lane >= 64).astype(F32)]


def forward_kernel(pick_ref, bias_ref, keep_ref, x_ref, sel_ref, vec_ref, wq_hbm, wp_hbm, w1_hbm, w2_hbm, qd_ref, qu_hbm, pd_ref, pu_ref,
                   wqf, wpf, w1f, w2f, vecf_out, qkv_out, n1_out, c1_out, prob_out, oh_out, att_out, c2_out, mid_out, n2_out,
                   wq_own, wq, wp, xp, vecf, qu, qkv, n1, c1, qkvw, n1w, c1w, prob, opad, sendb, oh, att, c2, mid, n2,
                   xs_sem, xr_sem, as_sem, ar_sem, loc_sem, out_sem, g_send, g_recv, g_own):
    net = Net()
    s, other = net.s, 1 - net.s
    rows, width = x_ref.shape
    half = wq.shape[1] // 3
    rb = wq_own.shape[0]
    fr1, fc = w1_hbm.shape
    fr2 = w2_hbm.shape[0]
    n_fc1, n_fc2 = 4, 4

    pre = []
    for part in range(3):
        cols = pl.ds(pl.multiple_of(part * width + s * half, 128), half)
        pre.append(pltpu.make_async_copy(wq_hbm.at[:, cols], wq_own.at[:, pl.ds(part * half, half)], loc_sem.at[part]))
        pre.append(pltpu.make_async_copy(qu_hbm.at[:, cols], qu.at[:, pl.ds(part * half, half)], loc_sem.at[3 + part]))
    for copy in pre:
        copy.start()
    net.barrier()

    chunk = rows // 2
    xsend = []
    for i in range(2):
        part = pl.ds(i * chunk, chunk)
        copy = pltpu.make_async_remote_copy(
            src_ref=x_ref.at[part, :], dst_ref=xp.at[part, :], send_sem=xs_sem.at[i], recv_sem=xr_sem.at[i],
            device_id=net.partner, device_id_type=MESH)
        copy.start()
        xsend.append(copy)
    for copy in pre:
        copy.wait()

    items = [(vec_ref, lambda b: vecf.at[pl.ds(b * 16, 16), :]),
             (wq_own, lambda b: wq.at[pl.ds(b * rb, rb), :]),
             (wp_hbm, lambda b: wp.at[pl.ds(b * rb, rb), :])]
    for j in range(n_fc1):
        cols = pl.ds(j * (fc // n_fc1), fc // n_fc1)
        items.append((w1_hbm.at[:, cols], lambda b, cols=cols: w1f.at[pl.ds(b * fr1, fr1), cols]))
    sub = fr2 // n_fc2
    for j in range(n_fc2):
        items.append((w2_hbm.at[pl.ds(j * sub, sub), :],
                      lambda b, j=j: w2f.at[pl.ds(b * fr2 + j * sub, sub), :]))
    gather = Gather(net, items, g_send, g_recv, g_own)
    last = len(items) - 1

    gather.start(0)
    gather.start(1)
    zeros = jnp.zeros((PAD, 128), BF16)
    opad[0:PAD, :] = zeros
    opad[PAD + WINDOW:2 * PAD + WINDOW, :] = zeros
    gather.start(2)
    gather.from_z(0)
    gather.from_z(1)
    gather.from_x(0)
    gather.from_x(1)
    gather.start(3)
    gather.from_core(0)
    gather.from_core(1)

    gain1 = full_vector(vecf, 0)
    shift1 = full_vector(vecf, 1)

    def project(src, src_row, row):
        v = src[pl.ds(src_row, chunk), :].astype(F32)
        h, unused = norm_parts(v)
        normed = (h * gain1 + shift1).astype(BF16)
        at = pl.ds(row, chunk)
        n1[at, :] = normed
        inner = (mm(normed, qd_ref[...]) * sel_ref[at, :]).astype(BF16)
        c1[at, :] = inner
        for part in range(3):
            cols = pl.ds(part * half, half)
            qkv[at, cols] = (mm(normed, wq[:, cols]) + mm(inner, qu[:, cols])).astype(BF16)

    @pl.loop(0, 2)
    def _(i):
        project(x_ref, pl.multiple_of(i * chunk, chunk), pl.multiple_of(s * rows + i * chunk, chunk))

    gather.from_z(2)
    for i in range(2):
        xsend[i].wait_recv()
        project(xp, i * chunk, pl.multiple_of(other * rows + i * chunk, chunk))

    gather.from_x(2)
    gather.start(4)
    outs = []

    def put(src, dst):
        copy = pltpu.make_async_copy(src, dst, out_sem.at[len(outs)])
        copy.start()
        outs.append(copy)

    put(wq, wqf)
    put(vecf, vecf_out)
    for src, dst in ((qkv, qkvw), (n1, n1w), (c1, c1w)):
        step = min(src.shape[1], 512)
        for col in range(0, src.shape[1], step):
            dst[:, col:col + step] = choose(pick_ref, lambda at: src[at:at + WINDOW, col:col + step])
    put(qkvw, qkv_out)
    put(n1w, n1_out)
    put(c1w, c1_out)
    bias = bias_ref[0:1, :]
    halves = lane_halves()
    asend = []
    for pair in range(half // 128):
        k2 = qkvw[:, half + pair * 128:half + (pair + 1) * 128]
        v2 = qkvw[:, 2 * half + pair * 128:2 * half + (pair + 1) * 128]
        vs = [(v2 * hm.astype(BF16)) for hm in halves]

        @pl.loop(0, WINDOW // QROWS)
        def _(b):
            r0 = pl.multiple_of(b * QROWS, QROWS)
            q2 = qkvw[pl.ds(r0, QROWS), pair * 128:(pair + 1) * 128]
            q2 = q2 * jnp.asarray(HEAD_DIM ** (-0.5), BF16)
            total = None
            for hd in range(2):
                scores = mm_nt(q2 * halves[hd].astype(BF16), k2) + bias
                weights = jnp.exp(scores - jnp.max(scores, axis=1, keepdims=True))
                weights = (weights * (1.0 / jnp.sum(weights, axis=1, keepdims=True))).astype(BF16)
                prob[2 * pair + hd, pl.ds(r0, QROWS), :] = weights
                part = mm(weights, vs[hd])
                total = part if total is None else total + part
            total = (total * keep_ref[pl.ds(r0, QROWS), :]).astype(BF16)
            opad[pl.ds(PAD + r0, QROWS), :] = total
            oh[pl.ds(r0, QROWS), pair * 128:(pair + 1) * 128] = total

        def own_rows(who):
            return choose(pick_ref, lambda at: opad[pl.ds(pl.multiple_of(who * rows + PAD - at, STEP), rows), :])

        sendb[pair] = own_rows(other)
        cols = pl.ds(pl.multiple_of(s * half + pair * 128, 128), 128)
        copy = pltpu.make_async_remote_copy(
            src_ref=sendb.at[pair], dst_ref=att.at[:, cols], send_sem=as_sem.at[pair], recv_sem=ar_sem.at[pair],
            device_id=net.partner, device_id_type=MESH)
        copy.start()
        asend.append(copy)
        att[:, cols] = own_rows(s)
        if pair == 0:
            gather.from_core(2)
            put(wp, wpf)
        if pair == 1:
            gather.from_z(3)
        if pair == 2:
            gather.start(5)
            gather.from_x(3)
        if pair == 3:
            gather.from_z(4)
    put(prob, prob_out)
    put(oh, oh_out)
    for copy in asend:
        copy.wait_recv()
    put(att, att_out)

    bias_p = full_vector(vecf, 2)
    gain2 = full_vector(vecf, 3)
    shift2 = full_vector(vecf, 4)

    @pl.loop(0, 2)
    def _(i):
        at = pl.ds(pl.multiple_of(i * chunk, chunk), chunk)
        rows_in = att[at, :]
        inner = (mm(rows_in, pd_ref[...]) * sel_ref[pl.ds(pl.multiple_of(s * rows + i * chunk, chunk), chunk), :]).astype(BF16)
        c2[at, :] = inner
        branch = mm(rows_in, wp[...]) + mm(inner, pu_ref[...]) + bias_p
        middle = x_ref[at, :].astype(F32) + branch
        mid[at, :] = middle
        h, unused = norm_parts(middle)
        n2[at, :] = (h * gain2 + shift2).astype(BF16)

    put(c2, c2_out)
    put(mid, mid_out)
    put(n2, n2_out)
    gather.from_core(3)
    for i in range(4, last + 1):
        if i + 2 <= last:
            gather.start(i + 2)
        gather.from_x(i)
        if i + 1 <= last:
            gather.from_z(i + 1)
        gather.from_core(i)
    for copy in outs:
        copy.wait()
    for copy in xsend + asend:
        copy.wait_send()
    gather.finish()


def any_spec():
    return pl.BlockSpec(memory_space=pl.ANY)


def vmem_spec():
    return pl.BlockSpec(memory_space=pltpu.VMEM)


def run_forward(pick, bias, keep, x, sel, vec, wq, wp, w1, w2, qd, qu, pd, pu):
    rows, width = x.shape
    toks = sel.shape[0]
    half = width // 2
    ff = w1.shape[1]
    dma = pltpu.SemaphoreType.DMA
    n_items = 11
    sds = jax.ShapeDtypeStruct
    out_shape = (
        sds((width, 3 * half), BF16), sds((width, width), BF16), sds((width, ff), BF16), sds((ff, width), BF16),
        sds((256, 128), F32), sds((WINDOW, 3 * half), BF16), sds((WINDOW, width), BF16), sds((WINDOW, 128), BF16),
        sds((half // 64, WINDOW, WINDOW), BF16), sds((WINDOW, half), BF16), sds((rows, width), BF16), sds((rows, 128), BF16),
        sds((rows, width), F32), sds((rows, width), BF16))
    scratch = [
        pltpu.VMEM((wq.shape[0], 3 * half), BF16), pltpu.VMEM((width, 3 * half), BF16), pltpu.VMEM((width, width), BF16),
        pltpu.VMEM((rows, width), BF16), pltpu.VMEM((256, 128), F32), pltpu.VMEM((128, 3 * half), BF16),
        pltpu.VMEM((toks, 3 * half), BF16), pltpu.VMEM((toks, width), BF16), pltpu.VMEM((toks, 128), BF16),
        pltpu.VMEM((WINDOW, 3 * half), BF16), pltpu.VMEM((WINDOW, width), BF16), pltpu.VMEM((WINDOW, 128), BF16),
        pltpu.VMEM((half // 64, WINDOW, WINDOW), BF16), pltpu.VMEM((2 * PAD + WINDOW, 128), BF16),
        pltpu.VMEM((half // 128, rows, 128), BF16), pltpu.VMEM((WINDOW, half), BF16), pltpu.VMEM((rows, width), BF16),
        pltpu.VMEM((rows, 128), BF16), pltpu.VMEM((rows, width), F32), pltpu.VMEM((rows, width), BF16),
        dma((2,)), dma((2,)), dma((4,)), dma((4,)), dma((6,)), dma((12,)),
        dma((n_items, 15)), dma((n_items, 16)), dma((n_items,))]
    return pl.pallas_call(
        forward_kernel, out_shape=out_shape,
        in_specs=[vmem_spec()] * 6 + [any_spec(), any_spec(), any_spec(), any_spec(),
                  vmem_spec(), any_spec(), vmem_spec(), vmem_spec()],
        out_specs=tuple(any_spec() for unused in out_shape), scratch_shapes=scratch,
        compiler_params=pltpu.CompilerParams(collective_id=1, has_side_effects=True, vmem_limit_bytes=VMEM_LIMIT),
        name="forward")(pick, bias, keep, x, sel, vec, wq, wp, w1, w2, qd, qu, pd, pu)


FFB = 512


def ffn_kernel(n2_ref, mid_ref, g_ref, sel_ref, w1_ref, w2_ref, u1_ref, d1_ref, u2_ref, d2_ref, vec_ref,
               out_ref, gm_ref, gr_ref, oacc, gacc, u4, e3, c3, e4, c3t, e4t, act_s, gh_s):
    j = pl.program_id(0)
    steps = pl.num_programs(0)
    rows = n2_ref.shape[0]
    half = rows // 2
    ff = FFB * 8

    @pl.when(j == 0)
    def _():
        c = (mm(n2_ref[...], d1_ref[...]) * sel_ref[...])
        e = (mm_nt(g_ref[...], u2_ref[...]) * sel_ref[...])
        c3[...] = c.astype(BF16)
        e4[...] = e.astype(BF16)
        c3t[...] = c.T.astype(BF16)
        e4t[...] = e.T.astype(BF16)
        oacc[...] = jnp.zeros_like(oacc)
        gacc[...] = jnp.zeros_like(gacc)
        u4[...] = jnp.zeros_like(u4)
        e3[...] = jnp.zeros_like(e3)

    bias = jnp.concatenate([vec_ref[pl.ds(2 * j * 16 + 6, 1), :], vec_ref[pl.ds(2 * j * 16 + 7, 1), :],
                            vec_ref[pl.ds((2 * j + 1) * 16 + 6, 1), :], vec_ref[pl.ds((2 * j + 1) * 16 + 7, 1), :]], axis=1)

    @pl.loop(0, 2)
    def _(i):
        at = pl.ds(pl.multiple_of(i * half, half), half)
        hidden = mm(n2_ref[at, :], w1_ref[...]) + mm(c3[at, :], u1_ref[...]) + bias
        cdf = 0.5 * (1.0 + lax.erf(hidden * (0.5 ** 0.5)))
        pdf = jnp.exp(hidden * hidden * -0.5) * (0.5 / 3.141592653589793) ** 0.5
        active = (hidden * cdf).astype(BF16)
        act_s[at, :] = active
        grad_active = mm_nt(g_ref[at, :], w2_ref[...]) + mm_nt(e4[at, :], d2_ref[...])
        grad_hidden = (grad_active * (cdf + hidden * pdf)).astype(BF16)
        gh_s[at, :] = grad_hidden
        oacc[at, :] += mm(active, w2_ref[...])
        u4[at, :] += mm(active, d2_ref[...])
        gacc[at, :] += mm_nt(grad_hidden, w1_ref[...])
        e3[at, :] += mm_nt(grad_hidden, u1_ref[...])

    def compact(dense):
        total = dense[0:16]
        for k in range(1, 8):
            total = total + dense[16 * k:16 * (k + 1)]
        return total.astype(BF16)

    col = pl.multiple_of(j * FFB, FFB)
    gr_ref[:, pl.ds(col, FFB)] = compact(mm(c3t[...], gh_s[...]))
    gr_ref[:, pl.ds(pl.multiple_of(ff + j * FFB, FFB), FFB)] = compact(mm(e4t[...], act_s[...]))

    @pl.when(j == steps - 1)
    def _():
        e = e3[...] * sel_ref[...]
        c = u4[...] * sel_ref[...]
        gr_ref[:, 2 * ff:2 * ff + 1024] = compact(mm(e.T.astype(BF16), n2_ref[...]))
        gr_ref[:, 2 * ff + 1024:2 * ff + 2048] = compact(mm(c.T.astype(BF16), g_ref[...]))
        e3[...] = e
        u4[...] = c
        gain2 = full_vector(vec_ref, 3)
        bias2 = full_vector(vec_ref, 5)

        @pl.loop(0, 2)
        def _(i):
            at = pl.ds(pl.multiple_of(i * half, half), half)
            branch = oacc[at, :] + mm(u4[at, :].astype(BF16), u2_ref[...]) + bias2
            out_ref[at, :] = (mid_ref[at, :] + branch).astype(BF16)
            grad_n2 = gacc[at, :] + mm_nt(e3[at, :].astype(BF16), d1_ref[...])
            gm_ref[at, :] = g_ref[at, :].astype(F32) + norm_grad(mid_ref[at, :], gain2, grad_n2)


def run_ffn(n2, mid, g, sel_own, w1, w2, u1, d1, u2, d2, vec):
    rows, width = n2.shape
    ff = w1.shape[1]
    sds = jax.ShapeDtypeStruct

    def const(shape):
        return pl.BlockSpec(shape, lambda j: (0, 0), pipeline_mode=pl.Buffered(1))

    def outc(shape):
        return pl.BlockSpec(shape, lambda j: (0, 0))

    return pl.pallas_call(
        ffn_kernel, grid=(ff // FFB,),
        out_shape=(sds((rows, width), BF16), sds((rows, width), F32), sds((16, 2 * ff + 2 * width), BF16)),
        in_specs=[const((rows, width)), const((rows, width)), const((rows, width)), const((rows, 128)),
                  pl.BlockSpec((width, FFB), lambda j: (0, j)), pl.BlockSpec((FFB, width), lambda j: (j, 0)),
                  pl.BlockSpec((128, FFB), lambda j: (0, j)), const((width, 128)), const((128, width)),
                  pl.BlockSpec((FFB, 128), lambda j: (j, 0)), const((256, 128))],
        out_specs=(outc((rows, width)), outc((rows, width)), outc((16, 2 * ff + 2 * width))),
        scratch_shapes=[pltpu.VMEM((rows, width), F32), pltpu.VMEM((rows, width), F32), pltpu.VMEM((rows, 128), F32),
                        pltpu.VMEM((rows, 128), F32), pltpu.VMEM((rows, 128), BF16), pltpu.VMEM((rows, 128), BF16),
                        pltpu.VMEM((128, rows), BF16), pltpu.VMEM((128, rows), BF16), pltpu.VMEM((rows, FFB), BF16),
                        pltpu.VMEM((rows, FFB), BF16)],
        compiler_params=pltpu.CompilerParams(vmem_limit_bytes=VMEM_LIMIT),
        name="feedforward")(n2, mid, g, sel_own, w1, w2, u1, d1, u2, d2, vec)


def compact_rows(dense):
    total = dense[0:16]
    for k in range(1, 8):
        total = total + dense[16 * k:16 * (k + 1)]
    return total.astype(BF16)


def backward_kernel(pick_ref, keep_ref, sel_w_ref, gm_ref, sel_ref, att_ref, c2_ref, oh_ref, pd_ref, pu_ref, qd_ref, gf_ref, wp_ref,
                    wq_hbm, qkv_hbm, n1_hbm, c1_hbm, prob_hbm, qu_hbm,
                    gall, gn_out,
                    wq, qkv, n1, c1, prob, qu, g1, e2, gsend, do_s, first_own, first_send, first_in, gq, qsend, qdown, qdown_in, qown,
                    gpad, psend, prcv, gn,
                    loc_sem, ds_sem, dr_sem, fs_sem, fr_sem, qs_sem, qr_sem, ps_sem, pr_sem, out_sem, g_send, g_recv, g_own):
    net = Net()
    s, other = net.s, 1 - net.s
    rows, width = gm_ref.shape
    half = wq.shape[1] // 3
    chunk = rows // 2
    ffn_cols = gf_ref.shape[1]

    loads = [pltpu.make_async_copy(src, dst, loc_sem.at[i]) for i, (src, dst) in enumerate(
        [(qkv_hbm, qkv), (prob_hbm, prob), (wq_hbm, wq), (n1_hbm, n1), (c1_hbm, c1)])]
    for part in range(3):
        cols = pl.ds(pl.multiple_of(part * width + s * half, 128), half)
        loads.append(pltpu.make_async_copy(qu_hbm.at[:, cols], qu.at[:, pl.ds(part * half, half)], loc_sem.at[5 + part]))
    for copy in loads:
        copy.start()
    net.barrier()

    @pl.loop(0, 2)
    def _(i):
        at = pl.ds(pl.multiple_of(i * chunk, chunk), chunk)
        low = gm_ref[at, :].astype(BF16)
        g1[at, :] = low
        e2[at, :] = mm_nt(low, pu_ref[...]) * sel_ref[at, :]

    def grad_att(i, who):
        at = pl.ds(i * chunk, chunk)
        heads = pl.ds(pl.multiple_of(who * half, half), half)
        return (mm_nt(g1[at, :], wp_ref[heads, :]) + mm_nt(e2[at, :].astype(BF16), pd_ref[heads, :])).astype(BF16)

    dsend = []
    for i in range(2):
        gsend[i] = grad_att(i, other)
        copy = pltpu.make_async_remote_copy(
            src_ref=gsend.at[i], dst_ref=do_s.at[pl.ds(pl.multiple_of(s * rows + i * chunk, chunk), chunk), :],
            send_sem=ds_sem.at[i], recv_sem=dr_sem.at[i], device_id=net.partner, device_id_type=MESH)
        copy.start()
        dsend.append(copy)
    first_own[:, 0:ffn_cols] = gf_ref[...]
    first_own[:, ffn_cols:ffn_cols + width] = compact_rows(mm_tn(c2_ref[...], g1[...]))
    first_own[:, ffn_cols + width:ffn_cols + 2 * width] = compact_rows(mm_tn(e2[...].astype(BF16), att_ref[...]))
    fsend = pltpu.make_async_remote_copy(
        src_ref=first_own, dst_ref=first_in, send_sem=fs_sem.at[0], recv_sem=fr_sem.at[0],
        device_id=net.partner, device_id_type=MESH)
    fsend.start()
    for i in range(2):
        do_s[pl.ds(pl.multiple_of(s * rows + i * chunk, chunk), chunk), :] = grad_att(i, s)
    n_first = first_own.shape[1]
    items = [(first_send, lambda b: gall.at[pl.ds(b * 16, 16), pl.ds(0, n_first)]),
             (qown, lambda b: gall.at[pl.ds(b * 16, 16), pl.ds(n_first, 4 * width)])]
    gather = Gather(net, items, g_send, g_recv, g_own)
    zeros = jnp.zeros((PAD, width), F32)
    gpad[0:PAD, :] = zeros
    gpad[PAD + WINDOW:2 * PAD + WINDOW, :] = zeros
    for copy in loads:
        copy.wait()
    for copy in dsend:
        copy.wait_recv()
    fsend.wait_recv()
    first_send[...] = (first_own[...].astype(F32) + first_in[...].astype(F32)).astype(BF16)
    gather.start(0)

    halves = lane_halves()
    scale = HEAD_DIM ** (-0.5)
    keep = keep_ref[...].astype(BF16)
    for pair in range(half // 128):
        cols = slice(pair * 128, (pair + 1) * 128)
        k2 = qkv[:, half + pair * 128:half + (pair + 1) * 128]
        v2 = qkv[:, 2 * half + pair * 128:2 * half + (pair + 1) * 128]
        q2 = qkv[:, cols] * jnp.asarray(scale, BF16)
        do2 = choose(pick_ref, lambda at: do_s[at:at + WINDOW, cols]) * keep
        inner = do2.astype(F32) * oh_ref[:, cols].astype(F32)
        gv = gk = gqq = None
        for hd in range(2):
            hm = halves[hd].astype(BF16)
            weights = prob[2 * pair + hd]
            grad_p = mm_nt(do2 * hm, v2)
            row_inner = jnp.sum(inner * halves[hd], axis=1, keepdims=True)
            grad_s = (weights.astype(F32) * (grad_p - row_inner)).astype(BF16)
            dv = mm_tn(weights, do2 * hm)
            dk = mm_tn(grad_s, q2 * hm)
            dq = mm(grad_s, k2 * hm)
            gv = dv if gv is None else gv + dv
            gk = dk if gk is None else gk + dk
            gqq = dq if gqq is None else gqq + dq
        gq[:, cols] = (gqq * scale).astype(BF16)
        gq[:, half + pair * 128:half + (pair + 1) * 128] = gk.astype(BF16)
        gq[:, 2 * half + pair * 128:2 * half + (pair + 1) * 128] = gv.astype(BF16)
        if pair == 1:
            gather.from_z(0)
        if pair == 2:
            gather.from_x(0)

    up = compact_rows(mm_tn(c1[...], gq[...]))
    e1 = (mm_nt(gq[...], qu[...]) * sel_w_ref[...]).astype(BF16)
    down = mm_tn(e1, n1[...])
    qdown[...] = compact_rows(down)
    qsends = []
    for part in range(3):
        cols = pl.ds(pl.multiple_of(part * width + s * half, 128), half)
        qsend[:, pl.ds(part * half, half)] = up[:, part * half:(part + 1) * half]
        qown[:, cols] = up[:, part * half:(part + 1) * half]
        qsends.append(pltpu.make_async_remote_copy(
            src_ref=qsend.at[:, pl.ds(part * half, half)], dst_ref=qown.at[:, cols], send_sem=qs_sem.at[part],
            recv_sem=qr_sem.at[part], device_id=net.partner, device_id_type=MESH))
    qsends.append(pltpu.make_async_remote_copy(
        src_ref=qdown, dst_ref=qdown_in, send_sem=qs_sem.at[3],
        recv_sem=qr_sem.at[3], device_id=net.partner, device_id_type=MESH))
    for copy in qsends:
        copy.start()

    @pl.loop(0, 2)
    def _(i):
        at = pl.ds(pl.multiple_of(i * QROWS, QROWS), QROWS)
        e1_rows = (mm_nt(gq[at, :], qu[...]) * sel_w_ref[at, :]).astype(BF16)
        gpad[pl.ds(pl.multiple_of(PAD + i * QROWS, STEP), QROWS), :] = mm_nt(gq[at, :], wq[...]) + mm_nt(e1_rows, qd_ref[...])

    psends = []
    for i in range(2):
        psend[i] = choose(pick_ref, lambda at: gpad[
            pl.ds(pl.multiple_of(other * rows + PAD + i * chunk - at, STEP), chunk), :]).astype(BF16)
        copy = pltpu.make_async_remote_copy(
            src_ref=psend.at[i], dst_ref=prcv.at[i], send_sem=ps_sem.at[i], recv_sem=pr_sem.at[i],
            device_id=net.partner, device_id_type=MESH)
        copy.start()
        psends.append(copy)
    for copy in qsends:
        copy.wait_recv()
    qown[:, 3 * width:4 * width] = (qdown[...].astype(F32) + qdown_in[...].astype(F32)).astype(BF16)
    gather.start(1)
    gather.from_core(0)
    gather.from_z(1)
    gather.from_x(1)
    gather.from_core(1)
    outs = []
    for i in range(2):
        psends[i].wait_recv()
        rows_at = pl.ds(i * chunk, chunk)
        gn[rows_at, :] = prcv[i].astype(F32) + choose(pick_ref, lambda at: gpad[
            pl.ds(pl.multiple_of(s * rows + PAD + i * chunk - at, STEP), chunk), :])
        copy = pltpu.make_async_copy(gn.at[rows_at, :], gn_out.at[rows_at, :], out_sem.at[i])
        copy.start()
        outs.append(copy)
    for copy in outs:
        copy.wait()
    for copy in dsend + [fsend] + qsends + psends:
        copy.wait_send()
    gather.finish()


def run_backward(pick, keep, sel_w, gm, sel, att, c2, oh, pd, pu, qd, gf, wp, wq, qkv, n1, c1, prob, qu):
    rows, width = gm.shape
    toks = 2 * rows
    half = width // 2
    dma = pltpu.SemaphoreType.DMA
    sds = jax.ShapeDtypeStruct
    n_first = gf.shape[1] + 2 * width
    out_shape = (sds((256, n_first + 4 * width), BF16), sds((rows, width), F32))
    chunk = rows // 2
    scratch = [
        pltpu.VMEM(wq.shape, BF16), pltpu.VMEM(qkv.shape, BF16), pltpu.VMEM(n1.shape, BF16), pltpu.VMEM(c1.shape, BF16),
        pltpu.VMEM(prob.shape, BF16), pltpu.VMEM((128, 3 * half), BF16), pltpu.VMEM((rows, width), BF16),
        pltpu.VMEM((rows, 128), F32), pltpu.VMEM((2, chunk, half), BF16), pltpu.VMEM((toks, half), BF16),
        pltpu.VMEM((16, n_first), BF16), pltpu.VMEM((16, n_first), BF16), pltpu.VMEM((16, n_first), BF16),
        pltpu.VMEM((WINDOW, 3 * half), BF16), pltpu.VMEM((16, 3 * half), BF16), pltpu.VMEM((16, width), BF16),
        pltpu.VMEM((16, width), BF16), pltpu.VMEM((16, 4 * width), BF16), pltpu.VMEM((2 * PAD + WINDOW, width), F32), pltpu.VMEM((2, chunk, width), BF16),
        pltpu.VMEM((2, chunk, width), BF16), pltpu.VMEM((rows, width), F32),
        dma((8,)), dma((2,)), dma((2,)), dma((1,)), dma((1,)), dma((4,)), dma((4,)), dma((2,)), dma((2,)), dma((2,)),
        dma((2, 15)), dma((2, 16)), dma((2,))]
    return pl.pallas_call(
        backward_kernel, out_shape=out_shape,
        in_specs=[vmem_spec()] * 13 + [any_spec()] * 6,
        out_specs=tuple(any_spec() for unused in out_shape), scratch_shapes=scratch,
        compiler_params=pltpu.CompilerParams(collective_id=2, has_side_effects=True, vmem_limit_bytes=VMEM_LIMIT),
        name="backward")(pick, keep, sel_w, gm, sel, att, c2, oh, pd, pu, qd, gf, wp, wq, qkv, n1, c1, prob, qu)


def expand_kernel(vec_ref, f1u, f2d, f1d, f2u, pu, pdn, qu, qd, gn, x, gm,
                  gt_out, qd_out, qu_out, pd_out, pu_out, f1d_out, f1u_out, f2d_out, f2u_out):
    ids = jnp.concatenate([jnp.broadcast_to(vec_ref[16 * p + 8:16 * p + 9, :], (16, 128)) for p in range(16)], axis=0)
    r = lax.broadcasted_iota(jnp.int32, (256, 128), 0) % 16
    col = lax.broadcasted_iota(jnp.int32, (256, 128), 1)
    pick = ((ids.astype(jnp.int32) == col // 16) & (r == col % 16)).astype(F32)
    pick_t = pick.T.astype(BF16)
    for src, dst in ((f1u, f1u_out), (f2u, f2u_out), (pu, pu_out), (qu, qu_out)):
        dst[...] = mm(pick_t, src[...])
    for src, dst in ((f1d, f1d_out), (f2d, f2d_out), (pdn, pd_out), (qd, qd_out)):
        dst[...] = mm(pick_t, src[...]).T
    gain1 = full_vector(vec_ref, 0)
    gt_out[...] = gm[...] + norm_grad(x[...].astype(F32), gain1, gn[...])


def run_expand(vec, gall, gn, x, gm):
    rows, width = gn.shape
    ff = 4 * width
    n = 4
    sds = jax.ShapeDtypeStruct

    def part(cols, offset):
        return pl.BlockSpec((256, cols), lambda j: (0, offset // cols + j))

    def by_row(shape):
        return pl.BlockSpec(shape, lambda j: (j, 0))

    def by_col(shape):
        return pl.BlockSpec(shape, lambda j: (0, j))

    q = width // n
    return pl.pallas_call(
        expand_kernel, grid=(n,),
        out_shape=(sds((rows, width), F32), sds((width, 128), F32), sds((128, 3 * width), F32), sds((width, 128), F32),
                   sds((128, width), F32), sds((width, 128), F32), sds((128, ff), F32), sds((ff, 128), F32), sds((128, width), F32)),
        in_specs=[pl.BlockSpec((256, 128), lambda j: (0, 0)), part(ff // n, 0), part(ff // n, ff), part(q, 2 * ff),
                  part(q, 2 * ff + width), part(q, 2 * ff + 2 * width), part(q, 2 * ff + 3 * width),
                  part(3 * q, 2 * ff + 4 * width), part(q, 2 * ff + 7 * width),
                  by_row((rows // n, width)), by_row((rows // n, width)), by_row((rows // n, width))],
        out_specs=(by_row((rows // n, width)), by_row((q, 128)), by_col((128, 3 * q)), by_row((q, 128)), by_col((128, q)),
                   by_row((q, 128)), by_col((128, ff // n)), by_row((ff // n, 128)), by_col((128, q))),
        compiler_params=pltpu.CompilerParams(vmem_limit_bytes=VMEM_LIMIT),
        name="expand")(vec, *([gall] * 8), gn, x, gm)


def per_device_fast(tokens, grad_out, segments, padding, adapter_ids, norm1_gain, norm1_bias, w_qkv, w_proj, proj_bias,
                    norm2_gain, norm2_bias, w_fc1, fc1_bias, w_fc2, fc2_bias, qkv_down, qkv_up, proj_down, proj_up,
                    fc1_down, fc1_up, fc2_down, fc2_up):
    rows = tokens.shape[1]
    x = tokens[0]
    g = grad_out[0]
    seg = segments[0]
    start = jnp.sum((seg == 0).astype(jnp.int32))
    base = start // STEP * STEP
    pick = jnp.broadcast_to((base == jnp.arange(8, dtype=jnp.int32) * STEP).astype(F32)[:, None], (8, 128))
    inside = jnp.arange(WINDOW, dtype=jnp.int32) + (base - start)
    inside = (inside >= 0) & (inside < IMG)
    bias = jnp.broadcast_to(jnp.where(inside, 0.0, masked_score).astype(F32)[None, :], (8, WINDOW))
    keep = jnp.broadcast_to(inside.astype(F32)[:, None], (WINDOW, 128))
    sel = selection(seg, adapter_ids[0], qkv_down.shape[1])
    sel_own = lax.dynamic_slice_in_dim(sel, lax.axis_index("seq") * rows, rows, 0)
    sel_w = lax.dynamic_slice_in_dim(sel, base, WINDOW, 0)
    odd = (lax.axis_index("fsdp") % 2).astype(F32)
    six = jnp.stack([norm1_gain, norm1_bias, proj_bias, norm2_gain, norm2_bias, fc2_bias]).astype(F32)
    vec = jnp.concatenate([
        jnp.concatenate([six * (1.0 - odd), six * odd], axis=1), fc1_bias.astype(F32).reshape(2, 128),
        jnp.broadcast_to(adapter_ids[0].astype(F32)[:, None], (1, 128)), jnp.zeros((7, 128), F32)], axis=0)
    (wq, wp, w1, w2, vecf, qkv, n1, c1, prob, oh, att, c2, mid, n2) = run_forward(
        pick, bias, keep, x, sel, vec, w_qkv, w_proj, w_fc1, w_fc2, qkv_down, qkv_up, proj_down, proj_up)
    out, gm, gf = run_ffn(n2, mid, g, sel_own, w1, w2, fc1_up, fc1_down, fc2_up, fc2_down, vecf)
    gall, gn = run_backward(pick, keep, sel_w, gm, sel_own, att, c2, oh, proj_down, proj_up, qkv_down, gf, wp, wq, qkv, n1, c1, prob, qkv_up)
    gt, gqd, gqu, gpd, gpu, gf1d, gf1u, gf2d, gf2u = run_expand(vecf, gall, gn, x, gm)
    return out[None], gt[None], gqd, gqu, gpd, gpu, gf1d, gf1u, gf2d, gf2u


def solution(mesh):
    sizes = dict(mesh.shape)
    small = sizes == {"seq": 2, "fsdp": 16}

    def per_device_any(*args):
        tokens, adapter_ids = args[0], args[4]
        one_image = tokens.shape[1:] == (512, 1024) and adapter_ids.shape[1] == 1
        return (per_device_fast if small and one_image else per_device)(*args)

    return jax.shard_map(
        per_device_any,
        mesh=mesh,
        in_specs=(
            P("fsdp", "seq", None),
            P("fsdp", "seq", None),
            P("fsdp", None),
            P("fsdp", None),
            P("fsdp", None),
            P("fsdp"),
            P("fsdp"),
            P("fsdp", None),
            P("fsdp", None),
            P("fsdp"),
            P("fsdp"),
            P("fsdp"),
            P("fsdp", None),
            P("fsdp"),
            P("fsdp", None),
            P("fsdp"),
            P(),
            P(),
            P(),
            P(),
            P(),
            P(),
            P(),
            P(),
        ),
        out_specs=(
            P("fsdp", "seq", None),
            P("fsdp", "seq", None),
            P(),
            P(),
            P(),
            P(),
            P(),
            P(),
            P(),
            P(),
        ),
        check_vma=False,
    )
```

```python
from functools import partial

import jax
import jax.numpy as jnp
from jax import lax
from jax.experimental import pallas as pl
from jax.experimental.pallas import tpu as pltpu
from jax.sharding import PartitionSpec as P

HEAD_DIM = 64
IMG = 577
RANK = 16
QBLOCK = 512


norm_eps = 1e-06
masked_score = -1e30


def matmul(left_side, right_side):
    return jnp.dot(left_side, right_side, preferred_element_type=jnp.float32)


def matmul_nt(left_side, right_side):
    return jnp.einsum("tk,jk->tj", left_side, right_side, preferred_element_type=jnp.float32)


def matmul_tn(left_side, right_side):
    return jnp.einsum("ti,to->io", left_side, right_side, preferred_element_type=jnp.float32)


def layer_norm(values, norm_gain, norm_shift):
    centre = jnp.mean(values, axis=-1, keepdims=True)
    centred = values - centre
    spread = jnp.mean(centred * centred, axis=-1, keepdims=True)
    return centred * lax.rsqrt(spread + norm_eps) * norm_gain + norm_shift


def norm_backward(values, norm_gain, norm_shift, grad_in):

    def apply_norm(inputs):
        return layer_norm(inputs, norm_gain, norm_shift)

    unused, pullback = jax.vjp(apply_norm, values)
    return pullback(grad_in)[0]


def selection(seg_own, image_adapters, columns):
    images = jnp.arange(image_adapters.shape[0], dtype=jnp.int32)
    image_match = seg_own[:, None] - 1 == images[None, :]
    token_adapter = jnp.sum(jnp.where(image_match, image_adapters[None, :], 0), axis=1)
    present = jnp.any(image_match, axis=1)
    column = jnp.arange(columns, dtype=jnp.int32) // RANK
    chosen = (token_adapter[:, None] == column[None, :]) & present[:, None]
    return chosen.astype(jnp.float32)


def adapter_forward(inputs_b, weight, down_map, up_map, select):
    inner_term = (matmul(inputs_b, down_map) * select).astype(jnp.bfloat16)
    return (matmul(inputs_b, weight) + matmul(inner_term, up_map), inner_term)


def adapter_backward(inputs_b, inner_term, grad_in, weight, down_map, up_map, select):
    grad_up = matmul_tn(inner_term, grad_in)
    grad_inner = (matmul_nt(grad_in, up_map) * select).astype(jnp.bfloat16)
    grad_down = matmul_tn(inputs_b, grad_inner)
    grad_inputs = matmul_nt(grad_in, weight) + matmul_nt(grad_inner, down_map)
    return (grad_inputs, grad_down, grad_up)


def block_scores(query_block, key_heads, seg_block, seg_keys, keep_keys):
    score_scale = HEAD_DIM ** (-0.5)
    scores = (
        jnp.einsum("qhd,khd->hqk", query_block, key_heads, preferred_element_type=jnp.float32)
        * score_scale
    )
    allowed = (seg_block[:, None] == seg_keys[None, :]) & (keep_keys[None, :] == 1)
    return jnp.where(allowed[None, :, :], scores, masked_score)


def split_heads(head_rows):
    all_rows = head_rows.shape[0]
    local_heads = head_rows.shape[2] // HEAD_DIM
    query_heads = head_rows[:, 0].reshape(all_rows, local_heads, HEAD_DIM)
    key_heads = head_rows[:, 1].reshape(all_rows, local_heads, HEAD_DIM)
    value_heads = head_rows[:, 2].reshape(all_rows, local_heads, HEAD_DIM)
    return (query_heads, key_heads, value_heads)


def key_window(all_rows):
    return min(all_rows, (QBLOCK + 2 * IMG - 2 + 127) // 128 * 128)


def window_start(block_index, all_rows, window):
    first = block_index * QBLOCK - (IMG - 1)
    return jnp.clip(first, 0, all_rows - window)


def attention_forward(head_rows, seg_all, keep_all):
    all_rows = head_rows.shape[0]
    block_count = all_rows // QBLOCK
    window = key_window(all_rows)
    query_heads, key_heads, value_heads = split_heads(head_rows)
    local_heads = query_heads.shape[1]

    def one_block(block_parts):
        query_block, seg_block, keep_block, block_index = block_parts
        start = window_start(block_index, all_rows, window)
        keys_near = lax.dynamic_slice_in_dim(key_heads, start, window, 0)
        values_near = lax.dynamic_slice_in_dim(value_heads, start, window, 0)
        seg_near = lax.dynamic_slice_in_dim(seg_all, start, window, 0)
        keep_near = lax.dynamic_slice_in_dim(keep_all, start, window, 0)
        scores = block_scores(query_block, keys_near, seg_block, seg_near, keep_near)
        row_max = jnp.max(scores, axis=2, keepdims=True)
        weights = jnp.exp(scores - row_max)
        row_sum = jnp.sum(weights, axis=2, keepdims=True)
        probs_low = (weights / row_sum).astype(jnp.bfloat16)
        result = jnp.einsum(
            "hqk,khd->qhd", probs_low, values_near, preferred_element_type=jnp.float32
        )
        result = result * keep_block[:, None, None].astype(jnp.float32)
        return (result.astype(jnp.bfloat16), row_max, row_sum)

    block_ids = jnp.arange(block_count, dtype=jnp.int32)
    blocked = (
        query_heads.reshape(block_count, QBLOCK, local_heads, HEAD_DIM),
        seg_all.reshape(block_count, QBLOCK),
        keep_all.reshape(block_count, QBLOCK),
        block_ids,
    )
    results, block_max, block_sums = lax.map(one_block, blocked)
    return (results.reshape(all_rows, local_heads * HEAD_DIM), block_max, block_sums)


def attention_backward(head_rows, grad_rows, seg_all, keep_all, block_max, block_sums):
    all_rows = head_rows.shape[0]
    block_count = all_rows // QBLOCK
    window = key_window(all_rows)
    query_heads, key_heads, value_heads = split_heads(head_rows)
    local_heads = query_heads.shape[1]
    score_scale = HEAD_DIM ** (-0.5)

    def one_block(running, block_parts):
        grad_keys, grad_values = running
        query_block, seg_block, keep_block, grad_block, row_max, row_sum, block_index = block_parts
        start = window_start(block_index, all_rows, window)
        keys_near = lax.dynamic_slice_in_dim(key_heads, start, window, 0)
        values_near = lax.dynamic_slice_in_dim(value_heads, start, window, 0)
        seg_near = lax.dynamic_slice_in_dim(seg_all, start, window, 0)
        keep_near = lax.dynamic_slice_in_dim(keep_all, start, window, 0)
        scores = block_scores(query_block, keys_near, seg_block, seg_near, keep_near)
        probs = jnp.exp(scores - row_max) / row_sum
        grad_result = grad_block * keep_block[:, None, None].astype(jnp.bfloat16)
        values_term = jnp.einsum(
            "hqk,qhd->khd",
            probs.astype(jnp.bfloat16),
            grad_result,
            preferred_element_type=jnp.float32,
        )
        grad_probs = jnp.einsum(
            "qhd,khd->hqk", grad_result, values_near, preferred_element_type=jnp.float32
        )
        row_inner = jnp.sum(probs * grad_probs, axis=2, keepdims=True)
        grad_scores = (probs * (grad_probs - row_inner)).astype(jnp.bfloat16)
        grad_query = (
            jnp.einsum("hqk,khd->qhd", grad_scores, keys_near, preferred_element_type=jnp.float32)
            * score_scale
        )
        keys_term = (
            jnp.einsum("hqk,qhd->khd", grad_scores, query_block, preferred_element_type=jnp.float32)
            * score_scale
        )
        grad_keys = lax.dynamic_update_slice_in_dim(
            grad_keys, lax.dynamic_slice_in_dim(grad_keys, start, window, 0) + keys_term, start, 0
        )
        grad_values = lax.dynamic_update_slice_in_dim(
            grad_values,
            lax.dynamic_slice_in_dim(grad_values, start, window, 0) + values_term,
            start,
            0,
        )
        return ((grad_keys, grad_values), grad_query)

    zero_heads = jnp.zeros((all_rows, local_heads, HEAD_DIM), jnp.float32)
    block_ids = jnp.arange(block_count, dtype=jnp.int32)
    blocked = (
        query_heads.reshape(block_count, QBLOCK, local_heads, HEAD_DIM),
        seg_all.reshape(block_count, QBLOCK),
        keep_all.reshape(block_count, QBLOCK),
        grad_rows.reshape(block_count, QBLOCK, local_heads, HEAD_DIM),
        block_max,
        block_sums,
        block_ids,
    )
    (grad_keys, grad_values), grad_queries = lax.scan(one_block, (zero_heads, zero_heads), blocked)
    flat_width = local_heads * HEAD_DIM
    stacked = jnp.stack(
        [
            grad_queries.reshape(all_rows, flat_width),
            grad_keys.reshape(all_rows, flat_width),
            grad_values.reshape(all_rows, flat_width),
        ],
        axis=1,
    )
    return stacked.astype(jnp.bfloat16)


def per_device(
    tokens,
    grad_out,
    segments,
    padding,
    adapter_ids,
    norm1_gain,
    norm1_bias,
    w_qkv,
    w_proj,
    proj_bias,
    norm2_gain,
    norm2_bias,
    w_fc1,
    fc1_bias,
    w_fc2,
    fc2_bias,
    qkv_down,
    qkv_up,
    proj_down,
    proj_up,
    fc1_down,
    fc1_up,
    fc2_down,
    fc2_up,
):
    tok_rows = tokens.shape[1]
    feat_width = tokens.shape[2]
    inputs = tokens[0].astype(jnp.float32)
    seg_all = segments[0]
    keep_all = padding[0]
    offset = lax.axis_index("seq") * tok_rows
    seg_own = lax.dynamic_slice_in_dim(seg_all, offset, tok_rows)
    select = selection(seg_own, adapter_ids[0], qkv_down.shape[1])
    gain_one, shift_one, qkv_weight, proj_weight, proj_shift = (
        lax.all_gather(norm1_gain, "fsdp", axis=0, tiled=True),
        lax.all_gather(norm1_bias, "fsdp", axis=0, tiled=True),
        lax.all_gather(w_qkv, "fsdp", axis=0, tiled=True),
        lax.all_gather(w_proj, "fsdp", axis=0, tiled=True),
        lax.all_gather(proj_bias, "fsdp", axis=0, tiled=True),
    )
    gain_one = gain_one.astype(jnp.float32)
    shift_one = shift_one.astype(jnp.float32)
    normed_one = layer_norm(inputs, gain_one, shift_one).astype(jnp.bfloat16)
    qkv_main, inner_one = adapter_forward(normed_one, qkv_weight, qkv_down, qkv_up, select)
    qkv_low = qkv_main.astype(jnp.bfloat16).reshape(tok_rows, 3, feat_width)
    head_rows = lax.all_to_all(qkv_low, "seq", split_axis=2, concat_axis=0, tiled=True)
    attended_heads, block_max, block_sums = attention_forward(head_rows, seg_all, keep_all)
    attended = lax.all_to_all(attended_heads, "seq", split_axis=0, concat_axis=1, tiled=True)
    branch_one, inner_two = adapter_forward(attended, proj_weight, proj_down, proj_up, select)
    middle = inputs + (branch_one + proj_shift.astype(jnp.float32))
    gain_two, shift_two, fc1_weight, fc2_shift, fc2_weight, fc1_shift = (
        lax.all_gather(norm2_gain, "fsdp", axis=0, tiled=True),
        lax.all_gather(norm2_bias, "fsdp", axis=0, tiled=True),
        lax.all_gather(w_fc1, "fsdp", axis=0, tiled=True),
        lax.all_gather(fc2_bias, "fsdp", axis=0, tiled=True),
        lax.all_gather(w_fc2, "fsdp", axis=0, tiled=True),
        lax.all_gather(fc1_bias, "fsdp", axis=0, tiled=True),
    )
    gain_two = gain_two.astype(jnp.float32)
    shift_two = shift_two.astype(jnp.float32)
    normed_two = layer_norm(middle, gain_two, shift_two).astype(jnp.bfloat16)
    hidden_main, inner_three = adapter_forward(normed_two, fc1_weight, fc1_down, fc1_up, select)
    hidden = hidden_main + fc1_shift.astype(jnp.float32)
    active = jax.nn.gelu(hidden, approximate=False).astype(jnp.bfloat16)
    branch_two, inner_four = adapter_forward(active, fc2_weight, fc2_down, fc2_up, select)
    output = (middle + (branch_two + fc2_shift.astype(jnp.float32))).astype(jnp.bfloat16)
    fc1_back, fc2_back = (
        lax.all_gather(w_fc1, "fsdp", axis=0, tiled=True),
        lax.all_gather(w_fc2, "fsdp", axis=0, tiled=True),
    )
    grad_top = grad_out[0]
    grad_active, grad_fc2_down, grad_fc2_up = adapter_backward(
        active, inner_four, grad_top, fc2_back, fc2_down, fc2_up, select
    )
    unused, gelu_back = jax.vjp(partial(jax.nn.gelu, approximate=False), hidden)
    grad_hidden = gelu_back(grad_active)[0].astype(jnp.bfloat16)
    grad_normed_two, grad_fc1_down, grad_fc1_up = adapter_backward(
        normed_two, inner_three, grad_hidden, fc1_back, fc1_down, fc1_up, select
    )
    grad_middle = grad_top.astype(jnp.float32) + norm_backward(
        middle, gain_two, shift_two, grad_normed_two
    )
    qkv_back, proj_back = (
        lax.all_gather(w_qkv, "fsdp", axis=0, tiled=True),
        lax.all_gather(w_proj, "fsdp", axis=0, tiled=True),
    )
    grad_branch_one = grad_middle.astype(jnp.bfloat16)
    grad_attended, grad_proj_down, grad_proj_up = adapter_backward(
        attended, inner_two, grad_branch_one, proj_back, proj_down, proj_up, select
    )
    grad_head_rows = lax.all_to_all(
        grad_attended.astype(jnp.bfloat16), "seq", split_axis=1, concat_axis=0, tiled=True
    )
    grad_qkv_heads = attention_backward(
        head_rows, grad_head_rows, seg_all, keep_all, block_max, block_sums
    )
    grad_qkv = lax.all_to_all(
        grad_qkv_heads, "seq", split_axis=0, concat_axis=2, tiled=True
    ).reshape(tok_rows, 3 * feat_width)
    grad_normed_one, grad_qkv_down, grad_qkv_up = adapter_backward(
        normed_one, inner_one, grad_qkv, qkv_back, qkv_down, qkv_up, select
    )
    grad_tokens = grad_middle + norm_backward(inputs, gain_one, shift_one, grad_normed_one)
    summed = lax.psum(
        (
            grad_qkv_down,
            grad_qkv_up,
            grad_proj_down,
            grad_proj_up,
            grad_fc1_down,
            grad_fc1_up,
            grad_fc2_down,
            grad_fc2_up,
        ),
        ("seq", "fsdp"),
    )
    return (
        output[None],
        grad_tokens[None],
        summed[0],
        summed[1],
        summed[2],
        summed[3],
        summed[4],
        summed[5],
        summed[6],
        summed[7],
    )


F32 = jnp.float32
BF16 = jnp.bfloat16
MESH = pl.DeviceIdType.MESH
VMEM_LIMIT = 64 * 1000 * 1000


def mm(a, b):
    return lax.dot_general(a, b, (((1,), (0,)), ((), ())), preferred_element_type=F32)


def mm_nt(a, b):
    return lax.dot_general(a, b, (((1,), (1,)), ((), ())), preferred_element_type=F32)


def mm_tn(a, b):
    return lax.dot_general(a, b, (((0,), (0,)), ((), ())), preferred_element_type=F32)


def norm_parts(v):
    mean = jnp.mean(v, axis=-1, keepdims=True)
    centred = v - mean
    r = lax.rsqrt(jnp.mean(centred * centred, axis=-1, keepdims=True) + norm_eps)
    return centred * r, r


def norm_grad(v, gain, grad_y):
    h, r = norm_parts(v)
    d = grad_y * gain
    return r * (d - jnp.mean(d, axis=-1, keepdims=True) - h * jnp.mean(d * h, axis=-1, keepdims=True))


class Net:
    def __init__(self):
        self.s = lax.axis_index("seq")
        self.f = lax.axis_index("fsdp")
        self.z = self.f // 4
        self.x = (self.f // 2) % 2
        self.c = self.f % 2
        self.partner = {"seq": 1 - self.s}
        self.x_peer = {"fsdp": self.block(self.z, 1 - self.x, self.c)}
        self.c_peer = {"fsdp": self.block(self.z, self.x, 1 - self.c)}

    def block(self, z, x, c):
        return (z * 2 + x) * 2 + c

    def z_peer(self, d):
        return {"fsdp": self.block((self.z + d) % 4, self.x, self.c)}

    def barrier(self):
        sem = pltpu.get_barrier_semaphore()
        peers = [self.partner, self.x_peer, self.c_peer] + [self.z_peer(d) for d in (1, 2, 3)]
        for peer in peers:
            pl.semaphore_signal(sem, inc=1, device_id=peer, device_id_type=MESH)
        pl.semaphore_wait(sem, len(peers))


class Block:
    def __init__(self, src, piece, send_sem, recv_sem, own_sem, plane=None):
        self.src, self.piece, self.plane = src, piece, plane
        self.send_sem, self.recv_sem, self.own_sem = send_sem, recv_sem, own_sem


class Gather:
    def __init__(self, net):
        self.net = net

    def copy(self, it, src, block, k, peer):
        return pltpu.make_async_remote_copy(
            src_ref=src, dst_ref=it.piece(block), send_sem=it.send_sem(k), recv_sem=it.recv_sem(block),
            device_id=peer, device_id_type=MESH)

    def arrive(self, it, block):
        piece = it.piece(block)
        self.copy(it, piece, block, 0, self.net.c_peer).wait_recv()
        return piece

    def here(self, it, body):
        if it.plane is None:
            body()
        else:
            pl.when(self.net.s == it.plane)(body)

    def own(self, it):
        return pltpu.make_async_copy(it.src, it.piece(self.net.f), it.own_sem)

    def start(self, it):
        net = self.net

        def along():
            for d in (2, 1, 3):
                self.copy(it, it.src, net.f, d - 1, net.z_peer(d)).start()
            self.copy(it, it.src, net.f, 3, net.x_peer).start()

        self.here(it, along)
        self.copy(it, it.src, net.f, 4, net.c_peer).start()
        self.own(it).start()

    def from_z(self, it):
        net = self.net

        def body():
            for n, d in enumerate((1, 3, 2)):
                block = net.block((net.z + d) % 4, net.x, net.c)
                piece = self.arrive(it, block)
                self.copy(it, piece, block, 5 + 2 * n, net.x_peer).start()
                if it.plane is not None:
                    self.copy(it, piece, block, 15 + n, net.partner).start()
                self.copy(it, piece, block, 6 + 2 * n, net.c_peer).start()

        self.here(it, body)

    def from_x(self, it):
        net = self.net

        def body():
            for n, d in enumerate((0, 1, 3, 2)):
                block = net.block((net.z + d) % 4, 1 - net.x, net.c)
                piece = self.arrive(it, block)
                if it.plane is not None:
                    self.copy(it, piece, block, 18 + n, net.partner).start()
                self.copy(it, piece, block, 11 + n, net.c_peer).start()

        self.here(it, body)

    def from_seq(self, it):
        net = self.net
        if it.plane is None:
            return

        @pl.when(net.s != it.plane)
        def _():
            for n, (d, x) in enumerate(((1, net.x), (3, net.x), (2, net.x), (0, 1 - net.x), (1, 1 - net.x),
                                        (3, 1 - net.x), (2, 1 - net.x))):
                block = net.block((net.z + d) % 4, x, net.c)
                piece = self.arrive(it, block)
                self.copy(it, piece, block, 5 + n, net.c_peer).start()

    def from_core(self, it):
        net = self.net

        @pl.loop(0, 8)
        def _(n):
            self.arrive(it, 2 * n + 1 - net.c)

        self.own(it).wait()

    def finish(self, it):
        net = self.net

        def sent(first, end):
            @pl.loop(first, end)
            def _(k):
                self.copy(it, it.src, net.f, k, net.c_peer).wait_send()

        if it.plane is None:
            sent(0, 15)
            return

        @pl.when(net.s == it.plane)
        def _():
            sent(0, 22)

        @pl.when(net.s != it.plane)
        def _():
            sent(4, 12)


def full_vector(vec_ref, row, blocks=16, rows=16):
    parts = []
    for k in range(blocks // 2):
        even = vec_ref[2 * k * rows + row:2 * k * rows + row + 1, :]
        odd = vec_ref[(2 * k + 1) * rows + row:(2 * k + 1) * rows + row + 1, :]
        parts.append(even + odd)
    return jnp.concatenate(parts, axis=1)


WINDOW = 640
STEP = 64
PAD = 384
QROWS = 320
FFB = 512


class Image:
    def __init__(self, seg_ref, id_ref):
        self.start = jnp.sum((seg_ref[...] == 0).astype(F32), axis=1, keepdims=True)
        ident = id_ref[...].astype(F32)
        self.pick = []
        base = jnp.zeros((1, 1), F32)
        for k in range(PAD // STEP + 1):
            mark = ((self.start >= k * STEP) & (self.start < (k + 1) * STEP)).astype(F32)
            self.pick.append(mark)
            base = base + mark * float(k * STEP)
        self.shift = base - self.start
        lane = lax.broadcasted_iota(jnp.int32, (1, 128), 1).astype(F32)
        self.columns = ((lane >= ident * RANK) & (lane < (ident + 1) * RANK)).astype(F32)

    def choose(self, load):
        total = None
        for k, mark in enumerate(self.pick):
            value = load(k * STEP)
            value = value * mark.astype(value.dtype)
            total = value if total is None else total + value
        return total

    def inside(self, shape, axis, first=0):
        at = (lax.broadcasted_iota(jnp.int32, shape, axis) + first).astype(F32) + self.shift
        return (at >= 0) & (at < IMG)

    def select(self, first, rows):
        at = (lax.broadcasted_iota(jnp.int32, (rows, 1), 0) + first).astype(F32)
        return (at >= self.start).astype(F32) * self.columns

    def select_window(self, first, rows):
        at = (lax.broadcasted_iota(jnp.int32, (rows, 1), 0) + first).astype(F32) + self.shift
        return (at >= 0).astype(F32) * self.columns


def lane_halves():
    lane = lax.broadcasted_iota(jnp.int32, (1, 128), 1)
    return [(lane < 64).astype(F32), (lane >= 64).astype(F32)]


def compact_rows(dense):
    total = dense[0:16]
    for k in range(1, 8):
        total = total + dense[16 * k:16 * (k + 1)]
    return total.astype(BF16)


N_FC1 = 8
N_FC2 = 4
N_ITEMS = 3 + N_FC2 + N_FC1


def forward_kernel(seg_ref, id_ref, x_ref, vec_ref, qd_ref, pd_ref, pu_ref, wq_hbm, wp_hbm, w1_hbm, w2_hbm,
                   qu_hbm, g_hbm, u1_hbm, d1_hbm, u2_hbm, d2_hbm,
                   wqf, wpf, vecf_out, qkv_out, n1_out, c1_out, prob_out, oh_out, att_out, c2_out, gm_out, gr_out, out_out,
                   wq_own, wq, wp, w1, w2, xp, vecf, qu, g, u1, d1, u2, d2, qkv, n1, c1, qkvw, n1w, c1w, prob, opad, sendb,
                   oh, att, c2, mid, n2, oacc, gacc, u4, e3, c3, e4, c3t, e4t, act_s, gh_s, gr,
                   xs_sem, xr_sem, as_sem, ar_sem, loc_sem, out_sem, prob_sem, g_send, g_recv, g_own):
    net = Net()
    s, other = net.s, 1 - net.s
    rows, width = x_ref.shape
    half = wq.shape[1] // 3
    rb = wq_own.shape[0]
    fr1 = w1_hbm.shape[0]
    fr2 = w2_hbm.shape[0]
    ff = w1.shape[1]
    chunk = rows // 2

    pre = []
    for part in range(3):
        cols = pl.ds(pl.multiple_of(part * width + s * half, 128), half)
        pre.append(pltpu.make_async_copy(wq_hbm.at[:, cols], wq_own.at[:, pl.ds(part * half, half)], loc_sem.at[part]))
    late = []
    for part in range(3):
        cols = pl.ds(pl.multiple_of(part * width + s * half, 128), half)
        late.append(pltpu.make_async_copy(qu_hbm.at[:, cols], qu.at[:, pl.ds(part * half, half)], loc_sem.at[3 + part]))
    for n, (src, dst) in enumerate(((g_hbm, g), (u1_hbm, u1), (d1_hbm, d1), (u2_hbm, u2), (d2_hbm, d2))):
        late.append(pltpu.make_async_copy(src, dst, loc_sem.at[6 + n]))
    for copy in pre + late:
        copy.start()
    net.barrier()

    def x_copy(i):
        part = pl.ds(i * chunk, chunk)
        return pltpu.make_async_remote_copy(
            src_ref=x_ref.at[part, :], dst_ref=xp.at[part, :], send_sem=xs_sem.at[i], recv_sem=xr_sem.at[i],
            device_id=net.partner, device_id_type=MESH)

    for i in range(2):
        x_copy(i).start()
    for copy in pre:
        copy.wait()

    def block(n, src, piece, plane=None):
        return Block(src, piece, lambda k: g_send.at[n, k], lambda b: g_recv.at[n, b], g_own.at[n], plane)

    sub = fr2 // N_FC2
    vec_it = block(0, vec_ref, lambda b: vecf.at[pl.ds(b * 16, 16), :])
    wq_it = block(1, wq_own, lambda b: wq.at[pl.ds(b * rb, rb), :])
    wp_it = block(2, wp_hbm, lambda b: wp.at[pl.ds(b * rb, rb), :])
    fc2_it = [block(3 + j, w2_hbm.at[pl.ds(j * sub, sub), :], lambda b, j=j: w2.at[pl.ds(b * fr2 + j * sub, sub), :],
                    (0, 1, None, None)[j]) for j in range(N_FC2)]

    def fc1_it(j):
        cols = pl.ds(j * FFB if isinstance(j, int) else pl.multiple_of(j * FFB, FFB), FFB)
        return block(3 + N_FC2 + j, w1_hbm.at[:, cols], lambda b: w1.at[pl.ds(b * fr1, fr1), cols], j % 2)

    gather = Gather(net)
    gather.start(vec_it)
    gather.start(wq_it)
    image = Image(seg_ref, id_ref)
    zeros = jnp.zeros((PAD, 128), BF16)
    opad[0:PAD, :] = zeros
    opad[PAD + WINDOW:2 * PAD + WINDOW, :] = zeros
    gather.from_z(vec_it)
    gather.from_z(wq_it)
    gather.start(wp_it)
    gather.from_x(vec_it)
    gather.from_x(wq_it)
    gather.start(fc2_it[0])
    gather.start(fc2_it[1])
    for copy in late:
        copy.wait()
    gather.from_core(vec_it)
    gather.from_core(wq_it)

    gain1 = full_vector(vecf, 0)
    shift1 = full_vector(vecf, 1)

    def project(src, src_row, row):
        v = src[pl.ds(src_row, chunk), :].astype(F32)
        h, unused = norm_parts(v)
        normed = (h * gain1 + shift1).astype(BF16)
        at = pl.ds(row, chunk)
        n1[at, :] = normed
        inner = (mm(normed, qd_ref[...]) * image.select(row, chunk)).astype(BF16)
        c1[at, :] = inner
        for part in range(3):
            cols = pl.ds(part * half, half)
            qkv[at, cols] = (mm(normed, wq[:, cols]) + mm(inner, qu[:, cols])).astype(BF16)

    @pl.loop(0, 2)
    def _(i):
        project(x_ref, pl.multiple_of(i * chunk, chunk), pl.multiple_of(s * rows + i * chunk, chunk))

    gather.from_z(wp_it)
    gather.start(fc2_it[2])

    @pl.loop(0, 2)
    def _(i):
        pltpu.make_async_remote_copy(
            src_ref=x_ref.at[pl.ds(0, chunk), :], dst_ref=xp.at[pl.ds(0, chunk), :], send_sem=xs_sem.at[i],
            recv_sem=xr_sem.at[i], device_id=net.partner, device_id_type=MESH).wait_recv()
        project(xp, pl.multiple_of(i * chunk, chunk), pl.multiple_of(other * rows + i * chunk, chunk))

    gather.from_x(wp_it)
    gather.from_z(fc2_it[0])
    gather.from_z(fc2_it[1])
    outs = []

    def put(src, dst):
        copy = pltpu.make_async_copy(src, dst, out_sem.at[len(outs)])
        copy.start()
        outs.append(copy)

    put(wq, wqf)
    put(vecf, vecf_out)
    for src, dst in ((qkv, qkvw), (n1, n1w), (c1, c1w)):
        step = min(src.shape[1], 512)

        @pl.loop(0, src.shape[1] // step)
        def _(n, src=src, dst=dst, step=step):
            cols = pl.ds(pl.multiple_of(n * step, step), step)
            dst[:, cols] = image.choose(lambda at: src[at:at + WINDOW, cols])
    put(qkvw, qkv_out)
    put(n1w, n1_out)
    put(c1w, c1_out)
    bias = jnp.where(image.inside((1, WINDOW), 1), 0.0, masked_score).astype(F32)
    halves = lane_halves()

    def prob_copy(pair):
        slot = lax.rem(pair, 2)
        return pltpu.make_async_copy(prob.at[slot], prob_out.at[pl.ds(2 * pair, 2)], prob_sem.at[slot])

    def att_copy(pair):
        cols = pl.ds(pl.multiple_of(s * half + pair * 128, 128), 128)
        return pltpu.make_async_remote_copy(
            src_ref=sendb.at[pair], dst_ref=att.at[:, cols], send_sem=as_sem.at[pair], recv_sem=ar_sem.at[pair],
            device_id=net.partner, device_id_type=MESH)

    pairs = half // 128

    @pl.loop(0, pairs)
    def _(pair):
        def cols(part):
            return pl.ds(pl.multiple_of(part * half + pair * 128, 128), 128)

        k2 = qkvw[:, cols(1)]
        v2 = qkvw[:, cols(2)]
        vs = [(v2 * hm.astype(BF16)) for hm in halves]
        slot = lax.rem(pair, 2)

        @pl.when(pair >= 2)
        def _():
            prob_copy(pair).wait()

        @pl.loop(0, WINDOW // QROWS)
        def _(b):
            r0 = pl.multiple_of(b * QROWS, QROWS)
            q2 = qkvw[pl.ds(r0, QROWS), cols(0)]
            q2 = q2 * jnp.asarray(HEAD_DIM ** (-0.5), BF16)
            total = None
            for hd in range(2):
                scores = mm_nt(q2 * halves[hd].astype(BF16), k2) + bias
                weights = jnp.exp(scores - jnp.max(scores, axis=1, keepdims=True))
                weights = (weights * (1.0 / jnp.sum(weights, axis=1, keepdims=True))).astype(BF16)
                prob[slot, hd, pl.ds(r0, QROWS), :] = weights
                part = mm(weights, vs[hd])
                total = part if total is None else total + part
            total = (total * image.inside((QROWS, 1), 0, r0).astype(F32)).astype(BF16)
            opad[pl.ds(PAD + r0, QROWS), :] = total
            oh[pl.ds(r0, QROWS), cols(0)] = total

        prob_copy(pair).start()

        def own_rows(who):
            return image.choose(lambda at: opad[pl.ds(pl.multiple_of(who * rows + PAD - at, STEP), rows), :])

        sendb[pair] = own_rows(other)
        att_copy(pair).start()
        att[:, pl.ds(pl.multiple_of(s * half + pair * 128, 128), 128)] = own_rows(s)

        @pl.when(pair == 0)
        def _():
            gather.from_core(wp_it)
            gather.from_x(fc2_it[0])
            gather.from_x(fc2_it[1])

        @pl.when(pair == 1)
        def _():
            gather.start(fc2_it[3])
            gather.from_z(fc2_it[2])

        @pl.when(pair == 2)
        def _():
            gather.from_seq(fc2_it[0])
            gather.from_seq(fc2_it[1])
            gather.start(fc1_it(0))
            gather.start(fc1_it(1))

        @pl.when(pair == 3)
        def _():
            gather.from_x(fc2_it[2])
            gather.from_z(fc2_it[3])

    put(wp, wpf)
    put(oh, oh_out)

    @pl.loop(0, pairs)
    def _(pair):
        att_copy(pair).wait_recv()

    put(att, att_out)
    bias_p = full_vector(vecf, 2)
    gain2 = full_vector(vecf, 3)
    shift2 = full_vector(vecf, 4)

    @pl.loop(0, 2)
    def _(i):
        at = pl.ds(pl.multiple_of(i * chunk, chunk), chunk)
        rows_in = att[at, :]
        own_select = image.select(s * rows + i * chunk, chunk)
        inner = (mm(rows_in, pd_ref[...]) * own_select).astype(BF16)
        c2[at, :] = inner
        branch = mm(rows_in, wp[...]) + mm(inner, pu_ref[...]) + bias_p
        middle = x_ref[at, :].astype(F32) + branch
        mid[at, :] = middle
        h, unused = norm_parts(middle)
        normed = (h * gain2 + shift2).astype(BF16)
        n2[at, :] = normed
        c = mm(normed, d1[...]) * own_select
        e = mm_nt(g[at, :], u2[...]) * own_select
        c3[at, :] = c.astype(BF16)
        e4[at, :] = e.astype(BF16)
        oacc[at, :] = jnp.zeros((chunk, width), F32)
        gacc[at, :] = jnp.zeros((chunk, width), F32)
        u4[at, :] = jnp.zeros((chunk, 128), F32)
        e3[at, :] = jnp.zeros((chunk, 128), F32)

    c3t[...] = c3[...].T
    e4t[...] = e4[...].T
    put(c2, c2_out)
    gather.start(fc1_it(2))
    gather.from_z(fc1_it(0))
    gather.from_z(fc1_it(1))
    gather.from_x(fc2_it[3])
    gather.start(fc1_it(3))
    gather.from_x(fc1_it(0))
    gather.from_x(fc1_it(1))
    gather.from_z(fc1_it(2))
    gather.start(fc1_it(4))
    for j in range(N_FC2):
        gather.from_core(fc2_it[j])
    gather.from_seq(fc1_it(0))

    @pl.loop(0, N_FC1)
    def _(j):
        @pl.when(j + 5 < N_FC1)
        def _():
            gather.start(fc1_it(j + 5))

        @pl.when(j + 3 < N_FC1)
        def _():
            gather.from_z(fc1_it(j + 3))

        @pl.when(j + 2 < N_FC1)
        def _():
            gather.from_x(fc1_it(j + 2))

        @pl.when(j + 1 < N_FC1)
        def _():
            gather.from_seq(fc1_it(j + 1))

        gather.from_core(fc1_it(j))
        bias = jnp.concatenate([vecf[pl.ds(2 * j * 16 + 6, 1), :], vecf[pl.ds(2 * j * 16 + 7, 1), :],
                                vecf[pl.ds((2 * j + 1) * 16 + 6, 1), :], vecf[pl.ds((2 * j + 1) * 16 + 7, 1), :]], axis=1)
        col = pl.ds(pl.multiple_of(j * FFB, FFB), FFB)

        @pl.loop(0, 2)
        def _(i):
            at = pl.ds(pl.multiple_of(i * chunk, chunk), chunk)
            hidden = mm(n2[at, :], w1[:, col]) + mm(c3[at, :], u1[:, col]) + bias
            cdf = 0.5 * (1.0 + lax.erf(hidden * (0.5 ** 0.5)))
            pdf = jnp.exp(hidden * hidden * -0.5) * (0.5 / 3.141592653589793) ** 0.5
            active = (hidden * cdf).astype(BF16)
            act_s[at, :] = active
            grad_active = mm_nt(g[at, :], w2[col, :]) + mm_nt(e4[at, :], d2[col, :])
            grad_hidden = (grad_active * (cdf + hidden * pdf)).astype(BF16)
            gh_s[at, :] = grad_hidden
            oacc[at, :] += mm(active, w2[col, :])
            u4[at, :] += mm(active, d2[col, :])
            gacc[at, :] += mm_nt(grad_hidden, w1[:, col])
            e3[at, :] += mm_nt(grad_hidden, u1[:, col])

        gr[:, col] = compact_rows(mm(c3t[...], gh_s[...]))
        gr[:, pl.ds(pl.multiple_of(ff + j * FFB, FFB), FFB)] = compact_rows(mm(e4t[...], act_s[...]))

    bias2 = full_vector(vecf, 5)

    @pl.loop(0, 2)
    def _(i):
        at = pl.ds(pl.multiple_of(i * chunk, chunk), chunk)
        own_select = image.select(s * rows + i * chunk, chunk)
        c = (u4[at, :] * own_select).astype(BF16)
        e = (e3[at, :] * own_select).astype(BF16)
        c3[at, :] = c
        e4[at, :] = e
        act_out = mid[at, :] + (oacc[at, :] + mm(c, u2[...]) + bias2)
        xp[at, :] = act_out.astype(BF16)
        grad_n2 = gacc[at, :] + mm_nt(e, d1[...])
        gacc[at, :] = g[at, :].astype(F32) + norm_grad(mid[at, :], gain2, grad_n2)

    put(xp, out_out)
    put(gacc, gm_out)
    gr[:, 2 * ff:2 * ff + width] = compact_rows(mm_tn(e4[...], n2[...]))
    gr[:, 2 * ff + width:2 * ff + 2 * width] = compact_rows(mm_tn(c3[...], g[...]))
    put(gr, gr_out)
    for copy in outs:
        copy.wait()
    for pair in range(pairs - 2, pairs):
        prob_copy(pair).wait()
    for i in range(2):
        x_copy(i).wait_send()

    @pl.loop(0, pairs)
    def _(pair):
        att_copy(pair).wait_send()

    for it in [vec_it, wq_it, wp_it] + fc2_it:
        gather.finish(it)

    @pl.loop(0, N_FC1)
    def _(j):
        gather.finish(fc1_it(j))


def any_spec():
    return pl.BlockSpec(memory_space=pl.ANY)


def vmem_spec():
    return pl.BlockSpec(memory_space=pltpu.VMEM)


def run_forward(seg, ident, x, vec, qd, pd, pu, wq, wp, w1, w2, qu, g, u1, d1, u2, d2):
    rows, width = x.shape
    toks = seg.shape[1]
    half = width // 2
    ff = w1.shape[1]
    dma = pltpu.SemaphoreType.DMA
    sds = jax.ShapeDtypeStruct
    gcols = 2 * ff + 2 * width
    out_shape = (
        sds((width, 3 * half), BF16), sds((width, width), BF16), sds((256, 128), F32),
        sds((WINDOW, 3 * half), BF16), sds((WINDOW, width), BF16), sds((WINDOW, 128), BF16),
        sds((half // 64, WINDOW, WINDOW), BF16), sds((WINDOW, half), BF16), sds((rows, width), BF16), sds((rows, 128), BF16),
        sds((rows, width), F32), sds((16, gcols), BF16), sds((rows, width), BF16))

    def low(*shape):
        return pltpu.VMEM(shape, BF16)

    def full(*shape):
        return pltpu.VMEM(shape, F32)

    scratch = [
        low(wq.shape[0], 3 * half), low(width, 3 * half), low(width, width), low(width, ff), low(ff, width),
        low(rows, width), full(256, 128), low(128, 3 * half), low(rows, width), low(128, ff), low(width, 128),
        low(128, width), low(ff, 128), low(toks, 3 * half), low(toks, width), low(toks, 128),
        low(WINDOW, 3 * half), low(WINDOW, width), low(WINDOW, 128), low(2, 2, WINDOW, WINDOW), low(2 * PAD + WINDOW, 128),
        low(half // 128, rows, 128), low(WINDOW, half), low(rows, width), low(rows, 128), full(rows, width), low(rows, width),
        full(rows, width), full(rows, width), full(rows, 128), full(rows, 128), low(rows, 128), low(rows, 128),
        low(128, rows), low(128, rows), low(rows, FFB), low(rows, FFB), low(16, gcols),
        dma((2,)), dma((2,)), dma((4,)), dma((4,)), dma((11,)), dma((12,)), dma((2,)),
        dma((N_ITEMS, 22)), dma((N_ITEMS, 16)), dma((N_ITEMS,))]
    return pl.pallas_call(
        forward_kernel, out_shape=out_shape, in_specs=[vmem_spec()] * 7 + [any_spec()] * 10,
        out_specs=tuple(any_spec() for unused in out_shape), scratch_shapes=scratch,
        compiler_params=pltpu.CompilerParams(collective_id=1, has_side_effects=True, vmem_limit_bytes=VMEM_LIMIT),
        name="forward")(seg, ident, x, vec, qd, pd, pu, wq, wp, w1, w2, qu, g, u1, d1, u2, d2)


def backward_kernel(seg_ref, id_ref, gm_ref, att_ref, c2_ref, oh_ref, pd_ref, pu_ref, qd_ref, gf_ref, wp_ref,
                    wq_hbm, qkv_hbm, n1_hbm, c1_hbm, prob_hbm, qu_hbm,
                    gall, gn_out,
                    wq, qkv, n1, c1, prob, qu, g1, e2, gsend, do_s, first_own, first_send, first_in, gq, qsend, qdown, qdown_in, qown,
                    gpad, psend, prcv, gn,
                    loc_sem, ds_sem, dr_sem, fs_sem, fr_sem, qs_sem, qr_sem, ps_sem, pr_sem, out_sem, g_send, g_recv, g_own):
    net = Net()
    s, other = net.s, 1 - net.s
    image = Image(seg_ref, id_ref)
    rows, width = gm_ref.shape
    half = wq.shape[1] // 3
    chunk = rows // 2
    ffn_cols = gf_ref.shape[1]

    loads = [pltpu.make_async_copy(src, dst, loc_sem.at[i]) for i, (src, dst) in enumerate(
        [(qkv_hbm, qkv), (prob_hbm, prob), (wq_hbm, wq), (n1_hbm, n1), (c1_hbm, c1)])]
    for part in range(3):
        cols = pl.ds(pl.multiple_of(part * width + s * half, 128), half)
        loads.append(pltpu.make_async_copy(qu_hbm.at[:, cols], qu.at[:, pl.ds(part * half, half)], loc_sem.at[5 + part]))
    for copy in loads:
        copy.start()
    net.barrier()

    @pl.loop(0, 2)
    def _(i):
        at = pl.ds(pl.multiple_of(i * chunk, chunk), chunk)
        low = gm_ref[at, :].astype(BF16)
        g1[at, :] = low
        e2[at, :] = mm_nt(low, pu_ref[...]) * image.select(s * rows + i * chunk, chunk)

    def grad_att(i, who):
        at = pl.ds(i * chunk, chunk)
        heads = pl.ds(pl.multiple_of(who * half, half), half)
        return (mm_nt(g1[at, :], wp_ref[heads, :]) + mm_nt(e2[at, :].astype(BF16), pd_ref[heads, :])).astype(BF16)

    dsend = []
    for i in range(2):
        gsend[i] = grad_att(i, other)
        copy = pltpu.make_async_remote_copy(
            src_ref=gsend.at[i], dst_ref=do_s.at[pl.ds(pl.multiple_of(s * rows + i * chunk, chunk), chunk), :],
            send_sem=ds_sem.at[i], recv_sem=dr_sem.at[i], device_id=net.partner, device_id_type=MESH)
        copy.start()
        dsend.append(copy)
    first_own[:, 0:ffn_cols] = gf_ref[...]
    first_own[:, ffn_cols:ffn_cols + width] = compact_rows(mm_tn(c2_ref[...], g1[...]))
    first_own[:, ffn_cols + width:ffn_cols + 2 * width] = compact_rows(mm_tn(e2[...].astype(BF16), att_ref[...]))
    fsend = pltpu.make_async_remote_copy(
        src_ref=first_own, dst_ref=first_in, send_sem=fs_sem.at[0], recv_sem=fr_sem.at[0],
        device_id=net.partner, device_id_type=MESH)
    fsend.start()
    for i in range(2):
        do_s[pl.ds(pl.multiple_of(s * rows + i * chunk, chunk), chunk), :] = grad_att(i, s)
    n_first = first_own.shape[1]
    items = [Block(src, lambda b, cols=cols: gall.at[pl.ds(b * 16, 16), cols], lambda k, n=n: g_send.at[n, k],
                   lambda b, n=n: g_recv.at[n, b], g_own.at[n])
             for n, (src, cols) in enumerate(((first_send, pl.ds(0, n_first)), (qown, pl.ds(n_first, 4 * width))))]
    gather = Gather(net)
    zeros = jnp.zeros((PAD, width), F32)
    gpad[0:PAD, :] = zeros
    gpad[PAD + WINDOW:2 * PAD + WINDOW, :] = zeros
    for copy in loads:
        copy.wait()
    for copy in dsend:
        copy.wait_recv()
    fsend.wait_recv()
    first_send[...] = (first_own[...].astype(F32) + first_in[...].astype(F32)).astype(BF16)
    gather.start(items[0])

    halves = lane_halves()
    scale = HEAD_DIM ** (-0.5)
    keep = image.inside((WINDOW, 1), 0).astype(BF16)
    for pair in range(half // 128):
        cols = slice(pair * 128, (pair + 1) * 128)
        k2 = qkv[:, half + pair * 128:half + (pair + 1) * 128]
        v2 = qkv[:, 2 * half + pair * 128:2 * half + (pair + 1) * 128]
        q2 = qkv[:, cols] * jnp.asarray(scale, BF16)
        do2 = image.choose(lambda at: do_s[at:at + WINDOW, cols]) * keep
        inner = do2.astype(F32) * oh_ref[:, cols].astype(F32)
        gv = gk = gqq = None
        for hd in range(2):
            hm = halves[hd].astype(BF16)
            weights = prob[2 * pair + hd]
            grad_p = mm_nt(do2 * hm, v2)
            row_inner = jnp.sum(inner * halves[hd], axis=1, keepdims=True)
            grad_s = (weights.astype(F32) * (grad_p - row_inner)).astype(BF16)
            dv = mm_tn(weights, do2 * hm)
            dk = mm_tn(grad_s, q2 * hm)
            dq = mm(grad_s, k2 * hm)
            gv = dv if gv is None else gv + dv
            gk = dk if gk is None else gk + dk
            gqq = dq if gqq is None else gqq + dq
        gq[:, cols] = (gqq * scale).astype(BF16)
        gq[:, half + pair * 128:half + (pair + 1) * 128] = gk.astype(BF16)
        gq[:, 2 * half + pair * 128:2 * half + (pair + 1) * 128] = gv.astype(BF16)
        if pair == 1:
            gather.from_z(items[0])
        if pair == 2:
            gather.from_x(items[0])

    up = compact_rows(mm_tn(c1[...], gq[...]))
    e1 = (mm_nt(gq[...], qu[...]) * image.select_window(0, WINDOW)).astype(BF16)
    down = mm_tn(e1, n1[...])
    qdown[...] = compact_rows(down)
    qsends = []
    for part in range(3):
        cols = pl.ds(pl.multiple_of(part * width + s * half, 128), half)
        qsend[:, pl.ds(part * half, half)] = up[:, part * half:(part + 1) * half]
        qown[:, cols] = up[:, part * half:(part + 1) * half]
        qsends.append(pltpu.make_async_remote_copy(
            src_ref=qsend.at[:, pl.ds(part * half, half)], dst_ref=qown.at[:, cols], send_sem=qs_sem.at[part],
            recv_sem=qr_sem.at[part], device_id=net.partner, device_id_type=MESH))
    qsends.append(pltpu.make_async_remote_copy(
        src_ref=qdown, dst_ref=qdown_in, send_sem=qs_sem.at[3],
        recv_sem=qr_sem.at[3], device_id=net.partner, device_id_type=MESH))
    for copy in qsends:
        copy.start()

    @pl.loop(0, 2)
    def _(i):
        at = pl.ds(pl.multiple_of(i * QROWS, QROWS), QROWS)
        e1_rows = (mm_nt(gq[at, :], qu[...]) * image.select_window(i * QROWS, QROWS)).astype(BF16)
        gpad[pl.ds(pl.multiple_of(PAD + i * QROWS, STEP), QROWS), :] = mm_nt(gq[at, :], wq[...]) + mm_nt(e1_rows, qd_ref[...])

    psends = []
    for i in range(2):
        psend[i] = image.choose(lambda at: gpad[
            pl.ds(pl.multiple_of(other * rows + PAD + i * chunk - at, STEP), chunk), :]).astype(BF16)
        copy = pltpu.make_async_remote_copy(
            src_ref=psend.at[i], dst_ref=prcv.at[i], send_sem=ps_sem.at[i], recv_sem=pr_sem.at[i],
            device_id=net.partner, device_id_type=MESH)
        copy.start()
        psends.append(copy)
    for copy in qsends:
        copy.wait_recv()
    qown[:, 3 * width:4 * width] = (qdown[...].astype(F32) + qdown_in[...].astype(F32)).astype(BF16)
    gather.start(items[1])
    gather.from_core(items[0])
    gather.from_z(items[1])
    gather.from_x(items[1])
    gather.from_core(items[1])
    outs = []
    for i in range(2):
        psends[i].wait_recv()
        rows_at = pl.ds(i * chunk, chunk)
        gn[rows_at, :] = prcv[i].astype(F32) + image.choose(lambda at: gpad[
            pl.ds(pl.multiple_of(s * rows + PAD + i * chunk - at, STEP), chunk), :])
        copy = pltpu.make_async_copy(gn.at[rows_at, :], gn_out.at[rows_at, :], out_sem.at[i])
        copy.start()
        outs.append(copy)
    for copy in outs:
        copy.wait()
    for copy in dsend + [fsend] + qsends + psends:
        copy.wait_send()
    for it in items:
        gather.finish(it)


def run_backward(seg, ident, gm, att, c2, oh, pd, pu, qd, gf, wp, wq, qkv, n1, c1, prob, qu):
    rows, width = gm.shape
    toks = 2 * rows
    half = width // 2
    dma = pltpu.SemaphoreType.DMA
    sds = jax.ShapeDtypeStruct
    n_first = gf.shape[1] + 2 * width
    out_shape = (sds((256, n_first + 4 * width), BF16), sds((rows, width), F32))
    chunk = rows // 2
    scratch = [
        pltpu.VMEM(wq.shape, BF16), pltpu.VMEM(qkv.shape, BF16), pltpu.VMEM(n1.shape, BF16), pltpu.VMEM(c1.shape, BF16),
        pltpu.VMEM(prob.shape, BF16), pltpu.VMEM((128, 3 * half), BF16), pltpu.VMEM((rows, width), BF16),
        pltpu.VMEM((rows, 128), F32), pltpu.VMEM((2, chunk, half), BF16), pltpu.VMEM((toks, half), BF16),
        pltpu.VMEM((16, n_first), BF16), pltpu.VMEM((16, n_first), BF16), pltpu.VMEM((16, n_first), BF16),
        pltpu.VMEM((WINDOW, 3 * half), BF16), pltpu.VMEM((16, 3 * half), BF16), pltpu.VMEM((16, width), BF16),
        pltpu.VMEM((16, width), BF16), pltpu.VMEM((16, 4 * width), BF16), pltpu.VMEM((2 * PAD + WINDOW, width), F32), pltpu.VMEM((2, chunk, width), BF16),
        pltpu.VMEM((2, chunk, width), BF16), pltpu.VMEM((rows, width), F32),
        dma((8,)), dma((2,)), dma((2,)), dma((1,)), dma((1,)), dma((4,)), dma((4,)), dma((2,)), dma((2,)), dma((2,)),
        dma((2, 15)), dma((2, 16)), dma((2,))]
    return pl.pallas_call(
        backward_kernel, out_shape=out_shape,
        in_specs=[vmem_spec()] * 11 + [any_spec()] * 6,
        out_specs=tuple(any_spec() for unused in out_shape), scratch_shapes=scratch,
        compiler_params=pltpu.CompilerParams(collective_id=2, has_side_effects=True, vmem_limit_bytes=VMEM_LIMIT),
        name="backward")(seg, ident, gm, att, c2, oh, pd, pu, qd, gf, wp, wq, qkv, n1, c1, prob, qu)


def expand_kernel(vec_ref, f1u, f2d, f1d, f2u, pu, pdn, qu, qd, gn, x, gm,
                  gt_out, qd_out, qu_out, pd_out, pu_out, f1d_out, f1u_out, f2d_out, f2u_out):
    ids = jnp.concatenate([jnp.broadcast_to(vec_ref[16 * p + 8:16 * p + 9, :], (16, 128)) for p in range(16)], axis=0)
    r = lax.broadcasted_iota(jnp.int32, (256, 128), 0) % 16
    col = lax.broadcasted_iota(jnp.int32, (256, 128), 1)
    pick = ((ids.astype(jnp.int32) == col // 16) & (r == col % 16)).astype(F32)
    pick_t = pick.T.astype(BF16)
    for src, dst in ((f1u, f1u_out), (f2u, f2u_out), (pu, pu_out), (qu, qu_out)):
        dst[...] = mm(pick_t, src[...])
    for src, dst in ((f1d, f1d_out), (f2d, f2d_out), (pdn, pd_out), (qd, qd_out)):
        dst[...] = mm(pick_t, src[...]).T
    gain1 = full_vector(vec_ref, 0)
    gt_out[...] = gm[...] + norm_grad(x[...].astype(F32), gain1, gn[...])


def run_expand(vec, gall, gn, x, gm):
    rows, width = gn.shape
    ff = 4 * width
    n = 4
    sds = jax.ShapeDtypeStruct

    def part(cols, offset):
        return pl.BlockSpec((256, cols), lambda j: (0, offset // cols + j))

    def by_row(shape):
        return pl.BlockSpec(shape, lambda j: (j, 0))

    def by_col(shape):
        return pl.BlockSpec(shape, lambda j: (0, j))

    q = width // n
    return pl.pallas_call(
        expand_kernel, grid=(n,),
        out_shape=(sds((rows, width), F32), sds((width, 128), F32), sds((128, 3 * width), F32), sds((width, 128), F32),
                   sds((128, width), F32), sds((width, 128), F32), sds((128, ff), F32), sds((ff, 128), F32), sds((128, width), F32)),
        in_specs=[pl.BlockSpec((256, 128), lambda j: (0, 0)), part(ff // n, 0), part(ff // n, ff), part(q, 2 * ff),
                  part(q, 2 * ff + width), part(q, 2 * ff + 2 * width), part(q, 2 * ff + 3 * width),
                  part(3 * q, 2 * ff + 4 * width), part(q, 2 * ff + 7 * width),
                  by_row((rows // n, width)), by_row((rows // n, width)), by_row((rows // n, width))],
        out_specs=(by_row((rows // n, width)), by_row((q, 128)), by_col((128, 3 * q)), by_row((q, 128)), by_col((128, q)),
                   by_row((q, 128)), by_col((128, ff // n)), by_row((ff // n, 128)), by_col((128, q))),
        compiler_params=pltpu.CompilerParams(vmem_limit_bytes=VMEM_LIMIT),
        name="expand")(vec, *([gall] * 8), gn, x, gm)


def per_device_fast(tokens, grad_out, segments, padding, adapter_ids, norm1_gain, norm1_bias, w_qkv, w_proj, proj_bias,
                    norm2_gain, norm2_bias, w_fc1, fc1_bias, w_fc2, fc2_bias, qkv_down, qkv_up, proj_down, proj_up,
                    fc1_down, fc1_up, fc2_down, fc2_up):
    x = tokens[0]
    odd = (lax.axis_index("fsdp") % 2).astype(F32)
    six = jnp.stack([norm1_gain, norm1_bias, proj_bias, norm2_gain, norm2_bias, fc2_bias]).astype(F32)
    vec = jnp.concatenate([
        jnp.concatenate([six * (1.0 - odd), six * odd], axis=1), fc1_bias.astype(F32).reshape(2, 128),
        jnp.broadcast_to(adapter_ids[0].astype(F32)[:, None], (1, 128)), jnp.zeros((7, 128), F32)], axis=0)
    (wq, wp, vecf, qkv, n1, c1, prob, oh, att, c2, gm, gf, out) = run_forward(
        segments, adapter_ids, x, vec, qkv_down, proj_down, proj_up, w_qkv, w_proj, w_fc1, w_fc2, qkv_up,
        grad_out[0], fc1_up, fc1_down, fc2_up, fc2_down)
    gall, gn = run_backward(segments, adapter_ids, gm, att, c2, oh, proj_down, proj_up, qkv_down, gf, wp, wq, qkv, n1, c1, prob, qkv_up)
    gt, gqd, gqu, gpd, gpu, gf1d, gf1u, gf2d, gf2u = run_expand(vecf, gall, gn, x, gm)
    return out[None], gt[None], gqd, gqu, gpd, gpu, gf1d, gf1u, gf2d, gf2u


def solution(mesh):
    sizes = dict(mesh.shape)
    small = sizes == {"seq": 2, "fsdp": 16}

    def per_device_any(*args):
        tokens, adapter_ids = args[0], args[4]
        one_image = tokens.shape[1:] == (512, 1024) and adapter_ids.shape[1] == 1
        return (per_device_fast if small and one_image else per_device)(*args)

    return jax.shard_map(
        per_device_any,
        mesh=mesh,
        in_specs=(
            P("fsdp", "seq", None),
            P("fsdp", "seq", None),
            P("fsdp", None),
            P("fsdp", None),
            P("fsdp", None),
            P("fsdp"),
            P("fsdp"),
            P("fsdp", None),
            P("fsdp", None),
            P("fsdp"),
            P("fsdp"),
            P("fsdp"),
            P("fsdp", None),
            P("fsdp"),
            P("fsdp", None),
            P("fsdp"),
            P(),
            P(),
            P(),
            P(),
            P(),
            P(),
            P(),
            P(),
        ),
        out_specs=(
            P("fsdp", "seq", None),
            P("fsdp", "seq", None),
            P(),
            P(),
            P(),
            P(),
            P(),
            P(),
            P(),
            P(),
        ),
        check_vma=False,
    )
```

```python
from functools import partial

import jax
import jax.numpy as jnp
from jax import lax
from jax.experimental import pallas as pl
from jax.experimental.pallas import tpu as pltpu
from jax.sharding import PartitionSpec as P

HEAD_DIM = 64
IMG = 577
RANK = 16
QBLOCK = 512


norm_eps = 1e-06
masked_score = -1e30


def matmul(left_side, right_side):
    return jnp.dot(left_side, right_side, preferred_element_type=jnp.float32)


def matmul_nt(left_side, right_side):
    return jnp.einsum("tk,jk->tj", left_side, right_side, preferred_element_type=jnp.float32)


def matmul_tn(left_side, right_side):
    return jnp.einsum("ti,to->io", left_side, right_side, preferred_element_type=jnp.float32)


def layer_norm(values, norm_gain, norm_shift):
    centre = jnp.mean(values, axis=-1, keepdims=True)
    centred = values - centre
    spread = jnp.mean(centred * centred, axis=-1, keepdims=True)
    return centred * lax.rsqrt(spread + norm_eps) * norm_gain + norm_shift


def norm_backward(values, norm_gain, norm_shift, grad_in):

    def apply_norm(inputs):
        return layer_norm(inputs, norm_gain, norm_shift)

    unused, pullback = jax.vjp(apply_norm, values)
    return pullback(grad_in)[0]


def selection(seg_own, image_adapters, columns):
    images = jnp.arange(image_adapters.shape[0], dtype=jnp.int32)
    image_match = seg_own[:, None] - 1 == images[None, :]
    token_adapter = jnp.sum(jnp.where(image_match, image_adapters[None, :], 0), axis=1)
    present = jnp.any(image_match, axis=1)
    column = jnp.arange(columns, dtype=jnp.int32) // RANK
    chosen = (token_adapter[:, None] == column[None, :]) & present[:, None]
    return chosen.astype(jnp.float32)


def adapter_forward(inputs_b, weight, down_map, up_map, select):
    inner_term = (matmul(inputs_b, down_map) * select).astype(jnp.bfloat16)
    return (matmul(inputs_b, weight) + matmul(inner_term, up_map), inner_term)


def adapter_backward(inputs_b, inner_term, grad_in, weight, down_map, up_map, select):
    grad_up = matmul_tn(inner_term, grad_in)
    grad_inner = (matmul_nt(grad_in, up_map) * select).astype(jnp.bfloat16)
    grad_down = matmul_tn(inputs_b, grad_inner)
    grad_inputs = matmul_nt(grad_in, weight) + matmul_nt(grad_inner, down_map)
    return (grad_inputs, grad_down, grad_up)


def block_scores(query_block, key_heads, seg_block, seg_keys, keep_keys):
    score_scale = HEAD_DIM ** (-0.5)
    scores = (
        jnp.einsum("qhd,khd->hqk", query_block, key_heads, preferred_element_type=jnp.float32)
        * score_scale
    )
    allowed = (seg_block[:, None] == seg_keys[None, :]) & (keep_keys[None, :] == 1)
    return jnp.where(allowed[None, :, :], scores, masked_score)


def split_heads(head_rows):
    all_rows = head_rows.shape[0]
    local_heads = head_rows.shape[2] // HEAD_DIM
    query_heads = head_rows[:, 0].reshape(all_rows, local_heads, HEAD_DIM)
    key_heads = head_rows[:, 1].reshape(all_rows, local_heads, HEAD_DIM)
    value_heads = head_rows[:, 2].reshape(all_rows, local_heads, HEAD_DIM)
    return (query_heads, key_heads, value_heads)


def key_window(all_rows):
    return min(all_rows, (QBLOCK + 2 * IMG - 2 + 127) // 128 * 128)


def window_start(block_index, all_rows, window):
    first = block_index * QBLOCK - (IMG - 1)
    return jnp.clip(first, 0, all_rows - window)


def attention_forward(head_rows, seg_all, keep_all):
    all_rows = head_rows.shape[0]
    block_count = all_rows // QBLOCK
    window = key_window(all_rows)
    query_heads, key_heads, value_heads = split_heads(head_rows)
    local_heads = query_heads.shape[1]

    def one_block(block_parts):
        query_block, seg_block, keep_block, block_index = block_parts
        start = window_start(block_index, all_rows, window)
        keys_near = lax.dynamic_slice_in_dim(key_heads, start, window, 0)
        values_near = lax.dynamic_slice_in_dim(value_heads, start, window, 0)
        seg_near = lax.dynamic_slice_in_dim(seg_all, start, window, 0)
        keep_near = lax.dynamic_slice_in_dim(keep_all, start, window, 0)
        scores = block_scores(query_block, keys_near, seg_block, seg_near, keep_near)
        row_max = jnp.max(scores, axis=2, keepdims=True)
        weights = jnp.exp(scores - row_max)
        row_sum = jnp.sum(weights, axis=2, keepdims=True)
        probs_low = (weights / row_sum).astype(jnp.bfloat16)
        result = jnp.einsum(
            "hqk,khd->qhd", probs_low, values_near, preferred_element_type=jnp.float32
        )
        result = result * keep_block[:, None, None].astype(jnp.float32)
        return (result.astype(jnp.bfloat16), row_max, row_sum)

    block_ids = jnp.arange(block_count, dtype=jnp.int32)
    blocked = (
        query_heads.reshape(block_count, QBLOCK, local_heads, HEAD_DIM),
        seg_all.reshape(block_count, QBLOCK),
        keep_all.reshape(block_count, QBLOCK),
        block_ids,
    )
    results, block_max, block_sums = lax.map(one_block, blocked)
    return (results.reshape(all_rows, local_heads * HEAD_DIM), block_max, block_sums)


def attention_backward(head_rows, grad_rows, seg_all, keep_all, block_max, block_sums):
    all_rows = head_rows.shape[0]
    block_count = all_rows // QBLOCK
    window = key_window(all_rows)
    query_heads, key_heads, value_heads = split_heads(head_rows)
    local_heads = query_heads.shape[1]
    score_scale = HEAD_DIM ** (-0.5)

    def one_block(running, block_parts):
        grad_keys, grad_values = running
        query_block, seg_block, keep_block, grad_block, row_max, row_sum, block_index = block_parts
        start = window_start(block_index, all_rows, window)
        keys_near = lax.dynamic_slice_in_dim(key_heads, start, window, 0)
        values_near = lax.dynamic_slice_in_dim(value_heads, start, window, 0)
        seg_near = lax.dynamic_slice_in_dim(seg_all, start, window, 0)
        keep_near = lax.dynamic_slice_in_dim(keep_all, start, window, 0)
        scores = block_scores(query_block, keys_near, seg_block, seg_near, keep_near)
        probs = jnp.exp(scores - row_max) / row_sum
        grad_result = grad_block * keep_block[:, None, None].astype(jnp.bfloat16)
        values_term = jnp.einsum(
            "hqk,qhd->khd",
            probs.astype(jnp.bfloat16),
            grad_result,
            preferred_element_type=jnp.float32,
        )
        grad_probs = jnp.einsum(
            "qhd,khd->hqk", grad_result, values_near, preferred_element_type=jnp.float32
        )
        row_inner = jnp.sum(probs * grad_probs, axis=2, keepdims=True)
        grad_scores = (probs * (grad_probs - row_inner)).astype(jnp.bfloat16)
        grad_query = (
            jnp.einsum("hqk,khd->qhd", grad_scores, keys_near, preferred_element_type=jnp.float32)
            * score_scale
        )
        keys_term = (
            jnp.einsum("hqk,qhd->khd", grad_scores, query_block, preferred_element_type=jnp.float32)
            * score_scale
        )
        grad_keys = lax.dynamic_update_slice_in_dim(
            grad_keys, lax.dynamic_slice_in_dim(grad_keys, start, window, 0) + keys_term, start, 0
        )
        grad_values = lax.dynamic_update_slice_in_dim(
            grad_values,
            lax.dynamic_slice_in_dim(grad_values, start, window, 0) + values_term,
            start,
            0,
        )
        return ((grad_keys, grad_values), grad_query)

    zero_heads = jnp.zeros((all_rows, local_heads, HEAD_DIM), jnp.float32)
    block_ids = jnp.arange(block_count, dtype=jnp.int32)
    blocked = (
        query_heads.reshape(block_count, QBLOCK, local_heads, HEAD_DIM),
        seg_all.reshape(block_count, QBLOCK),
        keep_all.reshape(block_count, QBLOCK),
        grad_rows.reshape(block_count, QBLOCK, local_heads, HEAD_DIM),
        block_max,
        block_sums,
        block_ids,
    )
    (grad_keys, grad_values), grad_queries = lax.scan(one_block, (zero_heads, zero_heads), blocked)
    flat_width = local_heads * HEAD_DIM
    stacked = jnp.stack(
        [
            grad_queries.reshape(all_rows, flat_width),
            grad_keys.reshape(all_rows, flat_width),
            grad_values.reshape(all_rows, flat_width),
        ],
        axis=1,
    )
    return stacked.astype(jnp.bfloat16)


def per_device(
    tokens,
    grad_out,
    segments,
    padding,
    adapter_ids,
    norm1_gain,
    norm1_bias,
    w_qkv,
    w_proj,
    proj_bias,
    norm2_gain,
    norm2_bias,
    w_fc1,
    fc1_bias,
    w_fc2,
    fc2_bias,
    qkv_down,
    qkv_up,
    proj_down,
    proj_up,
    fc1_down,
    fc1_up,
    fc2_down,
    fc2_up,
):
    tok_rows = tokens.shape[1]
    feat_width = tokens.shape[2]
    inputs = tokens[0].astype(jnp.float32)
    seg_all = segments[0]
    keep_all = padding[0]
    offset = lax.axis_index("seq") * tok_rows
    seg_own = lax.dynamic_slice_in_dim(seg_all, offset, tok_rows)
    select = selection(seg_own, adapter_ids[0], qkv_down.shape[1])
    gain_one, shift_one, qkv_weight, proj_weight, proj_shift = (
        lax.all_gather(norm1_gain, "fsdp", axis=0, tiled=True),
        lax.all_gather(norm1_bias, "fsdp", axis=0, tiled=True),
        lax.all_gather(w_qkv, "fsdp", axis=0, tiled=True),
        lax.all_gather(w_proj, "fsdp", axis=0, tiled=True),
        lax.all_gather(proj_bias, "fsdp", axis=0, tiled=True),
    )
    gain_one = gain_one.astype(jnp.float32)
    shift_one = shift_one.astype(jnp.float32)
    normed_one = layer_norm(inputs, gain_one, shift_one).astype(jnp.bfloat16)
    qkv_main, inner_one = adapter_forward(normed_one, qkv_weight, qkv_down, qkv_up, select)
    qkv_low = qkv_main.astype(jnp.bfloat16).reshape(tok_rows, 3, feat_width)
    head_rows = lax.all_to_all(qkv_low, "seq", split_axis=2, concat_axis=0, tiled=True)
    attended_heads, block_max, block_sums = attention_forward(head_rows, seg_all, keep_all)
    attended = lax.all_to_all(attended_heads, "seq", split_axis=0, concat_axis=1, tiled=True)
    branch_one, inner_two = adapter_forward(attended, proj_weight, proj_down, proj_up, select)
    middle = inputs + (branch_one + proj_shift.astype(jnp.float32))
    gain_two, shift_two, fc1_weight, fc2_shift, fc2_weight, fc1_shift = (
        lax.all_gather(norm2_gain, "fsdp", axis=0, tiled=True),
        lax.all_gather(norm2_bias, "fsdp", axis=0, tiled=True),
        lax.all_gather(w_fc1, "fsdp", axis=0, tiled=True),
        lax.all_gather(fc2_bias, "fsdp", axis=0, tiled=True),
        lax.all_gather(w_fc2, "fsdp", axis=0, tiled=True),
        lax.all_gather(fc1_bias, "fsdp", axis=0, tiled=True),
    )
    gain_two = gain_two.astype(jnp.float32)
    shift_two = shift_two.astype(jnp.float32)
    normed_two = layer_norm(middle, gain_two, shift_two).astype(jnp.bfloat16)
    hidden_main, inner_three = adapter_forward(normed_two, fc1_weight, fc1_down, fc1_up, select)
    hidden = hidden_main + fc1_shift.astype(jnp.float32)
    active = jax.nn.gelu(hidden, approximate=False).astype(jnp.bfloat16)
    branch_two, inner_four = adapter_forward(active, fc2_weight, fc2_down, fc2_up, select)
    output = (middle + (branch_two + fc2_shift.astype(jnp.float32))).astype(jnp.bfloat16)
    fc1_back, fc2_back = (
        lax.all_gather(w_fc1, "fsdp", axis=0, tiled=True),
        lax.all_gather(w_fc2, "fsdp", axis=0, tiled=True),
    )
    grad_top = grad_out[0]
    grad_active, grad_fc2_down, grad_fc2_up = adapter_backward(
        active, inner_four, grad_top, fc2_back, fc2_down, fc2_up, select
    )
    unused, gelu_back = jax.vjp(partial(jax.nn.gelu, approximate=False), hidden)
    grad_hidden = gelu_back(grad_active)[0].astype(jnp.bfloat16)
    grad_normed_two, grad_fc1_down, grad_fc1_up = adapter_backward(
        normed_two, inner_three, grad_hidden, fc1_back, fc1_down, fc1_up, select
    )
    grad_middle = grad_top.astype(jnp.float32) + norm_backward(
        middle, gain_two, shift_two, grad_normed_two
    )
    qkv_back, proj_back = (
        lax.all_gather(w_qkv, "fsdp", axis=0, tiled=True),
        lax.all_gather(w_proj, "fsdp", axis=0, tiled=True),
    )
    grad_branch_one = grad_middle.astype(jnp.bfloat16)
    grad_attended, grad_proj_down, grad_proj_up = adapter_backward(
        attended, inner_two, grad_branch_one, proj_back, proj_down, proj_up, select
    )
    grad_head_rows = lax.all_to_all(
        grad_attended.astype(jnp.bfloat16), "seq", split_axis=1, concat_axis=0, tiled=True
    )
    grad_qkv_heads = attention_backward(
        head_rows, grad_head_rows, seg_all, keep_all, block_max, block_sums
    )
    grad_qkv = lax.all_to_all(
        grad_qkv_heads, "seq", split_axis=0, concat_axis=2, tiled=True
    ).reshape(tok_rows, 3 * feat_width)
    grad_normed_one, grad_qkv_down, grad_qkv_up = adapter_backward(
        normed_one, inner_one, grad_qkv, qkv_back, qkv_down, qkv_up, select
    )
    grad_tokens = grad_middle + norm_backward(inputs, gain_one, shift_one, grad_normed_one)
    summed = lax.psum(
        (
            grad_qkv_down,
            grad_qkv_up,
            grad_proj_down,
            grad_proj_up,
            grad_fc1_down,
            grad_fc1_up,
            grad_fc2_down,
            grad_fc2_up,
        ),
        ("seq", "fsdp"),
    )
    return (
        output[None],
        grad_tokens[None],
        summed[0],
        summed[1],
        summed[2],
        summed[3],
        summed[4],
        summed[5],
        summed[6],
        summed[7],
    )


F32 = jnp.float32
BF16 = jnp.bfloat16
MESH = pl.DeviceIdType.MESH
VMEM_LIMIT = 64 * 1000 * 1000


def mm(a, b):
    return lax.dot_general(a, b, (((1,), (0,)), ((), ())), preferred_element_type=F32)


def mm_nt(a, b):
    return lax.dot_general(a, b, (((1,), (1,)), ((), ())), preferred_element_type=F32)


def mm_tn(a, b):
    return lax.dot_general(a, b, (((0,), (0,)), ((), ())), preferred_element_type=F32)


def norm_parts(v):
    mean = jnp.mean(v, axis=-1, keepdims=True)
    centred = v - mean
    r = lax.rsqrt(jnp.mean(centred * centred, axis=-1, keepdims=True) + norm_eps)
    return centred * r, r


def norm_grad(v, gain, grad_y):
    h, r = norm_parts(v)
    d = grad_y * gain
    return r * (d - jnp.mean(d, axis=-1, keepdims=True) - h * jnp.mean(d * h, axis=-1, keepdims=True))


class Net:
    def __init__(self):
        self.s = lax.axis_index("seq")
        self.f = lax.axis_index("fsdp")
        self.z = self.f // 4
        self.x = (self.f // 2) % 2
        self.c = self.f % 2
        self.partner = {"seq": 1 - self.s}
        self.x_peer = {"fsdp": self.block(self.z, 1 - self.x, self.c)}
        self.c_peer = {"fsdp": self.block(self.z, self.x, 1 - self.c)}

    def block(self, z, x, c):
        return (z * 2 + x) * 2 + c

    def z_peer(self, d):
        return {"fsdp": self.block((self.z + d) % 4, self.x, self.c)}

    def meet(self, peers):
        sem = pltpu.get_barrier_semaphore()
        for peer in peers:
            pl.semaphore_signal(sem, inc=1, device_id=peer, device_id_type=MESH)
        pl.semaphore_wait(sem, len(peers))

    def plane_peer(self, d):
        return {"fsdp": (self.f + d) % 16}

    def plane_barrier(self):
        self.meet([self.partner] + [self.plane_peer(d) for d in range(1, 16)])

    def barrier(self):
        self.meet([self.partner, self.x_peer, self.c_peer] + [self.z_peer(d) for d in (1, 2, 3)])


class Block:
    def __init__(self, src, piece, send_sem, recv_sem, own_sem, plane=2):
        self.src, self.piece, self.plane = src, piece, plane
        self.send_sem, self.recv_sem, self.own_sem = send_sem, recv_sem, own_sem


class Gather:
    def __init__(self, net):
        self.net = net

    def copy(self, it, src, block, k, peer):
        return pltpu.make_async_remote_copy(
            src_ref=src, dst_ref=it.piece(block), send_sem=it.send_sem(k), recv_sem=it.recv_sem(block),
            device_id=peer, device_id_type=MESH)

    def arrive(self, it, block):
        piece = it.piece(block)
        self.copy(it, piece, block, 0, self.net.c_peer).wait_recv()
        return piece

    def here(self, it, body):
        if isinstance(it.plane, int) and it.plane == 2:
            body()
        else:
            pl.when((self.net.s == it.plane) | (it.plane == 2))(body)

    def hand_on(self, it, copies):
        if isinstance(it.plane, int):
            if it.plane != 2:
                for copy in copies:
                    copy.start()
            return

        @pl.when(it.plane != 2)
        def _():
            for copy in copies:
                copy.start()

    def own(self, it):
        return pltpu.make_async_copy(it.src, it.piece(self.net.f), it.own_sem)

    def start(self, it):
        net = self.net

        def along():
            for d in (2, 1, 3):
                self.copy(it, it.src, net.f, d - 1, net.z_peer(d)).start()
            self.copy(it, it.src, net.f, 3, net.x_peer).start()

        self.here(it, along)
        self.copy(it, it.src, net.f, 4, net.c_peer).start()
        self.own(it).start()

    def from_z(self, it):
        net = self.net

        def body():
            pieces = []
            for n, d in enumerate((1, 3, 2)):
                block = net.block((net.z + d) % 4, net.x, net.c)
                piece = self.arrive(it, block)
                self.copy(it, piece, block, 5 + 2 * n, net.x_peer).start()
                self.copy(it, piece, block, 6 + 2 * n, net.c_peer).start()
                pieces.append((piece, block))
            self.hand_on(it, [self.copy(it, piece, block, 15 + n, net.partner) for n, (piece, block) in enumerate(pieces)])

        self.here(it, body)

    def from_x(self, it):
        net = self.net

        def body():
            pieces = []
            for n, d in enumerate((0, 1, 3, 2)):
                block = net.block((net.z + d) % 4, 1 - net.x, net.c)
                piece = self.arrive(it, block)
                self.copy(it, piece, block, 11 + n, net.c_peer).start()
                pieces.append((piece, block))
            self.hand_on(it, [self.copy(it, piece, block, 18 + n, net.partner) for n, (piece, block) in enumerate(pieces)])

        self.here(it, body)

    def from_seq(self, it):
        net = self.net
        if isinstance(it.plane, int) and it.plane == 2:
            return

        @pl.when((net.s != it.plane) & (it.plane != 2))
        def _():
            for n, (d, x) in enumerate(((1, net.x), (3, net.x), (2, net.x), (0, 1 - net.x), (1, 1 - net.x),
                                        (3, 1 - net.x), (2, 1 - net.x))):
                block = net.block((net.z + d) % 4, x, net.c)
                piece = self.arrive(it, block)
                self.copy(it, piece, block, 5 + n, net.c_peer).start()

    def from_core(self, it):
        net = self.net

        @pl.loop(0, 8)
        def _(n):
            self.arrive(it, 2 * n + 1 - net.c)

        self.own(it).wait()

    def finish(self, it):
        net = self.net

        def sent(first, end):
            @pl.loop(first, end)
            def _(k):
                self.copy(it, it.src, net.f, k, net.c_peer).wait_send()

        if isinstance(it.plane, int) and it.plane == 2:
            sent(0, 15)
            return

        @pl.when(it.plane == 2)
        def _():
            sent(0, 15)

        @pl.when(net.s == it.plane)
        def _():
            sent(0, 22)

        @pl.when((net.s != it.plane) & (it.plane != 2))
        def _():
            sent(4, 12)


def full_vector(vec_ref, row, blocks=16, rows=16):
    parts = []
    for k in range(blocks // 2):
        even = vec_ref[2 * k * rows + row:2 * k * rows + row + 1, :]
        odd = vec_ref[(2 * k + 1) * rows + row:(2 * k + 1) * rows + row + 1, :]
        parts.append(even + odd)
    return jnp.concatenate(parts, axis=1)


WINDOW = 640
STEP = 64
PAD = 384
QROWS = 320
FFB = 512


class Image:
    def __init__(self, seg_ref, id_ref):
        self.start = jnp.sum((seg_ref[...] == 0).astype(F32), axis=1, keepdims=True)
        ident = id_ref[...].astype(F32)
        self.pick = []
        base = jnp.zeros((1, 1), F32)
        for k in range(PAD // STEP + 1):
            mark = ((self.start >= k * STEP) & (self.start < (k + 1) * STEP)).astype(F32)
            self.pick.append(mark)
            base = base + mark * float(k * STEP)
        self.shift = base - self.start
        lane = lax.broadcasted_iota(jnp.int32, (1, 128), 1).astype(F32)
        self.columns = ((lane >= ident * RANK) & (lane < (ident + 1) * RANK)).astype(F32)

    def choose(self, load):
        total = None
        for k, mark in enumerate(self.pick):
            value = load(k * STEP)
            value = value * mark.astype(value.dtype)
            total = value if total is None else total + value
        return total

    def inside(self, shape, axis, first=0):
        at = (lax.broadcasted_iota(jnp.int32, shape, axis) + first).astype(F32) + self.shift
        return (at >= 0) & (at < IMG)

    def select(self, first, rows):
        at = (lax.broadcasted_iota(jnp.int32, (rows, 1), 0) + first).astype(F32)
        return (at >= self.start).astype(F32) * self.columns

    def select_window(self, first, rows):
        at = (lax.broadcasted_iota(jnp.int32, (rows, 1), 0) + first).astype(F32) + self.shift
        return (at >= 0).astype(F32) * self.columns


def lane_halves():
    lane = lax.broadcasted_iota(jnp.int32, (1, 128), 1)
    return [(lane < 64).astype(F32), (lane >= 64).astype(F32)]


def compact_rows(dense):
    total = dense[0:16]
    for k in range(1, 8):
        total = total + dense[16 * k:16 * (k + 1)]
    return total.astype(BF16)


N_FC1 = 8
N_FC2 = 4
FIRST = 6
N_ITEMS = FIRST + N_FC2 + N_FC1


def forward_kernel(seg_ref, id_ref, x_ref, vec_ref, qd_ref, pd_ref, pu_ref, wq_hbm, wp_hbm, w1_hbm, w2_hbm,
                   qu_hbm, g_hbm, u1_hbm, d1_hbm, u2_hbm, d2_hbm,
                   wqf, wpf, vecf_out, qkv_out, n1_out, c1_out, prob_out, oh_out, att_out, c2_out, gm_out, gr_out, out_out,
                   wq_own, wq, wp, w1, w2, xp, vecf, qu, g, u1, d1, u2, d2, qkv, n1, c1, qkvw, n1w, c1w, prob, opad, sendb,
                   oh, att, c2, mid, n2, oacc, gacc, u4, e3, c3, e4, c3t, e4t, act_s, gh_s, gr,
                   xs_sem, xr_sem, as_sem, ar_sem, loc_sem, out_sem, prob_sem, g_send, g_recv, g_own):
    net = Net()
    s, other = net.s, 1 - net.s
    rows, width = x_ref.shape
    half = wq.shape[1] // 3
    rb = wq_own.shape[0]
    fr1 = w1_hbm.shape[0]
    fr2 = w2_hbm.shape[0]
    ff = w1.shape[1]
    chunk = rows // 2

    pre = []
    for part in range(3):
        cols = pl.ds(pl.multiple_of(part * width + s * half, 128), half)
        pre.append(pltpu.make_async_copy(wq_hbm.at[:, cols], wq_own.at[:, pl.ds(part * half, half)], loc_sem.at[part]))
    late = []
    for part in range(3):
        cols = pl.ds(pl.multiple_of(part * width + s * half, 128), half)
        late.append(pltpu.make_async_copy(qu_hbm.at[:, cols], qu.at[:, pl.ds(part * half, half)], loc_sem.at[3 + part]))
    for n, (src, dst) in enumerate(((g_hbm, g), (u1_hbm, u1), (d1_hbm, d1), (u2_hbm, u2), (d2_hbm, d2))):
        late.append(pltpu.make_async_copy(src, dst, loc_sem.at[6 + n]))
    for copy in pre + late:
        copy.start()
    net.barrier()

    def x_copy(i):
        part = pl.ds(i * chunk, chunk)
        return pltpu.make_async_remote_copy(
            src_ref=x_ref.at[part, :], dst_ref=xp.at[part, :], send_sem=xs_sem.at[i], recv_sem=xr_sem.at[i],
            device_id=net.partner, device_id_type=MESH)

    for i in range(2):
        x_copy(i).start()
    for copy in pre:
        copy.wait()

    def block(n, src, piece, plane=2):
        return Block(src, piece, lambda k: g_send.at[n, k], lambda b: g_recv.at[n, b], g_own.at[n], plane)

    def wq_part(part):
        cols = pl.ds(part * half, half)
        return block(1 + part, wq_own.at[:, cols], lambda b: wq.at[pl.ds(b * rb, rb), cols])

    def wp_part(part):
        cols = pl.ds(part * half, half)
        return block(4 + part, wp_hbm.at[:, cols], lambda b: wp.at[pl.ds(b * rb, rb), cols], part)

    sub = fr2 // N_FC2

    def times(j, size):
        return j * size if isinstance(j, int) else pl.multiple_of(j * size, size)

    def item(n):
        if isinstance(n, int) and n < FIRST:
            if n == 0:
                return block(0, vec_ref, lambda b: vecf.at[pl.ds(b * 16, 16), :])
            return wq_part(n - 1) if n < 4 else wp_part(n - 4)
        if isinstance(n, int):
            return fc2_it(n - FIRST) if n < FIRST + N_FC2 else fc1_it(n - FIRST - N_FC2)
        return fc1_it(n - FIRST - N_FC2)

    def fc2_it(j):
        at = pl.ds(times(j, sub), sub)
        return block(FIRST + j, w2_hbm.at[at, :], lambda b: w2.at[pl.ds(b * fr2 + times(j, sub), sub), :],
                     (0, 1, 2, 2)[j])

    def fc1_it(j):
        cols = pl.ds(times(j, FFB), FFB)
        return block(FIRST + N_FC2 + j, w1_hbm.at[:, cols], lambda b: w1.at[pl.ds(b * fr1, fr1), cols],
                     ((2, 2, 0, 1)[j % 4] if isinstance(j, int) else jnp.where(j % 4 < 2, 2, j % 4 - 2)))

    gather = Gather(net)
    stages = {"S": gather.start, "A": gather.from_z, "B": gather.from_x, "Y": gather.from_seq, "C": gather.from_core}

    def go(*steps):
        for step in steps:
            stages[step[0]](item(int(step[1:])))

    go("S0", "S1", "S2")
    image = Image(seg_ref, id_ref)
    zeros = jnp.zeros((PAD, 128), BF16)
    opad[0:PAD, :] = zeros
    opad[PAD + WINDOW:2 * PAD + WINDOW, :] = zeros
    go("A0", "A1", "S3", "A2", "S4", "S5", "B0", "B1", "A3", "S6", "S7", "B2", "A4", "A5", "S8")
    for copy in late:
        copy.wait()
    go("B3", "C0", "C1", "C2", "C3")

    gain1 = full_vector(vecf, 0)
    shift1 = full_vector(vecf, 1)

    def project(src, src_row, row):
        v = src[pl.ds(src_row, chunk), :].astype(F32)
        h, unused = norm_parts(v)
        normed = (h * gain1 + shift1).astype(BF16)
        at = pl.ds(row, chunk)
        n1[at, :] = normed
        inner = (mm(normed, qd_ref[...]) * image.select(row, chunk)).astype(BF16)
        c1[at, :] = inner
        for part in range(3):
            cols = pl.ds(part * half, half)
            qkv[at, cols] = (mm(normed, wq[:, cols]) + mm(inner, qu[:, cols])).astype(BF16)

    def own_rows_in(i):
        project(x_ref, i * chunk, pl.multiple_of(s * rows + i * chunk, chunk))

    def partner_rows_in(i):
        x_copy(i).wait_recv()
        project(xp, i * chunk, pl.multiple_of(other * rows + i * chunk, chunk))

    own_rows_in(0)
    own_rows_in(1)
    partner_rows_in(0)
    partner_rows_in(1)
    go("B4", "B5", "A6", "A7", "S9")
    outs = []

    def put(src, dst):
        copy = pltpu.make_async_copy(src, dst, out_sem.at[len(outs)])
        copy.start()
        outs.append(copy)

    put(wq, wqf)
    put(vecf, vecf_out)
    for src, dst in ((qkv, qkvw), (n1, n1w), (c1, c1w)):
        step = min(src.shape[1], 512)

        @pl.loop(0, src.shape[1] // step)
        def _(n, src=src, dst=dst, step=step):
            cols = pl.ds(pl.multiple_of(n * step, step), step)
            dst[:, cols] = image.choose(lambda at: src[at:at + WINDOW, cols])
    put(qkvw, qkv_out)
    put(n1w, n1_out)
    put(c1w, c1_out)
    bias = jnp.where(image.inside((1, WINDOW), 1), 0.0, masked_score).astype(F32)
    halves = lane_halves()

    def prob_copy(pair):
        slot = lax.rem(pair, 2)
        return pltpu.make_async_copy(prob.at[slot], prob_out.at[pl.ds(2 * pair, 2)], prob_sem.at[slot])

    def att_copy(pair):
        cols = pl.ds(pl.multiple_of(s * half + pair * 128, 128), 128)
        return pltpu.make_async_remote_copy(
            src_ref=sendb.at[pair], dst_ref=att.at[:, cols], send_sem=as_sem.at[pair], recv_sem=ar_sem.at[pair],
            device_id=net.partner, device_id_type=MESH)

    pairs = half // 128

    @pl.loop(0, pairs)
    def _(pair):
        def cols(part):
            return pl.ds(pl.multiple_of(part * half + pair * 128, 128), 128)

        for n, steps in enumerate(((), ("Y4", "Y5"), ("B6", "B7", "A8", "S10", "S11"), ("C4", "C5"))):
            @pl.when(pair == n)
            def _(steps=steps):
                go(*steps)

        k2 = qkvw[:, cols(1)]
        v2 = qkvw[:, cols(2)]
        vs = [(v2 * hm.astype(BF16)) for hm in halves]
        slot = lax.rem(pair, 2)

        @pl.when(pair >= 2)
        def _():
            prob_copy(pair).wait()

        @pl.loop(0, WINDOW // QROWS)
        def _(b):
            r0 = pl.multiple_of(b * QROWS, QROWS)
            q2 = qkvw[pl.ds(r0, QROWS), cols(0)]
            q2 = q2 * jnp.asarray(HEAD_DIM ** (-0.5), BF16)
            total = None
            for hd in range(2):
                scores = mm_nt(q2 * halves[hd].astype(BF16), k2) + bias
                weights = jnp.exp(scores - jnp.max(scores, axis=1, keepdims=True))
                weights = (weights * (1.0 / jnp.sum(weights, axis=1, keepdims=True))).astype(BF16)
                prob[slot, hd, pl.ds(r0, QROWS), :] = weights
                part = mm(weights, vs[hd])
                total = part if total is None else total + part
            total = (total * image.inside((QROWS, 1), 0, r0).astype(F32)).astype(BF16)
            opad[pl.ds(PAD + r0, QROWS), :] = total
            oh[pl.ds(r0, QROWS), cols(0)] = total

        prob_copy(pair).start()

        def own_rows(who):
            return image.choose(lambda at: opad[pl.ds(pl.multiple_of(who * rows + PAD - at, STEP), rows), :])

        sendb[pair] = own_rows(other)
        att_copy(pair).start()
        att[:, pl.ds(pl.multiple_of(s * half + pair * 128, 128), 128)] = own_rows(s)

    go("B8", "A9", "S12", "S13", "Y6", "Y7")
    put(wp, wpf)
    put(oh, oh_out)

    @pl.loop(0, pairs)
    def _(pair):
        att_copy(pair).wait_recv()

    put(att, att_out)
    go("A10", "S14")
    bias_p = full_vector(vecf, 2)
    gain2 = full_vector(vecf, 3)
    shift2 = full_vector(vecf, 4)

    @pl.loop(0, 2)
    def _(i):
        at = pl.ds(pl.multiple_of(i * chunk, chunk), chunk)
        rows_in = att[at, :]
        own_select = image.select(s * rows + i * chunk, chunk)
        inner = (mm(rows_in, pd_ref[...]) * own_select).astype(BF16)
        c2[at, :] = inner
        branch = mm(rows_in, wp[...]) + mm(inner, pu_ref[...]) + bias_p
        middle = x_ref[at, :].astype(F32) + branch
        mid[at, :] = middle
        h, unused = norm_parts(middle)
        normed = (h * gain2 + shift2).astype(BF16)
        n2[at, :] = normed
        c = mm(normed, d1[...]) * own_select
        e = mm_nt(g[at, :], u2[...]) * own_select
        c3[at, :] = c.astype(BF16)
        e4[at, :] = e.astype(BF16)
        oacc[at, :] = jnp.zeros((chunk, width), F32)
        gacc[at, :] = jnp.zeros((chunk, width), F32)
        u4[at, :] = jnp.zeros((chunk, 128), F32)
        e3[at, :] = jnp.zeros((chunk, 128), F32)

    c3t[...] = c3[...].T
    e4t[...] = e4[...].T
    put(c2, c2_out)
    go("B9", "A11", "S15", "C6", "C7", "C8", "C9", "B10", "A12", "A13", "S16", "S17", "B11")

    @pl.loop(0, N_FC1)
    def _(j):
        gather.from_core(fc1_it(j))
        bias = jnp.concatenate([vecf[pl.ds(2 * j * 16 + 6, 1), :], vecf[pl.ds(2 * j * 16 + 7, 1), :],
                                vecf[pl.ds((2 * j + 1) * 16 + 6, 1), :], vecf[pl.ds((2 * j + 1) * 16 + 7, 1), :]], axis=1)
        col = pl.ds(pl.multiple_of(j * FFB, FFB), FFB)

        @pl.loop(0, 2)
        def _(i):
            @pl.when((i == 1) & (j + 4 < N_FC1))
            def _():
                gather.from_z(fc1_it(j + 4))

            @pl.when((i == 1) & (j + 2 < N_FC1))
            def _():
                gather.from_x(fc1_it(j + 2))

            at = pl.ds(pl.multiple_of(i * chunk, chunk), chunk)
            hidden = mm(n2[at, :], w1[:, col]) + mm(c3[at, :], u1[:, col]) + bias
            cdf = 0.5 * (1.0 + lax.erf(hidden * (0.5 ** 0.5)))
            pdf = jnp.exp(hidden * hidden * -0.5) * (0.5 / 3.141592653589793) ** 0.5
            active = (hidden * cdf).astype(BF16)
            act_s[at, :] = active
            grad_active = mm_nt(g[at, :], w2[col, :]) + mm_nt(e4[at, :], d2[col, :])
            grad_hidden = (grad_active * (cdf + hidden * pdf)).astype(BF16)
            gh_s[at, :] = grad_hidden
            oacc[at, :] += mm(active, w2[col, :])
            u4[at, :] += mm(active, d2[col, :])
            gacc[at, :] += mm_nt(grad_hidden, w1[:, col])
            e3[at, :] += mm_nt(grad_hidden, u1[:, col])

        @pl.when(j + 1 < N_FC1)
        def _():
            gather.from_seq(fc1_it(j + 1))

        gr[:, col] = compact_rows(mm(c3t[...], gh_s[...]))
        gr[:, pl.ds(pl.multiple_of(ff + j * FFB, FFB), FFB)] = compact_rows(mm(e4t[...], act_s[...]))

    bias2 = full_vector(vecf, 5)

    @pl.loop(0, 2)
    def _(i):
        at = pl.ds(pl.multiple_of(i * chunk, chunk), chunk)
        own_select = image.select(s * rows + i * chunk, chunk)
        c = (u4[at, :] * own_select).astype(BF16)
        e = (e3[at, :] * own_select).astype(BF16)
        c3[at, :] = c
        e4[at, :] = e
        act_out = mid[at, :] + (oacc[at, :] + mm(c, u2[...]) + bias2)
        xp[at, :] = act_out.astype(BF16)
        grad_n2 = gacc[at, :] + mm_nt(e, d1[...])
        gacc[at, :] = g[at, :].astype(F32) + norm_grad(mid[at, :], gain2, grad_n2)

    put(xp, out_out)
    put(gacc, gm_out)
    gr[:, 2 * ff:2 * ff + width] = compact_rows(mm_tn(e4[...], n2[...]))
    gr[:, 2 * ff + width:2 * ff + 2 * width] = compact_rows(mm_tn(c3[...], g[...]))
    put(gr, gr_out)
    for copy in outs:
        copy.wait()
    for pair in range(pairs - 2, pairs):
        prob_copy(pair).wait()
    for i in range(2):
        x_copy(i).wait_send()

    @pl.loop(0, pairs)
    def _(pair):
        att_copy(pair).wait_send()

    for n in range(FIRST + N_FC2):
        gather.finish(item(n))

    @pl.loop(0, N_FC1)
    def _(j):
        gather.finish(fc1_it(j))


def any_spec():
    return pl.BlockSpec(memory_space=pl.ANY)


def vmem_spec():
    return pl.BlockSpec(memory_space=pltpu.VMEM)


def run_forward(seg, ident, x, vec, qd, pd, pu, wq, wp, w1, w2, qu, g, u1, d1, u2, d2):
    rows, width = x.shape
    toks = seg.shape[1]
    half = width // 2
    ff = w1.shape[1]
    dma = pltpu.SemaphoreType.DMA
    sds = jax.ShapeDtypeStruct
    gcols = 2 * ff + 2 * width
    out_shape = (
        sds((width, 3 * half), BF16), sds((width, width), BF16), sds((256, 128), F32),
        sds((WINDOW, 3 * half), BF16), sds((WINDOW, width), BF16), sds((WINDOW, 128), BF16),
        sds((half // 64, WINDOW, WINDOW), BF16), sds((WINDOW, half), BF16), sds((rows, width), BF16), sds((rows, 128), BF16),
        sds((rows, width), F32), sds((16, gcols), BF16), sds((rows, width), BF16))

    def low(*shape):
        return pltpu.VMEM(shape, BF16)

    def full(*shape):
        return pltpu.VMEM(shape, F32)

    scratch = [
        low(wq.shape[0], 3 * half), low(width, 3 * half), low(width, width), low(width, ff), low(ff, width),
        low(rows, width), full(256, 128), low(128, 3 * half), low(rows, width), low(128, ff), low(width, 128),
        low(128, width), low(ff, 128), low(toks, 3 * half), low(toks, width), low(toks, 128),
        low(WINDOW, 3 * half), low(WINDOW, width), low(WINDOW, 128), low(2, 2, WINDOW, WINDOW), low(2 * PAD + WINDOW, 128),
        low(half // 128, rows, 128), low(WINDOW, half), low(rows, width), low(rows, 128), full(rows, width), low(rows, width),
        full(rows, width), full(rows, width), full(rows, 128), full(rows, 128), low(rows, 128), low(rows, 128),
        low(128, rows), low(128, rows), low(rows, FFB), low(rows, FFB), low(16, gcols),
        dma((2,)), dma((2,)), dma((4,)), dma((4,)), dma((11,)), dma((12,)), dma((2,)),
        dma((N_ITEMS, 22)), dma((N_ITEMS, 16)), dma((N_ITEMS,))]
    return pl.pallas_call(
        forward_kernel, out_shape=out_shape, in_specs=[vmem_spec()] * 7 + [any_spec()] * 10,
        out_specs=tuple(any_spec() for unused in out_shape), scratch_shapes=scratch,
        compiler_params=pltpu.CompilerParams(collective_id=1, has_side_effects=True, vmem_limit_bytes=VMEM_LIMIT),
        name="forward")(seg, ident, x, vec, qd, pd, pu, wq, wp, w1, w2, qu, g, u1, d1, u2, d2)


FIRST_PARTS = 3


def adapter_rows(vec_ref):
    ids = jnp.concatenate([jnp.broadcast_to(vec_ref[16 * p + 8:16 * p + 9, :], (16, 128)) for p in range(16)], axis=0)
    r = lax.broadcasted_iota(jnp.int32, (256, 128), 0) % 16
    col = lax.broadcasted_iota(jnp.int32, (256, 128), 1)
    group = (col // 16).astype(F32)
    return ((ids == group) & (r == col % 16)).astype(F32).T.astype(BF16)


def backward_kernel(seg_ref, id_ref, vec_ref, gm_ref, att_ref, c2_ref, oh_ref, pd_ref, pu_ref, qd_ref, gf_ref, wp_ref,
                    wq_hbm, qkv_hbm, n1_hbm, c1_hbm, prob_hbm, qu_hbm,
                    gall, gn_out,
                    wq, qkv, n1, c1, prob, qu, g1, e2, gsend, do_s, first_own, first_in, last_own, last_in, first_sum, last_sum,
                    parts1, parts2, dense1, dense2, gq, gpad, psend, prcv, gn,
                    loc_sem, ds_sem, dr_sem, fs_sem, fr_sem, ps_sem, pr_sem, out_sem, t_send, t_recv, g_send, g_recv, g_own):
    net = Net()
    s, other = net.s, 1 - net.s
    image = Image(seg_ref, id_ref)
    rows, width = gm_ref.shape
    half = wq.shape[1] // 3
    chunk = rows // 2
    ffn_cols = gf_ref.shape[1]
    n_first = first_own.shape[1]
    own1, own2 = n_first // 16, 4 * width // 16

    loads = [pltpu.make_async_copy(src, dst, loc_sem.at[i]) for i, (src, dst) in enumerate(
        [(qkv_hbm, qkv), (prob_hbm, prob), (wq_hbm, wq), (n1_hbm, n1), (c1_hbm, c1)])]
    for part in range(3):
        cols = pl.ds(pl.multiple_of(part * width + s * half, 128), half)
        loads.append(pltpu.make_async_copy(qu_hbm.at[:, cols], qu.at[:, pl.ds(part * half, half)], loc_sem.at[5 + part]))
    for copy in loads:
        copy.start()
    net.plane_barrier()

    def to_partner(src, dst, send, recv):
        return pltpu.make_async_remote_copy(src_ref=src, dst_ref=dst, send_sem=send, recv_sem=recv,
                                            device_id=net.partner, device_id_type=MESH)

    @pl.loop(0, 2)
    def _(i):
        at = pl.ds(pl.multiple_of(i * chunk, chunk), chunk)
        low = gm_ref[at, :].astype(BF16)
        g1[at, :] = low
        e2[at, :] = mm_nt(low, pu_ref[...]) * image.select(s * rows + i * chunk, chunk)

    def grad_att(i, who):
        at = pl.ds(i * chunk, chunk)
        heads = pl.ds(pl.multiple_of(who * half, half), half)
        return (mm_nt(g1[at, :], wp_ref[heads, :]) + mm_nt(e2[at, :].astype(BF16), pd_ref[heads, :])).astype(BF16)

    dsend = []
    for i in range(2):
        gsend[i] = grad_att(i, other)
        copy = to_partner(gsend.at[i], do_s.at[pl.ds(pl.multiple_of(s * rows + i * chunk, chunk), chunk), :],
                          ds_sem.at[i], dr_sem.at[i])
        copy.start()
        dsend.append(copy)
    first_own[:, 0:ffn_cols] = gf_ref[...]
    first_own[:, ffn_cols:ffn_cols + width] = compact_rows(mm_tn(c2_ref[...], g1[...]))
    first_own[:, ffn_cols + width:ffn_cols + 2 * width] = compact_rows(mm_tn(e2[...].astype(BF16), att_ref[...]))
    fsend = to_partner(first_own, first_in, fs_sem.at[0], fr_sem.at[0])
    fsend.start()
    for i in range(2):
        do_s[pl.ds(pl.multiple_of(s * rows + i * chunk, chunk), chunk), :] = grad_att(i, s)
    zeros = jnp.zeros((PAD, width), F32)
    gpad[0:PAD, :] = zeros
    gpad[PAD + WINDOW:2 * PAD + WINDOW, :] = zeros
    last_own[...] = jnp.zeros_like(last_own)
    pick = adapter_rows(vec_ref)

    def turn(n, src, dst, cols, d):
        peer = (net.f + d) % 16
        return pltpu.make_async_remote_copy(
            src_ref=src.at[:, pl.ds(pl.multiple_of(peer * cols, 128), cols)],
            dst_ref=dst.at[pl.ds(pl.multiple_of(net.f * 16, 16), 16), :], send_sem=t_send.at[n, d],
            recv_sem=t_recv.at[n, net.f], device_id={"fsdp": peer}, device_id_type=MESH)

    def turn_start(n, src, dst, cols):
        @pl.loop(1, 16)
        def _(d):
            turn(n, src, dst, cols, d).start()

        dst[pl.ds(pl.multiple_of(net.f * 16, 16), 16), :] = src[:, pl.ds(pl.multiple_of(net.f * cols, 128), cols)]

    def turn_wait(n, src, dst, cols):
        @pl.loop(1, 16)
        def _(d):
            peer = (net.f + d) % 16
            pltpu.make_async_remote_copy(
                src_ref=src.at[:, pl.ds(0, cols)], dst_ref=dst.at[pl.ds(pl.multiple_of(peer * 16, 16), 16), :],
                send_sem=t_send.at[n, d], recv_sem=t_recv.at[n, peer], device_id={"fsdp": peer},
                device_id_type=MESH).wait_recv()

    def turn_finish(n, src, dst, cols):
        @pl.loop(1, 16)
        def _(d):
            turn(n, src, dst, cols, d).wait_send()

    def block(n, src, first, step, cols):
        return Block(src, lambda b: gall.at[:, pl.ds(pl.multiple_of(first + b * step, 128), cols)],
                     lambda k: g_send.at[n, k], lambda b: g_recv.at[n, b], g_own.at[n])

    share = own1 // FIRST_PARTS
    items = [block(n, dense1.at[:, pl.ds(n * share, share)], n * share, own1, share) for n in range(FIRST_PARTS)]
    items.append(block(FIRST_PARTS, dense2, n_first, own2, own2))
    gather = Gather(net)
    stages = {"S": gather.start, "A": gather.from_z, "B": gather.from_x, "C": gather.from_core}

    def go(*steps):
        for step in steps:
            stages[step[0]](items[int(step[1:])])

    for copy in loads:
        copy.wait()
    for copy in dsend:
        copy.wait_recv()

    halves = lane_halves()
    scale = HEAD_DIM ** (-0.5)
    keep = image.inside((WINDOW, 1), 0).astype(BF16)

    @pl.loop(0, half // 128)
    def _(pair):
        @pl.when(pair == 1)
        def _():
            fsend.wait_recv()
            first_sum[...] = (first_own[...].astype(F32) + first_in[...].astype(F32)).astype(BF16)
            turn_start(0, first_sum, parts1, own1)

        @pl.when(pair == 3)
        def _():
            turn_wait(0, first_sum, parts1, own1)
            for n in range(FIRST_PARTS):
                dense1[:, n * share:(n + 1) * share] = mm(pick, parts1[:, n * share:(n + 1) * share]).astype(BF16)
            go("S0", "S1", "S2")

        def cols(part):
            return pl.ds(pl.multiple_of(part * half + pair * 128, 128), 128)

        k2 = qkv[:, cols(1)]
        v2 = qkv[:, cols(2)]
        q2 = qkv[:, cols(0)] * jnp.asarray(scale, BF16)
        do2 = image.choose(lambda at: do_s[at:at + WINDOW, cols(0)]) * keep
        inner = do2.astype(F32) * oh_ref[:, cols(0)].astype(F32)
        gv = gk = gqq = None
        for hd in range(2):
            hm = halves[hd].astype(BF16)
            weights = prob[2 * pair + hd]
            grad_p = mm_nt(do2 * hm, v2)
            row_inner = jnp.sum(inner * halves[hd], axis=1, keepdims=True)
            grad_s = (weights.astype(F32) * (grad_p - row_inner)).astype(BF16)
            dv = mm_tn(weights, do2 * hm)
            dk = mm_tn(grad_s, q2 * hm)
            dq = mm(grad_s, k2 * hm)
            gv = dv if gv is None else gv + dv
            gk = dk if gk is None else gk + dk
            gqq = dq if gqq is None else gqq + dq
        gq[:, cols(0)] = (gqq * scale).astype(BF16)
        gq[:, cols(1)] = gk.astype(BF16)
        gq[:, cols(2)] = gv.astype(BF16)

    up = compact_rows(mm_tn(c1[...], gq[...]))
    e1 = (mm_nt(gq[...], qu[...]) * image.select_window(0, WINDOW)).astype(BF16)
    for part in range(3):
        last_own[:, pl.ds(pl.multiple_of(part * width + s * half, 128), half)] = up[:, part * half:(part + 1) * half]
    last_own[:, 3 * width:4 * width] = compact_rows(mm_tn(e1, n1[...]))
    lsend = to_partner(last_own, last_in, fs_sem.at[1], fr_sem.at[1])
    lsend.start()

    @pl.loop(0, 2)
    def _(i):
        at = pl.ds(pl.multiple_of(i * QROWS, QROWS), QROWS)
        e1_rows = (mm_nt(gq[at, :], qu[...]) * image.select_window(i * QROWS, QROWS)).astype(BF16)
        gpad[pl.ds(pl.multiple_of(PAD + i * QROWS, STEP), QROWS), :] = mm_nt(gq[at, :], wq[...]) + mm_nt(e1_rows, qd_ref[...])

    def rows_of(who, i):
        return image.choose(lambda at: gpad[pl.ds(pl.multiple_of(who * rows + PAD + i * chunk - at, STEP), chunk), :])

    psends = []
    for i in range(2):
        psend[i] = rows_of(other, i).astype(BF16)
        copy = to_partner(psend.at[i], prcv.at[i], ps_sem.at[i], pr_sem.at[i])
        copy.start()
        psends.append(copy)
    go("A0")
    lsend.wait_recv()
    last_sum[...] = (last_own[...].astype(F32) + last_in[...].astype(F32)).astype(BF16)
    turn_start(1, last_sum, parts2, own2)
    go("A1", "B0", "A2", "B1")
    turn_wait(1, last_sum, parts2, own2)
    dense2[...] = mm(pick, parts2[...]).astype(BF16)
    go("S3", "B2", "C0", "C1", "A3", "C2", "B3")
    outs = []
    for i in range(2):
        psends[i].wait_recv()
        rows_at = pl.ds(i * chunk, chunk)
        gn[rows_at, :] = prcv[i].astype(F32) + rows_of(s, i)
        copy = pltpu.make_async_copy(gn.at[rows_at, :], gn_out.at[rows_at, :], out_sem.at[i])
        copy.start()
        outs.append(copy)
    go("C3")
    for copy in outs:
        copy.wait()
    for copy in dsend + [fsend, lsend] + psends:
        copy.wait_send()
    turn_finish(0, first_sum, parts1, own1)
    turn_finish(1, last_sum, parts2, own2)
    for it in items:
        gather.finish(it)


def run_backward(seg, ident, vec, gm, att, c2, oh, pd, pu, qd, gf, wp, wq, qkv, n1, c1, prob, qu):
    rows, width = gm.shape
    toks = 2 * rows
    half = width // 2
    dma = pltpu.SemaphoreType.DMA
    sds = jax.ShapeDtypeStruct
    n_first = gf.shape[1] + 2 * width
    out_shape = (sds((128, n_first + 4 * width), BF16), sds((rows, width), F32))
    chunk = rows // 2

    def low(*shape):
        return pltpu.VMEM(shape, BF16)

    scratch = [
        low(*wq.shape), low(*qkv.shape), low(*n1.shape), low(*c1.shape), low(*prob.shape), low(128, 3 * half), low(rows, width),
        pltpu.VMEM((rows, 128), F32), low(2, chunk, half), low(toks, half), low(16, n_first), low(16, n_first),
        low(16, 4 * width), low(16, 4 * width), low(16, n_first), low(16, 4 * width), low(256, n_first // 16),
        low(256, width // 4), low(128, n_first // 16), low(128, width // 4), low(WINDOW, 3 * half),
        pltpu.VMEM((2 * PAD + WINDOW, width), F32), low(2, chunk, width), low(2, chunk, width), pltpu.VMEM((rows, width), F32),
        dma((8,)), dma((2,)), dma((2,)), dma((2,)), dma((2,)), dma((2,)), dma((2,)), dma((2,)), dma((2, 16)), dma((2, 16)),
        dma((FIRST_PARTS + 1, 22)), dma((FIRST_PARTS + 1, 16)), dma((FIRST_PARTS + 1,))]
    return pl.pallas_call(
        backward_kernel, out_shape=out_shape, in_specs=[vmem_spec()] * 12 + [any_spec()] * 6,
        out_specs=tuple(any_spec() for unused in out_shape), scratch_shapes=scratch,
        compiler_params=pltpu.CompilerParams(collective_id=2, has_side_effects=True, vmem_limit_bytes=VMEM_LIMIT),
        name="backward")(seg, ident, vec, gm, att, c2, oh, pd, pu, qd, gf, wp, wq, qkv, n1, c1, prob, qu)


def expand_kernel(vec_ref, f1u, f2d, f1d, f2u, pu, pdn, qu, qd, gn, x, gm,
                  gt_out, qd_out, qu_out, pd_out, pu_out, f1d_out, f1u_out, f2d_out, f2u_out):
    for src, dst in ((f1u, f1u_out), (f2u, f2u_out), (pu, pu_out), (qu, qu_out)):
        dst[...] = src[...].astype(F32)
    for src, dst in ((f1d, f1d_out), (f2d, f2d_out), (pdn, pd_out), (qd, qd_out)):
        dst[...] = src[...].astype(F32).T
    gain1 = full_vector(vec_ref, 0)
    gt_out[...] = gm[...] + norm_grad(x[...].astype(F32), gain1, gn[...])


def run_expand(vec, gall, gn, x, gm):
    rows, width = gn.shape
    ff = 4 * width
    n = 4
    sds = jax.ShapeDtypeStruct

    def part(cols, offset):
        return pl.BlockSpec((128, cols), lambda j: (0, offset // cols + j))

    def by_row(shape):
        return pl.BlockSpec(shape, lambda j: (j, 0))

    def by_col(shape):
        return pl.BlockSpec(shape, lambda j: (0, j))

    q = width // n
    return pl.pallas_call(
        expand_kernel, grid=(n,),
        out_shape=(sds((rows, width), F32), sds((width, 128), F32), sds((128, 3 * width), F32), sds((width, 128), F32),
                   sds((128, width), F32), sds((width, 128), F32), sds((128, ff), F32), sds((ff, 128), F32), sds((128, width), F32)),
        in_specs=[pl.BlockSpec((256, 128), lambda j: (0, 0)), part(ff // n, 0), part(ff // n, ff), part(q, 2 * ff),
                  part(q, 2 * ff + width), part(q, 2 * ff + 2 * width), part(q, 2 * ff + 3 * width),
                  part(3 * q, 2 * ff + 4 * width), part(q, 2 * ff + 7 * width),
                  by_row((rows // n, width)), by_row((rows // n, width)), by_row((rows // n, width))],
        out_specs=(by_row((rows // n, width)), by_row((q, 128)), by_col((128, 3 * q)), by_row((q, 128)), by_col((128, q)),
                   by_row((q, 128)), by_col((128, ff // n)), by_row((ff // n, 128)), by_col((128, q))),
        compiler_params=pltpu.CompilerParams(vmem_limit_bytes=VMEM_LIMIT),
        name="expand")(vec, *([gall] * 8), gn, x, gm)


def per_device_fast(tokens, grad_out, segments, padding, adapter_ids, norm1_gain, norm1_bias, w_qkv, w_proj, proj_bias,
                    norm2_gain, norm2_bias, w_fc1, fc1_bias, w_fc2, fc2_bias, qkv_down, qkv_up, proj_down, proj_up,
                    fc1_down, fc1_up, fc2_down, fc2_up):
    x = tokens[0]
    odd = (lax.axis_index("fsdp") % 2).astype(F32)
    six = jnp.stack([norm1_gain, norm1_bias, proj_bias, norm2_gain, norm2_bias, fc2_bias]).astype(F32)
    vec = jnp.concatenate([
        jnp.concatenate([six * (1.0 - odd), six * odd], axis=1), fc1_bias.astype(F32).reshape(2, 128),
        jnp.broadcast_to(adapter_ids[0].astype(F32)[:, None], (1, 128)), jnp.zeros((7, 128), F32)], axis=0)
    (wq, wp, vecf, qkv, n1, c1, prob, oh, att, c2, gm, gf, out) = run_forward(
        segments, adapter_ids, x, vec, qkv_down, proj_down, proj_up, w_qkv, w_proj, w_fc1, w_fc2, qkv_up,
        grad_out[0], fc1_up, fc1_down, fc2_up, fc2_down)
    gall, gn = run_backward(segments, adapter_ids, vecf, gm, att, c2, oh, proj_down, proj_up, qkv_down, gf, wp, wq, qkv, n1, c1, prob, qkv_up)
    gt, gqd, gqu, gpd, gpu, gf1d, gf1u, gf2d, gf2u = run_expand(vecf, gall, gn, x, gm)
    return out[None], gt[None], gqd, gqu, gpd, gpu, gf1d, gf1u, gf2d, gf2u


def solution(mesh):
    sizes = dict(mesh.shape)
    small = sizes == {"seq": 2, "fsdp": 16}

    def per_device_any(*args):
        tokens, adapter_ids = args[0], args[4]
        one_image = tokens.shape[1:] == (512, 1024) and adapter_ids.shape[1] == 1
        return (per_device_fast if small and one_image else per_device)(*args)

    return jax.shard_map(
        per_device_any,
        mesh=mesh,
        in_specs=(
            P("fsdp", "seq", None),
            P("fsdp", "seq", None),
            P("fsdp", None),
            P("fsdp", None),
            P("fsdp", None),
            P("fsdp"),
            P("fsdp"),
            P("fsdp", None),
            P("fsdp", None),
            P("fsdp"),
            P("fsdp"),
            P("fsdp"),
            P("fsdp", None),
            P("fsdp"),
            P("fsdp", None),
            P("fsdp"),
            P(),
            P(),
            P(),
            P(),
            P(),
            P(),
            P(),
            P(),
        ),
        out_specs=(
            P("fsdp", "seq", None),
            P("fsdp", "seq", None),
            P(),
            P(),
            P(),
            P(),
            P(),
            P(),
            P(),
            P(),
        ),
        check_vma=False,
    )
```

```python
from functools import partial

import jax
import jax.numpy as jnp
from jax import lax
from jax.experimental import pallas as pl
from jax.experimental.pallas import tpu as pltpu
from jax.sharding import PartitionSpec as P

HEAD_DIM = 64
IMG = 577
RANK = 16
QBLOCK = 512


norm_eps = 1e-06
masked_score = -1e30


def matmul(left_side, right_side):
    return jnp.dot(left_side, right_side, preferred_element_type=jnp.float32)


def matmul_nt(left_side, right_side):
    return jnp.einsum("tk,jk->tj", left_side, right_side, preferred_element_type=jnp.float32)


def matmul_tn(left_side, right_side):
    return jnp.einsum("ti,to->io", left_side, right_side, preferred_element_type=jnp.float32)


def layer_norm(values, norm_gain, norm_shift):
    centre = jnp.mean(values, axis=-1, keepdims=True)
    centred = values - centre
    spread = jnp.mean(centred * centred, axis=-1, keepdims=True)
    return centred * lax.rsqrt(spread + norm_eps) * norm_gain + norm_shift


def norm_backward(values, norm_gain, norm_shift, grad_in):

    def apply_norm(inputs):
        return layer_norm(inputs, norm_gain, norm_shift)

    unused, pullback = jax.vjp(apply_norm, values)
    return pullback(grad_in)[0]


def selection(seg_own, image_adapters, columns):
    images = jnp.arange(image_adapters.shape[0], dtype=jnp.int32)
    image_match = seg_own[:, None] - 1 == images[None, :]
    token_adapter = jnp.sum(jnp.where(image_match, image_adapters[None, :], 0), axis=1)
    present = jnp.any(image_match, axis=1)
    column = jnp.arange(columns, dtype=jnp.int32) // RANK
    chosen = (token_adapter[:, None] == column[None, :]) & present[:, None]
    return chosen.astype(jnp.float32)


def adapter_forward(inputs_b, weight, down_map, up_map, select):
    inner_term = (matmul(inputs_b, down_map) * select).astype(jnp.bfloat16)
    return (matmul(inputs_b, weight) + matmul(inner_term, up_map), inner_term)


def adapter_backward(inputs_b, inner_term, grad_in, weight, down_map, up_map, select):
    grad_up = matmul_tn(inner_term, grad_in)
    grad_inner = (matmul_nt(grad_in, up_map) * select).astype(jnp.bfloat16)
    grad_down = matmul_tn(inputs_b, grad_inner)
    grad_inputs = matmul_nt(grad_in, weight) + matmul_nt(grad_inner, down_map)
    return (grad_inputs, grad_down, grad_up)


def block_scores(query_block, key_heads, seg_block, seg_keys, keep_keys):
    score_scale = HEAD_DIM ** (-0.5)
    scores = (
        jnp.einsum("qhd,khd->hqk", query_block, key_heads, preferred_element_type=jnp.float32)
        * score_scale
    )
    allowed = (seg_block[:, None] == seg_keys[None, :]) & (keep_keys[None, :] == 1)
    return jnp.where(allowed[None, :, :], scores, masked_score)


def split_heads(head_rows):
    all_rows = head_rows.shape[0]
    local_heads = head_rows.shape[2] // HEAD_DIM
    query_heads = head_rows[:, 0].reshape(all_rows, local_heads, HEAD_DIM)
    key_heads = head_rows[:, 1].reshape(all_rows, local_heads, HEAD_DIM)
    value_heads = head_rows[:, 2].reshape(all_rows, local_heads, HEAD_DIM)
    return (query_heads, key_heads, value_heads)


def key_window(all_rows):
    return min(all_rows, (QBLOCK + 2 * IMG - 2 + 127) // 128 * 128)


def window_start(block_index, all_rows, window):
    first = block_index * QBLOCK - (IMG - 1)
    return jnp.clip(first, 0, all_rows - window)


def attention_forward(head_rows, seg_all, keep_all):
    all_rows = head_rows.shape[0]
    block_count = all_rows // QBLOCK
    window = key_window(all_rows)
    query_heads, key_heads, value_heads = split_heads(head_rows)
    local_heads = query_heads.shape[1]

    def one_block(block_parts):
        query_block, seg_block, keep_block, block_index = block_parts
        start = window_start(block_index, all_rows, window)
        keys_near = lax.dynamic_slice_in_dim(key_heads, start, window, 0)
        values_near = lax.dynamic_slice_in_dim(value_heads, start, window, 0)
        seg_near = lax.dynamic_slice_in_dim(seg_all, start, window, 0)
        keep_near = lax.dynamic_slice_in_dim(keep_all, start, window, 0)
        scores = block_scores(query_block, keys_near, seg_block, seg_near, keep_near)
        row_max = jnp.max(scores, axis=2, keepdims=True)
        weights = jnp.exp(scores - row_max)
        row_sum = jnp.sum(weights, axis=2, keepdims=True)
        probs_low = (weights / row_sum).astype(jnp.bfloat16)
        result = jnp.einsum(
            "hqk,khd->qhd", probs_low, values_near, preferred_element_type=jnp.float32
        )
        result = result * keep_block[:, None, None].astype(jnp.float32)
        return (result.astype(jnp.bfloat16), row_max, row_sum)

    block_ids = jnp.arange(block_count, dtype=jnp.int32)
    blocked = (
        query_heads.reshape(block_count, QBLOCK, local_heads, HEAD_DIM),
        seg_all.reshape(block_count, QBLOCK),
        keep_all.reshape(block_count, QBLOCK),
        block_ids,
    )
    results, block_max, block_sums = lax.map(one_block, blocked)
    return (results.reshape(all_rows, local_heads * HEAD_DIM), block_max, block_sums)


def attention_backward(head_rows, grad_rows, seg_all, keep_all, block_max, block_sums):
    all_rows = head_rows.shape[0]
    block_count = all_rows // QBLOCK
    window = key_window(all_rows)
    query_heads, key_heads, value_heads = split_heads(head_rows)
    local_heads = query_heads.shape[1]
    score_scale = HEAD_DIM ** (-0.5)

    def one_block(running, block_parts):
        grad_keys, grad_values = running
        query_block, seg_block, keep_block, grad_block, row_max, row_sum, block_index = block_parts
        start = window_start(block_index, all_rows, window)
        keys_near = lax.dynamic_slice_in_dim(key_heads, start, window, 0)
        values_near = lax.dynamic_slice_in_dim(value_heads, start, window, 0)
        seg_near = lax.dynamic_slice_in_dim(seg_all, start, window, 0)
        keep_near = lax.dynamic_slice_in_dim(keep_all, start, window, 0)
        scores = block_scores(query_block, keys_near, seg_block, seg_near, keep_near)
        probs = jnp.exp(scores - row_max) / row_sum
        grad_result = grad_block * keep_block[:, None, None].astype(jnp.bfloat16)
        values_term = jnp.einsum(
            "hqk,qhd->khd",
            probs.astype(jnp.bfloat16),
            grad_result,
            preferred_element_type=jnp.float32,
        )
        grad_probs = jnp.einsum(
            "qhd,khd->hqk", grad_result, values_near, preferred_element_type=jnp.float32
        )
        row_inner = jnp.sum(probs * grad_probs, axis=2, keepdims=True)
        grad_scores = (probs * (grad_probs - row_inner)).astype(jnp.bfloat16)
        grad_query = (
            jnp.einsum("hqk,khd->qhd", grad_scores, keys_near, preferred_element_type=jnp.float32)
            * score_scale
        )
        keys_term = (
            jnp.einsum("hqk,qhd->khd", grad_scores, query_block, preferred_element_type=jnp.float32)
            * score_scale
        )
        grad_keys = lax.dynamic_update_slice_in_dim(
            grad_keys, lax.dynamic_slice_in_dim(grad_keys, start, window, 0) + keys_term, start, 0
        )
        grad_values = lax.dynamic_update_slice_in_dim(
            grad_values,
            lax.dynamic_slice_in_dim(grad_values, start, window, 0) + values_term,
            start,
            0,
        )
        return ((grad_keys, grad_values), grad_query)

    zero_heads = jnp.zeros((all_rows, local_heads, HEAD_DIM), jnp.float32)
    block_ids = jnp.arange(block_count, dtype=jnp.int32)
    blocked = (
        query_heads.reshape(block_count, QBLOCK, local_heads, HEAD_DIM),
        seg_all.reshape(block_count, QBLOCK),
        keep_all.reshape(block_count, QBLOCK),
        grad_rows.reshape(block_count, QBLOCK, local_heads, HEAD_DIM),
        block_max,
        block_sums,
        block_ids,
    )
    (grad_keys, grad_values), grad_queries = lax.scan(one_block, (zero_heads, zero_heads), blocked)
    flat_width = local_heads * HEAD_DIM
    stacked = jnp.stack(
        [
            grad_queries.reshape(all_rows, flat_width),
            grad_keys.reshape(all_rows, flat_width),
            grad_values.reshape(all_rows, flat_width),
        ],
        axis=1,
    )
    return stacked.astype(jnp.bfloat16)


def per_device(
    tokens,
    grad_out,
    segments,
    padding,
    adapter_ids,
    norm1_gain,
    norm1_bias,
    w_qkv,
    w_proj,
    proj_bias,
    norm2_gain,
    norm2_bias,
    w_fc1,
    fc1_bias,
    w_fc2,
    fc2_bias,
    qkv_down,
    qkv_up,
    proj_down,
    proj_up,
    fc1_down,
    fc1_up,
    fc2_down,
    fc2_up,
):
    tok_rows = tokens.shape[1]
    feat_width = tokens.shape[2]
    inputs = tokens[0].astype(jnp.float32)
    seg_all = segments[0]
    keep_all = padding[0]
    offset = lax.axis_index("seq") * tok_rows
    seg_own = lax.dynamic_slice_in_dim(seg_all, offset, tok_rows)
    select = selection(seg_own, adapter_ids[0], qkv_down.shape[1])
    gain_one, shift_one, qkv_weight, proj_weight, proj_shift = (
        lax.all_gather(norm1_gain, "fsdp", axis=0, tiled=True),
        lax.all_gather(norm1_bias, "fsdp", axis=0, tiled=True),
        lax.all_gather(w_qkv, "fsdp", axis=0, tiled=True),
        lax.all_gather(w_proj, "fsdp", axis=0, tiled=True),
        lax.all_gather(proj_bias, "fsdp", axis=0, tiled=True),
    )
    gain_one = gain_one.astype(jnp.float32)
    shift_one = shift_one.astype(jnp.float32)
    normed_one = layer_norm(inputs, gain_one, shift_one).astype(jnp.bfloat16)
    qkv_main, inner_one = adapter_forward(normed_one, qkv_weight, qkv_down, qkv_up, select)
    qkv_low = qkv_main.astype(jnp.bfloat16).reshape(tok_rows, 3, feat_width)
    head_rows = lax.all_to_all(qkv_low, "seq", split_axis=2, concat_axis=0, tiled=True)
    attended_heads, block_max, block_sums = attention_forward(head_rows, seg_all, keep_all)
    attended = lax.all_to_all(attended_heads, "seq", split_axis=0, concat_axis=1, tiled=True)
    branch_one, inner_two = adapter_forward(attended, proj_weight, proj_down, proj_up, select)
    middle = inputs + (branch_one + proj_shift.astype(jnp.float32))
    gain_two, shift_two, fc1_weight, fc2_shift, fc2_weight, fc1_shift = (
        lax.all_gather(norm2_gain, "fsdp", axis=0, tiled=True),
        lax.all_gather(norm2_bias, "fsdp", axis=0, tiled=True),
        lax.all_gather(w_fc1, "fsdp", axis=0, tiled=True),
        lax.all_gather(fc2_bias, "fsdp", axis=0, tiled=True),
        lax.all_gather(w_fc2, "fsdp", axis=0, tiled=True),
        lax.all_gather(fc1_bias, "fsdp", axis=0, tiled=True),
    )
    gain_two = gain_two.astype(jnp.float32)
    shift_two = shift_two.astype(jnp.float32)
    normed_two = layer_norm(middle, gain_two, shift_two).astype(jnp.bfloat16)
    hidden_main, inner_three = adapter_forward(normed_two, fc1_weight, fc1_down, fc1_up, select)
    hidden = hidden_main + fc1_shift.astype(jnp.float32)
    active = jax.nn.gelu(hidden, approximate=False).astype(jnp.bfloat16)
    branch_two, inner_four = adapter_forward(active, fc2_weight, fc2_down, fc2_up, select)
    output = (middle + (branch_two + fc2_shift.astype(jnp.float32))).astype(jnp.bfloat16)
    fc1_back, fc2_back = (
        lax.all_gather(w_fc1, "fsdp", axis=0, tiled=True),
        lax.all_gather(w_fc2, "fsdp", axis=0, tiled=True),
    )
    grad_top = grad_out[0]
    grad_active, grad_fc2_down, grad_fc2_up = adapter_backward(
        active, inner_four, grad_top, fc2_back, fc2_down, fc2_up, select
    )
    unused, gelu_back = jax.vjp(partial(jax.nn.gelu, approximate=False), hidden)
    grad_hidden = gelu_back(grad_active)[0].astype(jnp.bfloat16)
    grad_normed_two, grad_fc1_down, grad_fc1_up = adapter_backward(
        normed_two, inner_three, grad_hidden, fc1_back, fc1_down, fc1_up, select
    )
    grad_middle = grad_top.astype(jnp.float32) + norm_backward(
        middle, gain_two, shift_two, grad_normed_two
    )
    qkv_back, proj_back = (
        lax.all_gather(w_qkv, "fsdp", axis=0, tiled=True),
        lax.all_gather(w_proj, "fsdp", axis=0, tiled=True),
    )
    grad_branch_one = grad_middle.astype(jnp.bfloat16)
    grad_attended, grad_proj_down, grad_proj_up = adapter_backward(
        attended, inner_two, grad_branch_one, proj_back, proj_down, proj_up, select
    )
    grad_head_rows = lax.all_to_all(
        grad_attended.astype(jnp.bfloat16), "seq", split_axis=1, concat_axis=0, tiled=True
    )
    grad_qkv_heads = attention_backward(
        head_rows, grad_head_rows, seg_all, keep_all, block_max, block_sums
    )
    grad_qkv = lax.all_to_all(
        grad_qkv_heads, "seq", split_axis=0, concat_axis=2, tiled=True
    ).reshape(tok_rows, 3 * feat_width)
    grad_normed_one, grad_qkv_down, grad_qkv_up = adapter_backward(
        normed_one, inner_one, grad_qkv, qkv_back, qkv_down, qkv_up, select
    )
    grad_tokens = grad_middle + norm_backward(inputs, gain_one, shift_one, grad_normed_one)
    summed = lax.psum(
        (
            grad_qkv_down,
            grad_qkv_up,
            grad_proj_down,
            grad_proj_up,
            grad_fc1_down,
            grad_fc1_up,
            grad_fc2_down,
            grad_fc2_up,
        ),
        ("seq", "fsdp"),
    )
    return (
        output[None],
        grad_tokens[None],
        summed[0],
        summed[1],
        summed[2],
        summed[3],
        summed[4],
        summed[5],
        summed[6],
        summed[7],
    )


F32 = jnp.float32
BF16 = jnp.bfloat16
MESH = pl.DeviceIdType.MESH
VMEM_LIMIT = 67_000_000


def mm(a, b):
    return lax.dot_general(a, b, (((1,), (0,)), ((), ())), preferred_element_type=F32)


def mm_nt(a, b):
    return lax.dot_general(a, b, (((1,), (1,)), ((), ())), preferred_element_type=F32)


def mm_tn(a, b):
    return lax.dot_general(a, b, (((0,), (0,)), ((), ())), preferred_element_type=F32)


def norm_parts(v):
    mean = jnp.mean(v, axis=-1, keepdims=True)
    centred = v - mean
    r = lax.rsqrt(jnp.mean(centred * centred, axis=-1, keepdims=True) + norm_eps)
    return centred * r, r


def norm_grad(v, gain, grad_y):
    h, r = norm_parts(v)
    d = grad_y * gain
    return r * (d - jnp.mean(d, axis=-1, keepdims=True) - h * jnp.mean(d * h, axis=-1, keepdims=True))


class Net:
    def __init__(self):
        self.s = lax.axis_index("seq")
        self.f = lax.axis_index("fsdp")
        self.z = self.f // 4
        self.x = (self.f // 2) % 2
        self.c = self.f % 2
        self.partner = {"seq": 1 - self.s}
        self.x_peer = {"fsdp": self.block(self.z, 1 - self.x, self.c)}
        self.c_peer = {"fsdp": self.block(self.z, self.x, 1 - self.c)}

    def block(self, z, x, c):
        return (z * 2 + x) * 2 + c

    def z_peer(self, d):
        return {"fsdp": self.block((self.z + d) % 4, self.x, self.c)}

    def meet(self, peers):
        sem = pltpu.get_barrier_semaphore()
        for peer in peers:
            pl.semaphore_signal(sem, inc=1, device_id=peer, device_id_type=MESH)
        pl.semaphore_wait(sem, len(peers))

    def plane_peer(self, d):
        return {"fsdp": (self.f + d) % 16}

    def plane_barrier(self):
        self.meet([self.partner] + [self.plane_peer(d) for d in range(1, 16)])

    def barrier(self):
        self.meet([self.partner, self.x_peer, self.c_peer] + [self.z_peer(d) for d in (1, 2, 3)])


class Block:
    def __init__(self, src, piece, some, sems, own_sem, plane=2):
        self.src, self.piece, self.some, self.plane, self.own_sem = src, piece, some, plane, own_sem
        self.sent, self.z, self.x, self.y1, self.y2, self.c = sems


N_SEMS = 6


class Gather:
    def __init__(self, net):
        self.net = net

    def send(self, it, src, block, sem, peer):
        pltpu.make_async_remote_copy(
            src_ref=src, dst_ref=it.piece(block), send_sem=it.sent, recv_sem=sem, device_id=peer,
            device_id_type=MESH).start()

    def total(self, it, n, sem):
        return pltpu.make_async_remote_copy(
            src_ref=it.some(n), dst_ref=it.some(n), send_sem=it.sent, recv_sem=sem, device_id=self.net.c_peer,
            device_id_type=MESH)

    def here(self, it, body):
        if isinstance(it.plane, int) and it.plane == 2:
            body()
        else:
            pl.when((self.net.s == it.plane) | (it.plane == 2))(body)

    def hand_on(self, it, pieces, sem):
        def body():
            for piece, block in pieces:
                self.send(it, piece, block, sem, self.net.partner)

        if not isinstance(it.plane, int):
            pl.when(it.plane != 2)(body)
        elif it.plane != 2:
            body()

    def own(self, it):
        return pltpu.make_async_copy(it.src, it.piece(self.net.f), it.own_sem)

    def column(self, it, x, ds):
        net = self.net
        blocks = [net.block((net.z + d) % 4, x, net.c) for d in ds]
        return [(it.piece(block), block) for block in blocks]

    def start(self, it):
        net = self.net

        def along():
            for d in (2, 1, 3):
                self.send(it, it.src, net.f, it.z, net.z_peer(d))
            self.send(it, it.src, net.f, it.x, net.x_peer)

        self.here(it, along)
        self.send(it, it.src, net.f, it.c, net.c_peer)
        self.own(it).start()

    def from_z(self, it):
        net = self.net

        def body():
            self.total(it, 3, it.z).wait_recv()
            pieces = self.column(it, net.x, (1, 3, 2))
            for piece, block in pieces:
                self.send(it, piece, block, it.x, net.x_peer)
            self.hand_on(it, pieces, it.y1)
            for piece, block in pieces:
                self.send(it, piece, block, it.c, net.c_peer)

        self.here(it, body)

    def from_x(self, it):
        net = self.net

        def body():
            self.total(it, 4, it.x).wait_recv()
            pieces = self.column(it, 1 - net.x, (0, 1, 3, 2))
            self.hand_on(it, pieces, it.y2)
            for piece, block in pieces:
                self.send(it, piece, block, it.c, net.c_peer)

        self.here(it, body)

    def from_seq(self, it):
        net = self.net
        if isinstance(it.plane, int) and it.plane == 2:
            return

        @pl.when((net.s != it.plane) & (it.plane != 2))
        def _():
            self.total(it, 3, it.y1).wait_recv()
            for piece, block in self.column(it, net.x, (1, 3, 2)):
                self.send(it, piece, block, it.c, net.c_peer)
            self.total(it, 4, it.y2).wait_recv()
            for piece, block in self.column(it, 1 - net.x, (0, 1, 3, 2)):
                self.send(it, piece, block, it.c, net.c_peer)

    def from_core(self, it):
        self.total(it, 8, it.c).wait_recv()
        self.own(it).wait()

    def finish(self, it):
        net = self.net
        if isinstance(it.plane, int) and it.plane == 2:
            self.total(it, 15, it.z).wait_send()
            return

        @pl.when(it.plane == 2)
        def _():
            self.total(it, 15, it.z).wait_send()

        @pl.when(net.s == it.plane)
        def _():
            self.total(it, 22, it.z).wait_send()

        @pl.when((net.s != it.plane) & (it.plane != 2))
        def _():
            self.total(it, 8, it.z).wait_send()


def full_vector(vec_ref, row, blocks=16, rows=16):
    parts = []
    for k in range(blocks // 2):
        even = vec_ref[2 * k * rows + row:2 * k * rows + row + 1, :]
        odd = vec_ref[(2 * k + 1) * rows + row:(2 * k + 1) * rows + row + 1, :]
        parts.append(even + odd)
    return jnp.concatenate(parts, axis=1)


WINDOW = 640
STEP = 64
PAD = 384
QROWS = 320
FFB = 512


class Image:
    def __init__(self, seg_ref, id_ref):
        self.start = jnp.sum((seg_ref[...] == 0).astype(F32), axis=1, keepdims=True)
        ident = id_ref[...].astype(F32)
        self.pick = []
        base = jnp.zeros((1, 1), F32)
        for k in range(PAD // STEP + 1):
            mark = ((self.start >= k * STEP) & (self.start < (k + 1) * STEP)).astype(F32)
            self.pick.append(mark)
            base = base + mark * float(k * STEP)
        self.shift = base - self.start
        lane = lax.broadcasted_iota(jnp.int32, (1, 128), 1).astype(F32)
        self.columns = ((lane >= ident * RANK) & (lane < (ident + 1) * RANK)).astype(F32)

    def choose(self, load):
        total = None
        for k, mark in enumerate(self.pick):
            value = load(k * STEP)
            value = value * mark.astype(value.dtype)
            total = value if total is None else total + value
        return total

    def inside(self, shape, axis, first=0):
        at = (lax.broadcasted_iota(jnp.int32, shape, axis) + first).astype(F32) + self.shift
        return (at >= 0) & (at < IMG)

    def select(self, first, rows):
        at = (lax.broadcasted_iota(jnp.int32, (rows, 1), 0) + first).astype(F32)
        return (at >= self.start).astype(F32) * self.columns

    def select_window(self, first, rows):
        at = (lax.broadcasted_iota(jnp.int32, (rows, 1), 0) + first).astype(F32) + self.shift
        return (at >= 0).astype(F32) * self.columns


def lane_halves():
    lane = lax.broadcasted_iota(jnp.int32, (1, 128), 1)
    return [(lane < 64).astype(F32), (lane >= 64).astype(F32)]


def compact_rows(dense):
    total = dense[0:16]
    for k in range(1, 8):
        total = total + dense[16 * k:16 * (k + 1)]
    return total.astype(BF16)


N_FC1 = 8
N_FC2 = 4
FIRST = 6
PLANES = (2, 2, 0, 1, 2, 2, 2, 2)
N_ITEMS = FIRST + N_FC2 + N_FC1


def block_kernel(seg_ref, id_ref, x_ref, vec_ref, qd_ref, pd_ref, pu_ref, wq_hbm, wp_hbm, w1_hbm, w2_hbm,
                 qu_hbm, g_hbm, u1_hbm, d1_hbm, u2_hbm, d2_hbm,
                 vecf_out, prob_out, gm_out, out_out, gall, gn_out,
                 wq_own, wq, wp, w1, w2, xp, vecf, qu, g, u1, d1, u2, d2, qkv, n1, c1, qkvw, n1w, c1w, prob, opad, sendb,
                 oh, att, c2, mid, n2, oacc, gacc, u4, e3, c3, e4, c3t, e4t, act_s, gh_s, gr,
                 do_s, gr_in, gr_sum, last_own, last_in, last_sum, parts0, parts1, parts2, dense0, dense1, dense2, prcv,
                 xs_sem, xr_sem, as_sem, ar_sem, loc_sem, out_sem, prob_sem, g_sem, g_own,
                 ds_sem, dr_sem, fs_sem, fr_sem, ps_sem, pr_sem, t_send, t_recv):
    net = Net()
    s, other = net.s, 1 - net.s
    rows, width = x_ref.shape
    half = wq.shape[1] // 3
    rb = wq_own.shape[0]
    fr1 = w1_hbm.shape[0]
    fr2 = w2_hbm.shape[0]
    ff = w1.shape[1]
    chunk = rows // 2

    pre = []
    for part in range(3):
        cols = pl.ds(pl.multiple_of(part * width + s * half, 128), half)
        pre.append(pltpu.make_async_copy(wq_hbm.at[:, cols], wq_own.at[:, pl.ds(part * half, half)], loc_sem.at[part]))
    late = []
    for part in range(3):
        cols = pl.ds(pl.multiple_of(part * width + s * half, 128), half)
        late.append(pltpu.make_async_copy(qu_hbm.at[:, cols], qu.at[:, pl.ds(part * half, half)], loc_sem.at[3 + part]))
    for n, (src, dst) in enumerate(((g_hbm, g), (u1_hbm, u1), (d1_hbm, d1), (u2_hbm, u2), (d2_hbm, d2))):
        late.append(pltpu.make_async_copy(src, dst, loc_sem.at[6 + n]))
    for copy in pre + late:
        copy.start()
    net.plane_barrier()

    def x_copy(i):
        part = pl.ds(i * chunk, chunk)
        return pltpu.make_async_remote_copy(
            src_ref=x_ref.at[part, :], dst_ref=xp.at[part, :], send_sem=xs_sem.at[i], recv_sem=xr_sem.at[i],
            device_id=net.partner, device_id_type=MESH)

    for i in range(2):
        x_copy(i).start()
    for copy in pre:
        copy.wait()

    def square(n):
        return w1.at[pl.ds(0, n * 64), pl.ds(0, half)] if n <= 16 else w1.at[pl.ds(0, n * 32), pl.ds(0, 2 * half)]

    def block(n, src, piece, plane=2, some=square):
        return Block(src, piece, some, [g_sem.at[k, n] for k in range(N_SEMS)], g_own.at[n], plane)

    def wq_part(part):
        cols = pl.ds(part * half, half)
        return block(1 + part, wq_own.at[:, cols], lambda b: wq.at[pl.ds(b * rb, rb), cols])

    def wp_part(part):
        cols = pl.ds(part * half, half)
        return block(4 + part, wp_hbm.at[:, cols], lambda b: wp.at[pl.ds(b * rb, rb), cols], part)

    sub = fr2 // N_FC2

    def times(j, size):
        return j * size if isinstance(j, int) else pl.multiple_of(j * size, size)

    def item(n):
        if isinstance(n, int) and n < FIRST:
            if n == 0:
                return block(0, vec_ref, lambda b: vecf.at[pl.ds(b * 16, 16), :], 2,
                             lambda n: vecf.at[pl.ds(0, n * 16), :])
            return wq_part(n - 1) if n < 4 else wp_part(n - 4)
        if isinstance(n, int):
            return fc2_it(n - FIRST) if n < FIRST + N_FC2 else fc1_it(n - FIRST - N_FC2)
        return fc1_it(n - FIRST - N_FC2)

    def fc2_it(j):
        at = pl.ds(times(j, sub), sub)
        return block(FIRST + j, w2_hbm.at[at, :], lambda b: w2.at[pl.ds(b * fr2 + times(j, sub), sub), :],
                     (0, 1, 2, 2)[j], lambda n: w2.at[pl.ds(0, n * sub), :])

    def fc1_it(j):
        cols = pl.ds(times(j, FFB), FFB)
        return block(FIRST + N_FC2 + j, w1_hbm.at[:, cols], lambda b: w1.at[pl.ds(b * fr1, fr1), cols],
                     (PLANES[j] if isinstance(j, int) else jnp.where(j // 2 == 1, j % 2, 2)))

    gather = Gather(net)
    stages = {"S": gather.start, "A": gather.from_z, "B": gather.from_x, "Y": gather.from_seq, "C": gather.from_core}

    def go(*steps):
        for step in steps:
            stages[step[0]](item(int(step[1:])))

    go("S0", "S1", "S2")
    image = Image(seg_ref, id_ref)
    zeros = jnp.zeros((PAD, 128), BF16)
    opad[0:PAD, :] = zeros
    opad[PAD + WINDOW:2 * PAD + WINDOW, :] = zeros
    go("A0", "A1", "S3", "A2", "S4", "S5", "B0", "B1", "A3", "S6", "S7", "B2", "A4", "A5", "S8")
    for copy in late:
        copy.wait()
    go("B3", "C0", "C1", "C2", "C3")

    gain1 = full_vector(vecf, 0)
    shift1 = full_vector(vecf, 1)

    def project(src, src_row, row):
        v = src[pl.ds(src_row, chunk), :].astype(F32)
        h, unused = norm_parts(v)
        normed = (h * gain1 + shift1).astype(BF16)
        at = pl.ds(row, chunk)
        n1[at, :] = normed
        inner = (mm(normed, qd_ref[...]) * image.select(row, chunk)).astype(BF16)
        c1[at, :] = inner
        for part in range(3):
            cols = pl.ds(part * half, half)
            qkv[at, cols] = (mm(normed, wq[:, cols]) + mm(inner, qu[:, cols])).astype(BF16)

    def own_rows_in(i):
        project(x_ref, i * chunk, pl.multiple_of(s * rows + i * chunk, chunk))

    def partner_rows_in(i):
        x_copy(i).wait_recv()
        project(xp, i * chunk, pl.multiple_of(other * rows + i * chunk, chunk))

    own_rows_in(0)
    own_rows_in(1)
    partner_rows_in(0)
    partner_rows_in(1)
    go("B4", "B5", "A6", "A7", "S9")
    outs = []

    def put(src, dst):
        copy = pltpu.make_async_copy(src, dst, out_sem.at[len(outs)])
        copy.start()
        outs.append(copy)

    put(vecf, vecf_out)
    for src, dst in ((qkv, qkvw), (n1, n1w), (c1, c1w)):
        step = min(src.shape[1], 512)

        @pl.loop(0, src.shape[1] // step)
        def _(n, src=src, dst=dst, step=step):
            cols = pl.ds(pl.multiple_of(n * step, step), step)
            dst[:, cols] = image.choose(lambda at: src[at:at + WINDOW, cols])
    bias = jnp.where(image.inside((1, WINDOW), 1), 0.0, masked_score).astype(F32)
    halves = lane_halves()

    def prob_copy(pair):
        slot = lax.rem(pair, 2)
        return pltpu.make_async_copy(prob.at[slot], prob_out.at[pl.ds(2 * pair, 2)], prob_sem.at[slot])

    def att_copy(pair):
        cols = pl.ds(pl.multiple_of(s * half + pair * 128, 128), 128)
        return pltpu.make_async_remote_copy(
            src_ref=sendb.at[pair], dst_ref=att.at[:, cols], send_sem=as_sem.at[pair], recv_sem=ar_sem.at[pair],
            device_id=net.partner, device_id_type=MESH)

    def to_partner(src, dst, send, recv):
        return pltpu.make_async_remote_copy(src_ref=src, dst_ref=dst, send_sem=send, recv_sem=recv,
                                            device_id=net.partner, device_id_type=MESH)

    pairs = half // 128

    @pl.loop(0, pairs)
    def _(pair):
        def cols(part):
            return pl.ds(pl.multiple_of(part * half + pair * 128, 128), 128)

        for n, steps in enumerate(((), ("Y4", "Y5"), ("B6", "B7", "A8", "S10", "S11"), ("C4", "C5"))):
            @pl.when(pair == n)
            def _(steps=steps):
                go(*steps)

        k2 = qkvw[:, cols(1)]
        v2 = qkvw[:, cols(2)]
        vs = [(v2 * hm.astype(BF16)) for hm in halves]
        slot = lax.rem(pair, 2)

        @pl.when(pair >= 2)
        def _():
            prob_copy(pair).wait()

        @pl.loop(0, WINDOW // QROWS)
        def _(b):
            r0 = pl.multiple_of(b * QROWS, QROWS)
            q2 = qkvw[pl.ds(r0, QROWS), cols(0)]
            q2 = q2 * jnp.asarray(HEAD_DIM ** (-0.5), BF16)
            total = None
            for hd in range(2):
                scores = mm_nt(q2 * halves[hd].astype(BF16), k2) + bias
                weights = jnp.exp(scores - jnp.max(scores, axis=1, keepdims=True))
                weights = (weights * (1.0 / jnp.sum(weights, axis=1, keepdims=True))).astype(BF16)
                prob[slot, hd, pl.ds(r0, QROWS), :] = weights
                part = mm(weights, vs[hd])
                total = part if total is None else total + part
            total = (total * image.inside((QROWS, 1), 0, r0).astype(F32)).astype(BF16)
            opad[pl.ds(PAD + r0, QROWS), :] = total
            oh[pl.ds(r0, QROWS), cols(0)] = total

        prob_copy(pair).start()

        def own_rows(who):
            return image.choose(lambda at: opad[pl.ds(pl.multiple_of(who * rows + PAD - at, STEP), rows), :])

        sendb[pair] = own_rows(other)
        att_copy(pair).start()
        att[:, pl.ds(pl.multiple_of(s * half + pair * 128, 128), 128)] = own_rows(s)

    go("B8", "A9", "S12", "S13", "Y6", "Y7")

    @pl.loop(0, pairs)
    def _(pair):
        att_copy(pair).wait_recv()

    go("A10", "S14")
    bias_p = full_vector(vecf, 2)
    gain2 = full_vector(vecf, 3)
    shift2 = full_vector(vecf, 4)

    @pl.loop(0, 2)
    def _(i):
        at = pl.ds(pl.multiple_of(i * chunk, chunk), chunk)
        rows_in = att[at, :]
        own_select = image.select(s * rows + i * chunk, chunk)
        inner = (mm(rows_in, pd_ref[...]) * own_select).astype(BF16)
        c2[at, :] = inner
        branch = mm(rows_in, wp[...]) + mm(inner, pu_ref[...]) + bias_p
        middle = x_ref[at, :].astype(F32) + branch
        mid[at, :] = middle
        h, unused = norm_parts(middle)
        normed = (h * gain2 + shift2).astype(BF16)
        n2[at, :] = normed
        c = mm(normed, d1[...]) * own_select
        e = mm_nt(g[at, :], u2[...]) * own_select
        c3[at, :] = c.astype(BF16)
        e4[at, :] = e.astype(BF16)
        oacc[at, :] = jnp.zeros((chunk, width), F32)
        gacc[at, :] = jnp.zeros((chunk, width), F32)
        u4[at, :] = jnp.zeros((chunk, 128), F32)
        e3[at, :] = jnp.zeros((chunk, 128), F32)

    c3t[...] = c3[...].T
    e4t[...] = e4[...].T
    go("B9", "A11", "S15", "C6", "C7", "C8", "C9", "B10", "A12", "A13", "S16", "S17")

    @pl.loop(0, N_FC1)
    def _(j):
        gather.from_core(fc1_it(j))
        bias = jnp.concatenate([vecf[pl.ds(2 * j * 16 + 6, 1), :], vecf[pl.ds(2 * j * 16 + 7, 1), :],
                                vecf[pl.ds((2 * j + 1) * 16 + 6, 1), :], vecf[pl.ds((2 * j + 1) * 16 + 7, 1), :]], axis=1)
        col = pl.ds(pl.multiple_of(j * FFB, FFB), FFB)

        for at in [pl.ds(0, rows)]:
            hidden = mm(n2[at, :], w1[:, col]) + mm(c3[at, :], u1[:, col]) + bias
            grad_active = mm_nt(g[at, :], w2[col, :]) + mm_nt(e4[at, :], d2[col, :])
            cdf = 0.5 * (1.0 + lax.erf(hidden * (0.5 ** 0.5)))
            pdf = jnp.exp(hidden * hidden * -0.5) * (0.5 / 3.141592653589793) ** 0.5
            active = (hidden * cdf).astype(BF16)
            act_s[at, :] = active
            grad_hidden = (grad_active * (cdf + hidden * pdf)).astype(BF16)
            gh_s[at, :] = grad_hidden
            oacc[at, :] += mm(active, w2[col, :])
            u4[at, :] += mm(active, d2[col, :])
            gacc[at, :] += mm_nt(grad_hidden, w1[:, col])
            e3[at, :] += mm_nt(grad_hidden, u1[:, col])

        @pl.when(j + 4 < N_FC1)
        def _():
            gather.from_z(fc1_it(j + 4))

        @pl.when(j == 0)
        def _():
            gather.from_x(fc1_it(1))

        @pl.when(j + 2 < N_FC1)
        def _():
            gather.from_x(fc1_it(j + 2))

        @pl.when(j + 1 < N_FC1)
        def _():
            gather.from_seq(fc1_it(j + 1))

        gr[:, col] = compact_rows(mm(c3t[...], gh_s[...]))
        gr[:, pl.ds(pl.multiple_of(ff + j * FFB, FFB), FFB)] = compact_rows(mm(e4t[...], act_s[...]))
        for first in (0, ff):
            cols = pl.ds(pl.multiple_of(first + j * FFB, FFB), FFB)
            to_partner(gr.at[:, cols], gr_in.at[:, cols], fs_sem.at[0], fr_sem.at[0]).start()

    bias2 = full_vector(vecf, 5)
    for n in range(FIRST + N_FC2):
        gather.finish(item(n))

    @pl.loop(0, N_FC1)
    def _(j):
        gather.finish(fc1_it(j))

    for pair in range(pairs - 2, pairs):
        prob_copy(pair).wait()

    def prob_load(pair):
        slot = lax.rem(pair, 2)
        return pltpu.make_async_copy(prob_out.at[pl.ds(2 * pair, 2)], prob.at[slot], prob_sem.at[slot])

    for pair in range(2):
        prob_load(pair).start()

    g1 = n1
    e2 = u4

    def grad_att(at, who):
        heads = pl.ds(pl.multiple_of(who * half, half), half)
        return (mm_nt(g1[at, :], wp[heads, :]) + mm_nt(e2[at, :].astype(BF16), pd_ref[heads, :])).astype(BF16)

    def d_copy(i):
        return to_partner(n1.at[pl.ds(rows + i * chunk, chunk), pl.ds(0, half)],
                          do_s.at[pl.ds(pl.multiple_of(s * rows + i * chunk, chunk), chunk), :], ds_sem.at[i], dr_sem.at[i])

    @pl.loop(0, 2)
    def _(i):
        at = pl.ds(pl.multiple_of(i * chunk, chunk), chunk)
        own_select = image.select(s * rows + i * chunk, chunk)
        c = (u4[at, :] * own_select).astype(BF16)
        e = (e3[at, :] * own_select).astype(BF16)
        c3[at, :] = c
        e4[at, :] = e
        grad_n2 = gacc[at, :] + mm_nt(e, d1[...])
        grad_mid = g[at, :].astype(F32) + norm_grad(mid[at, :], gain2, grad_n2)
        gacc[at, :] = grad_mid
        low = grad_mid.astype(BF16)
        g1[at, :] = low
        e2[at, :] = mm_nt(low, pu_ref[...]) * own_select
        n1[pl.ds(pl.multiple_of(rows + i * chunk, chunk), chunk), 0:half] = grad_att(at, other)
        d_copy(i).start()

    cols0 = 2 * ff
    cols1 = 4 * width
    gr[:, cols0:cols0 + width] = compact_rows(mm_tn(e4[...], n2[...]))
    gr[:, cols0 + width:cols0 + 2 * width] = compact_rows(mm_tn(c3[...], g[...]))
    gr[:, cols0 + 2 * width:cols0 + 3 * width] = compact_rows(mm_tn(c2[...], g1[0:rows, :]))
    gr[:, cols0 + 3 * width:cols0 + 4 * width] = compact_rows(mm_tn(e2[...].astype(BF16), att[...]))
    rest = pl.ds(cols0, cols1)
    rest_copy = to_partner(gr.at[:, rest], gr_in.at[:, rest], fs_sem.at[1], fr_sem.at[1])
    rest_copy.start()

    @pl.loop(0, 2)
    def _(i):
        at = pl.ds(pl.multiple_of(i * chunk, chunk), chunk)
        do_s[pl.ds(pl.multiple_of(s * rows + i * chunk, chunk), chunk), :] = grad_att(at, s)

    own0, own1 = cols0 // 16, cols1 // 16
    pick = adapter_rows(vecf)

    def turn_start(n, src, first, dst, cols):
        mine = pl.ds(pl.multiple_of(net.f * 16, 16), 16)

        @pl.loop(1, 16)
        def _(d):
            peer = (net.f + d) % 16
            pltpu.make_async_remote_copy(
                src_ref=src.at[:, pl.ds(pl.multiple_of(first + peer * cols, 128), cols)], dst_ref=dst.at[mine, :],
                send_sem=t_send.at[n], recv_sem=t_recv.at[n], device_id={"fsdp": peer}, device_id_type=MESH).start()

        dst[mine, :] = src[:, pl.ds(pl.multiple_of(first + net.f * cols, 128), cols)]

    def turn_total(n, dst):
        return pltpu.make_async_remote_copy(
            src_ref=dst.at[0:240, :], dst_ref=dst.at[0:240, :], send_sem=t_send.at[n], recv_sem=t_recv.at[n],
            device_id=net.c_peer, device_id_type=MESH)

    def result(n, src, first, step):
        return Block(src, lambda b: gall.at[:, pl.ds(pl.multiple_of(first + b * step, 128), 256)],
                     lambda m: gall.at[:, pl.ds(0, m * 256)], [g_sem.at[k, N_ITEMS + n] for k in range(N_SEMS)],
                     g_own.at[N_ITEMS + n])

    results = [result(0, dense0.at[:, pl.ds(0, 256)], 0, own0), result(1, dense0.at[:, pl.ds(256, 256)], 256, own0),
               result(2, dense1, cols0, own1), result(3, dense2, cols0 + cols1, own1)]

    def move(*steps):
        for step in steps:
            stages[step[0]](results[int(step[1:])])

    first_cols = pl.ds(0, cols0)
    first_copy = to_partner(gr.at[:, first_cols], gr_in.at[:, first_cols], fs_sem.at[0], fr_sem.at[0])
    first_copy.wait_recv()
    gr_sum[:, 0:cols0] = (gr[:, 0:cols0].astype(F32) + gr_in[:, 0:cols0].astype(F32)).astype(BF16)
    turn_start(0, gr_sum, 0, parts0, own0)

    @pl.loop(0, 2)
    def _(i):
        at = pl.ds(pl.multiple_of(i * chunk, chunk), chunk)
        branch = oacc[at, :] + mm(c3[at, :], u2[...]) + bias2
        xp[at, :] = (mid[at, :] + branch).astype(BF16)

    put(xp, out_out)
    put(gacc, gm_out)
    gpad = w2
    zeros = jnp.zeros((PAD, width), BF16)
    gpad[0:PAD, :] = zeros
    gpad[PAD + WINDOW:2 * PAD + WINDOW, :] = zeros
    last_own[...] = jnp.zeros_like(last_own)
    turn_total(0, parts0).wait_recv()
    dense0[...] = mm(pick, parts0[...]).astype(BF16)
    move("S0", "S1")
    for i in range(2):
        d_copy(i).wait_recv()

    gq = w1
    scale = HEAD_DIM ** (-0.5)
    keep = image.inside((WINDOW, 1), 0).astype(BF16)

    @pl.loop(0, pairs)
    def _(pair):
        @pl.when(pair == 2)
        def _():
            rest_copy.wait_recv()
            gr_sum[:, cols0:cols0 + cols1] = (gr[:, cols0:cols0 + cols1].astype(F32)
                                              + gr_in[:, cols0:cols0 + cols1].astype(F32)).astype(BF16)
            turn_start(1, gr_sum, cols0, parts1, own1)

        @pl.when(pair == 3)
        def _():
            move("A0")

        def cols(part):
            return pl.ds(pl.multiple_of(part * half + pair * 128, 128), 128)

        prob_load(pair).wait()
        slot = lax.rem(pair, 2)
        k2 = qkvw[:, cols(1)]
        v2 = qkvw[:, cols(2)]
        q2 = qkvw[:, cols(0)] * jnp.asarray(scale, BF16)
        do2 = image.choose(lambda at: do_s[at:at + WINDOW, cols(0)]) * keep
        inner = do2.astype(F32) * oh[:, cols(0)].astype(F32)
        gv = gk = gqq = None
        for hd in range(2):
            hm = halves[hd].astype(BF16)
            weights = prob[slot, hd]
            grad_p = mm_nt(do2 * hm, v2)
            row_inner = jnp.sum(inner * halves[hd], axis=1, keepdims=True)
            grad_s = (weights.astype(F32) * (grad_p - row_inner)).astype(BF16)
            dv = mm_tn(weights, do2 * hm)
            dk = mm_tn(grad_s, q2 * hm)
            dq = mm(grad_s, k2 * hm)
            gv = dv if gv is None else gv + dv
            gk = dk if gk is None else gk + dk
            gqq = dq if gqq is None else gqq + dq

        @pl.when(pair + 2 < pairs)
        def _():
            prob_load(pair + 2).start()

        gq[0:WINDOW, cols(0)] = (gqq * scale).astype(BF16)
        gq[0:WINDOW, cols(1)] = gk.astype(BF16)
        gq[0:WINDOW, cols(2)] = gv.astype(BF16)

    three = slice(0, 3 * half)
    c1[0:WINDOW, :] = (mm_nt(gq[0:WINDOW, three], qu[...]) * image.select_window(0, WINDOW)).astype(BF16)
    up = compact_rows(mm_tn(c1w[...], gq[0:WINDOW, three]))
    for part in range(3):
        last_own[:, pl.ds(pl.multiple_of(part * width + s * half, 128), half)] = up[:, part * half:(part + 1) * half]
    last_own[:, 3 * width:4 * width] = compact_rows(mm_tn(c1[0:WINDOW, :], n1w[...]))
    last_copy = to_partner(last_own, last_in, fs_sem.at[2], fr_sem.at[2])
    last_copy.start()
    move("A1")

    @pl.loop(0, 2)
    def _(i):
        at = pl.ds(pl.multiple_of(i * QROWS, QROWS), QROWS)
        gpad[pl.ds(pl.multiple_of(PAD + i * QROWS, STEP), QROWS), :] = (
            mm_nt(gq[at, three], wq[...]) + mm_nt(c1[at, :], qd_ref[...])).astype(BF16)

    def rows_of(who, i):
        return image.choose(lambda at: gpad[pl.ds(pl.multiple_of(who * rows + PAD + i * chunk - at, STEP), chunk), :])

    spot = 2 * PAD + WINDOW + 128

    def p_copy(i):
        return to_partner(gpad.at[pl.ds(spot + i * chunk, chunk), :], prcv.at[i], ps_sem.at[i], pr_sem.at[i])

    for i in range(2):
        gpad[spot + i * chunk:spot + (i + 1) * chunk, :] = rows_of(other, i)
        p_copy(i).start()
    last_copy.wait_recv()
    last_sum[...] = (last_own[...].astype(F32) + last_in[...].astype(F32)).astype(BF16)
    turn_start(2, last_sum, 0, parts2, own1)
    turn_total(1, parts1).wait_recv()
    dense1[...] = mm(pick, parts1[...]).astype(BF16)
    move("B0", "S2", "B1")
    turn_total(2, parts2).wait_recv()
    dense2[...] = mm(pick, parts2[...]).astype(BF16)
    move("S3", "C0", "A2", "C1", "A3", "B2", "C2", "B3")
    gn = oacc
    for i in range(2):
        p_copy(i).wait_recv()
        at = slice(i * chunk, (i + 1) * chunk)
        gn[at, :] = prcv[i].astype(F32) + rows_of(s, i).astype(F32)
        put(gn.at[at, :], gn_out.at[at, :])
    move("C3")
    for copy in outs:
        copy.wait()
    for i in range(2):
        x_copy(i).wait_send()
        d_copy(i).wait_send()
        p_copy(i).wait_send()
    for copy in (first_copy, rest_copy, last_copy):
        copy.wait_send()
    for n, dst in enumerate((parts0, parts1, parts2)):
        turn_total(n, dst).wait_send()
    for it in results:
        gather.finish(it)

    @pl.loop(0, pairs)
    def _(pair):
        att_copy(pair).wait_send()


def any_spec():
    return pl.BlockSpec(memory_space=pl.ANY)


def vmem_spec():
    return pl.BlockSpec(memory_space=pltpu.VMEM)


def adapter_rows(vec_ref):
    ids = jnp.concatenate([jnp.broadcast_to(vec_ref[16 * p + 8:16 * p + 9, :], (16, 128)) for p in range(16)], axis=0)
    r = lax.broadcasted_iota(jnp.int32, (256, 128), 0) % 16
    col = lax.broadcasted_iota(jnp.int32, (256, 128), 1)
    group = (col // 16).astype(F32)
    return ((ids == group) & (r == col % 16)).astype(F32).T.astype(BF16)


def run_block(seg, ident, x, vec, qd, pd, pu, wq, wp, w1, w2, qu, g, u1, d1, u2, d2):
    rows, width = x.shape
    toks = seg.shape[1]
    half = width // 2
    ff = w1.shape[1]
    chunk = rows // 2
    dma = pltpu.SemaphoreType.DMA
    sds = jax.ShapeDtypeStruct
    gcols = 2 * ff + 4 * width
    last = 4 * width
    out_shape = (
        sds((256, 128), F32), sds((half // 64, WINDOW, WINDOW), BF16), sds((rows, width), F32), sds((rows, width), BF16),
        sds((128, gcols + last), BF16), sds((rows, width), F32))

    def low(*shape):
        return pltpu.VMEM(shape, BF16)

    def full(*shape):
        return pltpu.VMEM(shape, F32)

    scratch = [
        low(wq.shape[0], 3 * half), low(width, 3 * half), low(width, width), low(width, ff), low(ff, width),
        low(rows, width), full(256, 128), low(128, 3 * half), low(rows, width), low(128, ff), low(width, 128),
        low(128, width), low(ff, 128), low(toks, 3 * half), low(toks, width), low(toks, 128),
        low(WINDOW, 3 * half), low(WINDOW, width), low(WINDOW, 128), low(2, 2, WINDOW, WINDOW), low(2 * PAD + WINDOW, 128),
        low(half // 128, rows, 128), low(WINDOW, half), low(rows, width), low(rows, 128), full(rows, width), low(rows, width),
        full(rows, width), full(rows, width), full(rows, 128), full(rows, 128), low(rows, 128), low(rows, 128),
        low(128, rows), low(128, rows), low(rows, FFB), low(rows, FFB), low(16, gcols),
        low(toks, half), low(16, gcols), low(16, gcols), low(16, last), low(16, last), low(16, last),
        low(256, 2 * ff // 16), low(256, last // 16), low(256, last // 16), low(128, 2 * ff // 16), low(128, last // 16),
        low(128, last // 16), low(2, chunk, width),
        dma((2,)), dma((2,)), dma((4,)), dma((4,)), dma((11,)), dma((12,)), dma((2,)),
        dma((N_SEMS, N_ITEMS + 4)), dma((N_ITEMS + 4,)),
        dma((2,)), dma((2,)), dma((3,)), dma((3,)), dma((2,)), dma((2,)), dma((3,)), dma((3,))]
    return pl.pallas_call(
        block_kernel, out_shape=out_shape, in_specs=[vmem_spec()] * 7 + [any_spec()] * 10,
        out_specs=tuple(any_spec() for unused in out_shape), scratch_shapes=scratch,
        compiler_params=pltpu.CompilerParams(collective_id=1, has_side_effects=True, vmem_limit_bytes=VMEM_LIMIT),
        name="block")(seg, ident, x, vec, qd, pd, pu, wq, wp, w1, w2, qu, g, u1, d1, u2, d2)


def expand_kernel(vec_ref, f1u, f2d, f1d, f2u, pu, pdn, qu, qd, gn, x, gm,
                  gt_out, qd_out, qu_out, pd_out, pu_out, f1d_out, f1u_out, f2d_out, f2u_out):
    for src, dst in ((f1u, f1u_out), (f2u, f2u_out), (pu, pu_out), (qu, qu_out)):
        dst[...] = src[...].astype(F32)
    for src, dst in ((f1d, f1d_out), (f2d, f2d_out), (pdn, pd_out), (qd, qd_out)):
        dst[...] = src[...].astype(F32).T
    gain1 = full_vector(vec_ref, 0)
    gt_out[...] = gm[...] + norm_grad(x[...].astype(F32), gain1, gn[...])


def run_expand(vec, gall, gn, x, gm):
    rows, width = gn.shape
    ff = 4 * width
    n = 4
    sds = jax.ShapeDtypeStruct

    def part(cols, offset):
        return pl.BlockSpec((128, cols), lambda j: (0, offset // cols + j))

    def by_row(shape):
        return pl.BlockSpec(shape, lambda j: (j, 0))

    def by_col(shape):
        return pl.BlockSpec(shape, lambda j: (0, j))

    q = width // n
    return pl.pallas_call(
        expand_kernel, grid=(n,),
        out_shape=(sds((rows, width), F32), sds((width, 128), F32), sds((128, 3 * width), F32), sds((width, 128), F32),
                   sds((128, width), F32), sds((width, 128), F32), sds((128, ff), F32), sds((ff, 128), F32), sds((128, width), F32)),
        in_specs=[pl.BlockSpec((256, 128), lambda j: (0, 0)), part(ff // n, 0), part(ff // n, ff), part(q, 2 * ff),
                  part(q, 2 * ff + width), part(q, 2 * ff + 2 * width), part(q, 2 * ff + 3 * width),
                  part(3 * q, 2 * ff + 4 * width), part(q, 2 * ff + 7 * width),
                  by_row((rows // n, width)), by_row((rows // n, width)), by_row((rows // n, width))],
        out_specs=(by_row((rows // n, width)), by_row((q, 128)), by_col((128, 3 * q)), by_row((q, 128)), by_col((128, q)),
                   by_row((q, 128)), by_col((128, ff // n)), by_row((ff // n, 128)), by_col((128, q))),
        compiler_params=pltpu.CompilerParams(vmem_limit_bytes=VMEM_LIMIT),
        name="expand")(vec, *([gall] * 8), gn, x, gm)


def per_device_fast(tokens, grad_out, segments, padding, adapter_ids, norm1_gain, norm1_bias, w_qkv, w_proj, proj_bias,
                    norm2_gain, norm2_bias, w_fc1, fc1_bias, w_fc2, fc2_bias, qkv_down, qkv_up, proj_down, proj_up,
                    fc1_down, fc1_up, fc2_down, fc2_up):
    x = tokens[0]
    odd = (lax.axis_index("fsdp") % 2).astype(F32)
    six = jnp.stack([norm1_gain, norm1_bias, proj_bias, norm2_gain, norm2_bias, fc2_bias]).astype(F32)
    vec = jnp.concatenate([
        jnp.concatenate([six * (1.0 - odd), six * odd], axis=1), fc1_bias.astype(F32).reshape(2, 128),
        jnp.broadcast_to(adapter_ids[0].astype(F32)[:, None], (1, 128)), jnp.zeros((7, 128), F32)], axis=0)
    vecf, unused, gm, out, gall, gn = run_block(
        segments, adapter_ids, x, vec, qkv_down, proj_down, proj_up, w_qkv, w_proj, w_fc1, w_fc2, qkv_up,
        grad_out[0], fc1_up, fc1_down, fc2_up, fc2_down)
    gt, gqd, gqu, gpd, gpu, gf1d, gf1u, gf2d, gf2u = run_expand(vecf, gall, gn, x, gm)
    return out[None], gt[None], gqd, gqu, gpd, gpu, gf1d, gf1u, gf2d, gf2u


def solution(mesh):
    sizes = dict(mesh.shape)
    small = sizes == {"seq": 2, "fsdp": 16}

    def per_device_any(*args):
        tokens, adapter_ids = args[0], args[4]
        one_image = tokens.shape[1:] == (512, 1024) and adapter_ids.shape[1] == 1
        return (per_device_fast if small and one_image else per_device)(*args)

    return jax.shard_map(
        per_device_any,
        mesh=mesh,
        in_specs=(
            P("fsdp", "seq", None),
            P("fsdp", "seq", None),
            P("fsdp", None),
            P("fsdp", None),
            P("fsdp", None),
            P("fsdp"),
            P("fsdp"),
            P("fsdp", None),
            P("fsdp", None),
            P("fsdp"),
            P("fsdp"),
            P("fsdp"),
            P("fsdp", None),
            P("fsdp"),
            P("fsdp", None),
            P("fsdp"),
            P(),
            P(),
            P(),
            P(),
            P(),
            P(),
            P(),
            P(),
        ),
        out_specs=(
            P("fsdp", "seq", None),
            P("fsdp", "seq", None),
            P(),
            P(),
            P(),
            P(),
            P(),
            P(),
            P(),
            P(),
        ),
        check_vma=False,
    )
```

```python
from functools import partial

import jax
import jax.numpy as jnp
from jax import lax
from jax.experimental import pallas as pl
from jax.experimental.pallas import tpu as pltpu
from jax.sharding import PartitionSpec as P

HEAD_DIM = 64
IMG = 577
RANK = 16
QBLOCK = 512


norm_eps = 1e-06
masked_score = -1e30


def matmul(left_side, right_side):
    return jnp.dot(left_side, right_side, preferred_element_type=jnp.float32)


def matmul_nt(left_side, right_side):
    return jnp.einsum("tk,jk->tj", left_side, right_side, preferred_element_type=jnp.float32)


def matmul_tn(left_side, right_side):
    return jnp.einsum("ti,to->io", left_side, right_side, preferred_element_type=jnp.float32)


def layer_norm(values, norm_gain, norm_shift):
    centre = jnp.mean(values, axis=-1, keepdims=True)
    centred = values - centre
    spread = jnp.mean(centred * centred, axis=-1, keepdims=True)
    return centred * lax.rsqrt(spread + norm_eps) * norm_gain + norm_shift


def norm_backward(values, norm_gain, norm_shift, grad_in):

    def apply_norm(inputs):
        return layer_norm(inputs, norm_gain, norm_shift)

    unused, pullback = jax.vjp(apply_norm, values)
    return pullback(grad_in)[0]


def selection(seg_own, image_adapters, columns):
    images = jnp.arange(image_adapters.shape[0], dtype=jnp.int32)
    image_match = seg_own[:, None] - 1 == images[None, :]
    token_adapter = jnp.sum(jnp.where(image_match, image_adapters[None, :], 0), axis=1)
    present = jnp.any(image_match, axis=1)
    column = jnp.arange(columns, dtype=jnp.int32) // RANK
    chosen = (token_adapter[:, None] == column[None, :]) & present[:, None]
    return chosen.astype(jnp.float32)


def adapter_forward(inputs_b, weight, down_map, up_map, select):
    inner_term = (matmul(inputs_b, down_map) * select).astype(jnp.bfloat16)
    return (matmul(inputs_b, weight) + matmul(inner_term, up_map), inner_term)


def adapter_backward(inputs_b, inner_term, grad_in, weight, down_map, up_map, select):
    grad_up = matmul_tn(inner_term, grad_in)
    grad_inner = (matmul_nt(grad_in, up_map) * select).astype(jnp.bfloat16)
    grad_down = matmul_tn(inputs_b, grad_inner)
    grad_inputs = matmul_nt(grad_in, weight) + matmul_nt(grad_inner, down_map)
    return (grad_inputs, grad_down, grad_up)


def block_scores(query_block, key_heads, seg_block, seg_keys, keep_keys):
    score_scale = HEAD_DIM ** (-0.5)
    scores = (
        jnp.einsum("qhd,khd->hqk", query_block, key_heads, preferred_element_type=jnp.float32)
        * score_scale
    )
    allowed = (seg_block[:, None] == seg_keys[None, :]) & (keep_keys[None, :] == 1)
    return jnp.where(allowed[None, :, :], scores, masked_score)


def split_heads(head_rows):
    all_rows = head_rows.shape[0]
    local_heads = head_rows.shape[2] // HEAD_DIM
    query_heads = head_rows[:, 0].reshape(all_rows, local_heads, HEAD_DIM)
    key_heads = head_rows[:, 1].reshape(all_rows, local_heads, HEAD_DIM)
    value_heads = head_rows[:, 2].reshape(all_rows, local_heads, HEAD_DIM)
    return (query_heads, key_heads, value_heads)


def key_window(all_rows):
    return min(all_rows, (QBLOCK + 2 * IMG - 2 + 127) // 128 * 128)


def window_start(block_index, all_rows, window):
    first = block_index * QBLOCK - (IMG - 1)
    return jnp.clip(first, 0, all_rows - window)


def attention_forward(head_rows, seg_all, keep_all):
    all_rows = head_rows.shape[0]
    block_count = all_rows // QBLOCK
    window = key_window(all_rows)
    query_heads, key_heads, value_heads = split_heads(head_rows)
    local_heads = query_heads.shape[1]

    def one_block(block_parts):
        query_block, seg_block, keep_block, block_index = block_parts
        start = window_start(block_index, all_rows, window)
        keys_near = lax.dynamic_slice_in_dim(key_heads, start, window, 0)
        values_near = lax.dynamic_slice_in_dim(value_heads, start, window, 0)
        seg_near = lax.dynamic_slice_in_dim(seg_all, start, window, 0)
        keep_near = lax.dynamic_slice_in_dim(keep_all, start, window, 0)
        scores = block_scores(query_block, keys_near, seg_block, seg_near, keep_near)
        row_max = jnp.max(scores, axis=2, keepdims=True)
        weights = jnp.exp(scores - row_max)
        row_sum = jnp.sum(weights, axis=2, keepdims=True)
        probs_low = (weights / row_sum).astype(jnp.bfloat16)
        result = jnp.einsum(
            "hqk,khd->qhd", probs_low, values_near, preferred_element_type=jnp.float32
        )
        result = result * keep_block[:, None, None].astype(jnp.float32)
        return (result.astype(jnp.bfloat16), row_max, row_sum)

    block_ids = jnp.arange(block_count, dtype=jnp.int32)
    blocked = (
        query_heads.reshape(block_count, QBLOCK, local_heads, HEAD_DIM),
        seg_all.reshape(block_count, QBLOCK),
        keep_all.reshape(block_count, QBLOCK),
        block_ids,
    )
    results, block_max, block_sums = lax.map(one_block, blocked)
    return (results.reshape(all_rows, local_heads * HEAD_DIM), block_max, block_sums)


def attention_backward(head_rows, grad_rows, seg_all, keep_all, block_max, block_sums):
    all_rows = head_rows.shape[0]
    block_count = all_rows // QBLOCK
    window = key_window(all_rows)
    query_heads, key_heads, value_heads = split_heads(head_rows)
    local_heads = query_heads.shape[1]
    score_scale = HEAD_DIM ** (-0.5)

    def one_block(running, block_parts):
        grad_keys, grad_values = running
        query_block, seg_block, keep_block, grad_block, row_max, row_sum, block_index = block_parts
        start = window_start(block_index, all_rows, window)
        keys_near = lax.dynamic_slice_in_dim(key_heads, start, window, 0)
        values_near = lax.dynamic_slice_in_dim(value_heads, start, window, 0)
        seg_near = lax.dynamic_slice_in_dim(seg_all, start, window, 0)
        keep_near = lax.dynamic_slice_in_dim(keep_all, start, window, 0)
        scores = block_scores(query_block, keys_near, seg_block, seg_near, keep_near)
        probs = jnp.exp(scores - row_max) / row_sum
        grad_result = grad_block * keep_block[:, None, None].astype(jnp.bfloat16)
        values_term = jnp.einsum(
            "hqk,qhd->khd",
            probs.astype(jnp.bfloat16),
            grad_result,
            preferred_element_type=jnp.float32,
        )
        grad_probs = jnp.einsum(
            "qhd,khd->hqk", grad_result, values_near, preferred_element_type=jnp.float32
        )
        row_inner = jnp.sum(probs * grad_probs, axis=2, keepdims=True)
        grad_scores = (probs * (grad_probs - row_inner)).astype(jnp.bfloat16)
        grad_query = (
            jnp.einsum("hqk,khd->qhd", grad_scores, keys_near, preferred_element_type=jnp.float32)
            * score_scale
        )
        keys_term = (
            jnp.einsum("hqk,qhd->khd", grad_scores, query_block, preferred_element_type=jnp.float32)
            * score_scale
        )
        grad_keys = lax.dynamic_update_slice_in_dim(
            grad_keys, lax.dynamic_slice_in_dim(grad_keys, start, window, 0) + keys_term, start, 0
        )
        grad_values = lax.dynamic_update_slice_in_dim(
            grad_values,
            lax.dynamic_slice_in_dim(grad_values, start, window, 0) + values_term,
            start,
            0,
        )
        return ((grad_keys, grad_values), grad_query)

    zero_heads = jnp.zeros((all_rows, local_heads, HEAD_DIM), jnp.float32)
    block_ids = jnp.arange(block_count, dtype=jnp.int32)
    blocked = (
        query_heads.reshape(block_count, QBLOCK, local_heads, HEAD_DIM),
        seg_all.reshape(block_count, QBLOCK),
        keep_all.reshape(block_count, QBLOCK),
        grad_rows.reshape(block_count, QBLOCK, local_heads, HEAD_DIM),
        block_max,
        block_sums,
        block_ids,
    )
    (grad_keys, grad_values), grad_queries = lax.scan(one_block, (zero_heads, zero_heads), blocked)
    flat_width = local_heads * HEAD_DIM
    stacked = jnp.stack(
        [
            grad_queries.reshape(all_rows, flat_width),
            grad_keys.reshape(all_rows, flat_width),
            grad_values.reshape(all_rows, flat_width),
        ],
        axis=1,
    )
    return stacked.astype(jnp.bfloat16)


def per_device(
    tokens,
    grad_out,
    segments,
    padding,
    adapter_ids,
    norm1_gain,
    norm1_bias,
    w_qkv,
    w_proj,
    proj_bias,
    norm2_gain,
    norm2_bias,
    w_fc1,
    fc1_bias,
    w_fc2,
    fc2_bias,
    qkv_down,
    qkv_up,
    proj_down,
    proj_up,
    fc1_down,
    fc1_up,
    fc2_down,
    fc2_up,
):
    tok_rows = tokens.shape[1]
    feat_width = tokens.shape[2]
    inputs = tokens[0].astype(jnp.float32)
    seg_all = segments[0]
    keep_all = padding[0]
    offset = lax.axis_index("seq") * tok_rows
    seg_own = lax.dynamic_slice_in_dim(seg_all, offset, tok_rows)
    select = selection(seg_own, adapter_ids[0], qkv_down.shape[1])
    gain_one, shift_one, qkv_weight, proj_weight, proj_shift = (
        lax.all_gather(norm1_gain, "fsdp", axis=0, tiled=True),
        lax.all_gather(norm1_bias, "fsdp", axis=0, tiled=True),
        lax.all_gather(w_qkv, "fsdp", axis=0, tiled=True),
        lax.all_gather(w_proj, "fsdp", axis=0, tiled=True),
        lax.all_gather(proj_bias, "fsdp", axis=0, tiled=True),
    )
    gain_one = gain_one.astype(jnp.float32)
    shift_one = shift_one.astype(jnp.float32)
    normed_one = layer_norm(inputs, gain_one, shift_one).astype(jnp.bfloat16)
    qkv_main, inner_one = adapter_forward(normed_one, qkv_weight, qkv_down, qkv_up, select)
    qkv_low = qkv_main.astype(jnp.bfloat16).reshape(tok_rows, 3, feat_width)
    head_rows = lax.all_to_all(qkv_low, "seq", split_axis=2, concat_axis=0, tiled=True)
    attended_heads, block_max, block_sums = attention_forward(head_rows, seg_all, keep_all)
    attended = lax.all_to_all(attended_heads, "seq", split_axis=0, concat_axis=1, tiled=True)
    branch_one, inner_two = adapter_forward(attended, proj_weight, proj_down, proj_up, select)
    middle = inputs + (branch_one + proj_shift.astype(jnp.float32))
    gain_two, shift_two, fc1_weight, fc2_shift, fc2_weight, fc1_shift = (
        lax.all_gather(norm2_gain, "fsdp", axis=0, tiled=True),
        lax.all_gather(norm2_bias, "fsdp", axis=0, tiled=True),
        lax.all_gather(w_fc1, "fsdp", axis=0, tiled=True),
        lax.all_gather(fc2_bias, "fsdp", axis=0, tiled=True),
        lax.all_gather(w_fc2, "fsdp", axis=0, tiled=True),
        lax.all_gather(fc1_bias, "fsdp", axis=0, tiled=True),
    )
    gain_two = gain_two.astype(jnp.float32)
    shift_two = shift_two.astype(jnp.float32)
    normed_two = layer_norm(middle, gain_two, shift_two).astype(jnp.bfloat16)
    hidden_main, inner_three = adapter_forward(normed_two, fc1_weight, fc1_down, fc1_up, select)
    hidden = hidden_main + fc1_shift.astype(jnp.float32)
    active = jax.nn.gelu(hidden, approximate=False).astype(jnp.bfloat16)
    branch_two, inner_four = adapter_forward(active, fc2_weight, fc2_down, fc2_up, select)
    output = (middle + (branch_two + fc2_shift.astype(jnp.float32))).astype(jnp.bfloat16)
    fc1_back, fc2_back = (
        lax.all_gather(w_fc1, "fsdp", axis=0, tiled=True),
        lax.all_gather(w_fc2, "fsdp", axis=0, tiled=True),
    )
    grad_top = grad_out[0]
    grad_active, grad_fc2_down, grad_fc2_up = adapter_backward(
        active, inner_four, grad_top, fc2_back, fc2_down, fc2_up, select
    )
    unused, gelu_back = jax.vjp(partial(jax.nn.gelu, approximate=False), hidden)
    grad_hidden = gelu_back(grad_active)[0].astype(jnp.bfloat16)
    grad_normed_two, grad_fc1_down, grad_fc1_up = adapter_backward(
        normed_two, inner_three, grad_hidden, fc1_back, fc1_down, fc1_up, select
    )
    grad_middle = grad_top.astype(jnp.float32) + norm_backward(
        middle, gain_two, shift_two, grad_normed_two
    )
    qkv_back, proj_back = (
        lax.all_gather(w_qkv, "fsdp", axis=0, tiled=True),
        lax.all_gather(w_proj, "fsdp", axis=0, tiled=True),
    )
    grad_branch_one = grad_middle.astype(jnp.bfloat16)
    grad_attended, grad_proj_down, grad_proj_up = adapter_backward(
        attended, inner_two, grad_branch_one, proj_back, proj_down, proj_up, select
    )
    grad_head_rows = lax.all_to_all(
        grad_attended.astype(jnp.bfloat16), "seq", split_axis=1, concat_axis=0, tiled=True
    )
    grad_qkv_heads = attention_backward(
        head_rows, grad_head_rows, seg_all, keep_all, block_max, block_sums
    )
    grad_qkv = lax.all_to_all(
        grad_qkv_heads, "seq", split_axis=0, concat_axis=2, tiled=True
    ).reshape(tok_rows, 3 * feat_width)
    grad_normed_one, grad_qkv_down, grad_qkv_up = adapter_backward(
        normed_one, inner_one, grad_qkv, qkv_back, qkv_down, qkv_up, select
    )
    grad_tokens = grad_middle + norm_backward(inputs, gain_one, shift_one, grad_normed_one)
    summed = lax.psum(
        (
            grad_qkv_down,
            grad_qkv_up,
            grad_proj_down,
            grad_proj_up,
            grad_fc1_down,
            grad_fc1_up,
            grad_fc2_down,
            grad_fc2_up,
        ),
        ("seq", "fsdp"),
    )
    return (
        output[None],
        grad_tokens[None],
        summed[0],
        summed[1],
        summed[2],
        summed[3],
        summed[4],
        summed[5],
        summed[6],
        summed[7],
    )


F32 = jnp.float32
BF16 = jnp.bfloat16
MESH = pl.DeviceIdType.MESH
VMEM_LIMIT = 67_000_000


def mm(a, b):
    return lax.dot_general(a, b, (((1,), (0,)), ((), ())), preferred_element_type=F32)


def mm_nt(a, b):
    return lax.dot_general(a, b, (((1,), (1,)), ((), ())), preferred_element_type=F32)


def mm_tn(a, b):
    return lax.dot_general(a, b, (((0,), (0,)), ((), ())), preferred_element_type=F32)


def norm_parts(v):
    mean = jnp.mean(v, axis=-1, keepdims=True)
    centred = v - mean
    r = lax.rsqrt(jnp.mean(centred * centred, axis=-1, keepdims=True) + norm_eps)
    return centred * r, r


def norm_grad(v, gain, grad_y):
    h, r = norm_parts(v)
    d = grad_y * gain
    return r * (d - jnp.mean(d, axis=-1, keepdims=True) - h * jnp.mean(d * h, axis=-1, keepdims=True))


class Net:
    def __init__(self):
        self.s = lax.axis_index("seq")
        self.f = lax.axis_index("fsdp")
        self.z = self.f // 4
        self.x = (self.f // 2) % 2
        self.c = self.f % 2
        self.partner = {"seq": 1 - self.s}
        self.x_peer = {"fsdp": self.block(self.z, 1 - self.x, self.c)}
        self.c_peer = {"fsdp": self.block(self.z, self.x, 1 - self.c)}

    def block(self, z, x, c):
        return (z * 2 + x) * 2 + c

    def z_peer(self, d):
        return {"fsdp": self.block((self.z + d) % 4, self.x, self.c)}

    def meet(self, peers):
        sem = pltpu.get_barrier_semaphore()
        for peer in peers:
            pl.semaphore_signal(sem, inc=1, device_id=peer, device_id_type=MESH)
        pl.semaphore_wait(sem, len(peers))

    def plane_peer(self, d):
        return {"fsdp": (self.f + d) % 16}

    def plane_barrier(self):
        self.meet([self.partner] + [self.plane_peer(d) for d in range(1, 16)])

    def barrier(self):
        self.meet([self.partner, self.x_peer, self.c_peer] + [self.z_peer(d) for d in (1, 2, 3)])


class Block:
    def __init__(self, src, piece, some, sems, own_sem, plane=2):
        self.src, self.piece, self.some, self.plane, self.own_sem = src, piece, some, plane, own_sem
        self.sent, self.z, self.x, self.y1, self.y2, self.c = sems


N_SEMS = 6


class Gather:
    def __init__(self, net):
        self.net = net

    def send(self, it, src, block, sem, peer):
        pltpu.make_async_remote_copy(
            src_ref=src, dst_ref=it.piece(block), send_sem=it.sent, recv_sem=sem, device_id=peer,
            device_id_type=MESH).start()

    def total(self, it, n, sem):
        return pltpu.make_async_remote_copy(
            src_ref=it.some(n), dst_ref=it.some(n), send_sem=it.sent, recv_sem=sem, device_id=self.net.c_peer,
            device_id_type=MESH)

    def here(self, it, body):
        if isinstance(it.plane, int) and it.plane == 2:
            body()
        else:
            pl.when((self.net.s == it.plane) | (it.plane == 2))(body)

    def hand_on(self, it, pieces, sem):
        def body():
            for piece, block in pieces:
                self.send(it, piece, block, sem, self.net.partner)

        if not isinstance(it.plane, int):
            pl.when(it.plane != 2)(body)
        elif it.plane != 2:
            body()

    def own(self, it):
        return pltpu.make_async_copy(it.src, it.piece(self.net.f), it.own_sem)

    def column(self, it, x, ds):
        net = self.net
        blocks = [net.block((net.z + d) % 4, x, net.c) for d in ds]
        return [(it.piece(block), block) for block in blocks]

    def start(self, it):
        net = self.net

        def along():
            for d in (2, 1, 3):
                self.send(it, it.src, net.f, it.z, net.z_peer(d))
            self.send(it, it.src, net.f, it.x, net.x_peer)

        self.here(it, along)
        self.send(it, it.src, net.f, it.c, net.c_peer)
        self.own(it).start()

    def from_z(self, it):
        net = self.net

        def body():
            self.total(it, 3, it.z).wait_recv()
            pieces = self.column(it, net.x, (1, 3, 2))
            for piece, block in pieces:
                self.send(it, piece, block, it.x, net.x_peer)
            self.hand_on(it, pieces, it.y1)
            for piece, block in pieces:
                self.send(it, piece, block, it.c, net.c_peer)

        self.here(it, body)

    def from_x(self, it):
        net = self.net

        def body():
            self.total(it, 4, it.x).wait_recv()
            pieces = self.column(it, 1 - net.x, (0, 1, 3, 2))
            self.hand_on(it, pieces, it.y2)
            for piece, block in pieces:
                self.send(it, piece, block, it.c, net.c_peer)

        self.here(it, body)

    def from_seq(self, it):
        net = self.net
        if isinstance(it.plane, int) and it.plane == 2:
            return

        @pl.when((net.s != it.plane) & (it.plane != 2))
        def _():
            self.total(it, 3, it.y1).wait_recv()
            for piece, block in self.column(it, net.x, (1, 3, 2)):
                self.send(it, piece, block, it.c, net.c_peer)
            self.total(it, 4, it.y2).wait_recv()
            for piece, block in self.column(it, 1 - net.x, (0, 1, 3, 2)):
                self.send(it, piece, block, it.c, net.c_peer)

    def from_core(self, it):
        self.total(it, 8, it.c).wait_recv()
        self.own(it).wait()

    def finish(self, it):
        net = self.net
        if isinstance(it.plane, int) and it.plane == 2:
            self.total(it, 15, it.z).wait_send()
            return

        @pl.when(it.plane == 2)
        def _():
            self.total(it, 15, it.z).wait_send()

        @pl.when(net.s == it.plane)
        def _():
            self.total(it, 22, it.z).wait_send()

        @pl.when((net.s != it.plane) & (it.plane != 2))
        def _():
            self.total(it, 8, it.z).wait_send()


def full_vector(vec_ref, row, blocks=16, rows=16):
    parts = []
    for k in range(blocks // 2):
        even = vec_ref[2 * k * rows + row:2 * k * rows + row + 1, :]
        odd = vec_ref[(2 * k + 1) * rows + row:(2 * k + 1) * rows + row + 1, :]
        parts.append(even + odd)
    return jnp.concatenate(parts, axis=1)


WINDOW = 640
STEP = 64
PAD = 384
QROWS = 320
FFB = 512


class Image:
    def __init__(self, seg_ref, id_ref):
        self.start = jnp.sum((seg_ref[...] == 0).astype(F32), axis=1, keepdims=True)
        ident = id_ref[...].astype(F32)
        self.pick = []
        base = jnp.zeros((1, 1), F32)
        for k in range(PAD // STEP + 1):
            mark = ((self.start >= k * STEP) & (self.start < (k + 1) * STEP)).astype(F32)
            self.pick.append(mark)
            base = base + mark * float(k * STEP)
        self.shift = base - self.start
        lane = lax.broadcasted_iota(jnp.int32, (1, 128), 1).astype(F32)
        self.columns = ((lane >= ident * RANK) & (lane < (ident + 1) * RANK)).astype(F32)

    def choose(self, load):
        total = None
        for k, mark in enumerate(self.pick):
            value = load(k * STEP)
            value = value * mark.astype(value.dtype)
            total = value if total is None else total + value
        return total

    def inside(self, shape, axis, first=0):
        at = (lax.broadcasted_iota(jnp.int32, shape, axis) + first).astype(F32) + self.shift
        return (at >= 0) & (at < IMG)

    def select(self, first, rows):
        at = (lax.broadcasted_iota(jnp.int32, (rows, 1), 0) + first).astype(F32)
        return (at >= self.start).astype(F32) * self.columns

    def select_window(self, first, rows):
        at = (lax.broadcasted_iota(jnp.int32, (rows, 1), 0) + first).astype(F32) + self.shift
        return (at >= 0).astype(F32) * self.columns


def lane_halves():
    lane = lax.broadcasted_iota(jnp.int32, (1, 128), 1)
    return [(lane < 64).astype(F32), (lane >= 64).astype(F32)]


def compact_rows(dense):
    total = dense[0:16]
    for k in range(1, 8):
        total = total + dense[16 * k:16 * (k + 1)]
    return total.astype(BF16)


N_FC1 = 8
N_FC2 = 4
FIRST = 6
PLANES = (2, 2, 0, 1, 2, 2, 2, 2)
N_ITEMS = FIRST + N_FC2 + N_FC1


def block_kernel(seg_ref, id_ref, x_ref, vec_ref, qd_ref, pd_ref, pu_ref, wq_hbm, wp_hbm, w1_hbm, w2_hbm,
                 qu_hbm, g_hbm, u1_hbm, d1_hbm, u2_hbm, d2_hbm,
                 vecf_out, prob_out, gm_out, out_out, gall, gn_out,
                 wq_own, wq, wp, w1, w2, xp, vecf, qu, g, u1, d1, u2, d2, qkv, n1, c1, qkvw, n1w, c1w, prob, opad, sendb,
                 oh, att, c2, mid, n2, oacc, gacc, u4, e3, c3, e4, c3t, e4t, act_s, gh_s, gr,
                 do_s, gr_in, gr_sum, last_own, last_in, last_sum, parts0, parts1, parts2, dense0, dense1, dense2, prcv,
                 xs_sem, xr_sem, as_sem, ar_sem, loc_sem, out_sem, prob_sem, g_sem, g_own,
                 ds_sem, dr_sem, fs_sem, fr_sem, ps_sem, pr_sem, t_send, t_recv):
    net = Net()
    s, other = net.s, 1 - net.s
    rows, width = x_ref.shape
    half = wq.shape[1] // 3
    rb = wq_own.shape[0]
    fr1 = w1_hbm.shape[0]
    fr2 = w2_hbm.shape[0]
    ff = w1.shape[1]
    chunk = rows // 2

    pre = []
    for part in range(3):
        cols = pl.ds(pl.multiple_of(part * width + s * half, 128), half)
        pre.append(pltpu.make_async_copy(wq_hbm.at[:, cols], wq_own.at[:, pl.ds(part * half, half)], loc_sem.at[part]))
    late = []
    for part in range(3):
        cols = pl.ds(pl.multiple_of(part * width + s * half, 128), half)
        late.append(pltpu.make_async_copy(qu_hbm.at[:, cols], qu.at[:, pl.ds(part * half, half)], loc_sem.at[3 + part]))
    for n, (src, dst) in enumerate(((g_hbm, g), (u1_hbm, u1), (d1_hbm, d1), (u2_hbm, u2), (d2_hbm, d2))):
        late.append(pltpu.make_async_copy(src, dst, loc_sem.at[6 + n]))
    for copy in pre + late:
        copy.start()
    net.plane_barrier()

    def x_copy(i):
        part = pl.ds(i * chunk, chunk)
        return pltpu.make_async_remote_copy(
            src_ref=x_ref.at[part, :], dst_ref=xp.at[part, :], send_sem=xs_sem.at[i], recv_sem=xr_sem.at[i],
            device_id=net.partner, device_id_type=MESH)

    for i in range(2):
        x_copy(i).start()
    for copy in pre:
        copy.wait()

    def square(n):
        return w1.at[pl.ds(0, n * 64), pl.ds(0, half)] if n <= 16 else w1.at[pl.ds(0, n * 32), pl.ds(0, 2 * half)]

    def block(n, src, piece, plane=2, some=square):
        return Block(src, piece, some, [g_sem.at[k, n] for k in range(N_SEMS)], g_own.at[n], plane)

    def wq_part(part):
        cols = pl.ds(part * half, half)
        return block(1 + part, wq_own.at[:, cols], lambda b: wq.at[pl.ds(b * rb, rb), cols])

    def wp_part(part):
        cols = pl.ds(part * half, half)
        return block(4 + part, wp_hbm.at[:, cols], lambda b: wp.at[pl.ds(b * rb, rb), cols], part)

    sub = fr2 // N_FC2

    def times(j, size):
        return j * size if isinstance(j, int) else pl.multiple_of(j * size, size)

    def item(n):
        if isinstance(n, int) and n < FIRST:
            if n == 0:
                return block(0, vec_ref, lambda b: vecf.at[pl.ds(b * 16, 16), :], 2,
                             lambda n: vecf.at[pl.ds(0, n * 16), :])
            return wq_part(n - 1) if n < 4 else wp_part(n - 4)
        if isinstance(n, int):
            return fc2_it(n - FIRST) if n < FIRST + N_FC2 else fc1_it(n - FIRST - N_FC2)
        return fc1_it(n - FIRST - N_FC2)

    def fc2_it(j):
        at = pl.ds(times(j, sub), sub)
        return block(FIRST + j, w2_hbm.at[at, :], lambda b: w2.at[pl.ds(b * fr2 + times(j, sub), sub), :],
                     (0, 1, 2, 2)[j], lambda n: w2.at[pl.ds(0, n * sub), :])

    def fc1_it(j):
        cols = pl.ds(times(j, FFB), FFB)
        return block(FIRST + N_FC2 + j, w1_hbm.at[:, cols], lambda b: w1.at[pl.ds(b * fr1, fr1), cols],
                     (PLANES[j] if isinstance(j, int) else jnp.where(j // 2 == 1, j % 2, 2)))

    gather = Gather(net)
    stages = {"S": gather.start, "A": gather.from_z, "B": gather.from_x, "Y": gather.from_seq, "C": gather.from_core}

    def go(*steps):
        for step in steps:
            stages[step[0]](item(int(step[1:])))

    go("S0", "S1", "S2")
    image = Image(seg_ref, id_ref)
    zeros = jnp.zeros((PAD, 128), BF16)
    opad[0:PAD, :] = zeros
    opad[PAD + WINDOW:2 * PAD + WINDOW, :] = zeros
    go("A0", "A1", "S3", "A2", "S4", "S5", "B0", "B1", "A3", "S6", "S7", "B2")
    for copy in late:
        copy.wait()
    go("B3", "C0", "C1", "C2", "C3")

    gain1 = full_vector(vecf, 0)
    shift1 = full_vector(vecf, 1)

    def project(src, src_row, row):
        v = src[pl.ds(src_row, chunk), :].astype(F32)
        h, unused = norm_parts(v)
        normed = (h * gain1 + shift1).astype(BF16)
        at = pl.ds(row, chunk)
        n1[at, :] = normed
        inner = (mm(normed, qd_ref[...]) * image.select(row, chunk)).astype(BF16)
        c1[at, :] = inner
        for part in range(3):
            cols = pl.ds(part * half, half)
            qkv[at, cols] = (mm(normed, wq[:, cols]) + mm(inner, qu[:, cols])).astype(BF16)

    def own_rows_in(i):
        project(x_ref, i * chunk, pl.multiple_of(s * rows + i * chunk, chunk))

    def partner_rows_in(i):
        x_copy(i).wait_recv()
        project(xp, i * chunk, pl.multiple_of(other * rows + i * chunk, chunk))

    own_rows_in(0)
    go("A4", "A5", "S8")
    own_rows_in(1)
    partner_rows_in(0)
    partner_rows_in(1)
    go("B4", "B5", "A6", "A7", "S9")
    outs = []

    def put(src, dst):
        copy = pltpu.make_async_copy(src, dst, out_sem.at[len(outs)])
        copy.start()
        outs.append(copy)

    put(vecf, vecf_out)
    for src, dst in ((qkv, qkvw), (n1, n1w), (c1, c1w)):
        step = min(src.shape[1], 512)

        @pl.loop(0, src.shape[1] // step)
        def _(n, src=src, dst=dst, step=step):
            cols = pl.ds(pl.multiple_of(n * step, step), step)
            dst[:, cols] = image.choose(lambda at: src[at:at + WINDOW, cols])
    bias = jnp.where(image.inside((1, WINDOW), 1), 0.0, masked_score).astype(F32)
    halves = lane_halves()

    def prob_copy(pair):
        slot = lax.rem(pair, 2)
        return pltpu.make_async_copy(prob.at[slot], prob_out.at[pl.ds(2 * pair, 2)], prob_sem.at[slot])

    def att_copy(pair):
        cols = pl.ds(pl.multiple_of(s * half + pair * 128, 128), 128)
        return pltpu.make_async_remote_copy(
            src_ref=sendb.at[pair], dst_ref=att.at[:, cols], send_sem=as_sem.at[pair], recv_sem=ar_sem.at[pair],
            device_id=net.partner, device_id_type=MESH)

    def to_partner(src, dst, send, recv):
        return pltpu.make_async_remote_copy(src_ref=src, dst_ref=dst, send_sem=send, recv_sem=recv,
                                            device_id=net.partner, device_id_type=MESH)

    pairs = half // 128

    @pl.loop(0, pairs)
    def _(pair):
        def cols(part):
            return pl.ds(pl.multiple_of(part * half + pair * 128, 128), 128)

        for n, steps in enumerate(((), ("Y4", "Y5"), ("A8", "S10", "S11"), ("C4", "C5"))):
            @pl.when(pair == n)
            def _(steps=steps):
                go(*steps)

        k2 = qkvw[:, cols(1)]
        v2 = qkvw[:, cols(2)]
        vs = [(v2 * hm.astype(BF16)) for hm in halves]
        slot = lax.rem(pair, 2)

        @pl.when(pair >= 2)
        def _():
            prob_copy(pair).wait()

        @pl.loop(0, WINDOW // QROWS)
        def _(b):
            r0 = pl.multiple_of(b * QROWS, QROWS)
            q2 = qkvw[pl.ds(r0, QROWS), cols(0)]
            q2 = q2 * jnp.asarray(HEAD_DIM ** (-0.5), BF16)
            total = None
            for hd in range(2):
                scores = mm_nt(q2 * halves[hd].astype(BF16), k2) + bias
                weights = jnp.exp(scores - jnp.max(scores, axis=1, keepdims=True))
                weights = (weights * (1.0 / jnp.sum(weights, axis=1, keepdims=True))).astype(BF16)
                prob[slot, hd, pl.ds(r0, QROWS), :] = weights
                part = mm(weights, vs[hd])
                total = part if total is None else total + part
            total = (total * image.inside((QROWS, 1), 0, r0).astype(F32)).astype(BF16)
            opad[pl.ds(PAD + r0, QROWS), :] = total
            oh[pl.ds(r0, QROWS), cols(0)] = total

        prob_copy(pair).start()

        def own_rows(who):
            return image.choose(lambda at: opad[pl.ds(pl.multiple_of(who * rows + PAD - at, STEP), rows), :])

        sendb[pair] = own_rows(other)
        att_copy(pair).start()
        att[:, pl.ds(pl.multiple_of(s * half + pair * 128, 128), 128)] = own_rows(s)

    go("B6", "B7")

    @pl.loop(0, pairs)
    def _(pair):
        att_copy(pair).wait_recv()

    go("A9", "S12", "S13")
    bias_p = full_vector(vecf, 2)
    gain2 = full_vector(vecf, 3)
    shift2 = full_vector(vecf, 4)

    @pl.loop(0, 2)
    def _(i):
        at = pl.ds(pl.multiple_of(i * chunk, chunk), chunk)
        rows_in = att[at, :]
        own_select = image.select(s * rows + i * chunk, chunk)
        inner = (mm(rows_in, pd_ref[...]) * own_select).astype(BF16)
        c2[at, :] = inner
        branch = mm(rows_in, wp[...]) + mm(inner, pu_ref[...]) + bias_p
        middle = x_ref[at, :].astype(F32) + branch
        mid[at, :] = middle
        h, unused = norm_parts(middle)
        normed = (h * gain2 + shift2).astype(BF16)
        n2[at, :] = normed
        c = mm(normed, d1[...]) * own_select
        e = mm_nt(g[at, :], u2[...]) * own_select
        c3[at, :] = c.astype(BF16)
        e4[at, :] = e.astype(BF16)
        oacc[at, :] = jnp.zeros((chunk, width), F32)
        gacc[at, :] = jnp.zeros((chunk, width), F32)
        u4[at, :] = jnp.zeros((chunk, 128), F32)
        e3[at, :] = jnp.zeros((chunk, 128), F32)

    c3t[...] = c3[...].T
    e4t[...] = e4[...].T
    go("B8", "A10", "S14", "Y6", "Y7", "B9", "A11", "S15", "C6", "C7", "C8", "C9", "B10", "A12", "A13", "S16", "S17")

    @pl.loop(0, N_FC1)
    def _(j):
        gather.from_core(fc1_it(j))
        bias = jnp.concatenate([vecf[pl.ds(2 * j * 16 + 6, 1), :], vecf[pl.ds(2 * j * 16 + 7, 1), :],
                                vecf[pl.ds((2 * j + 1) * 16 + 6, 1), :], vecf[pl.ds((2 * j + 1) * 16 + 7, 1), :]], axis=1)
        col = pl.ds(pl.multiple_of(j * FFB, FFB), FFB)

        for at in [pl.ds(0, rows)]:
            hidden = mm(n2[at, :], w1[:, col]) + mm(c3[at, :], u1[:, col]) + bias
            grad_active = mm_nt(g[at, :], w2[col, :]) + mm_nt(e4[at, :], d2[col, :])
            cdf = 0.5 * (1.0 + lax.erf(hidden * (0.5 ** 0.5)))
            pdf = jnp.exp(hidden * hidden * -0.5) * (0.5 / 3.141592653589793) ** 0.5
            active = (hidden * cdf).astype(BF16)
            act_s[at, :] = active
            grad_hidden = (grad_active * (cdf + hidden * pdf)).astype(BF16)
            gh_s[at, :] = grad_hidden
            oacc[at, :] += mm(active, w2[col, :])
            u4[at, :] += mm(active, d2[col, :])
            gacc[at, :] += mm_nt(grad_hidden, w1[:, col])
            e3[at, :] += mm_nt(grad_hidden, u1[:, col])

        @pl.when(j + 4 < N_FC1)
        def _():
            gather.from_z(fc1_it(j + 4))

        @pl.when(j == 0)
        def _():
            gather.from_x(fc1_it(1))

        @pl.when(j + 2 < N_FC1)
        def _():
            gather.from_x(fc1_it(j + 2))

        @pl.when(j + 1 < N_FC1)
        def _():
            gather.from_seq(fc1_it(j + 1))

        gr[:, col] = compact_rows(mm(c3t[...], gh_s[...]))
        gr[:, pl.ds(pl.multiple_of(ff + j * FFB, FFB), FFB)] = compact_rows(mm(e4t[...], act_s[...]))
        for first in (0, ff):
            cols = pl.ds(pl.multiple_of(first + j * FFB, FFB), FFB)
            to_partner(gr.at[:, cols], gr_in.at[:, cols], fs_sem.at[0], fr_sem.at[0]).start()

    bias2 = full_vector(vecf, 5)
    for n in range(FIRST + N_FC2):
        gather.finish(item(n))

    @pl.loop(0, N_FC1)
    def _(j):
        gather.finish(fc1_it(j))

    for pair in range(pairs - 2, pairs):
        prob_copy(pair).wait()

    def prob_load(pair):
        slot = lax.rem(pair, 2)
        return pltpu.make_async_copy(prob_out.at[pl.ds(2 * pair, 2)], prob.at[slot], prob_sem.at[slot])

    for pair in range(2):
        prob_load(pair).start()

    g1 = n1
    e2 = u4

    def grad_att(at, who):
        heads = pl.ds(pl.multiple_of(who * half, half), half)
        return (mm_nt(g1[at, :], wp[heads, :]) + mm_nt(e2[at, :].astype(BF16), pd_ref[heads, :])).astype(BF16)

    def d_copy(pair):
        cols = pl.ds(pair * 128 if isinstance(pair, int) else pl.multiple_of(pair * 128, 128), 128)
        return to_partner(n1.at[pl.ds(rows, rows), cols],
                          do_s.at[pl.ds(pl.multiple_of(s * rows, rows), rows), cols], ds_sem.at[pair], dr_sem.at[pair])

    @pl.loop(0, 2)
    def _(i):
        at = pl.ds(pl.multiple_of(i * chunk, chunk), chunk)
        own_select = image.select(s * rows + i * chunk, chunk)
        c = (u4[at, :] * own_select).astype(BF16)
        e = (e3[at, :] * own_select).astype(BF16)
        c3[at, :] = c
        e4[at, :] = e
        grad_n2 = gacc[at, :] + mm_nt(e, d1[...])
        grad_mid = g[at, :].astype(F32) + norm_grad(mid[at, :], gain2, grad_n2)
        gacc[at, :] = grad_mid
        low = grad_mid.astype(BF16)
        g1[at, :] = low
        e2[at, :] = mm_nt(low, pu_ref[...]) * own_select
        n1[pl.ds(pl.multiple_of(rows + i * chunk, chunk), chunk), 0:half] = grad_att(at, other)

    for pair in range(pairs):
        d_copy(pair).start()

    cols0 = 2 * ff
    cols1 = 4 * width
    gr[:, cols0:cols0 + width] = compact_rows(mm_tn(e4[...], n2[...]))
    gr[:, cols0 + width:cols0 + 2 * width] = compact_rows(mm_tn(c3[...], g[...]))
    gr[:, cols0 + 2 * width:cols0 + 3 * width] = compact_rows(mm_tn(c2[...], g1[0:rows, :]))
    gr[:, cols0 + 3 * width:cols0 + 4 * width] = compact_rows(mm_tn(e2[...].astype(BF16), att[...]))
    rest = pl.ds(cols0, cols1)
    rest_copy = to_partner(gr.at[:, rest], gr_in.at[:, rest], fs_sem.at[1], fr_sem.at[1])
    rest_copy.start()

    @pl.loop(0, 2)
    def _(i):
        at = pl.ds(pl.multiple_of(i * chunk, chunk), chunk)
        do_s[pl.ds(pl.multiple_of(s * rows + i * chunk, chunk), chunk), :] = grad_att(at, s)

    own0, own1 = cols0 // 16, cols1 // 16
    pick = adapter_rows(vecf)

    def turn_start(n, src, first, dst, cols):
        mine = pl.ds(pl.multiple_of(net.f * 16, 16), 16)

        @pl.loop(1, 16)
        def _(d):
            peer = (net.f + d) % 16
            pltpu.make_async_remote_copy(
                src_ref=src.at[:, pl.ds(pl.multiple_of(first + peer * cols, 128), cols)], dst_ref=dst.at[mine, :],
                send_sem=t_send.at[n], recv_sem=t_recv.at[n], device_id={"fsdp": peer}, device_id_type=MESH).start()

        dst[mine, :] = src[:, pl.ds(pl.multiple_of(first + net.f * cols, 128), cols)]

    def turn_total(n, dst):
        return pltpu.make_async_remote_copy(
            src_ref=dst.at[0:240, :], dst_ref=dst.at[0:240, :], send_sem=t_send.at[n], recv_sem=t_recv.at[n],
            device_id=net.c_peer, device_id_type=MESH)

    def result(n, src, first, step):
        return Block(src, lambda b: gall.at[:, pl.ds(pl.multiple_of(first + b * step, 128), 256)],
                     lambda m: gall.at[:, pl.ds(0, m * 256)], [g_sem.at[k, N_ITEMS + n] for k in range(N_SEMS)],
                     g_own.at[N_ITEMS + n])

    results = [result(0, dense0.at[:, pl.ds(0, 256)], 0, own0), result(1, dense0.at[:, pl.ds(256, 256)], 256, own0),
               result(2, dense1, cols0, own1), result(3, dense2, cols0 + cols1, own1)]

    def move(*steps):
        for step in steps:
            stages[step[0]](results[int(step[1:])])

    first_cols = pl.ds(0, cols0)
    first_copy = to_partner(gr.at[:, first_cols], gr_in.at[:, first_cols], fs_sem.at[0], fr_sem.at[0])
    first_copy.wait_recv()
    gr_sum[:, 0:cols0] = (gr[:, 0:cols0].astype(F32) + gr_in[:, 0:cols0].astype(F32)).astype(BF16)
    turn_start(0, gr_sum, 0, parts0, own0)

    @pl.loop(0, 2)
    def _(i):
        at = pl.ds(pl.multiple_of(i * chunk, chunk), chunk)
        branch = oacc[at, :] + mm(c3[at, :], u2[...]) + bias2
        xp[at, :] = (mid[at, :] + branch).astype(BF16)

    put(xp, out_out)
    put(gacc, gm_out)
    gpad = w2
    zeros = jnp.zeros((PAD, width), BF16)
    gpad[0:PAD, :] = zeros
    gpad[PAD + WINDOW:2 * PAD + WINDOW, :] = zeros
    last_own[...] = jnp.zeros_like(last_own)
    gq = w1
    scale = HEAD_DIM ** (-0.5)
    keep = image.inside((WINDOW, 1), 0).astype(BF16)

    @pl.loop(0, pairs)
    def _(pair):
        @pl.when(pair == 1)
        def _():
            turn_total(0, parts0).wait_recv()
            dense0[...] = mm(pick, parts0[...]).astype(BF16)
            move("S0", "S1")

        @pl.when(pair == 3)
        def _():
            rest_copy.wait_recv()
            gr_sum[:, cols0:cols0 + cols1] = (gr[:, cols0:cols0 + cols1].astype(F32)
                                              + gr_in[:, cols0:cols0 + cols1].astype(F32)).astype(BF16)
            turn_start(1, gr_sum, cols0, parts1, own1)

        def cols(part):
            return pl.ds(pl.multiple_of(part * half + pair * 128, 128), 128)

        prob_load(pair).wait()
        d_copy(pair).wait_recv()
        slot = lax.rem(pair, 2)
        k2 = qkvw[:, cols(1)]
        v2 = qkvw[:, cols(2)]
        q2 = qkvw[:, cols(0)] * jnp.asarray(scale, BF16)
        do2 = image.choose(lambda at: do_s[at:at + WINDOW, cols(0)]) * keep
        inner = do2.astype(F32) * oh[:, cols(0)].astype(F32)
        gv = gk = gqq = None
        for hd in range(2):
            hm = halves[hd].astype(BF16)
            weights = prob[slot, hd]
            grad_p = mm_nt(do2 * hm, v2)
            row_inner = jnp.sum(inner * halves[hd], axis=1, keepdims=True)
            grad_s = (weights.astype(F32) * (grad_p - row_inner)).astype(BF16)
            dv = mm_tn(weights, do2 * hm)
            dk = mm_tn(grad_s, q2 * hm)
            dq = mm(grad_s, k2 * hm)
            gv = dv if gv is None else gv + dv
            gk = dk if gk is None else gk + dk
            gqq = dq if gqq is None else gqq + dq

        @pl.when(pair + 2 < pairs)
        def _():
            prob_load(pair + 2).start()

        gq[0:WINDOW, cols(0)] = (gqq * scale).astype(BF16)
        gq[0:WINDOW, cols(1)] = gk.astype(BF16)
        gq[0:WINDOW, cols(2)] = gv.astype(BF16)

    three = slice(0, 3 * half)
    c1[0:WINDOW, :] = (mm_nt(gq[0:WINDOW, three], qu[...]) * image.select_window(0, WINDOW)).astype(BF16)
    up = compact_rows(mm_tn(c1w[...], gq[0:WINDOW, three]))
    for part in range(3):
        last_own[:, pl.ds(pl.multiple_of(part * width + s * half, 128), half)] = up[:, part * half:(part + 1) * half]
    last_own[:, 3 * width:4 * width] = compact_rows(mm_tn(c1[0:WINDOW, :], n1w[...]))
    last_copy = to_partner(last_own, last_in, fs_sem.at[2], fr_sem.at[2])
    last_copy.start()
    move("A0", "A1")

    @pl.loop(0, 2)
    def _(i):
        at = pl.ds(pl.multiple_of(i * QROWS, QROWS), QROWS)
        gpad[pl.ds(pl.multiple_of(PAD + i * QROWS, STEP), QROWS), :] = (
            mm_nt(gq[at, three], wq[...]) + mm_nt(c1[at, :], qd_ref[...])).astype(BF16)

    def rows_of(who, i):
        return image.choose(lambda at: gpad[pl.ds(pl.multiple_of(who * rows + PAD + i * chunk - at, STEP), chunk), :])

    spot = 2 * PAD + WINDOW + 128

    def p_copy(i):
        return to_partner(gpad.at[pl.ds(spot + i * chunk, chunk), :], prcv.at[i], ps_sem.at[i], pr_sem.at[i])

    for i in range(2):
        gpad[spot + i * chunk:spot + (i + 1) * chunk, :] = rows_of(other, i)
        p_copy(i).start()
    last_copy.wait_recv()
    last_sum[...] = (last_own[...].astype(F32) + last_in[...].astype(F32)).astype(BF16)
    turn_start(2, last_sum, 0, parts2, own1)
    turn_total(1, parts1).wait_recv()
    dense1[...] = mm(pick, parts1[...]).astype(BF16)
    move("B0", "S2", "B1")
    turn_total(2, parts2).wait_recv()
    dense2[...] = mm(pick, parts2[...]).astype(BF16)
    move("S3", "C0", "A2", "C1", "A3", "B2", "C2", "B3")
    gn = oacc
    for i in range(2):
        p_copy(i).wait_recv()
        at = slice(i * chunk, (i + 1) * chunk)
        gn[at, :] = prcv[i].astype(F32) + rows_of(s, i).astype(F32)
        put(gn.at[at, :], gn_out.at[at, :])
    move("C3")
    for copy in outs:
        copy.wait()
    for i in range(2):
        x_copy(i).wait_send()
        p_copy(i).wait_send()
    for copy in (first_copy, rest_copy, last_copy):
        copy.wait_send()
    for n, dst in enumerate((parts0, parts1, parts2)):
        turn_total(n, dst).wait_send()
    for it in results:
        gather.finish(it)

    @pl.loop(0, pairs)
    def _(pair):
        att_copy(pair).wait_send()
        d_copy(pair).wait_send()


def any_spec():
    return pl.BlockSpec(memory_space=pl.ANY)


def vmem_spec():
    return pl.BlockSpec(memory_space=pltpu.VMEM)


def adapter_rows(vec_ref):
    ids = jnp.concatenate([jnp.broadcast_to(vec_ref[16 * p + 8:16 * p + 9, :], (16, 128)) for p in range(16)], axis=0)
    r = lax.broadcasted_iota(jnp.int32, (256, 128), 0) % 16
    col = lax.broadcasted_iota(jnp.int32, (256, 128), 1)
    group = (col // 16).astype(F32)
    return ((ids == group) & (r == col % 16)).astype(F32).T.astype(BF16)


def run_block(seg, ident, x, vec, qd, pd, pu, wq, wp, w1, w2, qu, g, u1, d1, u2, d2):
    rows, width = x.shape
    toks = seg.shape[1]
    half = width // 2
    ff = w1.shape[1]
    chunk = rows // 2
    dma = pltpu.SemaphoreType.DMA
    sds = jax.ShapeDtypeStruct
    gcols = 2 * ff + 4 * width
    last = 4 * width
    out_shape = (
        sds((256, 128), F32), sds((half // 64, WINDOW, WINDOW), BF16), sds((rows, width), F32), sds((rows, width), BF16),
        sds((128, gcols + last), BF16), sds((rows, width), F32))

    def low(*shape):
        return pltpu.VMEM(shape, BF16)

    def full(*shape):
        return pltpu.VMEM(shape, F32)

    scratch = [
        low(wq.shape[0], 3 * half), low(width, 3 * half), low(width, width), low(width, ff), low(ff, width),
        low(rows, width), full(256, 128), low(128, 3 * half), low(rows, width), low(128, ff), low(width, 128),
        low(128, width), low(ff, 128), low(toks, 3 * half), low(toks, width), low(toks, 128),
        low(WINDOW, 3 * half), low(WINDOW, width), low(WINDOW, 128), low(2, 2, WINDOW, WINDOW), low(2 * PAD + WINDOW, 128),
        low(half // 128, rows, 128), low(WINDOW, half), low(rows, width), low(rows, 128), full(rows, width), low(rows, width),
        full(rows, width), full(rows, width), full(rows, 128), full(rows, 128), low(rows, 128), low(rows, 128),
        low(128, rows), low(128, rows), low(rows, FFB), low(rows, FFB), low(16, gcols),
        low(toks, half), low(16, gcols), low(16, gcols), low(16, last), low(16, last), low(16, last),
        low(256, 2 * ff // 16), low(256, last // 16), low(256, last // 16), low(128, 2 * ff // 16), low(128, last // 16),
        low(128, last // 16), low(2, chunk, width),
        dma((2,)), dma((2,)), dma((4,)), dma((4,)), dma((11,)), dma((12,)), dma((2,)),
        dma((N_SEMS, N_ITEMS + 4)), dma((N_ITEMS + 4,)),
        dma((4,)), dma((4,)), dma((3,)), dma((3,)), dma((2,)), dma((2,)), dma((3,)), dma((3,))]
    return pl.pallas_call(
        block_kernel, out_shape=out_shape, in_specs=[vmem_spec()] * 7 + [any_spec()] * 10,
        out_specs=tuple(any_spec() for unused in out_shape), scratch_shapes=scratch,
        compiler_params=pltpu.CompilerParams(collective_id=1, has_side_effects=True, vmem_limit_bytes=VMEM_LIMIT),
        name="block")(seg, ident, x, vec, qd, pd, pu, wq, wp, w1, w2, qu, g, u1, d1, u2, d2)


def expand_kernel(vec_ref, f1u, f2d, f1d, f2u, pu, pdn, qu, qd, gn, x, gm, out,
                  out_out, gt_out, qd_out, qu_out, pd_out, pu_out, f1d_out, f1u_out, f2d_out, f2u_out):
    for src, dst in ((f1u, f1u_out), (f2u, f2u_out), (pu, pu_out), (qu, qu_out)):
        dst[...] = src[...].astype(F32)
    for src, dst in ((f1d, f1d_out), (f2d, f2d_out), (pdn, pd_out), (qd, qd_out)):
        dst[...] = src[...].T.astype(F32)
    out_out[...] = out[...]
    gain1 = full_vector(vec_ref, 0)
    gt_out[...] = gm[...] + norm_grad(x[...].astype(F32), gain1, gn[...])


def run_expand(vec, gall, gn, x, gm, out):
    rows, width = gn.shape
    ff = 4 * width
    n = 2
    sds = jax.ShapeDtypeStruct

    def part(cols, offset):
        return pl.BlockSpec((128, cols), lambda j: (0, offset // cols + j))

    def by_row(shape):
        return pl.BlockSpec(shape, lambda j: (j, 0))

    def by_col(shape):
        return pl.BlockSpec(shape, lambda j: (0, j))

    q = width // n
    return pl.pallas_call(
        expand_kernel, grid=(n,),
        out_shape=(sds((rows, width), BF16), sds((rows, width), F32), sds((width, 128), F32), sds((128, 3 * width), F32), sds((width, 128), F32),
                   sds((128, width), F32), sds((width, 128), F32), sds((128, ff), F32), sds((ff, 128), F32), sds((128, width), F32)),
        in_specs=[pl.BlockSpec((256, 128), lambda j: (0, 0)), part(ff // n, 0), part(ff // n, ff), part(q, 2 * ff),
                  part(q, 2 * ff + width), part(q, 2 * ff + 2 * width), part(q, 2 * ff + 3 * width),
                  part(3 * q, 2 * ff + 4 * width), part(q, 2 * ff + 7 * width),
                  by_row((rows // n, width)), by_row((rows // n, width)), by_row((rows // n, width)), by_row((rows // n, width))],
        out_specs=(by_row((rows // n, width)), by_row((rows // n, width)), by_row((q, 128)), by_col((128, 3 * q)), by_row((q, 128)), by_col((128, q)),
                   by_row((q, 128)), by_col((128, ff // n)), by_row((ff // n, 128)), by_col((128, q))),
        compiler_params=pltpu.CompilerParams(vmem_limit_bytes=VMEM_LIMIT),
        name="expand")(vec, *([gall] * 8), gn, x, gm, out)


def per_device_fast(tokens, grad_out, segments, padding, adapter_ids, norm1_gain, norm1_bias, w_qkv, w_proj, proj_bias,
                    norm2_gain, norm2_bias, w_fc1, fc1_bias, w_fc2, fc2_bias, qkv_down, qkv_up, proj_down, proj_up,
                    fc1_down, fc1_up, fc2_down, fc2_up):
    x = tokens[0]
    odd = (lax.axis_index("fsdp") % 2).astype(F32)
    six = jnp.stack([norm1_gain, norm1_bias, proj_bias, norm2_gain, norm2_bias, fc2_bias]).astype(F32)
    vec = jnp.concatenate([
        jnp.concatenate([six * (1.0 - odd), six * odd], axis=1), fc1_bias.astype(F32).reshape(2, 128),
        jnp.broadcast_to(adapter_ids[0].astype(F32)[:, None], (1, 128)), jnp.zeros((7, 128), F32)], axis=0)
    vecf, unused, gm, out, gall, gn = run_block(
        segments, adapter_ids, x, vec, qkv_down, proj_down, proj_up, w_qkv, w_proj, w_fc1, w_fc2, qkv_up,
        grad_out[0], fc1_up, fc1_down, fc2_up, fc2_down)
    out, gt, gqd, gqu, gpd, gpu, gf1d, gf1u, gf2d, gf2u = run_expand(vecf, gall, gn, x, gm, out)
    return out[None], gt[None], gqd, gqu, gpd, gpu, gf1d, gf1u, gf2d, gf2u


def solution(mesh):
    sizes = dict(mesh.shape)
    small = sizes == {"seq": 2, "fsdp": 16}

    def per_device_any(*args):
        tokens, adapter_ids = args[0], args[4]
        one_image = tokens.shape[1:] == (512, 1024) and adapter_ids.shape[1] == 1
        return (per_device_fast if small and one_image else per_device)(*args)

    return jax.shard_map(
        per_device_any,
        mesh=mesh,
        in_specs=(
            P("fsdp", "seq", None),
            P("fsdp", "seq", None),
            P("fsdp", None),
            P("fsdp", None),
            P("fsdp", None),
            P("fsdp"),
            P("fsdp"),
            P("fsdp", None),
            P("fsdp", None),
            P("fsdp"),
            P("fsdp"),
            P("fsdp"),
            P("fsdp", None),
            P("fsdp"),
            P("fsdp", None),
            P("fsdp"),
            P(),
            P(),
            P(),
            P(),
            P(),
            P(),
            P(),
            P(),
        ),
        out_specs=(
            P("fsdp", "seq", None),
            P("fsdp", "seq", None),
            P(),
            P(),
            P(),
            P(),
            P(),
            P(),
            P(),
            P(),
        ),
        check_vma=False,
    )
```

```python
from functools import partial

import jax
import jax.numpy as jnp
from jax import lax
from jax.experimental import pallas as pl
from jax.experimental.pallas import tpu as pltpu
from jax.sharding import PartitionSpec as P

HEAD_DIM = 64
IMG = 577
RANK = 16
QBLOCK = 512


norm_eps = 1e-06
masked_score = -1e30


def matmul(left_side, right_side):
    return jnp.dot(left_side, right_side, preferred_element_type=jnp.float32)


def matmul_nt(left_side, right_side):
    return jnp.einsum("tk,jk->tj", left_side, right_side, preferred_element_type=jnp.float32)


def matmul_tn(left_side, right_side):
    return jnp.einsum("ti,to->io", left_side, right_side, preferred_element_type=jnp.float32)


def layer_norm(values, norm_gain, norm_shift):
    centre = jnp.mean(values, axis=-1, keepdims=True)
    centred = values - centre
    spread = jnp.mean(centred * centred, axis=-1, keepdims=True)
    return centred * lax.rsqrt(spread + norm_eps) * norm_gain + norm_shift


def norm_backward(values, norm_gain, norm_shift, grad_in):

    def apply_norm(inputs):
        return layer_norm(inputs, norm_gain, norm_shift)

    unused, pullback = jax.vjp(apply_norm, values)
    return pullback(grad_in)[0]


def selection(seg_own, image_adapters, columns):
    images = jnp.arange(image_adapters.shape[0], dtype=jnp.int32)
    image_match = seg_own[:, None] - 1 == images[None, :]
    token_adapter = jnp.sum(jnp.where(image_match, image_adapters[None, :], 0), axis=1)
    present = jnp.any(image_match, axis=1)
    column = jnp.arange(columns, dtype=jnp.int32) // RANK
    chosen = (token_adapter[:, None] == column[None, :]) & present[:, None]
    return chosen.astype(jnp.float32)


def adapter_forward(inputs_b, weight, down_map, up_map, select):
    inner_term = (matmul(inputs_b, down_map) * select).astype(jnp.bfloat16)
    return (matmul(inputs_b, weight) + matmul(inner_term, up_map), inner_term)


def adapter_backward(inputs_b, inner_term, grad_in, weight, down_map, up_map, select):
    grad_up = matmul_tn(inner_term, grad_in)
    grad_inner = (matmul_nt(grad_in, up_map) * select).astype(jnp.bfloat16)
    grad_down = matmul_tn(inputs_b, grad_inner)
    grad_inputs = matmul_nt(grad_in, weight) + matmul_nt(grad_inner, down_map)
    return (grad_inputs, grad_down, grad_up)


def block_scores(query_block, key_heads, seg_block, seg_keys, keep_keys):
    score_scale = HEAD_DIM ** (-0.5)
    scores = (
        jnp.einsum("qhd,khd->hqk", query_block, key_heads, preferred_element_type=jnp.float32)
        * score_scale
    )
    allowed = (seg_block[:, None] == seg_keys[None, :]) & (keep_keys[None, :] == 1)
    return jnp.where(allowed[None, :, :], scores, masked_score)


def split_heads(head_rows):
    all_rows = head_rows.shape[0]
    local_heads = head_rows.shape[2] // HEAD_DIM
    query_heads = head_rows[:, 0].reshape(all_rows, local_heads, HEAD_DIM)
    key_heads = head_rows[:, 1].reshape(all_rows, local_heads, HEAD_DIM)
    value_heads = head_rows[:, 2].reshape(all_rows, local_heads, HEAD_DIM)
    return (query_heads, key_heads, value_heads)


def key_window(all_rows):
    return min(all_rows, (QBLOCK + 2 * IMG - 2 + 127) // 128 * 128)


def window_start(block_index, all_rows, window):
    first = block_index * QBLOCK - (IMG - 1)
    return jnp.clip(first, 0, all_rows - window)


def attention_forward(head_rows, seg_all, keep_all):
    all_rows = head_rows.shape[0]
    block_count = all_rows // QBLOCK
    window = key_window(all_rows)
    query_heads, key_heads, value_heads = split_heads(head_rows)
    local_heads = query_heads.shape[1]

    def one_block(block_parts):
        query_block, seg_block, keep_block, block_index = block_parts
        start = window_start(block_index, all_rows, window)
        keys_near = lax.dynamic_slice_in_dim(key_heads, start, window, 0)
        values_near = lax.dynamic_slice_in_dim(value_heads, start, window, 0)
        seg_near = lax.dynamic_slice_in_dim(seg_all, start, window, 0)
        keep_near = lax.dynamic_slice_in_dim(keep_all, start, window, 0)
        scores = block_scores(query_block, keys_near, seg_block, seg_near, keep_near)
        row_max = jnp.max(scores, axis=2, keepdims=True)
        weights = jnp.exp(scores - row_max)
        row_sum = jnp.sum(weights, axis=2, keepdims=True)
        probs_low = (weights / row_sum).astype(jnp.bfloat16)
        result = jnp.einsum(
            "hqk,khd->qhd", probs_low, values_near, preferred_element_type=jnp.float32
        )
        result = result * keep_block[:, None, None].astype(jnp.float32)
        return (result.astype(jnp.bfloat16), row_max, row_sum)

    block_ids = jnp.arange(block_count, dtype=jnp.int32)
    blocked = (
        query_heads.reshape(block_count, QBLOCK, local_heads, HEAD_DIM),
        seg_all.reshape(block_count, QBLOCK),
        keep_all.reshape(block_count, QBLOCK),
        block_ids,
    )
    results, block_max, block_sums = lax.map(one_block, blocked)
    return (results.reshape(all_rows, local_heads * HEAD_DIM), block_max, block_sums)


def attention_backward(head_rows, grad_rows, seg_all, keep_all, block_max, block_sums):
    all_rows = head_rows.shape[0]
    block_count = all_rows // QBLOCK
    window = key_window(all_rows)
    query_heads, key_heads, value_heads = split_heads(head_rows)
    local_heads = query_heads.shape[1]
    score_scale = HEAD_DIM ** (-0.5)

    def one_block(running, block_parts):
        grad_keys, grad_values = running
        query_block, seg_block, keep_block, grad_block, row_max, row_sum, block_index = block_parts
        start = window_start(block_index, all_rows, window)
        keys_near = lax.dynamic_slice_in_dim(key_heads, start, window, 0)
        values_near = lax.dynamic_slice_in_dim(value_heads, start, window, 0)
        seg_near = lax.dynamic_slice_in_dim(seg_all, start, window, 0)
        keep_near = lax.dynamic_slice_in_dim(keep_all, start, window, 0)
        scores = block_scores(query_block, keys_near, seg_block, seg_near, keep_near)
        probs = jnp.exp(scores - row_max) / row_sum
        grad_result = grad_block * keep_block[:, None, None].astype(jnp.bfloat16)
        values_term = jnp.einsum(
            "hqk,qhd->khd",
            probs.astype(jnp.bfloat16),
            grad_result,
            preferred_element_type=jnp.float32,
        )
        grad_probs = jnp.einsum(
            "qhd,khd->hqk", grad_result, values_near, preferred_element_type=jnp.float32
        )
        row_inner = jnp.sum(probs * grad_probs, axis=2, keepdims=True)
        grad_scores = (probs * (grad_probs - row_inner)).astype(jnp.bfloat16)
        grad_query = (
            jnp.einsum("hqk,khd->qhd", grad_scores, keys_near, preferred_element_type=jnp.float32)
            * score_scale
        )
        keys_term = (
            jnp.einsum("hqk,qhd->khd", grad_scores, query_block, preferred_element_type=jnp.float32)
            * score_scale
        )
        grad_keys = lax.dynamic_update_slice_in_dim(
            grad_keys, lax.dynamic_slice_in_dim(grad_keys, start, window, 0) + keys_term, start, 0
        )
        grad_values = lax.dynamic_update_slice_in_dim(
            grad_values,
            lax.dynamic_slice_in_dim(grad_values, start, window, 0) + values_term,
            start,
            0,
        )
        return ((grad_keys, grad_values), grad_query)

    zero_heads = jnp.zeros((all_rows, local_heads, HEAD_DIM), jnp.float32)
    block_ids = jnp.arange(block_count, dtype=jnp.int32)
    blocked = (
        query_heads.reshape(block_count, QBLOCK, local_heads, HEAD_DIM),
        seg_all.reshape(block_count, QBLOCK),
        keep_all.reshape(block_count, QBLOCK),
        grad_rows.reshape(block_count, QBLOCK, local_heads, HEAD_DIM),
        block_max,
        block_sums,
        block_ids,
    )
    (grad_keys, grad_values), grad_queries = lax.scan(one_block, (zero_heads, zero_heads), blocked)
    flat_width = local_heads * HEAD_DIM
    stacked = jnp.stack(
        [
            grad_queries.reshape(all_rows, flat_width),
            grad_keys.reshape(all_rows, flat_width),
            grad_values.reshape(all_rows, flat_width),
        ],
        axis=1,
    )
    return stacked.astype(jnp.bfloat16)


def per_device(
    tokens,
    grad_out,
    segments,
    padding,
    adapter_ids,
    norm1_gain,
    norm1_bias,
    w_qkv,
    w_proj,
    proj_bias,
    norm2_gain,
    norm2_bias,
    w_fc1,
    fc1_bias,
    w_fc2,
    fc2_bias,
    qkv_down,
    qkv_up,
    proj_down,
    proj_up,
    fc1_down,
    fc1_up,
    fc2_down,
    fc2_up,
):
    tok_rows = tokens.shape[1]
    feat_width = tokens.shape[2]
    inputs = tokens[0].astype(jnp.float32)
    seg_all = segments[0]
    keep_all = padding[0]
    offset = lax.axis_index("seq") * tok_rows
    seg_own = lax.dynamic_slice_in_dim(seg_all, offset, tok_rows)
    select = selection(seg_own, adapter_ids[0], qkv_down.shape[1])
    gain_one, shift_one, qkv_weight, proj_weight, proj_shift = (
        lax.all_gather(norm1_gain, "fsdp", axis=0, tiled=True),
        lax.all_gather(norm1_bias, "fsdp", axis=0, tiled=True),
        lax.all_gather(w_qkv, "fsdp", axis=0, tiled=True),
        lax.all_gather(w_proj, "fsdp", axis=0, tiled=True),
        lax.all_gather(proj_bias, "fsdp", axis=0, tiled=True),
    )
    gain_one = gain_one.astype(jnp.float32)
    shift_one = shift_one.astype(jnp.float32)
    normed_one = layer_norm(inputs, gain_one, shift_one).astype(jnp.bfloat16)
    qkv_main, inner_one = adapter_forward(normed_one, qkv_weight, qkv_down, qkv_up, select)
    qkv_low = qkv_main.astype(jnp.bfloat16).reshape(tok_rows, 3, feat_width)
    head_rows = lax.all_to_all(qkv_low, "seq", split_axis=2, concat_axis=0, tiled=True)
    attended_heads, block_max, block_sums = attention_forward(head_rows, seg_all, keep_all)
    attended = lax.all_to_all(attended_heads, "seq", split_axis=0, concat_axis=1, tiled=True)
    branch_one, inner_two = adapter_forward(attended, proj_weight, proj_down, proj_up, select)
    middle = inputs + (branch_one + proj_shift.astype(jnp.float32))
    gain_two, shift_two, fc1_weight, fc2_shift, fc2_weight, fc1_shift = (
        lax.all_gather(norm2_gain, "fsdp", axis=0, tiled=True),
        lax.all_gather(norm2_bias, "fsdp", axis=0, tiled=True),
        lax.all_gather(w_fc1, "fsdp", axis=0, tiled=True),
        lax.all_gather(fc2_bias, "fsdp", axis=0, tiled=True),
        lax.all_gather(w_fc2, "fsdp", axis=0, tiled=True),
        lax.all_gather(fc1_bias, "fsdp", axis=0, tiled=True),
    )
    gain_two = gain_two.astype(jnp.float32)
    shift_two = shift_two.astype(jnp.float32)
    normed_two = layer_norm(middle, gain_two, shift_two).astype(jnp.bfloat16)
    hidden_main, inner_three = adapter_forward(normed_two, fc1_weight, fc1_down, fc1_up, select)
    hidden = hidden_main + fc1_shift.astype(jnp.float32)
    active = jax.nn.gelu(hidden, approximate=False).astype(jnp.bfloat16)
    branch_two, inner_four = adapter_forward(active, fc2_weight, fc2_down, fc2_up, select)
    output = (middle + (branch_two + fc2_shift.astype(jnp.float32))).astype(jnp.bfloat16)
    fc1_back, fc2_back = (
        lax.all_gather(w_fc1, "fsdp", axis=0, tiled=True),
        lax.all_gather(w_fc2, "fsdp", axis=0, tiled=True),
    )
    grad_top = grad_out[0]
    grad_active, grad_fc2_down, grad_fc2_up = adapter_backward(
        active, inner_four, grad_top, fc2_back, fc2_down, fc2_up, select
    )
    unused, gelu_back = jax.vjp(partial(jax.nn.gelu, approximate=False), hidden)
    grad_hidden = gelu_back(grad_active)[0].astype(jnp.bfloat16)
    grad_normed_two, grad_fc1_down, grad_fc1_up = adapter_backward(
        normed_two, inner_three, grad_hidden, fc1_back, fc1_down, fc1_up, select
    )
    grad_middle = grad_top.astype(jnp.float32) + norm_backward(
        middle, gain_two, shift_two, grad_normed_two
    )
    qkv_back, proj_back = (
        lax.all_gather(w_qkv, "fsdp", axis=0, tiled=True),
        lax.all_gather(w_proj, "fsdp", axis=0, tiled=True),
    )
    grad_branch_one = grad_middle.astype(jnp.bfloat16)
    grad_attended, grad_proj_down, grad_proj_up = adapter_backward(
        attended, inner_two, grad_branch_one, proj_back, proj_down, proj_up, select
    )
    grad_head_rows = lax.all_to_all(
        grad_attended.astype(jnp.bfloat16), "seq", split_axis=1, concat_axis=0, tiled=True
    )
    grad_qkv_heads = attention_backward(
        head_rows, grad_head_rows, seg_all, keep_all, block_max, block_sums
    )
    grad_qkv = lax.all_to_all(
        grad_qkv_heads, "seq", split_axis=0, concat_axis=2, tiled=True
    ).reshape(tok_rows, 3 * feat_width)
    grad_normed_one, grad_qkv_down, grad_qkv_up = adapter_backward(
        normed_one, inner_one, grad_qkv, qkv_back, qkv_down, qkv_up, select
    )
    grad_tokens = grad_middle + norm_backward(inputs, gain_one, shift_one, grad_normed_one)
    summed = lax.psum(
        (
            grad_qkv_down,
            grad_qkv_up,
            grad_proj_down,
            grad_proj_up,
            grad_fc1_down,
            grad_fc1_up,
            grad_fc2_down,
            grad_fc2_up,
        ),
        ("seq", "fsdp"),
    )
    return (
        output[None],
        grad_tokens[None],
        summed[0],
        summed[1],
        summed[2],
        summed[3],
        summed[4],
        summed[5],
        summed[6],
        summed[7],
    )


F32 = jnp.float32
BF16 = jnp.bfloat16
MESH = pl.DeviceIdType.MESH
VMEM_LIMIT = 67_000_000


def mm(a, b):
    return lax.dot_general(a, b, (((1,), (0,)), ((), ())), preferred_element_type=F32)


def mm_nt(a, b):
    return lax.dot_general(a, b, (((1,), (1,)), ((), ())), preferred_element_type=F32)


def mm_tn(a, b):
    return lax.dot_general(a, b, (((0,), (0,)), ((), ())), preferred_element_type=F32)


def norm_parts(v):
    mean = jnp.mean(v, axis=-1, keepdims=True)
    centred = v - mean
    r = lax.rsqrt(jnp.mean(centred * centred, axis=-1, keepdims=True) + norm_eps)
    return centred * r, r


def norm_grad(v, gain, grad_y):
    h, r = norm_parts(v)
    d = grad_y * gain
    return r * (d - jnp.mean(d, axis=-1, keepdims=True) - h * jnp.mean(d * h, axis=-1, keepdims=True))


class Net:
    def __init__(self):
        self.s = lax.axis_index("seq")
        self.f = lax.axis_index("fsdp")
        self.z = self.f // 4
        self.x = (self.f // 2) % 2
        self.c = self.f % 2
        self.partner = {"seq": 1 - self.s}
        self.x_peer = {"fsdp": self.block(self.z, 1 - self.x, self.c)}
        self.c_peer = {"fsdp": self.block(self.z, self.x, 1 - self.c)}

    def block(self, z, x, c):
        return (z * 2 + x) * 2 + c

    def z_peer(self, d):
        return {"fsdp": self.block((self.z + d) % 4, self.x, self.c)}

    def meet(self, peers):
        sem = pltpu.get_barrier_semaphore()
        for peer in peers:
            pl.semaphore_signal(sem, inc=1, device_id=peer, device_id_type=MESH)
        pl.semaphore_wait(sem, len(peers))

    def plane_peer(self, d):
        return {"fsdp": (self.f + d) % 16}

    def plane_barrier(self):
        self.meet([self.partner] + [self.plane_peer(d) for d in range(1, 16)])

    def barrier(self):
        self.meet([self.partner, self.x_peer, self.c_peer] + [self.z_peer(d) for d in (1, 2, 3)])


class Block:
    def __init__(self, src, piece, some, sems, own_sem, plane=2):
        self.src, self.piece, self.some, self.plane, self.own_sem = src, piece, some, plane, own_sem
        self.sent, self.z, self.x, self.y1, self.y2, self.c = sems


N_SEMS = 6


class Gather:
    def __init__(self, net):
        self.net = net

    def send(self, it, src, block, sem, peer):
        pltpu.make_async_remote_copy(
            src_ref=src, dst_ref=it.piece(block), send_sem=it.sent, recv_sem=sem, device_id=peer,
            device_id_type=MESH).start()

    def total(self, it, n, sem):
        return pltpu.make_async_remote_copy(
            src_ref=it.some(n), dst_ref=it.some(n), send_sem=it.sent, recv_sem=sem, device_id=self.net.c_peer,
            device_id_type=MESH)

    def here(self, it, body):
        if isinstance(it.plane, int) and it.plane == 2:
            body()
        else:
            pl.when((self.net.s == it.plane) | (it.plane == 2))(body)

    def hand_on(self, it, pieces, sem):
        def body():
            for piece, block in pieces:
                self.send(it, piece, block, sem, self.net.partner)

        if not isinstance(it.plane, int):
            pl.when(it.plane != 2)(body)
        elif it.plane != 2:
            body()

    def own(self, it):
        return pltpu.make_async_copy(it.src, it.piece(self.net.f), it.own_sem)

    def column(self, it, x, ds):
        net = self.net
        blocks = [net.block((net.z + d) % 4, x, net.c) for d in ds]
        return [(it.piece(block), block) for block in blocks]

    def start(self, it):
        net = self.net

        def along():
            for d in (2, 1, 3):
                self.send(it, it.src, net.f, it.z, net.z_peer(d))
            self.send(it, it.src, net.f, it.x, net.x_peer)

        self.here(it, along)
        self.send(it, it.src, net.f, it.c, net.c_peer)
        self.own(it).start()

    def from_z(self, it):
        net = self.net

        def body():
            self.total(it, 3, it.z).wait_recv()
            pieces = self.column(it, net.x, (1, 3, 2))
            for piece, block in pieces:
                self.send(it, piece, block, it.x, net.x_peer)
            self.hand_on(it, pieces, it.y1)
            for piece, block in pieces:
                self.send(it, piece, block, it.c, net.c_peer)

        self.here(it, body)

    def from_x(self, it):
        net = self.net

        def body():
            self.total(it, 4, it.x).wait_recv()
            pieces = self.column(it, 1 - net.x, (0, 1, 3, 2))
            self.hand_on(it, pieces, it.y2)
            for piece, block in pieces:
                self.send(it, piece, block, it.c, net.c_peer)

        self.here(it, body)

    def from_seq(self, it):
        net = self.net
        if isinstance(it.plane, int) and it.plane == 2:
            return

        @pl.when((net.s != it.plane) & (it.plane != 2))
        def _():
            self.total(it, 3, it.y1).wait_recv()
            for piece, block in self.column(it, net.x, (1, 3, 2)):
                self.send(it, piece, block, it.c, net.c_peer)
            self.total(it, 4, it.y2).wait_recv()
            for piece, block in self.column(it, 1 - net.x, (0, 1, 3, 2)):
                self.send(it, piece, block, it.c, net.c_peer)

    def from_core(self, it):
        self.total(it, 8, it.c).wait_recv()
        self.own(it).wait()

    def finish(self, it):
        net = self.net
        if isinstance(it.plane, int) and it.plane == 2:
            self.total(it, 15, it.z).wait_send()
            return

        @pl.when(it.plane == 2)
        def _():
            self.total(it, 15, it.z).wait_send()

        @pl.when(net.s == it.plane)
        def _():
            self.total(it, 22, it.z).wait_send()

        @pl.when((net.s != it.plane) & (it.plane != 2))
        def _():
            self.total(it, 8, it.z).wait_send()


def full_vector(vec_ref, row, blocks=16, rows=16):
    parts = []
    for k in range(blocks // 2):
        even = vec_ref[2 * k * rows + row:2 * k * rows + row + 1, :]
        odd = vec_ref[(2 * k + 1) * rows + row:(2 * k + 1) * rows + row + 1, :]
        parts.append(even + odd)
    return jnp.concatenate(parts, axis=1)


WINDOW = 640
STEP = 64
PAD = 384
QROWS = 320
FFB = 512


class Image:
    def __init__(self, seg_ref, id_ref):
        self.start = jnp.sum((seg_ref[...] == 0).astype(F32), axis=1, keepdims=True)
        ident = id_ref[...].astype(F32)
        self.pick = []
        base = jnp.zeros((1, 1), F32)
        for k in range(PAD // STEP + 1):
            mark = ((self.start >= k * STEP) & (self.start < (k + 1) * STEP)).astype(F32)
            self.pick.append(mark)
            base = base + mark * float(k * STEP)
        self.shift = base - self.start
        lane = lax.broadcasted_iota(jnp.int32, (1, 128), 1).astype(F32)
        self.columns = ((lane >= ident * RANK) & (lane < (ident + 1) * RANK)).astype(F32)

    def choose(self, load):
        total = None
        for k, mark in enumerate(self.pick):
            value = load(k * STEP)
            value = value * mark.astype(value.dtype)
            total = value if total is None else total + value
        return total

    def inside(self, shape, axis, first=0):
        at = (lax.broadcasted_iota(jnp.int32, shape, axis) + first).astype(F32) + self.shift
        return (at >= 0) & (at < IMG)

    def select(self, first, rows):
        at = (lax.broadcasted_iota(jnp.int32, (rows, 1), 0) + first).astype(F32)
        return (at >= self.start).astype(F32) * self.columns

    def select_window(self, first, rows):
        at = (lax.broadcasted_iota(jnp.int32, (rows, 1), 0) + first).astype(F32) + self.shift
        return (at >= 0).astype(F32) * self.columns


def lane_halves():
    lane = lax.broadcasted_iota(jnp.int32, (1, 128), 1)
    return [(lane < 64).astype(F32), (lane >= 64).astype(F32)]


def compact_rows(dense):
    total = dense[0:16]
    for k in range(1, 8):
        total = total + dense[16 * k:16 * (k + 1)]
    return total.astype(BF16)


N_FC1 = 8
N_FC2 = 4
FIRST = 6
PLANES = (2, 2, 0, 1, 2, 2, 2, 2)
N_ITEMS = FIRST + N_FC2 + N_FC1


def block_kernel(seg_ref, id_ref, x_ref, vec_ref, qd_ref, pd_ref, pu_ref, wq_hbm, wp_hbm, w1_hbm, w2_hbm,
                 qu_hbm, g_hbm, u1_hbm, d1_hbm, u2_hbm, d2_hbm,
                 vecf_out, prob_out, gm_out, out_out, gall, gn_out,
                 wq_own, wq, wp, w1, w2, xp, vecf, qu, g, u1, d1, u2, d2, qkv, n1, c1, qkvw, n1w, c1w, prob, opad, sendb,
                 oh, att, c2, mid, n2, oacc, gacc, u4, e3, c3, e4, c3t, e4t, act_s, gh_s, gr,
                 do_s, gr_in, gr_sum, last_own, last_in, last_sum, parts0, parts1, parts2, dense0, dense1, dense2, prcv,
                 xs_sem, xr_sem, as_sem, ar_sem, loc_sem, out_sem, prob_sem, g_sem, g_own,
                 ds_sem, dr_sem, fs_sem, fr_sem, ps_sem, pr_sem, t_send, t_recv):
    net = Net()
    s, other = net.s, 1 - net.s
    rows, width = x_ref.shape
    half = wq.shape[1] // 3
    rb = wq_own.shape[0]
    fr1 = w1_hbm.shape[0]
    fr2 = w2_hbm.shape[0]
    ff = w1.shape[1]
    chunk = rows // 2

    pre = []
    for part in range(3):
        cols = pl.ds(pl.multiple_of(part * width + s * half, 128), half)
        pre.append(pltpu.make_async_copy(wq_hbm.at[:, cols], wq_own.at[:, pl.ds(part * half, half)], loc_sem.at[part]))
    late = []
    for part in range(3):
        cols = pl.ds(pl.multiple_of(part * width + s * half, 128), half)
        late.append(pltpu.make_async_copy(qu_hbm.at[:, cols], qu.at[:, pl.ds(part * half, half)], loc_sem.at[3 + part]))
    for n, (src, dst) in enumerate(((g_hbm, g), (u1_hbm, u1), (d1_hbm, d1), (u2_hbm, u2), (d2_hbm, d2))):
        late.append(pltpu.make_async_copy(src, dst, loc_sem.at[6 + n]))
    for copy in pre + late:
        copy.start()
    net.plane_barrier()

    def x_copy(i):
        part = pl.ds(i * chunk, chunk)
        return pltpu.make_async_remote_copy(
            src_ref=x_ref.at[part, :], dst_ref=xp.at[part, :], send_sem=xs_sem.at[i], recv_sem=xr_sem.at[i],
            device_id=net.partner, device_id_type=MESH)

    for i in range(2):
        x_copy(i).start()
    for copy in pre:
        copy.wait()

    def square(n):
        return w1.at[pl.ds(0, n * 64), pl.ds(0, half)] if n <= 16 else w1.at[pl.ds(0, n * 32), pl.ds(0, 2 * half)]

    def block(n, src, piece, plane=2, some=square):
        return Block(src, piece, some, [g_sem.at[k, n] for k in range(N_SEMS)], g_own.at[n], plane)

    def wq_part(part):
        cols = pl.ds(part * half, half)
        return block(1 + part, wq_own.at[:, cols], lambda b: wq.at[pl.ds(b * rb, rb), cols])

    def wp_part(part):
        cols = pl.ds(part * half, half)
        return block(4 + part, wp_hbm.at[:, cols], lambda b: wp.at[pl.ds(b * rb, rb), cols], part)

    sub = fr2 // N_FC2

    def times(j, size):
        return j * size if isinstance(j, int) else pl.multiple_of(j * size, size)

    def item(n):
        if isinstance(n, int) and n < FIRST:
            if n == 0:
                return block(0, vec_ref, lambda b: vecf.at[pl.ds(b * 16, 16), :], 2,
                             lambda n: vecf.at[pl.ds(0, n * 16), :])
            return wq_part(n - 1) if n < 4 else wp_part(n - 4)
        if isinstance(n, int):
            return fc2_it(n - FIRST) if n < FIRST + N_FC2 else fc1_it(n - FIRST - N_FC2)
        return fc1_it(n - FIRST - N_FC2)

    def fc2_it(j):
        at = pl.ds(times(j, sub), sub)
        return block(FIRST + j, w2_hbm.at[at, :], lambda b: w2.at[pl.ds(b * fr2 + times(j, sub), sub), :],
                     (0, 1, 2, 2)[j], lambda n: w2.at[pl.ds(0, n * sub), :])

    def fc1_it(j):
        cols = pl.ds(times(j, FFB), FFB)
        return block(FIRST + N_FC2 + j, w1_hbm.at[:, cols], lambda b: w1.at[pl.ds(b * fr1, fr1), cols],
                     (PLANES[j] if isinstance(j, int) else jnp.where(j // 2 == 1, j % 2, 2)))

    gather = Gather(net)
    stages = {"S": gather.start, "A": gather.from_z, "B": gather.from_x, "Y": gather.from_seq, "C": gather.from_core}

    def go(*steps):
        for step in steps:
            stages[step[0]](item(int(step[1:])))

    go("S0", "S1", "S2")
    image = Image(seg_ref, id_ref)
    zeros = jnp.zeros((PAD, 128), BF16)
    opad[0:PAD, :] = zeros
    opad[PAD + WINDOW:2 * PAD + WINDOW, :] = zeros
    go("A0", "A1", "S3", "A2", "S4", "S5", "B0", "B1", "A3", "S6", "S7", "B2")
    for copy in late:
        copy.wait()
    go("B3", "C0", "C1", "C2", "C3")

    gain1 = full_vector(vecf, 0)
    shift1 = full_vector(vecf, 1)

    def project(src, src_row, row):
        v = src[pl.ds(src_row, chunk), :].astype(F32)
        h, unused = norm_parts(v)
        normed = (h * gain1 + shift1).astype(BF16)
        at = pl.ds(row, chunk)
        n1[at, :] = normed
        inner = (mm(normed, qd_ref[...]) * image.select(row, chunk)).astype(BF16)
        c1[at, :] = inner
        for part in range(3):
            cols = pl.ds(part * half, half)
            qkv[at, cols] = (mm(normed, wq[:, cols]) + mm(inner, qu[:, cols])).astype(BF16)

    def own_rows_in(i):
        project(x_ref, i * chunk, pl.multiple_of(s * rows + i * chunk, chunk))

    def partner_rows_in(i):
        x_copy(i).wait_recv()
        project(xp, i * chunk, pl.multiple_of(other * rows + i * chunk, chunk))

    own_rows_in(0)
    go("A4", "A5", "S8")
    own_rows_in(1)
    partner_rows_in(0)
    partner_rows_in(1)
    go("B4", "B5", "A6", "A7", "S9")
    outs = []

    def put(src, dst):
        copy = pltpu.make_async_copy(src, dst, out_sem.at[len(outs)])
        copy.start()
        outs.append(copy)

    put(vecf, vecf_out)
    for src, dst in ((qkv, qkvw), (n1, n1w), (c1, c1w)):
        step = min(src.shape[1], 512)

        @pl.loop(0, src.shape[1] // step)
        def _(n, src=src, dst=dst, step=step):
            cols = pl.ds(pl.multiple_of(n * step, step), step)
            dst[:, cols] = image.choose(lambda at: src[at:at + WINDOW, cols])
    bias = jnp.where(image.inside((1, WINDOW), 1), 0.0, masked_score).astype(F32)
    halves = lane_halves()

    def prob_copy(pair):
        slot = lax.rem(pair, 2)
        return pltpu.make_async_copy(prob.at[slot], prob_out.at[pl.ds(2 * pair, 2)], prob_sem.at[slot])

    def att_copy(pair):
        cols = pl.ds(pl.multiple_of(s * half + pair * 128, 128), 128)
        return pltpu.make_async_remote_copy(
            src_ref=sendb.at[pair], dst_ref=att.at[:, cols], send_sem=as_sem.at[pair], recv_sem=ar_sem.at[pair],
            device_id=net.partner, device_id_type=MESH)

    def to_partner(src, dst, send, recv):
        return pltpu.make_async_remote_copy(src_ref=src, dst_ref=dst, send_sem=send, recv_sem=recv,
                                            device_id=net.partner, device_id_type=MESH)

    pairs = half // 128

    @pl.loop(0, pairs)
    def _(pair):
        def cols(part):
            return pl.ds(pl.multiple_of(part * half + pair * 128, 128), 128)

        for n, steps in enumerate(((), ("Y4", "Y5"), ("A8", "S10", "S11"), ("C4", "C5"))):
            @pl.when(pair == n)
            def _(steps=steps):
                go(*steps)

        k2 = qkvw[:, cols(1)]
        v2 = qkvw[:, cols(2)]
        vs = [(v2 * hm.astype(BF16)) for hm in halves]
        slot = lax.rem(pair, 2)

        @pl.when(pair >= 2)
        def _():
            prob_copy(pair).wait()

        @pl.loop(0, WINDOW // QROWS)
        def _(b):
            r0 = pl.multiple_of(b * QROWS, QROWS)
            q2 = qkvw[pl.ds(r0, QROWS), cols(0)]
            q2 = q2 * jnp.asarray(HEAD_DIM ** (-0.5), BF16)
            total = None
            for hd in range(2):
                scores = mm_nt(q2 * halves[hd].astype(BF16), k2) + bias
                weights = jnp.exp(scores - jnp.max(scores, axis=1, keepdims=True))
                weights = (weights * (1.0 / jnp.sum(weights, axis=1, keepdims=True))).astype(BF16)
                prob[slot, hd, pl.ds(r0, QROWS), :] = weights
                part = mm(weights, vs[hd])
                total = part if total is None else total + part
            total = (total * image.inside((QROWS, 1), 0, r0).astype(F32)).astype(BF16)
            opad[pl.ds(PAD + r0, QROWS), :] = total
            oh[pl.ds(r0, QROWS), cols(0)] = total

        prob_copy(pair).start()

        def own_rows(who):
            return image.choose(lambda at: opad[pl.ds(pl.multiple_of(who * rows + PAD - at, STEP), rows), :])

        sendb[pair] = own_rows(other)
        att_copy(pair).start()
        att[:, pl.ds(pl.multiple_of(s * half + pair * 128, 128), 128)] = own_rows(s)

    go("B6", "B7")

    @pl.loop(0, pairs)
    def _(pair):
        att_copy(pair).wait_recv()

    go("A9", "S12", "S13")
    bias_p = full_vector(vecf, 2)
    gain2 = full_vector(vecf, 3)
    shift2 = full_vector(vecf, 4)

    @pl.loop(0, 2)
    def _(i):
        at = pl.ds(pl.multiple_of(i * chunk, chunk), chunk)
        rows_in = att[at, :]
        own_select = image.select(s * rows + i * chunk, chunk)
        inner = (mm(rows_in, pd_ref[...]) * own_select).astype(BF16)
        c2[at, :] = inner
        branch = mm(rows_in, wp[...]) + mm(inner, pu_ref[...]) + bias_p
        middle = x_ref[at, :].astype(F32) + branch
        mid[at, :] = middle
        h, unused = norm_parts(middle)
        normed = (h * gain2 + shift2).astype(BF16)
        n2[at, :] = normed
        c = mm(normed, d1[...]) * own_select
        e = mm_nt(g[at, :], u2[...]) * own_select
        c3[at, :] = c.astype(BF16)
        e4[at, :] = e.astype(BF16)
        oacc[at, :] = jnp.zeros((chunk, width), F32)
        gacc[at, :] = jnp.zeros((chunk, width), F32)
        u4[at, :] = jnp.zeros((chunk, 128), F32)
        e3[at, :] = jnp.zeros((chunk, 128), F32)

    c3t[...] = c3[...].T
    e4t[...] = e4[...].T
    go("B8", "A10", "S14", "Y6", "Y7", "B9", "A11", "S15", "C6", "C7", "C8", "C9", "B10", "A12", "A13", "S16", "S17")

    @pl.loop(0, N_FC1)
    def _(j):
        gather.from_core(fc1_it(j))
        bias = jnp.concatenate([vecf[pl.ds(2 * j * 16 + 6, 1), :], vecf[pl.ds(2 * j * 16 + 7, 1), :],
                                vecf[pl.ds((2 * j + 1) * 16 + 6, 1), :], vecf[pl.ds((2 * j + 1) * 16 + 7, 1), :]], axis=1)
        col = pl.ds(pl.multiple_of(j * FFB, FFB), FFB)

        for at in [pl.ds(0, rows)]:
            hidden = mm(n2[at, :], w1[:, col]) + mm(c3[at, :], u1[:, col]) + bias
            grad_active = mm_nt(g[at, :], w2[col, :]) + mm_nt(e4[at, :], d2[col, :])
            cdf = 0.5 * (1.0 + lax.erf(hidden * (0.5 ** 0.5)))
            pdf = jnp.exp(hidden * hidden * -0.5) * (0.5 / 3.141592653589793) ** 0.5
            active = (hidden * cdf).astype(BF16)
            act_s[at, :] = active
            grad_hidden = (grad_active * (cdf + hidden * pdf)).astype(BF16)
            gh_s[at, :] = grad_hidden
            oacc[at, :] += mm(active, w2[col, :])
            u4[at, :] += mm(active, d2[col, :])
            gacc[at, :] += mm_nt(grad_hidden, w1[:, col])
            e3[at, :] += mm_nt(grad_hidden, u1[:, col])

        gr[:, col] = compact_rows(mm(c3t[...], gh_s[...]))
        gr[:, pl.ds(pl.multiple_of(ff + j * FFB, FFB), FFB)] = compact_rows(mm(e4t[...], act_s[...]))
        for first in (0, ff):
            cols = pl.ds(pl.multiple_of(first + j * FFB, FFB), FFB)
            to_partner(gr.at[:, cols], gr_in.at[:, cols], fs_sem.at[0], fr_sem.at[0]).start()

        @pl.when(j + 4 < N_FC1)
        def _():
            gather.from_z(fc1_it(j + 4))

        @pl.when(j == 0)
        def _():
            gather.from_x(fc1_it(1))

        @pl.when(j + 2 < N_FC1)
        def _():
            gather.from_x(fc1_it(j + 2))

        @pl.when(j + 1 < N_FC1)
        def _():
            gather.from_seq(fc1_it(j + 1))

    bias2 = full_vector(vecf, 5)
    for n in range(FIRST + N_FC2):
        gather.finish(item(n))

    @pl.loop(0, N_FC1)
    def _(j):
        gather.finish(fc1_it(j))

    for pair in range(pairs - 2, pairs):
        prob_copy(pair).wait()

    def prob_load(pair):
        slot = lax.rem(pair, 2)
        return pltpu.make_async_copy(prob_out.at[pl.ds(2 * pair, 2)], prob.at[slot], prob_sem.at[slot])

    for pair in range(2):
        prob_load(pair).start()

    g1 = n1
    e2 = u4

    def grad_att(at, who):
        heads = pl.ds(pl.multiple_of(who * half, half), half)
        return (mm_nt(g1[at, :], wp[heads, :]) + mm_nt(e2[at, :].astype(BF16), pd_ref[heads, :])).astype(BF16)

    def d_copy(pair):
        cols = pl.ds(pair * 128 if isinstance(pair, int) else pl.multiple_of(pair * 128, 128), 128)
        return to_partner(n1.at[pl.ds(rows, rows), cols],
                          do_s.at[pl.ds(pl.multiple_of(s * rows, rows), rows), cols], ds_sem.at[pair], dr_sem.at[pair])

    @pl.loop(0, 2)
    def _(i):
        at = pl.ds(pl.multiple_of(i * chunk, chunk), chunk)
        own_select = image.select(s * rows + i * chunk, chunk)
        c = (u4[at, :] * own_select).astype(BF16)
        e = (e3[at, :] * own_select).astype(BF16)
        c3[at, :] = c
        e4[at, :] = e
        grad_n2 = gacc[at, :] + mm_nt(e, d1[...])
        grad_mid = g[at, :].astype(F32) + norm_grad(mid[at, :], gain2, grad_n2)
        gacc[at, :] = grad_mid
        low = grad_mid.astype(BF16)
        g1[at, :] = low
        e2[at, :] = mm_nt(low, pu_ref[...]) * own_select
        n1[pl.ds(pl.multiple_of(rows + i * chunk, chunk), chunk), 0:half] = grad_att(at, other)

    for pair in range(pairs):
        d_copy(pair).start()

    cols0 = 2 * ff
    cols1 = 4 * width
    gr[:, cols0:cols0 + width] = compact_rows(mm_tn(e4[...], n2[...]))
    gr[:, cols0 + width:cols0 + 2 * width] = compact_rows(mm_tn(c3[...], g[...]))
    gr[:, cols0 + 2 * width:cols0 + 3 * width] = compact_rows(mm_tn(c2[...], g1[0:rows, :]))
    gr[:, cols0 + 3 * width:cols0 + 4 * width] = compact_rows(mm_tn(e2[...].astype(BF16), att[...]))
    rest = pl.ds(cols0, cols1)
    rest_copy = to_partner(gr.at[:, rest], gr_in.at[:, rest], fs_sem.at[1], fr_sem.at[1])
    rest_copy.start()

    @pl.loop(0, 2)
    def _(i):
        at = pl.ds(pl.multiple_of(i * chunk, chunk), chunk)
        do_s[pl.ds(pl.multiple_of(s * rows + i * chunk, chunk), chunk), :] = grad_att(at, s)

    own0, own1 = cols0 // 16, cols1 // 16
    pick = adapter_rows(vecf)

    def turn_start(n, src, first, dst, cols):
        mine = pl.ds(pl.multiple_of(net.f * 16, 16), 16)

        @pl.loop(1, 16)
        def _(d):
            peer = (net.f + d) % 16
            pltpu.make_async_remote_copy(
                src_ref=src.at[:, pl.ds(pl.multiple_of(first + peer * cols, 128), cols)], dst_ref=dst.at[mine, :],
                send_sem=t_send.at[n], recv_sem=t_recv.at[n], device_id={"fsdp": peer}, device_id_type=MESH).start()

        dst[mine, :] = src[:, pl.ds(pl.multiple_of(first + net.f * cols, 128), cols)]

    def turn_total(n, dst):
        return pltpu.make_async_remote_copy(
            src_ref=dst.at[0:240, :], dst_ref=dst.at[0:240, :], send_sem=t_send.at[n], recv_sem=t_recv.at[n],
            device_id=net.c_peer, device_id_type=MESH)

    def result(n, src, first, step):
        return Block(src, lambda b: gall.at[:, pl.ds(pl.multiple_of(first + b * step, 128), 256)],
                     lambda m: gall.at[:, pl.ds(0, m * 256)], [g_sem.at[k, N_ITEMS + n] for k in range(N_SEMS)],
                     g_own.at[N_ITEMS + n])

    results = [result(0, dense0.at[:, pl.ds(0, 256)], 0, own0), result(1, dense0.at[:, pl.ds(256, 256)], 256, own0),
               result(2, dense1, cols0, own1), result(3, dense2, cols0 + cols1, own1)]

    def move(*steps):
        for step in steps:
            stages[step[0]](results[int(step[1:])])

    first_cols = pl.ds(0, cols0)
    first_copy = to_partner(gr.at[:, first_cols], gr_in.at[:, first_cols], fs_sem.at[0], fr_sem.at[0])
    first_copy.wait_recv()
    gr_sum[:, 0:cols0] = (gr[:, 0:cols0].astype(F32) + gr_in[:, 0:cols0].astype(F32)).astype(BF16)
    turn_start(0, gr_sum, 0, parts0, own0)

    @pl.loop(0, 2)
    def _(i):
        at = pl.ds(pl.multiple_of(i * chunk, chunk), chunk)
        branch = oacc[at, :] + mm(c3[at, :], u2[...]) + bias2
        xp[at, :] = (mid[at, :] + branch).astype(BF16)

    put(xp, out_out)
    put(gacc, gm_out)
    gpad = w2
    zeros = jnp.zeros((PAD, width), BF16)
    gpad[0:PAD, :] = zeros
    gpad[PAD + WINDOW:2 * PAD + WINDOW, :] = zeros
    last_own[...] = jnp.zeros_like(last_own)
    gq = w1
    scale = HEAD_DIM ** (-0.5)
    keep = image.inside((WINDOW, 1), 0).astype(BF16)

    @pl.loop(0, pairs)
    def _(pair):
        @pl.when(pair == 1)
        def _():
            turn_total(0, parts0).wait_recv()
            dense0[...] = mm(pick, parts0[...]).astype(BF16)
            move("S0", "S1")

        def cols(part):
            return pl.ds(pl.multiple_of(part * half + pair * 128, 128), 128)

        prob_load(pair).wait()
        d_copy(pair).wait_recv()
        slot = lax.rem(pair, 2)
        k2 = qkvw[:, cols(1)]
        v2 = qkvw[:, cols(2)]
        q2 = qkvw[:, cols(0)] * jnp.asarray(scale, BF16)
        do2 = image.choose(lambda at: do_s[at:at + WINDOW, cols(0)]) * keep
        inner = do2.astype(F32) * oh[:, cols(0)].astype(F32)
        gv = gk = gqq = None
        for hd in range(2):
            hm = halves[hd].astype(BF16)
            weights = prob[slot, hd]
            grad_p = mm_nt(do2 * hm, v2)
            row_inner = jnp.sum(inner * halves[hd], axis=1, keepdims=True)
            grad_s = (weights.astype(F32) * (grad_p - row_inner)).astype(BF16)
            dv = mm_tn(weights, do2 * hm)
            dk = mm_tn(grad_s, q2 * hm)
            dq = mm(grad_s, k2 * hm)
            gv = dv if gv is None else gv + dv
            gk = dk if gk is None else gk + dk
            gqq = dq if gqq is None else gqq + dq

        @pl.when(pair + 2 < pairs)
        def _():
            prob_load(pair + 2).start()

        gq[0:WINDOW, cols(0)] = (gqq * scale).astype(BF16)
        gq[0:WINDOW, cols(1)] = gk.astype(BF16)
        gq[0:WINDOW, cols(2)] = gv.astype(BF16)

    rest_copy.wait_recv()
    gr_sum[:, cols0:cols0 + cols1] = (gr[:, cols0:cols0 + cols1].astype(F32)
                                      + gr_in[:, cols0:cols0 + cols1].astype(F32)).astype(BF16)
    turn_start(1, gr_sum, cols0, parts1, own1)
    three = slice(0, 3 * half)
    c1[0:WINDOW, :] = (mm_nt(gq[0:WINDOW, three], qu[...]) * image.select_window(0, WINDOW)).astype(BF16)
    up = compact_rows(mm_tn(c1w[...], gq[0:WINDOW, three]))
    for part in range(3):
        last_own[:, pl.ds(pl.multiple_of(part * width + s * half, 128), half)] = up[:, part * half:(part + 1) * half]
    last_own[:, 3 * width:4 * width] = compact_rows(mm_tn(c1[0:WINDOW, :], n1w[...]))
    last_copy = to_partner(last_own, last_in, fs_sem.at[2], fr_sem.at[2])
    last_copy.start()
    move("A0", "A1")

    @pl.loop(0, 2)
    def _(i):
        at = pl.ds(pl.multiple_of(i * QROWS, QROWS), QROWS)
        gpad[pl.ds(pl.multiple_of(PAD + i * QROWS, STEP), QROWS), :] = (
            mm_nt(gq[at, three], wq[...]) + mm_nt(c1[at, :], qd_ref[...])).astype(BF16)

    def rows_of(who, i):
        return image.choose(lambda at: gpad[pl.ds(pl.multiple_of(who * rows + PAD + i * chunk - at, STEP), chunk), :])

    spot = 2 * PAD + WINDOW + 128

    def p_copy(i):
        return to_partner(gpad.at[pl.ds(spot + i * chunk, chunk), :], prcv.at[i], ps_sem.at[i], pr_sem.at[i])

    for i in range(2):
        gpad[spot + i * chunk:spot + (i + 1) * chunk, :] = rows_of(other, i)
        p_copy(i).start()
    last_copy.wait_recv()
    last_sum[...] = (last_own[...].astype(F32) + last_in[...].astype(F32)).astype(BF16)
    turn_start(2, last_sum, 0, parts2, own1)
    turn_total(1, parts1).wait_recv()
    dense1[...] = mm(pick, parts1[...]).astype(BF16)
    move("B0", "S2", "B1")
    turn_total(2, parts2).wait_recv()
    dense2[...] = mm(pick, parts2[...]).astype(BF16)
    gn = oacc

    def grad_in(i):
        p_copy(i).wait_recv()
        at = slice(i * chunk, (i + 1) * chunk)
        gn[at, :] = prcv[i].astype(F32) + rows_of(s, i).astype(F32)
        put(gn.at[at, :], gn_out.at[at, :])

    move("S3", "C0", "A2", "C1", "A3", "B2")
    grad_in(0)
    move("C2", "B3")
    grad_in(1)
    move("C3")
    for copy in outs:
        copy.wait()
    for i in range(2):
        x_copy(i).wait_send()
        p_copy(i).wait_send()
    for copy in (first_copy, rest_copy, last_copy):
        copy.wait_send()
    for n, dst in enumerate((parts0, parts1, parts2)):
        turn_total(n, dst).wait_send()
    for it in results:
        gather.finish(it)

    @pl.loop(0, pairs)
    def _(pair):
        att_copy(pair).wait_send()
        d_copy(pair).wait_send()


def any_spec():
    return pl.BlockSpec(memory_space=pl.ANY)


def vmem_spec():
    return pl.BlockSpec(memory_space=pltpu.VMEM)


def adapter_rows(vec_ref):
    ids = jnp.concatenate([jnp.broadcast_to(vec_ref[16 * p + 8:16 * p + 9, :], (16, 128)) for p in range(16)], axis=0)
    r = lax.broadcasted_iota(jnp.int32, (256, 128), 0) % 16
    col = lax.broadcasted_iota(jnp.int32, (256, 128), 1)
    group = (col // 16).astype(F32)
    return ((ids == group) & (r == col % 16)).astype(F32).T.astype(BF16)


def run_block(seg, ident, x, vec, qd, pd, pu, wq, wp, w1, w2, qu, g, u1, d1, u2, d2):
    rows, width = x.shape
    toks = seg.shape[1]
    half = width // 2
    ff = w1.shape[1]
    chunk = rows // 2
    dma = pltpu.SemaphoreType.DMA
    sds = jax.ShapeDtypeStruct
    gcols = 2 * ff + 4 * width
    last = 4 * width
    out_shape = (
        sds((256, 128), F32), sds((half // 64, WINDOW, WINDOW), BF16), sds((rows, width), F32), sds((rows, width), BF16),
        sds((128, gcols + last), BF16), sds((rows, width), F32))

    def low(*shape):
        return pltpu.VMEM(shape, BF16)

    def full(*shape):
        return pltpu.VMEM(shape, F32)

    scratch = [
        low(wq.shape[0], 3 * half), low(width, 3 * half), low(width, width), low(width, ff), low(ff, width),
        low(rows, width), full(256, 128), low(128, 3 * half), low(rows, width), low(128, ff), low(width, 128),
        low(128, width), low(ff, 128), low(toks, 3 * half), low(toks, width), low(toks, 128),
        low(WINDOW, 3 * half), low(WINDOW, width), low(WINDOW, 128), low(2, 2, WINDOW, WINDOW), low(2 * PAD + WINDOW, 128),
        low(half // 128, rows, 128), low(WINDOW, half), low(rows, width), low(rows, 128), full(rows, width), low(rows, width),
        full(rows, width), full(rows, width), full(rows, 128), full(rows, 128), low(rows, 128), low(rows, 128),
        low(128, rows), low(128, rows), low(rows, FFB), low(rows, FFB), low(16, gcols),
        low(toks, half), low(16, gcols), low(16, gcols), low(16, last), low(16, last), low(16, last),
        low(256, 2 * ff // 16), low(256, last // 16), low(256, last // 16), low(128, 2 * ff // 16), low(128, last // 16),
        low(128, last // 16), low(2, chunk, width),
        dma((2,)), dma((2,)), dma((4,)), dma((4,)), dma((11,)), dma((12,)), dma((2,)),
        dma((N_SEMS, N_ITEMS + 4)), dma((N_ITEMS + 4,)),
        dma((4,)), dma((4,)), dma((3,)), dma((3,)), dma((2,)), dma((2,)), dma((3,)), dma((3,))]
    return pl.pallas_call(
        block_kernel, out_shape=out_shape, in_specs=[vmem_spec()] * 7 + [any_spec()] * 10,
        out_specs=tuple(any_spec() for unused in out_shape), scratch_shapes=scratch,
        compiler_params=pltpu.CompilerParams(collective_id=1, has_side_effects=True, vmem_limit_bytes=VMEM_LIMIT),
        name="block")(seg, ident, x, vec, qd, pd, pu, wq, wp, w1, w2, qu, g, u1, d1, u2, d2)


def expand_kernel(vec_ref, f1u, f2d, f1d, f2u, pu, pdn, qu, qd, gn, x, gm, out,
                  out_out, gt_out, qd_out, qu_out, pd_out, pu_out, f1d_out, f1u_out, f2d_out, f2u_out):
    for src, dst in ((f1u, f1u_out), (f2u, f2u_out), (pu, pu_out), (qu, qu_out)):
        dst[...] = src[...].astype(F32)
    for src, dst in ((f1d, f1d_out), (f2d, f2d_out), (pdn, pd_out), (qd, qd_out)):
        dst[...] = src[...].T.astype(F32)
    out_out[...] = out[...]
    gain1 = full_vector(vec_ref, 0)
    gt_out[...] = gm[...] + norm_grad(x[...].astype(F32), gain1, gn[...])


def run_expand(vec, gall, gn, x, gm, out):
    rows, width = gn.shape
    ff = 4 * width
    n = 2
    sds = jax.ShapeDtypeStruct

    def part(cols, offset):
        return pl.BlockSpec((128, cols), lambda j: (0, offset // cols + j))

    def by_row(shape):
        return pl.BlockSpec(shape, lambda j: (j, 0))

    def by_col(shape):
        return pl.BlockSpec(shape, lambda j: (0, j))

    q = width // n
    return pl.pallas_call(
        expand_kernel, grid=(n,),
        out_shape=(sds((rows, width), BF16), sds((rows, width), F32), sds((width, 128), F32), sds((128, 3 * width), F32), sds((width, 128), F32),
                   sds((128, width), F32), sds((width, 128), F32), sds((128, ff), F32), sds((ff, 128), F32), sds((128, width), F32)),
        in_specs=[pl.BlockSpec((256, 128), lambda j: (0, 0)), part(ff // n, 0), part(ff // n, ff), part(q, 2 * ff),
                  part(q, 2 * ff + width), part(q, 2 * ff + 2 * width), part(q, 2 * ff + 3 * width),
                  part(3 * q, 2 * ff + 4 * width), part(q, 2 * ff + 7 * width),
                  by_row((rows // n, width)), by_row((rows // n, width)), by_row((rows // n, width)), by_row((rows // n, width))],
        out_specs=(by_row((rows // n, width)), by_row((rows // n, width)), by_row((q, 128)), by_col((128, 3 * q)), by_row((q, 128)), by_col((128, q)),
                   by_row((q, 128)), by_col((128, ff // n)), by_row((ff // n, 128)), by_col((128, q))),
        compiler_params=pltpu.CompilerParams(vmem_limit_bytes=VMEM_LIMIT),
        name="expand")(vec, *([gall] * 8), gn, x, gm, out)


def per_device_fast(tokens, grad_out, segments, padding, adapter_ids, norm1_gain, norm1_bias, w_qkv, w_proj, proj_bias,
                    norm2_gain, norm2_bias, w_fc1, fc1_bias, w_fc2, fc2_bias, qkv_down, qkv_up, proj_down, proj_up,
                    fc1_down, fc1_up, fc2_down, fc2_up):
    x = tokens[0]
    odd = (lax.axis_index("fsdp") % 2).astype(F32)
    six = jnp.stack([norm1_gain, norm1_bias, proj_bias, norm2_gain, norm2_bias, fc2_bias]).astype(F32)
    vec = jnp.concatenate([
        jnp.concatenate([six * (1.0 - odd), six * odd], axis=1), fc1_bias.astype(F32).reshape(2, 128),
        jnp.broadcast_to(adapter_ids[0].astype(F32)[:, None], (1, 128)), jnp.zeros((7, 128), F32)], axis=0)
    vecf, unused, gm, out, gall, gn = run_block(
        segments, adapter_ids, x, vec, qkv_down, proj_down, proj_up, w_qkv, w_proj, w_fc1, w_fc2, qkv_up,
        grad_out[0], fc1_up, fc1_down, fc2_up, fc2_down)
    out, gt, gqd, gqu, gpd, gpu, gf1d, gf1u, gf2d, gf2u = run_expand(vecf, gall, gn, x, gm, out)
    return out[None], gt[None], gqd, gqu, gpd, gpu, gf1d, gf1u, gf2d, gf2u


def solution(mesh):
    sizes = dict(mesh.shape)
    small = sizes == {"seq": 2, "fsdp": 16}

    def per_device_any(*args):
        tokens, adapter_ids = args[0], args[4]
        one_image = tokens.shape[1:] == (512, 1024) and adapter_ids.shape[1] == 1
        return (per_device_fast if small and one_image else per_device)(*args)

    return jax.shard_map(
        per_device_any,
        mesh=mesh,
        in_specs=(
            P("fsdp", "seq", None),
            P("fsdp", "seq", None),
            P("fsdp", None),
            P("fsdp", None),
            P("fsdp", None),
            P("fsdp"),
            P("fsdp"),
            P("fsdp", None),
            P("fsdp", None),
            P("fsdp"),
            P("fsdp"),
            P("fsdp"),
            P("fsdp", None),
            P("fsdp"),
            P("fsdp", None),
            P("fsdp"),
            P(),
            P(),
            P(),
            P(),
            P(),
            P(),
            P(),
            P(),
        ),
        out_specs=(
            P("fsdp", "seq", None),
            P("fsdp", "seq", None),
            P(),
            P(),
            P(),
            P(),
            P(),
            P(),
            P(),
            P(),
        ),
        check_vma=False,
    )
```

```python
from functools import partial

import jax
import jax.numpy as jnp
from jax import lax
from jax.experimental import pallas as pl
from jax.experimental.pallas import tpu as pltpu
from jax.sharding import PartitionSpec as P

HEAD_DIM = 64
IMG = 577
RANK = 16
QBLOCK = 512


norm_eps = 1e-06
masked_score = -1e30


def matmul(left_side, right_side):
    return jnp.dot(left_side, right_side, preferred_element_type=jnp.float32)


def matmul_nt(left_side, right_side):
    return jnp.einsum("tk,jk->tj", left_side, right_side, preferred_element_type=jnp.float32)


def matmul_tn(left_side, right_side):
    return jnp.einsum("ti,to->io", left_side, right_side, preferred_element_type=jnp.float32)


def layer_norm(values, norm_gain, norm_shift):
    centre = jnp.mean(values, axis=-1, keepdims=True)
    centred = values - centre
    spread = jnp.mean(centred * centred, axis=-1, keepdims=True)
    return centred * lax.rsqrt(spread + norm_eps) * norm_gain + norm_shift


def norm_backward(values, norm_gain, norm_shift, grad_in):

    def apply_norm(inputs):
        return layer_norm(inputs, norm_gain, norm_shift)

    unused, pullback = jax.vjp(apply_norm, values)
    return pullback(grad_in)[0]


def selection(seg_own, image_adapters, columns):
    images = jnp.arange(image_adapters.shape[0], dtype=jnp.int32)
    image_match = seg_own[:, None] - 1 == images[None, :]
    token_adapter = jnp.sum(jnp.where(image_match, image_adapters[None, :], 0), axis=1)
    present = jnp.any(image_match, axis=1)
    column = jnp.arange(columns, dtype=jnp.int32) // RANK
    chosen = (token_adapter[:, None] == column[None, :]) & present[:, None]
    return chosen.astype(jnp.float32)


def adapter_forward(inputs_b, weight, down_map, up_map, select):
    inner_term = (matmul(inputs_b, down_map) * select).astype(jnp.bfloat16)
    return (matmul(inputs_b, weight) + matmul(inner_term, up_map), inner_term)


def adapter_backward(inputs_b, inner_term, grad_in, weight, down_map, up_map, select):
    grad_up = matmul_tn(inner_term, grad_in)
    grad_inner = (matmul_nt(grad_in, up_map) * select).astype(jnp.bfloat16)
    grad_down = matmul_tn(inputs_b, grad_inner)
    grad_inputs = matmul_nt(grad_in, weight) + matmul_nt(grad_inner, down_map)
    return (grad_inputs, grad_down, grad_up)


def block_scores(query_block, key_heads, seg_block, seg_keys, keep_keys):
    score_scale = HEAD_DIM ** (-0.5)
    scores = (
        jnp.einsum("qhd,khd->hqk", query_block, key_heads, preferred_element_type=jnp.float32)
        * score_scale
    )
    allowed = (seg_block[:, None] == seg_keys[None, :]) & (keep_keys[None, :] == 1)
    return jnp.where(allowed[None, :, :], scores, masked_score)


def split_heads(head_rows):
    all_rows = head_rows.shape[0]
    local_heads = head_rows.shape[2] // HEAD_DIM
    query_heads = head_rows[:, 0].reshape(all_rows, local_heads, HEAD_DIM)
    key_heads = head_rows[:, 1].reshape(all_rows, local_heads, HEAD_DIM)
    value_heads = head_rows[:, 2].reshape(all_rows, local_heads, HEAD_DIM)
    return (query_heads, key_heads, value_heads)


def key_window(all_rows):
    return min(all_rows, (QBLOCK + 2 * IMG - 2 + 127) // 128 * 128)


def window_start(block_index, all_rows, window):
    first = block_index * QBLOCK - (IMG - 1)
    return jnp.clip(first, 0, all_rows - window)


def attention_forward(head_rows, seg_all, keep_all):
    all_rows = head_rows.shape[0]
    block_count = all_rows // QBLOCK
    window = key_window(all_rows)
    query_heads, key_heads, value_heads = split_heads(head_rows)
    local_heads = query_heads.shape[1]

    def one_block(block_parts):
        query_block, seg_block, keep_block, block_index = block_parts
        start = window_start(block_index, all_rows, window)
        keys_near = lax.dynamic_slice_in_dim(key_heads, start, window, 0)
        values_near = lax.dynamic_slice_in_dim(value_heads, start, window, 0)
        seg_near = lax.dynamic_slice_in_dim(seg_all, start, window, 0)
        keep_near = lax.dynamic_slice_in_dim(keep_all, start, window, 0)
        scores = block_scores(query_block, keys_near, seg_block, seg_near, keep_near)
        row_max = jnp.max(scores, axis=2, keepdims=True)
        weights = jnp.exp(scores - row_max)
        row_sum = jnp.sum(weights, axis=2, keepdims=True)
        probs_low = (weights / row_sum).astype(jnp.bfloat16)
        result = jnp.einsum(
            "hqk,khd->qhd", probs_low, values_near, preferred_element_type=jnp.float32
        )
        result = result * keep_block[:, None, None].astype(jnp.float32)
        return (result.astype(jnp.bfloat16), row_max, row_sum)

    block_ids = jnp.arange(block_count, dtype=jnp.int32)
    blocked = (
        query_heads.reshape(block_count, QBLOCK, local_heads, HEAD_DIM),
        seg_all.reshape(block_count, QBLOCK),
        keep_all.reshape(block_count, QBLOCK),
        block_ids,
    )
    results, block_max, block_sums = lax.map(one_block, blocked)
    return (results.reshape(all_rows, local_heads * HEAD_DIM), block_max, block_sums)


def attention_backward(head_rows, grad_rows, seg_all, keep_all, block_max, block_sums):
    all_rows = head_rows.shape[0]
    block_count = all_rows // QBLOCK
    window = key_window(all_rows)
    query_heads, key_heads, value_heads = split_heads(head_rows)
    local_heads = query_heads.shape[1]
    score_scale = HEAD_DIM ** (-0.5)

    def one_block(running, block_parts):
        grad_keys, grad_values = running
        query_block, seg_block, keep_block, grad_block, row_max, row_sum, block_index = block_parts
        start = window_start(block_index, all_rows, window)
        keys_near = lax.dynamic_slice_in_dim(key_heads, start, window, 0)
        values_near = lax.dynamic_slice_in_dim(value_heads, start, window, 0)
        seg_near = lax.dynamic_slice_in_dim(seg_all, start, window, 0)
        keep_near = lax.dynamic_slice_in_dim(keep_all, start, window, 0)
        scores = block_scores(query_block, keys_near, seg_block, seg_near, keep_near)
        probs = jnp.exp(scores - row_max) / row_sum
        grad_result = grad_block * keep_block[:, None, None].astype(jnp.bfloat16)
        values_term = jnp.einsum(
            "hqk,qhd->khd",
            probs.astype(jnp.bfloat16),
            grad_result,
            preferred_element_type=jnp.float32,
        )
        grad_probs = jnp.einsum(
            "qhd,khd->hqk", grad_result, values_near, preferred_element_type=jnp.float32
        )
        row_inner = jnp.sum(probs * grad_probs, axis=2, keepdims=True)
        grad_scores = (probs * (grad_probs - row_inner)).astype(jnp.bfloat16)
        grad_query = (
            jnp.einsum("hqk,khd->qhd", grad_scores, keys_near, preferred_element_type=jnp.float32)
            * score_scale
        )
        keys_term = (
            jnp.einsum("hqk,qhd->khd", grad_scores, query_block, preferred_element_type=jnp.float32)
            * score_scale
        )
        grad_keys = lax.dynamic_update_slice_in_dim(
            grad_keys, lax.dynamic_slice_in_dim(grad_keys, start, window, 0) + keys_term, start, 0
        )
        grad_values = lax.dynamic_update_slice_in_dim(
            grad_values,
            lax.dynamic_slice_in_dim(grad_values, start, window, 0) + values_term,
            start,
            0,
        )
        return ((grad_keys, grad_values), grad_query)

    zero_heads = jnp.zeros((all_rows, local_heads, HEAD_DIM), jnp.float32)
    block_ids = jnp.arange(block_count, dtype=jnp.int32)
    blocked = (
        query_heads.reshape(block_count, QBLOCK, local_heads, HEAD_DIM),
        seg_all.reshape(block_count, QBLOCK),
        keep_all.reshape(block_count, QBLOCK),
        grad_rows.reshape(block_count, QBLOCK, local_heads, HEAD_DIM),
        block_max,
        block_sums,
        block_ids,
    )
    (grad_keys, grad_values), grad_queries = lax.scan(one_block, (zero_heads, zero_heads), blocked)
    flat_width = local_heads * HEAD_DIM
    stacked = jnp.stack(
        [
            grad_queries.reshape(all_rows, flat_width),
            grad_keys.reshape(all_rows, flat_width),
            grad_values.reshape(all_rows, flat_width),
        ],
        axis=1,
    )
    return stacked.astype(jnp.bfloat16)


def per_device(
    tokens,
    grad_out,
    segments,
    padding,
    adapter_ids,
    norm1_gain,
    norm1_bias,
    w_qkv,
    w_proj,
    proj_bias,
    norm2_gain,
    norm2_bias,
    w_fc1,
    fc1_bias,
    w_fc2,
    fc2_bias,
    qkv_down,
    qkv_up,
    proj_down,
    proj_up,
    fc1_down,
    fc1_up,
    fc2_down,
    fc2_up,
):
    tok_rows = tokens.shape[1]
    feat_width = tokens.shape[2]
    inputs = tokens[0].astype(jnp.float32)
    seg_all = segments[0]
    keep_all = padding[0]
    offset = lax.axis_index("seq") * tok_rows
    seg_own = lax.dynamic_slice_in_dim(seg_all, offset, tok_rows)
    select = selection(seg_own, adapter_ids[0], qkv_down.shape[1])
    gain_one, shift_one, qkv_weight, proj_weight, proj_shift = (
        lax.all_gather(norm1_gain, "fsdp", axis=0, tiled=True),
        lax.all_gather(norm1_bias, "fsdp", axis=0, tiled=True),
        lax.all_gather(w_qkv, "fsdp", axis=0, tiled=True),
        lax.all_gather(w_proj, "fsdp", axis=0, tiled=True),
        lax.all_gather(proj_bias, "fsdp", axis=0, tiled=True),
    )
    gain_one = gain_one.astype(jnp.float32)
    shift_one = shift_one.astype(jnp.float32)
    normed_one = layer_norm(inputs, gain_one, shift_one).astype(jnp.bfloat16)
    qkv_main, inner_one = adapter_forward(normed_one, qkv_weight, qkv_down, qkv_up, select)
    qkv_low = qkv_main.astype(jnp.bfloat16).reshape(tok_rows, 3, feat_width)
    head_rows = lax.all_to_all(qkv_low, "seq", split_axis=2, concat_axis=0, tiled=True)
    attended_heads, block_max, block_sums = attention_forward(head_rows, seg_all, keep_all)
    attended = lax.all_to_all(attended_heads, "seq", split_axis=0, concat_axis=1, tiled=True)
    branch_one, inner_two = adapter_forward(attended, proj_weight, proj_down, proj_up, select)
    middle = inputs + (branch_one + proj_shift.astype(jnp.float32))
    gain_two, shift_two, fc1_weight, fc2_shift, fc2_weight, fc1_shift = (
        lax.all_gather(norm2_gain, "fsdp", axis=0, tiled=True),
        lax.all_gather(norm2_bias, "fsdp", axis=0, tiled=True),
        lax.all_gather(w_fc1, "fsdp", axis=0, tiled=True),
        lax.all_gather(fc2_bias, "fsdp", axis=0, tiled=True),
        lax.all_gather(w_fc2, "fsdp", axis=0, tiled=True),
        lax.all_gather(fc1_bias, "fsdp", axis=0, tiled=True),
    )
    gain_two = gain_two.astype(jnp.float32)
    shift_two = shift_two.astype(jnp.float32)
    normed_two = layer_norm(middle, gain_two, shift_two).astype(jnp.bfloat16)
    hidden_main, inner_three = adapter_forward(normed_two, fc1_weight, fc1_down, fc1_up, select)
    hidden = hidden_main + fc1_shift.astype(jnp.float32)
    active = jax.nn.gelu(hidden, approximate=False).astype(jnp.bfloat16)
    branch_two, inner_four = adapter_forward(active, fc2_weight, fc2_down, fc2_up, select)
    output = (middle + (branch_two + fc2_shift.astype(jnp.float32))).astype(jnp.bfloat16)
    fc1_back, fc2_back = (
        lax.all_gather(w_fc1, "fsdp", axis=0, tiled=True),
        lax.all_gather(w_fc2, "fsdp", axis=0, tiled=True),
    )
    grad_top = grad_out[0]
    grad_active, grad_fc2_down, grad_fc2_up = adapter_backward(
        active, inner_four, grad_top, fc2_back, fc2_down, fc2_up, select
    )
    unused, gelu_back = jax.vjp(partial(jax.nn.gelu, approximate=False), hidden)
    grad_hidden = gelu_back(grad_active)[0].astype(jnp.bfloat16)
    grad_normed_two, grad_fc1_down, grad_fc1_up = adapter_backward(
        normed_two, inner_three, grad_hidden, fc1_back, fc1_down, fc1_up, select
    )
    grad_middle = grad_top.astype(jnp.float32) + norm_backward(
        middle, gain_two, shift_two, grad_normed_two
    )
    qkv_back, proj_back = (
        lax.all_gather(w_qkv, "fsdp", axis=0, tiled=True),
        lax.all_gather(w_proj, "fsdp", axis=0, tiled=True),
    )
    grad_branch_one = grad_middle.astype(jnp.bfloat16)
    grad_attended, grad_proj_down, grad_proj_up = adapter_backward(
        attended, inner_two, grad_branch_one, proj_back, proj_down, proj_up, select
    )
    grad_head_rows = lax.all_to_all(
        grad_attended.astype(jnp.bfloat16), "seq", split_axis=1, concat_axis=0, tiled=True
    )
    grad_qkv_heads = attention_backward(
        head_rows, grad_head_rows, seg_all, keep_all, block_max, block_sums
    )
    grad_qkv = lax.all_to_all(
        grad_qkv_heads, "seq", split_axis=0, concat_axis=2, tiled=True
    ).reshape(tok_rows, 3 * feat_width)
    grad_normed_one, grad_qkv_down, grad_qkv_up = adapter_backward(
        normed_one, inner_one, grad_qkv, qkv_back, qkv_down, qkv_up, select
    )
    grad_tokens = grad_middle + norm_backward(inputs, gain_one, shift_one, grad_normed_one)
    summed = lax.psum(
        (
            grad_qkv_down,
            grad_qkv_up,
            grad_proj_down,
            grad_proj_up,
            grad_fc1_down,
            grad_fc1_up,
            grad_fc2_down,
            grad_fc2_up,
        ),
        ("seq", "fsdp"),
    )
    return (
        output[None],
        grad_tokens[None],
        summed[0],
        summed[1],
        summed[2],
        summed[3],
        summed[4],
        summed[5],
        summed[6],
        summed[7],
    )


F32 = jnp.float32
BF16 = jnp.bfloat16
MESH = pl.DeviceIdType.MESH
VMEM_LIMIT = 67_000_000


def mm(a, b):
    return lax.dot_general(a, b, (((1,), (0,)), ((), ())), preferred_element_type=F32)


def mm_nt(a, b):
    return lax.dot_general(a, b, (((1,), (1,)), ((), ())), preferred_element_type=F32)


def mm_tn(a, b):
    return lax.dot_general(a, b, (((0,), (0,)), ((), ())), preferred_element_type=F32)


def norm_parts(v):
    mean = jnp.mean(v, axis=-1, keepdims=True)
    centred = v - mean
    r = lax.rsqrt(jnp.mean(centred * centred, axis=-1, keepdims=True) + norm_eps)
    return centred * r, r


def norm_grad(v, gain, grad_y):
    h, r = norm_parts(v)
    d = grad_y * gain
    return r * (d - jnp.mean(d, axis=-1, keepdims=True) - h * jnp.mean(d * h, axis=-1, keepdims=True))


class Net:
    def __init__(self):
        self.s = lax.axis_index("seq")
        self.f = lax.axis_index("fsdp")
        self.z = self.f // 4
        self.x = (self.f // 2) % 2
        self.c = self.f % 2
        self.partner = {"seq": 1 - self.s}
        self.x_peer = {"fsdp": self.block(self.z, 1 - self.x, self.c)}
        self.c_peer = {"fsdp": self.block(self.z, self.x, 1 - self.c)}

    def block(self, z, x, c):
        return (z * 2 + x) * 2 + c

    def z_peer(self, d):
        return {"fsdp": self.block((self.z + d) % 4, self.x, self.c)}

    def meet(self, peers):
        sem = pltpu.get_barrier_semaphore()
        for peer in peers:
            pl.semaphore_signal(sem, inc=1, device_id=peer, device_id_type=MESH)
        pl.semaphore_wait(sem, len(peers))

    def plane_peer(self, d):
        return {"fsdp": (self.f + d) % 16}

    def plane_barrier(self):
        self.meet([self.partner] + [self.plane_peer(d) for d in range(1, 16)])

    def barrier(self):
        self.meet([self.partner, self.x_peer, self.c_peer] + [self.z_peer(d) for d in (1, 2, 3)])


class Block:
    def __init__(self, src, piece, some, sems, own_sem, plane=2):
        self.src, self.piece, self.some, self.plane, self.own_sem = src, piece, some, plane, own_sem
        self.sent, self.z, self.x, self.y1, self.y2, self.c = sems


N_SEMS = 6


class Gather:
    def __init__(self, net):
        self.net = net

    def send(self, it, src, block, sem, peer):
        pltpu.make_async_remote_copy(
            src_ref=src, dst_ref=it.piece(block), send_sem=it.sent, recv_sem=sem, device_id=peer,
            device_id_type=MESH).start()

    def total(self, it, n, sem):
        return pltpu.make_async_remote_copy(
            src_ref=it.some(n), dst_ref=it.some(n), send_sem=it.sent, recv_sem=sem, device_id=self.net.c_peer,
            device_id_type=MESH)

    def here(self, it, body):
        if isinstance(it.plane, int) and it.plane == 2:
            body()
        else:
            pl.when((self.net.s == it.plane) | (it.plane == 2))(body)

    def hand_on(self, it, pieces, sem):
        def body():
            for piece, block in pieces:
                self.send(it, piece, block, sem, self.net.partner)

        if not isinstance(it.plane, int):
            pl.when(it.plane != 2)(body)
        elif it.plane != 2:
            body()

    def own(self, it):
        return pltpu.make_async_copy(it.src, it.piece(self.net.f), it.own_sem)

    def column(self, it, x, ds):
        net = self.net
        blocks = [net.block((net.z + d) % 4, x, net.c) for d in ds]
        return [(it.piece(block), block) for block in blocks]

    def start(self, it):
        net = self.net

        def along():
            for d in (2, 1, 3):
                self.send(it, it.src, net.f, it.z, net.z_peer(d))
            self.send(it, it.src, net.f, it.x, net.x_peer)

        self.here(it, along)
        self.send(it, it.src, net.f, it.c, net.c_peer)
        self.own(it).start()

    def from_z(self, it):
        net = self.net

        def body():
            self.total(it, 3, it.z).wait_recv()
            pieces = self.column(it, net.x, (1, 3, 2))
            for piece, block in pieces:
                self.send(it, piece, block, it.x, net.x_peer)
            self.hand_on(it, pieces, it.y1)
            for piece, block in pieces:
                self.send(it, piece, block, it.c, net.c_peer)

        self.here(it, body)

    def from_x(self, it):
        net = self.net

        def body():
            self.total(it, 4, it.x).wait_recv()
            pieces = self.column(it, 1 - net.x, (0, 1, 3, 2))
            self.hand_on(it, pieces, it.y2)
            for piece, block in pieces:
                self.send(it, piece, block, it.c, net.c_peer)

        self.here(it, body)

    def from_seq(self, it):
        net = self.net
        if isinstance(it.plane, int) and it.plane == 2:
            return

        @pl.when((net.s != it.plane) & (it.plane != 2))
        def _():
            self.total(it, 3, it.y1).wait_recv()
            for piece, block in self.column(it, net.x, (1, 3, 2)):
                self.send(it, piece, block, it.c, net.c_peer)
            self.total(it, 4, it.y2).wait_recv()
            for piece, block in self.column(it, 1 - net.x, (0, 1, 3, 2)):
                self.send(it, piece, block, it.c, net.c_peer)

    def from_core(self, it):
        self.total(it, 8, it.c).wait_recv()
        self.own(it).wait()

    def finish(self, it):
        net = self.net
        if isinstance(it.plane, int) and it.plane == 2:
            self.total(it, 15, it.z).wait_send()
            return

        @pl.when(it.plane == 2)
        def _():
            self.total(it, 15, it.z).wait_send()

        @pl.when(net.s == it.plane)
        def _():
            self.total(it, 22, it.z).wait_send()

        @pl.when((net.s != it.plane) & (it.plane != 2))
        def _():
            self.total(it, 8, it.z).wait_send()


def full_vector(vec_ref, row, blocks=16, rows=16):
    parts = []
    for k in range(blocks // 2):
        even = vec_ref[2 * k * rows + row:2 * k * rows + row + 1, :]
        odd = vec_ref[(2 * k + 1) * rows + row:(2 * k + 1) * rows + row + 1, :]
        parts.append(even + odd)
    return jnp.concatenate(parts, axis=1)


WINDOW = 640
STEP = 64
PAD = 384
QROWS = 320
FFB = 512


class Image:
    def __init__(self, seg_ref, id_ref):
        self.start = jnp.sum((seg_ref[...] == 0).astype(F32), axis=1, keepdims=True)
        ident = id_ref[...].astype(F32)
        self.pick = []
        base = jnp.zeros((1, 1), F32)
        for k in range(PAD // STEP + 1):
            mark = ((self.start >= k * STEP) & (self.start < (k + 1) * STEP)).astype(F32)
            self.pick.append(mark)
            base = base + mark * float(k * STEP)
        self.shift = base - self.start
        lane = lax.broadcasted_iota(jnp.int32, (1, 128), 1).astype(F32)
        self.columns = ((lane >= ident * RANK) & (lane < (ident + 1) * RANK)).astype(F32)

    def choose(self, load):
        total = None
        for k, mark in enumerate(self.pick):
            value = load(k * STEP)
            value = value * mark.astype(value.dtype)
            total = value if total is None else total + value
        return total

    def inside(self, shape, axis, first=0):
        at = (lax.broadcasted_iota(jnp.int32, shape, axis) + first).astype(F32) + self.shift
        return (at >= 0) & (at < IMG)

    def select(self, first, rows):
        at = (lax.broadcasted_iota(jnp.int32, (rows, 1), 0) + first).astype(F32)
        return (at >= self.start).astype(F32) * self.columns

    def select_window(self, first, rows):
        at = (lax.broadcasted_iota(jnp.int32, (rows, 1), 0) + first).astype(F32) + self.shift
        return (at >= 0).astype(F32) * self.columns


def lane_halves():
    lane = lax.broadcasted_iota(jnp.int32, (1, 128), 1)
    return [(lane < 64).astype(F32), (lane >= 64).astype(F32)]


def compact_rows(dense):
    total = dense[0:16]
    for k in range(1, 8):
        total = total + dense[16 * k:16 * (k + 1)]
    return total.astype(BF16)


N_FC1 = 8
N_FC2 = 4
FIRST = 6
PLANES = (2, 2, 0, 1, 2, 2, 2, 2)
N_ITEMS = FIRST + N_FC2 + N_FC1


def block_kernel(seg_ref, id_ref, vec_ref, x_hbm, qd_hbm, pd_hbm, pu_hbm, wq_hbm, wp_hbm, w1_hbm, w2_hbm,
                 qu_hbm, g_hbm, u1_hbm, d1_hbm, u2_hbm, d2_hbm,
                 vecf_out, prob_out, gm_out, out_out, gall, gn_out,
                 x_ref, qd_ref, pd_ref, pu_ref, wq_own, wq, wp, w1, w2, xp, vecf, qu, g, u1, d1, u2, d2, qkv, n1, c1, qkvw, n1w, c1w, prob, opad, sendb,
                 oh, att, c2, mid, n2, oacc, gacc, u4, e3, c3, e4, c3t, e4t, act_s, gh_s, gr,
                 do_s, gr_in, gr_sum, last_own, last_in, last_sum, parts0, parts1, parts2, dense0, dense1, dense2, prcv,
                 xs_sem, xr_sem, as_sem, ar_sem, loc_sem, out_sem, prob_sem, g_sem, g_own,
                 ds_sem, dr_sem, fs_sem, fr_sem, ps_sem, pr_sem, t_send, t_recv):
    net = Net()
    s, other = net.s, 1 - net.s
    rows, width = x_ref.shape
    half = wq.shape[1] // 3
    rb = wq_own.shape[0]
    fr1 = w1_hbm.shape[0]
    fr2 = w2_hbm.shape[0]
    ff = w1.shape[1]
    chunk = rows // 2

    pre = []
    for part in range(3):
        cols = pl.ds(pl.multiple_of(part * width + s * half, 128), half)
        pre.append(pltpu.make_async_copy(wq_hbm.at[:, cols], wq_own.at[:, pl.ds(part * half, half)], loc_sem.at[part]))
    late = []
    for part in range(3):
        cols = pl.ds(pl.multiple_of(part * width + s * half, 128), half)
        late.append(pltpu.make_async_copy(qu_hbm.at[:, cols], qu.at[:, pl.ds(part * half, half)], loc_sem.at[3 + part]))
    for n, (src, dst) in enumerate(((x_hbm, x_ref), (qd_hbm, qd_ref), (g_hbm, g), (u1_hbm, u1), (d1_hbm, d1),
                                  (u2_hbm, u2), (d2_hbm, d2), (pd_hbm, pd_ref), (pu_hbm, pu_ref))):
        late.append(pltpu.make_async_copy(src, dst, loc_sem.at[6 + n]))
    for copy in pre + late:
        copy.start()
    net.plane_barrier()

    def x_copy(i):
        part = pl.ds(i * chunk, chunk)
        return pltpu.make_async_remote_copy(
            src_ref=x_hbm.at[part, :], dst_ref=xp.at[part, :], send_sem=xs_sem.at[i], recv_sem=xr_sem.at[i],
            device_id=net.partner, device_id_type=MESH)

    for i in range(2):
        x_copy(i).start()
    for copy in pre:
        copy.wait()

    def square(n):
        return w1.at[pl.ds(0, n * 64), pl.ds(0, half)] if n <= 16 else w1.at[pl.ds(0, n * 32), pl.ds(0, 2 * half)]

    def block(n, src, piece, plane=2, some=square):
        return Block(src, piece, some, [g_sem.at[k, n] for k in range(N_SEMS)], g_own.at[n], plane)

    def wq_part(part):
        cols = pl.ds(part * half, half)
        return block(1 + part, wq_own.at[:, cols], lambda b: wq.at[pl.ds(b * rb, rb), cols])

    def wp_part(part):
        cols = pl.ds(part * half, half)
        return block(4 + part, wp_hbm.at[:, cols], lambda b: wp.at[pl.ds(b * rb, rb), cols], part)

    sub = fr2 // N_FC2

    def times(j, size):
        return j * size if isinstance(j, int) else pl.multiple_of(j * size, size)

    def item(n):
        if isinstance(n, int) and n < FIRST:
            if n == 0:
                return block(0, vec_ref, lambda b: vecf.at[pl.ds(b * 16, 16), :], 2,
                             lambda n: vecf.at[pl.ds(0, n * 16), :])
            return wq_part(n - 1) if n < 4 else wp_part(n - 4)
        if isinstance(n, int):
            return fc2_it(n - FIRST) if n < FIRST + N_FC2 else fc1_it(n - FIRST - N_FC2)
        return fc1_it(n - FIRST - N_FC2)

    def fc2_it(j):
        at = pl.ds(times(j, sub), sub)
        return block(FIRST + j, w2_hbm.at[at, :], lambda b: w2.at[pl.ds(b * fr2 + times(j, sub), sub), :],
                     (0, 1, 2, 2)[j], lambda n: w2.at[pl.ds(0, n * sub), :])

    def fc1_it(j):
        cols = pl.ds(times(j, FFB), FFB)
        return block(FIRST + N_FC2 + j, w1_hbm.at[:, cols], lambda b: w1.at[pl.ds(b * fr1, fr1), cols],
                     (PLANES[j] if isinstance(j, int) else jnp.where(j // 2 == 1, j % 2, 2)))

    gather = Gather(net)
    stages = {"S": gather.start, "A": gather.from_z, "B": gather.from_x, "Y": gather.from_seq, "C": gather.from_core}

    def go(*steps):
        for step in steps:
            stages[step[0]](item(int(step[1:])))

    go("S0", "S1", "S2")
    image = Image(seg_ref, id_ref)
    zeros = jnp.zeros((PAD, 128), BF16)
    opad[0:PAD, :] = zeros
    opad[PAD + WINDOW:2 * PAD + WINDOW, :] = zeros
    go("A0", "A1", "S3", "A2", "S4", "S5", "B0", "B1", "A3", "S6", "S7", "B2")
    for copy in late:
        copy.wait()
    go("B3", "C0", "C1", "C2", "C3")

    gain1 = full_vector(vecf, 0)
    shift1 = full_vector(vecf, 1)

    def project(src, src_row, row):
        v = src[pl.ds(src_row, chunk), :].astype(F32)
        h, unused = norm_parts(v)
        normed = (h * gain1 + shift1).astype(BF16)
        at = pl.ds(row, chunk)
        n1[at, :] = normed
        inner = (mm(normed, qd_ref[...]) * image.select(row, chunk)).astype(BF16)
        c1[at, :] = inner
        for part in range(3):
            cols = pl.ds(part * half, half)
            qkv[at, cols] = (mm(normed, wq[:, cols]) + mm(inner, qu[:, cols])).astype(BF16)

    def own_rows_in(i):
        project(x_ref, i * chunk, pl.multiple_of(s * rows + i * chunk, chunk))

    def partner_rows_in(i):
        x_copy(i).wait_recv()
        project(xp, i * chunk, pl.multiple_of(other * rows + i * chunk, chunk))

    own_rows_in(0)
    go("A4", "A5", "S8")
    own_rows_in(1)
    partner_rows_in(0)
    partner_rows_in(1)
    go("B4", "B5", "A6", "A7", "S9")
    outs = []

    def put(src, dst):
        copy = pltpu.make_async_copy(src, dst, out_sem.at[len(outs)])
        copy.start()
        outs.append(copy)

    put(vecf, vecf_out)
    for src, dst in ((qkv, qkvw), (n1, n1w), (c1, c1w)):
        step = min(src.shape[1], 512)

        @pl.loop(0, src.shape[1] // step)
        def _(n, src=src, dst=dst, step=step):
            cols = pl.ds(pl.multiple_of(n * step, step), step)
            dst[:, cols] = image.choose(lambda at: src[at:at + WINDOW, cols])
    bias = jnp.where(image.inside((1, WINDOW), 1), 0.0, masked_score).astype(F32)
    halves = lane_halves()

    def prob_copy(pair):
        slot = lax.rem(pair, 2)
        return pltpu.make_async_copy(prob.at[slot], prob_out.at[pl.ds(2 * pair, 2)], prob_sem.at[slot])

    def att_copy(pair):
        cols = pl.ds(pl.multiple_of(s * half + pair * 128, 128), 128)
        return pltpu.make_async_remote_copy(
            src_ref=sendb.at[pair], dst_ref=att.at[:, cols], send_sem=as_sem.at[pair], recv_sem=ar_sem.at[pair],
            device_id=net.partner, device_id_type=MESH)

    def to_partner(src, dst, send, recv):
        return pltpu.make_async_remote_copy(src_ref=src, dst_ref=dst, send_sem=send, recv_sem=recv,
                                            device_id=net.partner, device_id_type=MESH)

    pairs = half // 128

    @pl.loop(0, pairs)
    def _(pair):
        def cols(part):
            return pl.ds(pl.multiple_of(part * half + pair * 128, 128), 128)

        for n, steps in enumerate(((), ("Y4", "Y5"), ("A8", "S10", "S11"), ("C4", "C5"))):
            @pl.when(pair == n)
            def _(steps=steps):
                go(*steps)

        k2 = qkvw[:, cols(1)]
        v2 = qkvw[:, cols(2)]
        vs = [(v2 * hm.astype(BF16)) for hm in halves]
        slot = lax.rem(pair, 2)

        @pl.when(pair >= 2)
        def _():
            prob_copy(pair).wait()

        @pl.loop(0, WINDOW // QROWS)
        def _(b):
            r0 = pl.multiple_of(b * QROWS, QROWS)
            q2 = qkvw[pl.ds(r0, QROWS), cols(0)]
            q2 = q2 * jnp.asarray(HEAD_DIM ** (-0.5), BF16)
            total = None
            for hd in range(2):
                scores = mm_nt(q2 * halves[hd].astype(BF16), k2) + bias
                weights = jnp.exp(scores - jnp.max(scores, axis=1, keepdims=True))
                weights = (weights * (1.0 / jnp.sum(weights, axis=1, keepdims=True))).astype(BF16)
                prob[slot, hd, pl.ds(r0, QROWS), :] = weights
                part = mm(weights, vs[hd])
                total = part if total is None else total + part
            total = (total * image.inside((QROWS, 1), 0, r0).astype(F32)).astype(BF16)
            opad[pl.ds(PAD + r0, QROWS), :] = total
            oh[pl.ds(r0, QROWS), cols(0)] = total

        prob_copy(pair).start()

        def own_rows(who):
            return image.choose(lambda at: opad[pl.ds(pl.multiple_of(who * rows + PAD - at, STEP), rows), :])

        sendb[pair] = own_rows(other)
        att_copy(pair).start()
        att[:, pl.ds(pl.multiple_of(s * half + pair * 128, 128), 128)] = own_rows(s)

    go("B6", "B7")

    @pl.loop(0, pairs)
    def _(pair):
        att_copy(pair).wait_recv()

    go("A9", "S12", "S13")
    bias_p = full_vector(vecf, 2)
    gain2 = full_vector(vecf, 3)
    shift2 = full_vector(vecf, 4)

    @pl.loop(0, 2)
    def _(i):
        at = pl.ds(pl.multiple_of(i * chunk, chunk), chunk)
        rows_in = att[at, :]
        own_select = image.select(s * rows + i * chunk, chunk)
        inner = (mm(rows_in, pd_ref[...]) * own_select).astype(BF16)
        c2[at, :] = inner
        branch = mm(rows_in, wp[...]) + mm(inner, pu_ref[...]) + bias_p
        middle = x_ref[at, :].astype(F32) + branch
        mid[at, :] = middle
        h, unused = norm_parts(middle)
        normed = (h * gain2 + shift2).astype(BF16)
        n2[at, :] = normed
        c = mm(normed, d1[...]) * own_select
        e = mm_nt(g[at, :], u2[...]) * own_select
        c3[at, :] = c.astype(BF16)
        e4[at, :] = e.astype(BF16)
        oacc[at, :] = jnp.zeros((chunk, width), F32)
        gacc[at, :] = jnp.zeros((chunk, width), F32)
        u4[at, :] = jnp.zeros((chunk, 128), F32)
        e3[at, :] = jnp.zeros((chunk, 128), F32)

    c3t[...] = c3[...].T
    e4t[...] = e4[...].T
    go("B8", "A10", "S14", "Y6", "Y7", "B9", "A11", "S15", "C6", "C7", "C8", "C9", "B10", "A12", "A13", "S16", "S17")

    @pl.loop(0, N_FC1)
    def _(j):
        gather.from_core(fc1_it(j))
        bias = jnp.concatenate([vecf[pl.ds(2 * j * 16 + 6, 1), :], vecf[pl.ds(2 * j * 16 + 7, 1), :],
                                vecf[pl.ds((2 * j + 1) * 16 + 6, 1), :], vecf[pl.ds((2 * j + 1) * 16 + 7, 1), :]], axis=1)
        col = pl.ds(pl.multiple_of(j * FFB, FFB), FFB)

        for at in [pl.ds(0, rows)]:
            hidden = mm(n2[at, :], w1[:, col]) + mm(c3[at, :], u1[:, col]) + bias
            grad_active = mm_nt(g[at, :], w2[col, :]) + mm_nt(e4[at, :], d2[col, :])
            cdf = 0.5 * (1.0 + lax.erf(hidden * (0.5 ** 0.5)))
            pdf = jnp.exp(hidden * hidden * -0.5) * (0.5 / 3.141592653589793) ** 0.5
            active = (hidden * cdf).astype(BF16)
            act_s[at, :] = active
            grad_hidden = (grad_active * (cdf + hidden * pdf)).astype(BF16)
            gh_s[at, :] = grad_hidden
            oacc[at, :] += mm(active, w2[col, :])
            u4[at, :] += mm(active, d2[col, :])
            gacc[at, :] += mm_nt(grad_hidden, w1[:, col])
            e3[at, :] += mm_nt(grad_hidden, u1[:, col])

        gr[:, col] = compact_rows(mm(c3t[...], gh_s[...]))
        gr[:, pl.ds(pl.multiple_of(ff + j * FFB, FFB), FFB)] = compact_rows(mm(e4t[...], act_s[...]))
        for first in (0, ff):
            cols = pl.ds(pl.multiple_of(first + j * FFB, FFB), FFB)
            to_partner(gr.at[:, cols], gr_in.at[:, cols], fs_sem.at[0], fr_sem.at[0]).start()

        @pl.when(j + 4 < N_FC1)
        def _():
            gather.from_z(fc1_it(j + 4))

        @pl.when(j == 0)
        def _():
            gather.from_x(fc1_it(1))

        @pl.when(j + 2 < N_FC1)
        def _():
            gather.from_x(fc1_it(j + 2))

        @pl.when(j + 1 < N_FC1)
        def _():
            gather.from_seq(fc1_it(j + 1))

    bias2 = full_vector(vecf, 5)
    for n in range(FIRST + N_FC2):
        gather.finish(item(n))

    @pl.loop(0, N_FC1)
    def _(j):
        gather.finish(fc1_it(j))

    for pair in range(pairs - 2, pairs):
        prob_copy(pair).wait()

    def prob_load(pair):
        slot = lax.rem(pair, 2)
        return pltpu.make_async_copy(prob_out.at[pl.ds(2 * pair, 2)], prob.at[slot], prob_sem.at[slot])

    for pair in range(2):
        prob_load(pair).start()

    g1 = n1
    e2 = u4

    def grad_att(at, who):
        heads = pl.ds(pl.multiple_of(who * half, half), half)
        return (mm_nt(g1[at, :], wp[heads, :]) + mm_nt(e2[at, :].astype(BF16), pd_ref[heads, :])).astype(BF16)

    def d_copy(pair):
        cols = pl.ds(pair * 128 if isinstance(pair, int) else pl.multiple_of(pair * 128, 128), 128)
        return to_partner(n1.at[pl.ds(rows, rows), cols],
                          do_s.at[pl.ds(pl.multiple_of(s * rows, rows), rows), cols], ds_sem.at[pair], dr_sem.at[pair])

    @pl.loop(0, 2)
    def _(i):
        at = pl.ds(pl.multiple_of(i * chunk, chunk), chunk)
        own_select = image.select(s * rows + i * chunk, chunk)
        c = (u4[at, :] * own_select).astype(BF16)
        e = (e3[at, :] * own_select).astype(BF16)
        c3[at, :] = c
        e4[at, :] = e
        grad_n2 = gacc[at, :] + mm_nt(e, d1[...])
        grad_mid = g[at, :].astype(F32) + norm_grad(mid[at, :], gain2, grad_n2)
        gacc[at, :] = grad_mid
        low = grad_mid.astype(BF16)
        g1[at, :] = low
        e2[at, :] = mm_nt(low, pu_ref[...]) * own_select
        n1[pl.ds(pl.multiple_of(rows + i * chunk, chunk), chunk), 0:half] = grad_att(at, other)

    for pair in range(pairs):
        d_copy(pair).start()

    cols0 = 2 * ff
    cols1 = 4 * width
    gr[:, cols0:cols0 + width] = compact_rows(mm_tn(e4[...], n2[...]))
    gr[:, cols0 + width:cols0 + 2 * width] = compact_rows(mm_tn(c3[...], g[...]))
    gr[:, cols0 + 2 * width:cols0 + 3 * width] = compact_rows(mm_tn(c2[...], g1[0:rows, :]))
    gr[:, cols0 + 3 * width:cols0 + 4 * width] = compact_rows(mm_tn(e2[...].astype(BF16), att[...]))
    rest = pl.ds(cols0, cols1)
    rest_copy = to_partner(gr.at[:, rest], gr_in.at[:, rest], fs_sem.at[1], fr_sem.at[1])
    rest_copy.start()

    @pl.loop(0, 2)
    def _(i):
        at = pl.ds(pl.multiple_of(i * chunk, chunk), chunk)
        do_s[pl.ds(pl.multiple_of(s * rows + i * chunk, chunk), chunk), :] = grad_att(at, s)

    own0, own1 = cols0 // 16, cols1 // 16
    pick = adapter_rows(vecf)

    def turn_start(n, src, first, dst, cols):
        mine = pl.ds(pl.multiple_of(net.f * 16, 16), 16)

        @pl.loop(1, 16)
        def _(d):
            peer = (net.f + d) % 16
            pltpu.make_async_remote_copy(
                src_ref=src.at[:, pl.ds(pl.multiple_of(first + peer * cols, 128), cols)], dst_ref=dst.at[mine, :],
                send_sem=t_send.at[n], recv_sem=t_recv.at[n], device_id={"fsdp": peer}, device_id_type=MESH).start()

        dst[mine, :] = src[:, pl.ds(pl.multiple_of(first + net.f * cols, 128), cols)]

    def turn_total(n, dst):
        return pltpu.make_async_remote_copy(
            src_ref=dst.at[0:240, :], dst_ref=dst.at[0:240, :], send_sem=t_send.at[n], recv_sem=t_recv.at[n],
            device_id=net.c_peer, device_id_type=MESH)

    def result(n, src, first, step):
        return Block(src, lambda b: gall.at[:, pl.ds(pl.multiple_of(first + b * step, 128), 256)],
                     lambda m: gall.at[:, pl.ds(0, m * 256)], [g_sem.at[k, N_ITEMS + n] for k in range(N_SEMS)],
                     g_own.at[N_ITEMS + n])

    results = [result(0, dense0.at[:, pl.ds(0, 256)], 0, own0), result(1, dense0.at[:, pl.ds(256, 256)], 256, own0),
               result(2, dense1, cols0, own1), result(3, dense2, cols0 + cols1, own1)]

    def move(*steps):
        for step in steps:
            stages[step[0]](results[int(step[1:])])

    first_cols = pl.ds(0, cols0)
    first_copy = to_partner(gr.at[:, first_cols], gr_in.at[:, first_cols], fs_sem.at[0], fr_sem.at[0])
    first_copy.wait_recv()
    gr_sum[:, 0:cols0] = (gr[:, 0:cols0].astype(F32) + gr_in[:, 0:cols0].astype(F32)).astype(BF16)
    turn_start(0, gr_sum, 0, parts0, own0)

    @pl.loop(0, 2)
    def _(i):
        at = pl.ds(pl.multiple_of(i * chunk, chunk), chunk)
        branch = oacc[at, :] + mm(c3[at, :], u2[...]) + bias2
        xp[at, :] = (mid[at, :] + branch).astype(BF16)

    put(xp, out_out)
    put(gacc, gm_out)
    gpad = w2
    zeros = jnp.zeros((PAD, width), BF16)
    gpad[0:PAD, :] = zeros
    gpad[PAD + WINDOW:2 * PAD + WINDOW, :] = zeros
    last_own[...] = jnp.zeros_like(last_own)
    gq = w1
    scale = HEAD_DIM ** (-0.5)
    keep = image.inside((WINDOW, 1), 0).astype(BF16)

    @pl.loop(0, pairs)
    def _(pair):
        @pl.when(pair == 1)
        def _():
            turn_total(0, parts0).wait_recv()
            dense0[...] = mm(pick, parts0[...]).astype(BF16)
            move("S0", "S1")

        def cols(part):
            return pl.ds(pl.multiple_of(part * half + pair * 128, 128), 128)

        prob_load(pair).wait()
        d_copy(pair).wait_recv()
        slot = lax.rem(pair, 2)
        k2 = qkvw[:, cols(1)]
        v2 = qkvw[:, cols(2)]
        q2 = qkvw[:, cols(0)] * jnp.asarray(scale, BF16)
        do2 = image.choose(lambda at: do_s[at:at + WINDOW, cols(0)]) * keep
        inner = do2.astype(F32) * oh[:, cols(0)].astype(F32)
        gv = gk = gqq = None
        for hd in range(2):
            hm = halves[hd].astype(BF16)
            weights = prob[slot, hd]
            grad_p = mm_nt(do2 * hm, v2)
            row_inner = jnp.sum(inner * halves[hd], axis=1, keepdims=True)
            grad_s = (weights.astype(F32) * (grad_p - row_inner)).astype(BF16)
            dv = mm_tn(weights, do2 * hm)
            dk = mm_tn(grad_s, q2 * hm)
            dq = mm(grad_s, k2 * hm)
            gv = dv if gv is None else gv + dv
            gk = dk if gk is None else gk + dk
            gqq = dq if gqq is None else gqq + dq

        @pl.when(pair + 2 < pairs)
        def _():
            prob_load(pair + 2).start()

        gq[0:WINDOW, cols(0)] = (gqq * scale).astype(BF16)
        gq[0:WINDOW, cols(1)] = gk.astype(BF16)
        gq[0:WINDOW, cols(2)] = gv.astype(BF16)

    rest_copy.wait_recv()
    gr_sum[:, cols0:cols0 + cols1] = (gr[:, cols0:cols0 + cols1].astype(F32)
                                      + gr_in[:, cols0:cols0 + cols1].astype(F32)).astype(BF16)
    turn_start(1, gr_sum, cols0, parts1, own1)
    three = slice(0, 3 * half)
    c1[0:WINDOW, :] = (mm_nt(gq[0:WINDOW, three], qu[...]) * image.select_window(0, WINDOW)).astype(BF16)
    up = compact_rows(mm_tn(c1w[...], gq[0:WINDOW, three]))
    for part in range(3):
        last_own[:, pl.ds(pl.multiple_of(part * width + s * half, 128), half)] = up[:, part * half:(part + 1) * half]
    last_own[:, 3 * width:4 * width] = compact_rows(mm_tn(c1[0:WINDOW, :], n1w[...]))
    last_copy = to_partner(last_own, last_in, fs_sem.at[2], fr_sem.at[2])
    last_copy.start()
    move("A0", "A1")

    @pl.loop(0, 2)
    def _(i):
        at = pl.ds(pl.multiple_of(i * QROWS, QROWS), QROWS)
        gpad[pl.ds(pl.multiple_of(PAD + i * QROWS, STEP), QROWS), :] = (
            mm_nt(gq[at, three], wq[...]) + mm_nt(c1[at, :], qd_ref[...])).astype(BF16)

    def rows_of(who, i):
        return image.choose(lambda at: gpad[pl.ds(pl.multiple_of(who * rows + PAD + i * chunk - at, STEP), chunk), :])

    spot = 2 * PAD + WINDOW + 128

    def p_copy(i):
        return to_partner(gpad.at[pl.ds(spot + i * chunk, chunk), :], prcv.at[i], ps_sem.at[i], pr_sem.at[i])

    for i in range(2):
        gpad[spot + i * chunk:spot + (i + 1) * chunk, :] = rows_of(other, i)
        p_copy(i).start()
    last_copy.wait_recv()
    last_sum[...] = (last_own[...].astype(F32) + last_in[...].astype(F32)).astype(BF16)
    turn_start(2, last_sum, 0, parts2, own1)
    turn_total(1, parts1).wait_recv()
    dense1[...] = mm(pick, parts1[...]).astype(BF16)
    move("B0", "S2", "B1")
    turn_total(2, parts2).wait_recv()
    dense2[...] = mm(pick, parts2[...]).astype(BF16)
    gn = oacc

    def grad_in(i):
        p_copy(i).wait_recv()
        at = slice(i * chunk, (i + 1) * chunk)
        gn[at, :] = prcv[i].astype(F32) + rows_of(s, i).astype(F32)
        put(gn.at[at, :], gn_out.at[at, :])

    move("S3", "C0", "A2", "C1", "A3", "B2")
    grad_in(0)
    move("C2", "B3")
    grad_in(1)
    move("C3")
    for copy in outs:
        copy.wait()
    for i in range(2):
        x_copy(i).wait_send()
        p_copy(i).wait_send()
    for copy in (first_copy, rest_copy, last_copy):
        copy.wait_send()
    for n, dst in enumerate((parts0, parts1, parts2)):
        turn_total(n, dst).wait_send()
    for it in results:
        gather.finish(it)

    @pl.loop(0, pairs)
    def _(pair):
        att_copy(pair).wait_send()
        d_copy(pair).wait_send()


def any_spec():
    return pl.BlockSpec(memory_space=pl.ANY)


def vmem_spec():
    return pl.BlockSpec(memory_space=pltpu.VMEM)


def adapter_rows(vec_ref):
    ids = jnp.concatenate([jnp.broadcast_to(vec_ref[16 * p + 8:16 * p + 9, :], (16, 128)) for p in range(16)], axis=0)
    r = lax.broadcasted_iota(jnp.int32, (256, 128), 0) % 16
    col = lax.broadcasted_iota(jnp.int32, (256, 128), 1)
    group = (col // 16).astype(F32)
    return ((ids == group) & (r == col % 16)).astype(F32).T.astype(BF16)


def run_block(seg, ident, x, vec, qd, pd, pu, wq, wp, w1, w2, qu, g, u1, d1, u2, d2):
    rows, width = x.shape
    toks = seg.shape[1]
    half = width // 2
    ff = w1.shape[1]
    chunk = rows // 2
    dma = pltpu.SemaphoreType.DMA
    sds = jax.ShapeDtypeStruct
    gcols = 2 * ff + 4 * width
    last = 4 * width
    out_shape = (
        sds((256, 128), F32), sds((half // 64, WINDOW, WINDOW), BF16), sds((rows, width), F32), sds((rows, width), BF16),
        sds((128, gcols + last), BF16), sds((rows, width), F32))

    def low(*shape):
        return pltpu.VMEM(shape, BF16)

    def full(*shape):
        return pltpu.VMEM(shape, F32)

    scratch = [
        low(rows, width), low(width, 128), low(width, 128), low(128, width), low(wq.shape[0], 3 * half), low(width, 3 * half), low(width, width), low(width, ff), low(ff, width),
        low(rows, width), full(256, 128), low(128, 3 * half), low(rows, width), low(128, ff), low(width, 128),
        low(128, width), low(ff, 128), low(toks, 3 * half), low(toks, width), low(toks, 128),
        low(WINDOW, 3 * half), low(WINDOW, width), low(WINDOW, 128), low(2, 2, WINDOW, WINDOW), low(2 * PAD + WINDOW, 128),
        low(half // 128, rows, 128), low(WINDOW, half), low(rows, width), low(rows, 128), full(rows, width), low(rows, width),
        full(rows, width), full(rows, width), full(rows, 128), full(rows, 128), low(rows, 128), low(rows, 128),
        low(128, rows), low(128, rows), low(rows, FFB), low(rows, FFB), low(16, gcols),
        low(toks, half), low(16, gcols), low(16, gcols), low(16, last), low(16, last), low(16, last),
        low(256, 2 * ff // 16), low(256, last // 16), low(256, last // 16), low(128, 2 * ff // 16), low(128, last // 16),
        low(128, last // 16), low(2, chunk, width),
        dma((2,)), dma((2,)), dma((4,)), dma((4,)), dma((15,)), dma((12,)), dma((2,)),
        dma((N_SEMS, N_ITEMS + 4)), dma((N_ITEMS + 4,)),
        dma((4,)), dma((4,)), dma((3,)), dma((3,)), dma((2,)), dma((2,)), dma((3,)), dma((3,))]
    return pl.pallas_call(
        block_kernel, out_shape=out_shape, in_specs=[vmem_spec()] * 3 + [any_spec()] * 14,
        out_specs=tuple(any_spec() for unused in out_shape), scratch_shapes=scratch,
        compiler_params=pltpu.CompilerParams(collective_id=1, has_side_effects=True, vmem_limit_bytes=VMEM_LIMIT),
        name="block")(seg, ident, vec, x, qd, pd, pu, wq, wp, w1, w2, qu, g, u1, d1, u2, d2)


def expand_kernel(vec_ref, f1u, f2d, f1d, f2u, pu, pdn, qu, qd, gn, x, gm, out,
                  out_out, gt_out, qd_out, qu_out, pd_out, pu_out, f1d_out, f1u_out, f2d_out, f2u_out):
    for src, dst in ((f1u, f1u_out), (f2u, f2u_out), (pu, pu_out), (qu, qu_out)):
        dst[...] = src[...].astype(F32)
    for src, dst in ((f1d, f1d_out), (f2d, f2d_out), (pdn, pd_out), (qd, qd_out)):
        dst[...] = src[...].T.astype(F32)
    out_out[...] = out[...]
    gain1 = full_vector(vec_ref, 0)
    gt_out[...] = gm[...] + norm_grad(x[...].astype(F32), gain1, gn[...])


def run_expand(vec, gall, gn, x, gm, out):
    rows, width = gn.shape
    ff = 4 * width
    n = 2
    sds = jax.ShapeDtypeStruct

    def part(cols, offset):
        return pl.BlockSpec((128, cols), lambda j: (0, offset // cols + j))

    def by_row(shape):
        return pl.BlockSpec(shape, lambda j: (j, 0))

    def by_col(shape):
        return pl.BlockSpec(shape, lambda j: (0, j))

    q = width // n
    return pl.pallas_call(
        expand_kernel, grid=(n,),
        out_shape=(sds((rows, width), BF16), sds((rows, width), F32), sds((width, 128), F32), sds((128, 3 * width), F32), sds((width, 128), F32),
                   sds((128, width), F32), sds((width, 128), F32), sds((128, ff), F32), sds((ff, 128), F32), sds((128, width), F32)),
        in_specs=[pl.BlockSpec((256, 128), lambda j: (0, 0)), part(ff // n, 0), part(ff // n, ff), part(q, 2 * ff),
                  part(q, 2 * ff + width), part(q, 2 * ff + 2 * width), part(q, 2 * ff + 3 * width),
                  part(3 * q, 2 * ff + 4 * width), part(q, 2 * ff + 7 * width),
                  by_row((rows // n, width)), by_row((rows // n, width)), by_row((rows // n, width)), by_row((rows // n, width))],
        out_specs=(by_row((rows // n, width)), by_row((rows // n, width)), by_row((q, 128)), by_col((128, 3 * q)), by_row((q, 128)), by_col((128, q)),
                   by_row((q, 128)), by_col((128, ff // n)), by_row((ff // n, 128)), by_col((128, q))),
        compiler_params=pltpu.CompilerParams(vmem_limit_bytes=VMEM_LIMIT),
        name="expand")(vec, *([gall] * 8), gn, x, gm, out)


def per_device_fast(tokens, grad_out, segments, padding, adapter_ids, norm1_gain, norm1_bias, w_qkv, w_proj, proj_bias,
                    norm2_gain, norm2_bias, w_fc1, fc1_bias, w_fc2, fc2_bias, qkv_down, qkv_up, proj_down, proj_up,
                    fc1_down, fc1_up, fc2_down, fc2_up):
    x = tokens[0]
    odd = (lax.axis_index("fsdp") % 2).astype(F32)
    six = jnp.stack([norm1_gain, norm1_bias, proj_bias, norm2_gain, norm2_bias, fc2_bias]).astype(F32)
    vec = jnp.concatenate([
        jnp.concatenate([six * (1.0 - odd), six * odd], axis=1), fc1_bias.astype(F32).reshape(2, 128),
        jnp.broadcast_to(adapter_ids[0].astype(F32)[:, None], (1, 128)), jnp.zeros((7, 128), F32)], axis=0)
    vecf, unused, gm, out, gall, gn = run_block(
        segments, adapter_ids, x, vec, qkv_down, proj_down, proj_up, w_qkv, w_proj, w_fc1, w_fc2, qkv_up,
        grad_out[0], fc1_up, fc1_down, fc2_up, fc2_down)
    out, gt, gqd, gqu, gpd, gpu, gf1d, gf1u, gf2d, gf2u = run_expand(vecf, gall, gn, x, gm, out)
    return out[None], gt[None], gqd, gqu, gpd, gpu, gf1d, gf1u, gf2d, gf2u


def solution(mesh):
    sizes = dict(mesh.shape)
    small = sizes == {"seq": 2, "fsdp": 16}

    def per_device_any(*args):
        tokens, adapter_ids = args[0], args[4]
        one_image = tokens.shape[1:] == (512, 1024) and adapter_ids.shape[1] == 1
        return (per_device_fast if small and one_image else per_device)(*args)

    return jax.shard_map(
        per_device_any,
        mesh=mesh,
        in_specs=(
            P("fsdp", "seq", None),
            P("fsdp", "seq", None),
            P("fsdp", None),
            P("fsdp", None),
            P("fsdp", None),
            P("fsdp"),
            P("fsdp"),
            P("fsdp", None),
            P("fsdp", None),
            P("fsdp"),
            P("fsdp"),
            P("fsdp"),
            P("fsdp", None),
            P("fsdp"),
            P("fsdp", None),
            P("fsdp"),
            P(),
            P(),
            P(),
            P(),
            P(),
            P(),
            P(),
            P(),
        ),
        out_specs=(
            P("fsdp", "seq", None),
            P("fsdp", "seq", None),
            P(),
            P(),
            P(),
            P(),
            P(),
            P(),
            P(),
            P(),
        ),
        check_vma=False,
    )
```
